128 devices in a mesh: fsdp: 128 (over z, y, x, core).
Axes of the slice: x: 4, y: 4, z: 4, core: 2. Of those that a mesh axis runs over, the one named last changes fastest.
Arguments:
- x: bfloat16 [512, 512, 512], P('fsdp')
- lengths: int32 [512], P('fsdp')
- d_y: bfloat16 [512, 512, 512], P('fsdp')
- w_attn: bfloat16 [2, 4, 512, 512], P(None, None, 'fsdp')
- b_attn: bfloat16 [2, 4, 512], P(None, None, 'fsdp')
- ln_par: bfloat16 [2, 4, 512], P(None, None, 'fsdp')
- w_up: bfloat16 [2, 512, 2048], P(None, 'fsdp')
- b_up: bfloat16 [2, 2048], P(None, 'fsdp')
- w_down: bfloat16 [2, 2048, 512], P(None, 'fsdp')
- b_down: bfloat16 [2, 512], P(None, 'fsdp')
Outputs:
- output 1: bfloat16 [512, 512, 512], P('fsdp')
- output 2: float32 [2, 4, 512, 512], P(None, None, 'fsdp')
- output 3: float32 [2, 4, 512], P(None, None, 'fsdp')
- output 4: float32 [2, 4, 512], P(None, None, 'fsdp')
- output 5: float32 [2, 512, 2048], P(None, 'fsdp')
- output 6: float32 [2, 2048], P(None, 'fsdp')
- output 7: float32 [2, 2048, 512], P(None, 'fsdp')
- output 8: float32 [2, 512], P(None, 'fsdp')
All inputs are finite; a program needn't handle non-finite values.
Results may differ from the reference program's by a relative error of at most 0.0133484.
Values are sent between devices in bfloat16 or wider.
A program may use at most 1 GiB of HBM per device.

```python
import jax
import jax.numpy as jnp
from jax import lax

MODEL_DIM = 512
FFN_DIM = 2048
HEAD_DIM = 64
NUM_LAYERS = 2
SEQ_LEN = 512
SEQ_DEV = 4
GROUP_SIZE = 128
EPS = 1e-5
THETA = 10000.0
NUM_HEADS = MODEL_DIM // HEAD_DIM
BATCH = SEQ_DEV * GROUP_SIZE
MIN_LEN = SEQ_LEN // 8


def setup_inputs(seed: int = 0) -> dict:
    key_list = jax.random.split(jax.random.key(seed), 10)
    seq_index = jnp.arange(BATCH)
    drawn_len = jax.random.randint(key_list[1], (BATCH,), MIN_LEN, SEQ_LEN + 1)
    lengths = jnp.where(seq_index == 0, SEQ_LEN, jnp.where(seq_index == 1, MIN_LEN, drawn_len)).astype(jnp.int32)
    act_shape = (BATCH, SEQ_LEN, MODEL_DIM)
    dy_scale = float(BATCH * SEQ_LEN) ** -0.25
    ln_base = jnp.array([1.0, 0.0, 1.0, 0.0], dtype=jnp.float32)[None, :, None]
    return {
        'x': jax.random.normal(key_list[0], act_shape, jnp.float32).astype(jnp.bfloat16),
        'lengths': lengths,
        'd_y': (dy_scale * jax.random.normal(key_list[2], act_shape, jnp.float32)).astype(jnp.bfloat16),
        'w_attn': (MODEL_DIM ** -0.5 * jax.random.normal(key_list[3], (NUM_LAYERS, 4, MODEL_DIM, MODEL_DIM), jnp.float32)).astype(jnp.bfloat16),
        'b_attn': (0.3 * jax.random.normal(key_list[4], (NUM_LAYERS, 4, MODEL_DIM), jnp.float32)).astype(jnp.bfloat16),
        'ln_par': (ln_base + 0.2 * jax.random.normal(key_list[5], (NUM_LAYERS, 4, MODEL_DIM), jnp.float32)).astype(jnp.bfloat16),
        'w_up': (MODEL_DIM ** -0.5 * jax.random.normal(key_list[6], (NUM_LAYERS, MODEL_DIM, FFN_DIM), jnp.float32)).astype(jnp.bfloat16),
        'b_up': (0.5 * jax.random.normal(key_list[7], (NUM_LAYERS, FFN_DIM), jnp.float32)).astype(jnp.bfloat16),
        'w_down': (FFN_DIM ** -0.5 * jax.random.normal(key_list[8], (NUM_LAYERS, FFN_DIM, MODEL_DIM), jnp.float32)).astype(jnp.bfloat16),
        'b_down': (0.3 * jax.random.normal(key_list[9], (NUM_LAYERS, MODEL_DIM), jnp.float32)).astype(jnp.bfloat16),
    }


def to_bf16(tensor):
    return tensor.astype(jnp.bfloat16).astype(jnp.float32)


def norm_fwd(x_in, gain, shift):
    row_mean = jnp.mean(x_in, axis=-1, keepdims=True)
    centered = x_in - row_mean
    variance = jnp.mean(centered * centered, axis=-1, keepdims=True)
    return centered * lax.rsqrt(variance + EPS) * gain + shift


def rotary_tables():
    half_dim = HEAD_DIM // 2
    inv_freq = 1.0 / (THETA ** (jnp.arange(half_dim, dtype=jnp.float32) * (2.0 / HEAD_DIM)))
    angles = jnp.arange(SEQ_LEN, dtype=jnp.float32)[:, None] * inv_freq[None, :]
    return jnp.cos(angles)[:, None, :], jnp.sin(angles)[:, None, :]


def rotate(tensor, cos_tab, sin_tab):
    half_dim = HEAD_DIM // 2
    first_half = tensor[..., :half_dim]
    second_half = tensor[..., half_dim:]
    return jnp.concatenate([first_half * cos_tab - second_half * sin_tab, second_half * cos_tab + first_half * sin_tab], axis=-1)


def layer_fwd(x, weights, lengths, tables):
    w_attn, b_attn, ln_par, w_up, b_up, w_down, b_down = weights
    cos_tab, sin_tab = tables
    num_seq = x.shape[0]
    h_one = to_bf16(norm_fwd(x, ln_par[0], ln_par[1]))
    projected = jnp.einsum('bld,kde->kble', h_one, w_attn[:3]) + b_attn[:3, None, None, :]
    projected = projected.reshape(3, num_seq, SEQ_LEN, NUM_HEADS, HEAD_DIM)
    query_rot = to_bf16(rotate(projected[0] * (HEAD_DIM ** -0.5), cos_tab, sin_tab))
    key_rot = to_bf16(rotate(projected[1], cos_tab, sin_tab))
    values = to_bf16(projected[2])
    scores = jnp.einsum('bqhd,bkhd->bhqk', query_rot, key_rot)
    key_valid = jnp.arange(SEQ_LEN)[None, None, None, :] < lengths[:, None, None, None]
    attn_probs = to_bf16(jax.nn.softmax(jnp.where(key_valid, scores, -1e30), axis=-1))
    context = to_bf16(jnp.einsum('bhqk,bkhd->bqhd', attn_probs, values)).reshape(num_seq, SEQ_LEN, MODEL_DIM)
    x_mid = to_bf16(x + jnp.einsum('bld,de->ble', context, w_attn[3]) + b_attn[3])
    h_two = to_bf16(norm_fwd(x_mid, ln_par[2], ln_par[3]))
    act_out = to_bf16(jax.nn.gelu(jnp.einsum('bld,df->blf', h_two, w_up) + b_up, approximate=False))
    return to_bf16(x_mid + jnp.einsum('blf,fd->bld', act_out, w_down) + b_down)


def reference(x, lengths, d_y, w_attn, b_attn, ln_par, w_up, b_up, w_down, b_down):
    params = tuple(tensor.astype(jnp.float32) for tensor in (w_attn, b_attn, ln_par, w_up, b_up, w_down, b_down))
    tables = rotary_tables()

    def stack_fwd(x_block, param_set, len_block):
        hidden = x_block
        for layer_idx in range(NUM_LAYERS):
            hidden = layer_fwd(hidden, tuple(tensor[layer_idx] for tensor in param_set), len_block, tables)
        return hidden

    def block_step(grad_acc, block_in):
        x_block, len_block, dy_block = block_in

        def block_fwd(x_local, param_local):
            return stack_fwd(x_local, param_local, len_block)

        _, pull_back = jax.vjp(block_fwd, x_block.astype(jnp.float32), params)
        d_x_block, d_params = pull_back(dy_block.astype(jnp.float32))
        return jax.tree.map(jnp.add, grad_acc, d_params), d_x_block.astype(jnp.bfloat16)

    grad_zero = jax.tree.map(jnp.zeros_like, params)
    blocks_in = (x.reshape(GROUP_SIZE, SEQ_DEV, SEQ_LEN, MODEL_DIM), lengths.reshape(GROUP_SIZE, SEQ_DEV), d_y.reshape(GROUP_SIZE, SEQ_DEV, SEQ_LEN, MODEL_DIM))
    grad_sum, d_x = lax.scan(block_step, grad_zero, blocks_in)
    return (d_x.reshape(BATCH, SEQ_LEN, MODEL_DIM), grad_sum[0], grad_sum[1], grad_sum[2], grad_sum[3], grad_sum[4], grad_sum[5], grad_sum[6])
```

```python
import math
import functools
import jax
import jax.numpy as jnp
from jax import lax
from jax.experimental import pallas as pl
from jax.experimental.pallas import tpu as pltpu
from jax.sharding import PartitionSpec as P

ZERO, ONE, TWO, THREE, FOUR = range(5)
EIGHT, SIXTEEN, WIDTH = 8, 16, 256

F32, BF16 = jnp.float32, jnp.bfloat16
SEQS, TOK, DIM, FFN, HEADS, HEAD, LANES = FOUR, 512, 512, 2048, EIGHT, 64, 128
HALF = HEAD // TWO
EPS = 1e-5
THETA = 10000.0
NEG_BIG = -1e30
B_ATTN, LN_PAR, B_UP, B_DOWN = ZERO, FOUR, EIGHT, 12


def nn(a, b):
    return lax.dot_general(a, b, (((ONE,), (ZERO,)), ((), ())), preferred_element_type=F32)


def nt(a, b):
    return lax.dot_general(a, b, (((ONE,), (ONE,)), ((), ())), preferred_element_type=F32)


def tn(a, b):
    return lax.dot_general(a, b, (((ZERO,), (ZERO,)), ((), ())), preferred_element_type=F32)


def lane_tiles(width=TOK, size=LANES):
    return [slice(i, i + size) for i in range(ZERO, width, size)]


def column(c_ref, lane, width=LANES):
    return jnp.broadcast_to(c_ref[:, lane:lane + ONE], (c_ref.shape[ZERO], width))


def total(value):
    return jnp.sum(value, axis=ZERO, keepdims=True)


def normed(x):
    centred = x - total(x) * (1.0 / DIM)
    rstd = lax.rsqrt(total(centred * centred) * (1.0 / DIM) + EPS)
    return centred * rstd, rstd


def norm_to(x_ref, c_ref, lane, h_ref):
    gain, shift = column(c_ref, lane), column(c_ref, lane + ONE)
    for cols in lane_tiles():
        h_ref[:, cols] = (normed(x_ref[:, cols].astype(F32))[ZERO] * gain + shift).astype(BF16)


def fold(value):
    parts = [value[:, cols] for cols in lane_tiles(value.shape[ONE])]
    return functools.reduce(jnp.add, parts)


def attn_fwd_kernel(first, len_ref, x_ref, w_ref, c_ref, cos_ref, sin_ref, *refs):
    if first:
        xt_ref, q_ref, k_ref, v_ref, p_ref, ctx_ref, h_ref, acc_ref = refs
        xt_ref[ZERO] = x_ref[ZERO].T
        xt_ref = xt_ref.at[ZERO]
    else:
        q_ref, k_ref, v_ref, p_ref, ctx_ref, h_ref, acc_ref = refs
        xt_ref = x_ref.at[ZERO]
    length = len_ref[pl.program_id(ZERO)]
    norm_to(xt_ref, c_ref, LN_PAR, h_ref)
    for m, out in enumerate((q_ref, k_ref, v_ref)):
        acc_ref[...] = nn(w_ref[m], h_ref[...])
        if m < TWO:
            scale = HEAD ** -0.5 if m == ZERO else 1.0
            for cols in lane_tiles():
                bias = column(c_ref, B_ATTN + m)
                for head in range(HEADS):
                    one, two = slice(HEAD * head, HEAD * head + HALF), slice(HEAD * head + HALF, HEAD * head + HEAD)
                    a = (acc_ref[one, cols] + bias[one]) * scale
                    b = (acc_ref[two, cols] + bias[two]) * scale
                    cos, sin = cos_ref[:, cols], sin_ref[:, cols]
                    out[ZERO, one, cols] = (a * cos - b * sin).astype(BF16)
                    out[ZERO, two, cols] = (b * cos + a * sin).astype(BF16)
        else:
            for cols in lane_tiles():
                out[ZERO, :, cols] = (acc_ref[:, cols] + column(c_ref, B_ATTN + m)).astype(BF16)

    key = lax.broadcasted_iota(jnp.int32, (SIXTEEN, TOK), ONE)
    row = lax.broadcasted_iota(jnp.int32, (SIXTEEN, TOK), ZERO)
    bias_rows = jnp.where((row == ZERO) & (key >= length), NEG_BIG, 0.0).astype(BF16)
    one_rows = jnp.where(row == ZERO, 1.0, 0.0).astype(BF16)

    @pl.loop(ZERO, HEADS)
    def _(head):
        rows = pl.ds(pl.multiple_of(head * HEAD, HEAD), HEAD)
        keys = jnp.concatenate([k_ref[ZERO, rows, :], bias_rows], axis=ZERO)
        for cols in lane_tiles(TOK, WIDTH):
            queries = jnp.concatenate([q_ref[ZERO, rows, cols], one_rows[:, cols]], axis=ZERO)
            scores = tn(keys, queries)
            weight = jnp.exp(scores - jnp.max(scores, axis=ZERO, keepdims=True))
            probs = (weight * (1.0 / total(weight))).astype(BF16)
            p_ref[ZERO, head, :, cols] = probs
            ctx_ref[ZERO, rows, cols] = nn(v_ref[ZERO, rows, :], probs)


def mlp_fwd_kernel(last, ctx_ref, x_ref, wo_ref, up_ref, *refs):
    if last:
        c_ref, mid_ref, act_ref, slope_ref, h_ref = refs
    else:
        down_ref, c_ref, mid_ref, act_ref, slope_ref, y_ref, h_ref = refs
    attn = nn(wo_ref[...], ctx_ref[ZERO].astype(BF16))
    for cols in lane_tiles():
        mid_ref[ZERO, :, cols] = (x_ref[ZERO, :, cols].astype(F32) + attn[:, cols] + column(c_ref, B_ATTN + THREE)).astype(BF16)
    norm_to(mid_ref.at[ZERO], c_ref, LN_PAR + TWO, h_ref)
    for part in range(FFN // DIM):
        rows = slice(DIM * part, DIM * part + DIM)
        pre = nn(up_ref[rows, :], h_ref[...])
        for cols in lane_tiles():
            z = pre[:, cols] + column(c_ref, B_UP + part)
            cdf = 0.5 * (1.0 + lax.erf(z * (1.0 / math.sqrt(2.0))))
            density = jnp.exp(-0.5 * z * z) * (1.0 / math.sqrt(2.0 * math.pi))
            act_ref[ZERO, rows, cols] = (z * cdf).astype(BF16)
            slope_ref[ZERO, rows, cols] = cdf + z * density
    if not last:
        out = nn(down_ref[...], act_ref[ZERO])
        for cols in lane_tiles():
            y_ref[ZERO, :, cols] = (mid_ref[ZERO, :, cols].astype(F32) + out[:, cols] + column(c_ref, B_DOWN)).astype(BF16)


def norm_back(dh, x, gain):
    xhat, rstd = normed(x)
    dxhat = dh * gain
    mean_one = total(dxhat) * (1.0 / DIM)
    mean_two = total(dxhat * xhat) * (1.0 / DIM)
    return rstd * (dxhat - mean_one - xhat * mean_two), xhat


def put_columns(out_ref, columns):
    lane = lax.broadcasted_iota(jnp.int32, (DIM, LANES), ONE)
    value = jnp.zeros((DIM, LANES), F32)
    for at, partial in columns:
        value = jnp.where(lane == at, jnp.sum(partial, axis=ONE, keepdims=True), value)
    out_ref[...] = value


def mlp_bwd_kernel(last, dy_ref, slope_ref, act_ref, mid_ref, ctx_ref, wo_ref, up_ref, down_ref, c_ref,
                   dmid_ref, dctx_ref, gwo_ref, gup_ref, gdown_ref, gc_ref, dyt_ref, dpre_ref, h_ref, dh_ref, sums_ref):
    seq = pl.program_id(ZERO)

    @pl.when(seq == ZERO)
    def _():
        for ref in (gwo_ref, gup_ref, gdown_ref, sums_ref):
            ref[...] = jnp.zeros_like(ref)

    if last:
        dyt_ref[...] = dy_ref[ZERO].T
    else:
        dyt_ref[...] = dy_ref[ZERO]
    norm_to(mid_ref.at[ZERO], c_ref, LN_PAR + TWO, h_ref)
    for part in range(FFN // DIM):
        rows = slice(DIM * part, DIM * part + DIM)
        dact = nn(down_ref[rows, :], dyt_ref[...])
        for cols in lane_tiles():
            dpre = dact[:, cols] * slope_ref[ZERO, rows, cols]
            sums_ref[part] += dpre
            dpre_ref[rows, cols] = dpre.astype(BF16)
        gdown_ref[rows, :] += nt(act_ref[ZERO, rows, :], dyt_ref[...])
        gup_ref[:, rows] += nt(h_ref[...], dpre_ref[rows, :])
    dh_ref[...] = nn(up_ref[...], dpre_ref[...])
    gain = column(c_ref, LN_PAR + TWO)
    for cols in lane_tiles():
        dh, dy = dh_ref[:, cols], dyt_ref[:, cols].astype(F32)
        dx, xhat = norm_back(dh, mid_ref[ZERO, :, cols].astype(F32), gain)
        dmid = (dy + dx).astype(BF16)
        dmid_ref[ZERO, :, cols] = dmid
        sums_ref[FOUR] += dh * xhat
        sums_ref[5] += dh
        sums_ref[6] += dy
        sums_ref[7] += dmid.astype(F32)
    gwo_ref[...] += nt(ctx_ref[ZERO].astype(BF16), dmid_ref[ZERO])
    dctx_ref[ZERO] = nn(wo_ref[...], dmid_ref[ZERO]).astype(BF16)

    @pl.when(seq == SEQS - ONE)
    def _():
        put_columns(gc_ref, [(B_UP + i, sums_ref[i]) for i in range(FOUR)] + [
            (LN_PAR + TWO, sums_ref[FOUR]), (LN_PAR + THREE, sums_ref[5]), (B_DOWN, sums_ref[6]), (B_ATTN + THREE, sums_ref[7])])


def attn_bwd_kernel(first, dctx_ref, ctx_ref, p_ref, q_ref, k_ref, v_ref, x_ref, dmid_ref, w_ref, c_ref, cos_ref, sin_ref,
                    dx_ref, gw_ref, gc_ref, dq_ref, dk_ref, dproj_ref, h_ref, dh_ref, sums_ref):
    seq = pl.program_id(ZERO)

    @pl.when(seq == ZERO)
    def _():
        gw_ref[...] = jnp.zeros_like(gw_ref)
        sums_ref[...] = jnp.zeros_like(sums_ref)

    @pl.loop(ZERO, HEADS)
    def _(head):
        rows = pl.ds(pl.multiple_of(head * HEAD, HEAD), HEAD)
        dk = jnp.zeros((HEAD, TOK), F32)
        dv = jnp.zeros((HEAD, TOK), F32)
        for cols in lane_tiles(TOK, WIDTH):
            dctx = dctx_ref[ZERO, rows, cols]
            delta = total(dctx.astype(F32) * ctx_ref[ZERO, rows, cols])
            dprobs = tn(v_ref[ZERO, rows, :], dctx)
            probs = p_ref[ZERO, head, :, cols]
            dscores = (probs.astype(F32) * (dprobs - delta)).astype(BF16)
            dv = dv + nt(dctx, probs)
            dk = dk + nt(q_ref[ZERO, rows, cols], dscores)
            dq_ref[rows, cols] = nn(k_ref[ZERO, rows, :], dscores)
        dk_ref[rows, :] = dk
        sums_ref[TWO, rows, :] += fold(dv)
        dproj_ref[TWO, rows, :] = dv.astype(BF16)

    for m, (ref, scale) in enumerate(((dq_ref, HEAD ** -0.5), (dk_ref, 1.0))):
        for cols in lane_tiles():
            for head in range(HEADS):
                one, two = slice(HEAD * head, HEAD * head + HALF), slice(HEAD * head + HALF, HEAD * head + HEAD)
                a, b = ref[one, cols] * scale, ref[two, cols] * scale
                cos, sin = cos_ref[:, cols], sin_ref[:, cols]
                for rows, value in ((one, a * cos + b * sin), (two, b * cos - a * sin)):
                    dproj_ref[m, rows, cols] = value.astype(BF16)
                    sums_ref[m, rows, :] += value
    norm_to(x_ref.at[ZERO], c_ref, LN_PAR, h_ref)
    for m in range(THREE):
        gw_ref[m] += nt(h_ref[...], dproj_ref[m])
    dh_ref[...] = functools.reduce(jnp.add, [nn(w_ref[m], dproj_ref[m]) for m in range(THREE)])
    gain = column(c_ref, LN_PAR)
    for cols in lane_tiles():
        dh = dh_ref[:, cols]
        dx, xhat = norm_back(dh, x_ref[ZERO, :, cols].astype(F32), gain)
        dx = (dmid_ref[ZERO, :, cols].astype(F32) + dx).astype(BF16)
        if first:
            dx_ref[ZERO, cols, :] = dx.T
        else:
            dx_ref[ZERO, :, cols] = dx
        sums_ref[THREE] += dh * xhat
        sums_ref[FOUR] += dh

    @pl.when(seq == SEQS - ONE)
    def _():
        put_columns(gc_ref, [(B_ATTN + i, sums_ref[i]) for i in range(THREE)] + [(LN_PAR, sums_ref[THREE]), (LN_PAR + ONE, sums_ref[FOUR])])


def seq_spec(shape):
    return pl.BlockSpec((ONE, *shape), lambda s: (s,) + (ZERO,) * len(shape))


def once(shape):
    return pl.BlockSpec(shape, lambda s: (ZERO,) * len(shape), pipeline_mode=pl.Buffered(ONE))


def act_shape(rows, dtype):
    return jax.ShapeDtypeStruct((SEQS, rows, TOK), dtype)


PARAMS = pltpu.CompilerParams(vmem_limit_bytes=60 << 20, dimension_semantics=("arbitrary",))
SQUARE, TALL, WIDE, COLS = (DIM, TOK), (FFN, TOK), (DIM, FFN), (DIM, LANES)


def attn_fwd(first, lengths, x, w, c, tables):
    smem = pl.BlockSpec(memory_space=pltpu.SMEM)
    outs = [act_shape(DIM, BF16)] * (FOUR if first else THREE)
    return pl.pallas_call(
        functools.partial(attn_fwd_kernel, first), grid=(SEQS,),
        out_shape=outs + [jax.ShapeDtypeStruct((SEQS, HEADS, TOK, TOK), BF16), act_shape(DIM, F32)],
        in_specs=[smem, seq_spec(SQUARE), once((THREE, DIM, DIM)), once(COLS), once((HALF, TOK)), once((HALF, TOK))],
        out_specs=[seq_spec(SQUARE)] * len(outs) + [seq_spec((HEADS, TOK, TOK)), seq_spec(SQUARE)],
        scratch_shapes=[pltpu.VMEM(SQUARE, BF16), pltpu.VMEM(SQUARE, F32)], compiler_params=PARAMS,
        name="attn_fwd")(lengths, x, w, c, *tables)


def mlp_fwd(last, ctx, x, wo, up, down, c):
    downs = [] if last else [down]
    return pl.pallas_call(
        functools.partial(mlp_fwd_kernel, last), grid=(SEQS,),
        out_shape=[act_shape(DIM, BF16), act_shape(FFN, BF16), act_shape(FFN, F32)] + [act_shape(DIM, BF16)] * len(downs),
        in_specs=[seq_spec(SQUARE)] * TWO + [once((DIM, DIM)), once((FFN, DIM))] + [once(WIDE)] * len(downs) + [once(COLS)],
        out_specs=[seq_spec(SQUARE), seq_spec(TALL), seq_spec(TALL)] + [seq_spec(SQUARE)] * len(downs),
        scratch_shapes=[pltpu.VMEM(SQUARE, BF16)], compiler_params=PARAMS, name="mlp_fwd")(ctx, x, wo, up, *downs, c)


def mlp_bwd(last, dy, slope, act, mid, ctx, wo, up, down, c):
    return pl.pallas_call(
        functools.partial(mlp_bwd_kernel, last), grid=(SEQS,),
        out_shape=[act_shape(DIM, BF16)] * TWO + [jax.ShapeDtypeStruct(s, F32) for s in ((DIM, DIM), WIDE, (FFN, DIM), COLS)],
        in_specs=[seq_spec(SQUARE), seq_spec(TALL), seq_spec(TALL), seq_spec(SQUARE), seq_spec(SQUARE),
                  once((DIM, DIM)), once(WIDE), once((FFN, DIM)), once(COLS)],
        out_specs=[seq_spec(SQUARE)] * TWO + [once((DIM, DIM)), once(WIDE), once((FFN, DIM)), once(COLS)],
        scratch_shapes=[pltpu.VMEM(SQUARE, BF16), pltpu.VMEM(TALL, BF16), pltpu.VMEM(SQUARE, BF16), pltpu.VMEM(SQUARE, F32),
                        pltpu.VMEM((EIGHT, DIM, LANES), F32)],
        compiler_params=PARAMS, name="mlp_bwd")(dy, slope, act, mid, ctx, wo, up, down, c)


def attn_bwd(first, dctx, ctx, probs, q, k, v, x, dmid, w, c, tables):
    return pl.pallas_call(
        functools.partial(attn_bwd_kernel, first), grid=(SEQS,),
        out_shape=[act_shape(DIM, BF16), jax.ShapeDtypeStruct((THREE, DIM, DIM), F32), jax.ShapeDtypeStruct(COLS, F32)],
        in_specs=[seq_spec(SQUARE)] * TWO + [seq_spec((HEADS, TOK, TOK))] + [seq_spec(SQUARE)] * 5 + [
            once((THREE, DIM, DIM)), once(COLS), once((HALF, TOK)), once((HALF, TOK))],
        out_specs=[seq_spec(SQUARE), once((THREE, DIM, DIM)), once(COLS)],
        scratch_shapes=[pltpu.VMEM(SQUARE, F32)] * TWO + [pltpu.VMEM((THREE, *SQUARE), BF16), pltpu.VMEM(SQUARE, BF16),
                        pltpu.VMEM(SQUARE, F32), pltpu.VMEM((5, DIM, LANES), F32)],
        compiler_params=PARAMS, name="attn_bwd")(dctx, ctx, probs, q, k, v, x, dmid, w, c, *tables)


def rotary_tables():
    inv_freq = 1.0 / (THETA ** (jnp.arange(HALF, dtype=F32) * (2.0 / HEAD)))
    angles = inv_freq[:, None] * jnp.arange(TOK, dtype=F32)[None, :]
    return jnp.cos(angles), jnp.sin(angles)


MESH = pl.DeviceIdType.MESH
AXIS = "fsdp"
ORDERS = ((TWO, ONE, ZERO), (ONE, ZERO, TWO), (ZERO, TWO, ONE))


class Place:
    def __init__(self):
        me = lax.axis_index(AXIS)
        self.me = me
        self.core = lax.rem(me, TWO)
        self.pos = (me // 32, lax.rem(me // EIGHT, FOUR), lax.rem(me // TWO, FOUR))
        self.partner = me + ONE - TWO * self.core

    def coord(self, dim, delta):
        return lax.rem(self.pos[dim] + (delta + FOUR), FOUR)

    def device(self, dim, delta):
        pos = list(self.pos)
        pos[dim] = self.coord(dim, delta)
        return pos[ZERO] * 32 + pos[ONE] * EIGHT + pos[TWO] * TWO + self.core

    def greet(self, reach=(ONE, -ONE)):
        self.greeted = THREE * len(reach) + ONE
        barrier = pltpu.get_barrier_semaphore()
        for dim in range(THREE):
            for delta in reach:
                pl.semaphore_signal(barrier, inc=ONE, device_id=(self.device(dim, delta),), device_id_type=MESH)
        pl.semaphore_signal(barrier, inc=ONE, device_id=(self.partner,), device_id_type=MESH)

    def met(self):
        pl.semaphore_wait(pltpu.get_barrier_semaphore(), self.greeted)


def remote(src, dst, send_sem, recv_sem, device):
    return pltpu.make_async_remote_copy(src_ref=src, dst_ref=dst, send_sem=send_sem, recv_sem=recv_sem,
                                        device_id=(device,), device_id_type=MESH)


class Gather:
    def __init__(self, place, buf, order, send, recv):
        self.place, self.buf, self.order, self.send, self.recv = place, buf, order, send, recv
        self.units = buf.shape[FOUR]

    def where(self, stage, at, half=None):
        dim = self.order[stage]
        index = list(self.place.pos)
        index[dim] = at
        for done in self.order[:stage]:
            index[done] = slice(ZERO, FOUR)
        unit = slice(ZERO, self.units)
        if half is not None:
            if stage > ZERO:
                index[self.order[ZERO]] = pl.ds(TWO * half, TWO)
            else:
                cut = (self.units + ONE) // TWO
                unit = slice(ZERO, cut) if half == ZERO else slice(cut, self.units)
        index = [pl.ds(i, ONE) if not isinstance(i, (slice, pl.Slice)) else i for i in index]
        return self.buf.at[index[ZERO], index[ONE], index[TWO], pl.ds(self.place.core, ONE), unit]

    def copies(self, stage, step, way):
        place, dim = self.place, self.order[stage]
        delta = ONE if way == ZERO else -ONE
        key = (stage * TWO + step) * TWO + way
        if step == ZERO:
            mine = self.where(stage, place.pos[dim])
            came = self.where(stage, place.coord(dim, -delta))
        else:
            if stage == ZERO and self.units == ONE and way == ONE:
                return None, None
            mine = self.where(stage, place.coord(dim, -delta), way)
            came = self.where(stage, place.coord(dim, -TWO * delta), way)
        def build(ref):
            return remote(ref, ref, self.send.at[key], self.recv.at[key], place.device(dim, delta))

        return lambda: build(mine), lambda: build(came)

    def step_a(self, stage):
        for way in (ZERO, ONE):
            self.copies(stage, ZERO, way)[ZERO]().start()

    def step_b(self, stage):
        for way in (ZERO, ONE):
            self.copies(stage, ZERO, way)[ONE]().wait_recv()
            out = self.copies(stage, ONE, way)[ZERO]
            if out is not None:
                out().start()

    def step_c(self, stage):
        for way in (ZERO, ONE):
            inc = self.copies(stage, ONE, way)[ONE]
            if inc is not None:
                inc().wait_recv()

    def share(self):
        half = self.buf.at[:, :, :, pl.ds(self.place.core, ONE)]
        return remote(half, half, self.send.at[12], self.recv.at[12], self.place.partner)

    def shared(self):
        half = self.buf.at[:, :, :, pl.ds(ONE - self.place.core, ONE)]
        remote(half, half, self.send.at[12], self.recv.at[12], self.place.partner).wait_recv()

    def drain(self):
        for stage in range(THREE):
            for step in range(TWO):
                for way in (ZERO, ONE):
                    out = self.copies(stage, step, way)[ZERO]
                    if out is not None:
                        out().wait_send()
        self.share().wait_send()


def gather_all(gathers):
    for stage in range(THREE):
        for g in gathers:
            g.step_a(stage)
        for g in gathers:
            g.step_b(stage)
        for g in gathers:
            g.step_c(stage)
    for g in gathers:
        g.share().start()
    for g in gathers:
        g.shared()
    for g in gathers:
        g.drain()


class Scatter:
    def __init__(self, place, grads, acc, got_a, got_b, order, send, recv):
        self.place, self.grads, self.acc, self.order = place, grads, acc, order
        self.got_a, self.got_b, self.send, self.recv = got_a, got_b, send, recv
        self.units = acc.shape[ZERO]

    def columns(self, core):
        return pl.ds(pl.multiple_of(core * WIDTH, WIDTH), WIDTH)

    def swap(self):
        place = self.place
        for u in range(self.units):
            remote(self.grads(u).at[:, :, :, :, self.columns(ONE - place.core)], self.acc.at[u],
                   self.send.at[20 + u], self.recv.at[20 + u], place.partner).start()

    def swapped(self):
        place = self.place
        for u in range(self.units):
            copy = remote(self.grads(u).at[:, :, :, :, self.columns(ONE - place.core)], self.acc.at[u],
                          self.send.at[20 + u], self.recv.at[20 + u], place.partner)
            copy.wait_recv()
            grad, acc = self.grads(u), self.acc

            @pl.loop(ZERO, SIXTEEN)
            def _(i):
                z, y = i // FOUR, lax.rem(i, FOUR)
                acc[u, z, y] = acc[u, z, y] + grad[z, y, :, :, self.columns(place.core)]

    def index(self, stage, at):
        index = [slice(ZERO, FOUR)] * THREE
        for done in self.order[:stage]:
            index[done] = pl.ds(self.place.pos[done], ONE)
        index[self.order[stage]] = pl.ds(at, ONE)
        return index

    def part(self, stage, at, half=None):
        columns = slice(ZERO, WIDTH) if half is None else slice(128 * half, 128 * half + 128)
        return self.acc.at[(slice(ZERO, self.units), *self.index(stage, at), slice(ZERO, EIGHT), columns)]

    def copy(self, stage, step, way):
        place, dim = self.place, self.order[stage]
        delta = ONE if way == ZERO else -ONE
        key = (stage * TWO + step) * TWO + way
        if step == ZERO:
            src, ref, half = self.part(stage, place.coord(dim, TWO), way), self.got_a, way
        else:
            src, ref, half = self.part(stage, place.coord(dim, delta)), self.got_b, None
        return src, ref, half, key, place.device(dim, delta)

    def start(self, stage, step, way):
        src, ref, half, key, device = self.copy(stage, step, way)
        remote(src, self.cast(ref, stage, way, half, src), self.send.at[key], self.recv.at[key], device).start()

    def wait(self, stage, step, way):
        src, ref, half, key, device = self.copy(stage, step, way)
        remote(src, self.cast(ref, stage, way, half, src), self.send.at[key], self.recv.at[key], device).wait_recv()

    def cast(self, ref, stage, way, half, src):
        columns = slice(ZERO, WIDTH) if half is None else slice(128 * half, 128 * half + 128)
        return ref[stage].at[(ZERO if half is not None else way, slice(ZERO, self.units), *([slice(None)] * THREE), slice(ZERO, EIGHT), columns)]

    def add(self, stage, at, refs, half):
        units = self.units
        shape = self.got_b[stage].shape[TWO:5]
        total = units * shape[ZERO] * shape[ONE] * shape[TWO]
        columns = slice(ZERO, WIDTH) if half is None else slice(128 * half, 128 * half + 128)
        base = [ZERO, ZERO, ZERO]
        for done in self.order[:stage]:
            base[done] = self.place.pos[done]
        base[self.order[stage]] = at
        acc = self.acc
        bunch = FOUR if total % FOUR == ZERO else ONE

        @pl.loop(ZERO, total // bunch)
        def _(k):
            for j in range(bunch):
                i = k * bunch + j
                u = i // (shape[ZERO] * shape[ONE] * shape[TWO])
                a = lax.rem(i // (shape[ONE] * shape[TWO]), shape[ZERO])
                b = lax.rem(i // shape[TWO], shape[ONE])
                c = lax.rem(i, shape[TWO])
                here = (u, base[ZERO] + a, base[ONE] + b, base[TWO] + c, slice(ZERO, EIGHT), columns)
                value = acc[here]
                for ref, way in refs:
                    value = value + ref[stage][ZERO if half is not None else way, u, a, b, c, :, columns]
                acc[here] = value

    def step_a(self, stage):
        for way in (ZERO, ONE):
            self.start(stage, ZERO, way)

    def step_b(self, stage):
        dim = self.order[stage]
        for way in (ZERO, ONE):
            delta = ONE if way == ZERO else -ONE
            self.wait(stage, ZERO, way)
            self.add(stage, self.place.coord(dim, delta), [(self.got_a, way)], way)
            self.start(stage, ONE, way)

    def step_c(self, stage):
        dim = self.order[stage]
        for way in (ZERO, ONE):
            self.wait(stage, ONE, way)
        self.add(stage, self.place.pos[dim], [(self.got_b, ZERO), (self.got_b, ONE)], None)

    def last(self, own, other):
        place = self.place
        z, y, x = place.pos
        src = self.acc.at[:, z, y, x]
        return remote(src, other, self.send.at[12], self.recv.at[12], place.partner)

    def drain(self, other):
        for stage in range(THREE):
            for step in range(TWO):
                for way in (ZERO, ONE):
                    src, ref, half, key, device = self.copy(stage, step, way)
                    remote(src, self.cast(ref, stage, way, half, src), self.send.at[key], self.recv.at[key], device).wait_send()
        for u in range(self.units):
            remote(self.grads(u).at[:, :, :, :, self.columns(ONE - self.place.core)], self.acc.at[u],
                   self.send.at[20 + u], self.recv.at[20 + u], self.place.partner).wait_send()
        self.last(None, other).wait_send()

    def result(self, unit, other):
        z, y, x = self.place.pos
        own, came = self.acc[unit, z, y, x], other[unit]
        first = self.place.core == ZERO
        return jnp.concatenate([jnp.where(first, own, came), jnp.where(first, came, own)], axis=ONE)


def landing_shapes(order, units, ways):
    shapes = []
    for stage in range(THREE):
        size = [FOUR, FOUR, FOUR]
        for done in order[:stage + ONE]:
            size[done] = ONE
        shapes.append((ways, units, *size, EIGHT, WIDTH))
    return shapes


class Small:
    def __init__(self, place, value, slots, send, recv):
        self.place, self.value, self.slots, self.send, self.recv = place, value, slots, send, recv

    def copies(self, stage):
        if stage == THREE:
            return [remote(self.value, self.slots.at[9], self.send.at[9], self.recv.at[9], self.place.partner)]
        return [remote(self.value, self.slots.at[stage * THREE + k], self.send.at[stage * THREE + k], self.recv.at[stage * THREE + k],
                       self.place.device(stage, delta)) for k, delta in enumerate((ONE, -ONE, TWO))]

    def start(self, stage):
        for copy in self.copies(stage):
            copy.start()

    def finish(self, stage):
        copies = self.copies(stage)
        for copy in copies:
            copy.wait()
        value = self.value[...]
        for k in range(len(copies)):
            value = value + self.slots[stage * THREE + k]
        self.value[...] = value


COLOURS = ((ZERO, THREE, FOUR, 5), (ONE, 6, 7, EIGHT), (TWO, 9, 10, 11))
KEYS = 28


def each_unit():
    for colour in range(THREE):
        for layer in range(TWO):
            for slot, unit in enumerate(COLOURS[colour]):
                yield colour, layer, layer * FOUR + slot, unit


def gather_kernel(packed, small, attn_out, up_out, down_out, attn_t, up_t, down_t, small_out, buf0, buf1, buf2, buf3, send, recv, local):
    place = Place()
    place.greet()
    z, y, x = place.pos
    bufs = (buf0, buf1, buf2)
    copies = [pltpu.make_async_copy(packed.at[k], bufs[k].at[z, y, x, place.core], local.at[k]) for k in range(THREE)]
    copies.append(pltpu.make_async_copy(small, buf3.at[z, y, x, place.core], local.at[THREE]))
    for copy in copies:
        copy.start()
    for copy in copies:
        copy.wait()
    place.met()
    gathers = [Gather(place, bufs[k], ORDERS[k], send.at[k], recv.at[k]) for k in range(THREE)]
    gathers.append(Gather(place, buf3, ORDERS[ZERO], send.at[THREE], recv.at[THREE]))
    gather_all(gathers)
    small_out[...] = buf3[...]

    for colour, layer, u, unit in each_unit():
        buf = bufs[colour]
        if unit < EIGHT:
            @pl.loop(ZERO, 32)
            def _(g):
                tiles = [buf[g // EIGHT, lax.rem(g // TWO, FOUR), lax.rem(g, TWO) * TWO + k // TWO, k % TWO, u].astype(F32) for k in range(FOUR)]
                rows = pl.ds(pl.multiple_of(g * SIXTEEN, SIXTEEN), SIXTEEN)
                for j, cols in enumerate(lane_tiles()):
                    block = jnp.concatenate([t[FOUR * j:FOUR * j + FOUR] for t in tiles], axis=ZERO).astype(BF16)
                    if unit < FOUR:
                        attn_out[layer, unit, rows, cols] = block
                    else:
                        up_out[layer, rows, DIM * (unit - FOUR) + cols.start:DIM * (unit - FOUR) + cols.stop] = block
        else:
            @pl.loop(ZERO, LANES)
            def _(d):
                rows = pl.ds(pl.multiple_of(d * SIXTEEN, SIXTEEN), SIXTEEN)
                down_out[layer, rows, lane_tiles()[unit - EIGHT]] = buf[d // 32, lax.rem(d // EIGHT, FOUR), lax.rem(d // TWO, FOUR), lax.rem(d, TWO), u]
    for layer in range(TWO):
        for k in range(FOUR):
            attn_t[layer, k] = attn_out[layer, k].T
            part = slice(DIM * k, DIM * k + DIM)
            up_t[layer, part, :] = up_out[layer, :, part].T
            down_t[layer, :, part] = down_out[layer, part, :].T


VMEM = pl.BlockSpec(memory_space=pltpu.VMEM)
HBM = pl.BlockSpec(memory_space=pl.ANY)
DMA = pltpu.SemaphoreType.DMA


def gather_params(packed, small):
    shapes = ((TWO, FOUR, DIM, DIM), (TWO, *WIDE), (TWO, FFN, DIM))
    both = shapes + (shapes[ZERO], shapes[TWO], shapes[ONE])
    tiny = (FOUR, FOUR, FOUR, TWO, ONE, ONE, LANES)
    return pl.pallas_call(
        gather_kernel,
        out_shape=[jax.ShapeDtypeStruct(s, BF16) for s in both] + [jax.ShapeDtypeStruct(tiny, F32)],
        in_specs=[HBM] * TWO,
        out_specs=[VMEM] * 7,
        scratch_shapes=[pltpu.VMEM((FOUR, FOUR, FOUR, TWO, EIGHT, SIXTEEN, LANES), BF16)] * THREE + [pltpu.VMEM(tiny, F32), DMA((FOUR, 13)), DMA((FOUR, 13)), DMA((FOUR,))],
        compiler_params=pltpu.CompilerParams(collective_id=ZERO, has_side_effects=True, vmem_limit_bytes=60 << 20),
        name="gather_params")(packed, small)


def scatter_kernel(*refs):
    place = Place()
    place.greet((ONE, -ONE, TWO))
    weights, refs = (refs[:FOUR], refs[FOUR:EIGHT]), refs[EIGHT:]
    small, attn_out, up_out, down_out, small_out = refs[:5]
    grads, accs, others, (sm, slots), refs = refs[5:EIGHT], refs[EIGHT:11], refs[11:14], refs[14:SIXTEEN], refs[SIXTEEN:]
    got_a = [refs[THREE * k:THREE * k + THREE] for k in range(THREE)]
    got_b = [refs[9 + THREE * k:9 + THREE * k + THREE] for k in range(THREE)]
    send, recv, ssend, srecv, local = refs[18:]
    copies = []
    for colour, layer, u, unit in each_unit():
        qkv, out, up, down = weights[layer]
        if unit < THREE:
            src = qkv.at[unit]
        elif unit == THREE:
            src = out
        elif unit < EIGHT:
            src = up.at[:, :, :, :, pl.ds(DIM * (unit - FOUR), DIM)]
        else:
            src = down.at[:, :, :, unit - EIGHT]
        copies.append(pltpu.make_async_copy(src, grads[colour].at[u], local.at[colour]))
    copies.append(pltpu.make_async_copy(small, sm, local.at[THREE]))
    for copy in copies:
        copy.start()
    for copy in copies:
        copy.wait()
    place.met()
    scatters = [Scatter(place, (lambda u, k=k: grads[k].at[u]), accs[k], got_a[k], got_b[k], ORDERS[k], send.at[k], recv.at[k])
                for k in range(THREE)]
    tiny = Small(place, sm, slots, ssend, srecv)
    for s in scatters:
        s.swap()
    tiny.start(ZERO)
    for s in scatters:
        s.swapped()
        s.step_a(ZERO)
    for stage in range(THREE):
        if stage:
            for s in scatters:
                s.step_a(stage)
        for s in scatters:
            s.step_b(stage)
        tiny.finish(stage)
        tiny.start(stage + ONE)
        for s in scatters:
            s.step_c(stage)
    for s, other in zip(scatters, others):
        s.last(None, other).start()
    tiny.finish(THREE)
    for s, other in zip(scatters, others):
        s.last(None, other).wait_recv()
    small_out[...] = sm[...]
    first = place.core == ZERO
    for colour, layer, u, unit in each_unit():
        full = scatters[colour].result(u, others[colour])
        if unit < EIGHT:
            mine = jnp.where(first, full[:FOUR], full[FOUR:])
            if unit < FOUR:
                attn_out[layer, unit] = mine
            else:
                up_out[layer, :, DIM * (unit - FOUR):DIM * (unit - THREE)] = mine
        else:
            at = EIGHT * (unit % TWO)

            @pl.when(place.core == (unit - EIGHT) // TWO)
            def _():
                down_out[layer, at:at + EIGHT] = full
    for s, other in zip(scatters, others):
        s.drain(other)


def scatter_grads(weights, small):
    acc, tiny = (EIGHT, FOUR, FOUR, FOUR, EIGHT, WIDTH), (32, DIM)
    scratch = [pltpu.VMEM((EIGHT, FOUR, FOUR, FOUR, EIGHT, DIM), F32)] * THREE + [pltpu.VMEM(acc, F32)] * THREE + [pltpu.VMEM((EIGHT, EIGHT, WIDTH), F32)] * THREE
    scratch += [pltpu.VMEM(tiny, F32), pltpu.VMEM((10, *tiny), F32)]
    for ways in (ONE, TWO):
        for order in ORDERS:
            scratch += [pltpu.VMEM(s, F32) for s in landing_shapes(order, EIGHT, ways)]
    scratch += [DMA((THREE, KEYS)), DMA((THREE, KEYS)), DMA((10,)), DMA((10,)), DMA((FOUR,))]
    grid = (FOUR, FOUR, FOUR)
    flat = []
    for qkv, out, up, down in weights:
        flat += [qkv.reshape(THREE, *grid, EIGHT, DIM), out.reshape(*grid, EIGHT, DIM), up.reshape(*grid, EIGHT, FFN), down.reshape(*grid, FOUR, EIGHT, DIM)]
    return pl.pallas_call(
        scatter_kernel,
        out_shape=[jax.ShapeDtypeStruct(s, F32) for s in ((TWO, FOUR, FOUR, DIM), (TWO, FOUR, FFN), (TWO, SIXTEEN, DIM), tiny)],
        in_specs=[HBM] * 9,
        out_specs=[VMEM] * FOUR,
        scratch_shapes=scratch,
        compiler_params=pltpu.CompilerParams(collective_id=ONE, has_side_effects=True, vmem_limit_bytes=63 << 20),
        name="scatter_grads")(*flat, small)


def pack_shards(w_attn, w_up, w_down):
    attn = w_attn.reshape(TWO, FOUR, FOUR, FOUR, LANES).transpose(ZERO, ONE, THREE, TWO, FOUR).reshape(TWO, FOUR, SIXTEEN, LANES)
    up = w_up.reshape(TWO, FOUR, FOUR, FOUR, LANES).transpose(ZERO, TWO, THREE, ONE, FOUR).reshape(TWO, FOUR, SIXTEEN, LANES)
    down = w_down.reshape(TWO, SIXTEEN, FOUR, LANES).transpose(ZERO, TWO, ONE, THREE)
    units = jnp.concatenate([attn, up, down], axis=ONE)
    return jnp.stack([jnp.concatenate([units[layer, jnp.array(c)] for layer in range(TWO)], axis=ZERO) for c in COLOURS])


def pack_small(b_attn, ln_par, b_up, b_down):
    row = jnp.concatenate([b_attn.reshape(TWO, SIXTEEN), ln_par.reshape(TWO, SIXTEEN), b_up, b_down, jnp.zeros((TWO, 12), b_up.dtype)], axis=ONE)
    return row.reshape(ONE, ONE, LANES).astype(F32)


def small_columns(small):
    small = small.reshape(LANES, TWO, 64)
    parts = small[:, :, :32].reshape(LANES, TWO, EIGHT, FOUR).transpose(ONE, ZERO, THREE, TWO).reshape(TWO, DIM, EIGHT)
    ups = small[:, :, 32:48].transpose(ONE, ZERO, TWO).reshape(TWO, FOUR, DIM).transpose(ZERO, TWO, ONE)
    down = small[:, :, 48:52].transpose(ONE, ZERO, TWO).reshape(TWO, DIM, ONE)
    return jnp.pad(jnp.concatenate([parts, ups, down], axis=TWO), ((ZERO, ZERO), (ZERO, ZERO), (ZERO, LANES - 13)))


def solution(mesh):
    batch_spec = P(AXIS)
    weight_specs = (P(None, None, AXIS, None), P(None, None, AXIS), P(None, None, AXIS),
                    P(None, AXIS, None), P(None, AXIS), P(None, AXIS, None), P(None, AXIS))

    def device_step(x, lengths, d_y, w_attn, b_attn, ln_par, w_up, b_up, w_down, b_down):
        tables = rotary_tables()
        attn, up, down, attn_t, up_t, down_t, small = gather_params(pack_shards(w_attn, w_up, w_down), pack_small(b_attn, ln_par, b_up, b_down))
        columns = small_columns(small)
        saved = []
        for l in range(TWO):
            first, last = l == ZERO, l == ONE
            c = columns[l]
            outs = attn_fwd(first, lengths, x, attn_t[l, :THREE], c, tables)
            if first:
                x, *outs = outs
            q, k, v, probs, ctx = outs
            mid, act, slope, *rest = mlp_fwd(last, ctx, x, attn_t[l, THREE], up_t[l], down_t[l], c)
            saved.append((x, q, k, v, probs, ctx, mid, act, slope))
            if rest:
                x = rest[ZERO]
        grad, weights, rows = d_y, [None] * TWO, [None] * TWO
        for l in (ONE, ZERO):
            x, q, k, v, probs, ctx, mid, act, slope = saved[l]
            c = columns[l]
            dmid, dctx, gwo, gup, gdown, gc_mlp = mlp_bwd(l == ONE, grad, slope, act, mid, ctx, attn[l, THREE], up[l], down[l], c)
            grad, gw, gc_attn = attn_bwd(l == ZERO, dctx, ctx, probs, q, k, v, x, dmid, attn[l, :THREE], c, tables)
            weights[l] = (gw, gwo, gup, gdown)
            rows[l] = (gc_mlp + gc_attn)[:, :SIXTEEN].T
        attn, up, down, small = scatter_grads(weights, jnp.concatenate(rows))
        me = lax.axis_index(AXIS)
        small = small.reshape(TWO, SIXTEEN, DIM)
        mine = lax.dynamic_slice(small, (ZERO, ZERO, FOUR * me), (TWO, SIXTEEN, FOUR))
        b_up_grad = lax.dynamic_slice(small[:, B_UP:B_DOWN].reshape(TWO, FFN), (ZERO, SIXTEEN * me), (TWO, SIXTEEN))
        return grad, attn, mine[:, :FOUR], mine[:, FOUR:EIGHT], up, b_up_grad, down, mine[:, 12]

    return jax.shard_map(device_step, mesh=mesh,
                         in_specs=(batch_spec, batch_spec, batch_spec) + weight_specs,
                         out_specs=(batch_spec,) + weight_specs,
                         check_vma=False)
```

```python
import math
import functools
import jax
import jax.numpy as jnp
from jax import lax
from jax.experimental import pallas as pl
from jax.experimental.pallas import tpu as pltpu
from jax.sharding import PartitionSpec as P

ZERO, ONE, TWO, THREE, FOUR = range(5)
EIGHT, SIXTEEN, WIDTH = 8, 16, 256

F32, BF16 = jnp.float32, jnp.bfloat16
SEQS, TOK, DIM, FFN, HEADS, HEAD, LANES = FOUR, 512, 512, 2048, EIGHT, 64, 128
HALF = HEAD // TWO
EPS = 1e-5
THETA = 10000.0
NEG_BIG = -1e30
B_ATTN, LN_PAR, B_UP, B_DOWN = ZERO, FOUR, EIGHT, 12


def nn(a, b):
    return lax.dot_general(a, b, (((ONE,), (ZERO,)), ((), ())), preferred_element_type=F32)


def nt(a, b):
    return lax.dot_general(a, b, (((ONE,), (ONE,)), ((), ())), preferred_element_type=F32)


def tn(a, b):
    return lax.dot_general(a, b, (((ZERO,), (ZERO,)), ((), ())), preferred_element_type=F32)


def lane_tiles(width=TOK, size=LANES):
    return [slice(i, i + size) for i in range(ZERO, width, size)]


def column(c_ref, lane, width=LANES):
    return jnp.broadcast_to(c_ref[:, lane:lane + ONE], (c_ref.shape[ZERO], width))


def total(value):
    return jnp.sum(value, axis=ZERO, keepdims=True)


def normed(x):
    centred = x - total(x) * (1.0 / DIM)
    rstd = lax.rsqrt(total(centred * centred) * (1.0 / DIM) + EPS)
    return centred * rstd, rstd


def norm_to(x_ref, c_ref, lane, h_ref):
    gain, shift = column(c_ref, lane), column(c_ref, lane + ONE)
    for cols in lane_tiles():
        h_ref[:, cols] = (normed(x_ref[:, cols].astype(F32))[ZERO] * gain + shift).astype(BF16)


def fold(value):
    parts = [value[:, cols] for cols in lane_tiles(value.shape[ONE])]
    return functools.reduce(jnp.add, parts)


def norm_back(dh, x, gain):
    xhat, rstd = normed(x)
    dxhat = dh * gain
    mean_one = total(dxhat) * (1.0 / DIM)
    mean_two = total(dxhat * xhat) * (1.0 / DIM)
    return rstd * (dxhat - mean_one - xhat * mean_two), xhat


def put_columns(out_ref, columns):
    lane = lax.broadcasted_iota(jnp.int32, (DIM, LANES), ONE)
    value = jnp.zeros((DIM, LANES), F32)
    for at, partial in columns:
        value = jnp.where(lane == at, jnp.sum(partial, axis=ONE, keepdims=True), value)
    out_ref[...] = value


def mlp_bwd_kernel(last, dy_ref, slope_ref, act_ref, mid_ref, ctx_ref, wo_ref, up_ref, down_ref, c_ref,
                   dmid_ref, dctx_ref, gwo_ref, gup_ref, gdown_ref, gc_ref, dyt_ref, dpre_ref, h_ref, dh_ref, sums_ref):
    seq = pl.program_id(ZERO)

    @pl.when(seq == ZERO)
    def _():
        for ref in (gwo_ref, gup_ref, gdown_ref, sums_ref):
            ref[...] = jnp.zeros_like(ref)

    if last:
        dyt_ref[...] = dy_ref[ZERO].T
    else:
        dyt_ref[...] = dy_ref[ZERO]
    norm_to(mid_ref.at[ZERO], c_ref, LN_PAR + TWO, h_ref)
    for part in range(FFN // DIM):
        rows = slice(DIM * part, DIM * part + DIM)
        dact = nn(down_ref[rows, :], dyt_ref[...])
        for cols in lane_tiles():
            dpre = dact[:, cols] * slope_ref[ZERO, rows, cols]
            sums_ref[part] += dpre
            dpre_ref[rows, cols] = dpre.astype(BF16)
        gdown_ref[rows, :] += nt(act_ref[ZERO, rows, :], dyt_ref[...])
        gup_ref[:, rows] += nt(h_ref[...], dpre_ref[rows, :])
    dh_ref[...] = nn(up_ref[...], dpre_ref[...])
    gain = column(c_ref, LN_PAR + TWO)
    for cols in lane_tiles():
        dh, dy = dh_ref[:, cols], dyt_ref[:, cols].astype(F32)
        dx, xhat = norm_back(dh, mid_ref[ZERO, :, cols].astype(F32), gain)
        dmid = (dy + dx).astype(BF16)
        dmid_ref[ZERO, :, cols] = dmid
        sums_ref[FOUR] += dh * xhat
        sums_ref[5] += dh
        sums_ref[6] += dy
        sums_ref[7] += dmid.astype(F32)
    gwo_ref[...] += nt(ctx_ref[ZERO].astype(BF16), dmid_ref[ZERO])
    dctx_ref[ZERO] = nn(wo_ref[...], dmid_ref[ZERO]).astype(BF16)

    @pl.when(seq == SEQS - ONE)
    def _():
        put_columns(gc_ref, [(B_UP + i, sums_ref[i]) for i in range(FOUR)] + [
            (LN_PAR + TWO, sums_ref[FOUR]), (LN_PAR + THREE, sums_ref[5]), (B_DOWN, sums_ref[6]), (B_ATTN + THREE, sums_ref[7])])


def attn_bwd_kernel(first, dctx_ref, ctx_ref, p_ref, q_ref, k_ref, v_ref, x_ref, dmid_ref, w_ref, c_ref, cos_ref, sin_ref,
                    dx_ref, gw_ref, gc_ref, dq_ref, dk_ref, dproj_ref, h_ref, dh_ref, sums_ref):
    seq = pl.program_id(ZERO)

    @pl.when(seq == ZERO)
    def _():
        gw_ref[...] = jnp.zeros_like(gw_ref)
        sums_ref[...] = jnp.zeros_like(sums_ref)

    @pl.loop(ZERO, HEADS)
    def _(head):
        rows = pl.ds(pl.multiple_of(head * HEAD, HEAD), HEAD)
        dk = jnp.zeros((HEAD, TOK), F32)
        dv = jnp.zeros((HEAD, TOK), F32)
        for cols in lane_tiles(TOK, WIDTH):
            dctx = dctx_ref[ZERO, rows, cols]
            delta = total(dctx.astype(F32) * ctx_ref[ZERO, rows, cols])
            dprobs = tn(v_ref[ZERO, rows, :], dctx)
            probs = p_ref[ZERO, head, :, cols]
            dscores = (probs.astype(F32) * (dprobs - delta)).astype(BF16)
            dv = dv + nt(dctx, probs)
            dk = dk + nt(q_ref[ZERO, rows, cols], dscores)
            dq_ref[rows, cols] = nn(k_ref[ZERO, rows, :], dscores)
        dk_ref[rows, :] = dk
        sums_ref[TWO, rows, :] += fold(dv)
        dproj_ref[TWO, rows, :] = dv.astype(BF16)

    for m, (ref, scale) in enumerate(((dq_ref, HEAD ** -0.5), (dk_ref, 1.0))):
        for cols in lane_tiles():
            for head in range(HEADS):
                one, two = slice(HEAD * head, HEAD * head + HALF), slice(HEAD * head + HALF, HEAD * head + HEAD)
                a, b = ref[one, cols] * scale, ref[two, cols] * scale
                cos, sin = cos_ref[:, cols], sin_ref[:, cols]
                for rows, value in ((one, a * cos + b * sin), (two, b * cos - a * sin)):
                    dproj_ref[m, rows, cols] = value.astype(BF16)
                    sums_ref[m, rows, :] += value
    norm_to(x_ref.at[ZERO], c_ref, LN_PAR, h_ref)
    for m in range(THREE):
        gw_ref[m] += nt(h_ref[...], dproj_ref[m])
    dh_ref[...] = functools.reduce(jnp.add, [nn(w_ref[m], dproj_ref[m]) for m in range(THREE)])
    gain = column(c_ref, LN_PAR)
    for cols in lane_tiles():
        dh = dh_ref[:, cols]
        dx, xhat = norm_back(dh, x_ref[ZERO, :, cols].astype(F32), gain)
        dx = (dmid_ref[ZERO, :, cols].astype(F32) + dx).astype(BF16)
        if first:
            dx_ref[ZERO, cols, :] = dx.T
        else:
            dx_ref[ZERO, :, cols] = dx
        sums_ref[THREE] += dh * xhat
        sums_ref[FOUR] += dh

    @pl.when(seq == SEQS - ONE)
    def _():
        put_columns(gc_ref, [(B_ATTN + i, sums_ref[i]) for i in range(THREE)] + [(LN_PAR, sums_ref[THREE]), (LN_PAR + ONE, sums_ref[FOUR])])


def seq_spec(shape):
    return pl.BlockSpec((ONE, *shape), lambda s: (s,) + (ZERO,) * len(shape))


def layer_seq(layer, shape):
    return pl.BlockSpec((None, ONE, *shape), lambda s: (layer, s) + (ZERO,) * len(shape))


def layer_once(layer, shape):
    return pl.BlockSpec((None, *shape), lambda s: (layer,) + (ZERO,) * len(shape), pipeline_mode=pl.Buffered(ONE))


def once(shape):
    return pl.BlockSpec(shape, lambda s: (ZERO,) * len(shape), pipeline_mode=pl.Buffered(ONE))


def act_shape(rows, dtype):
    return jax.ShapeDtypeStruct((SEQS, rows, TOK), dtype)


PARAMS = pltpu.CompilerParams(vmem_limit_bytes=60 << 20, dimension_semantics=("arbitrary",))
SQUARE, TALL, WIDE, COLS = (DIM, TOK), (FFN, TOK), (DIM, FFN), (DIM, LANES)


def mlp_bwd(layer, last, dy, slope, act, mid, ctx, wo, up, down, c):
    return pl.pallas_call(
        functools.partial(mlp_bwd_kernel, last), grid=(SEQS,),
        out_shape=[act_shape(DIM, BF16)] * TWO + [jax.ShapeDtypeStruct(s, F32) for s in ((DIM, DIM), WIDE, (FFN, DIM), COLS)],
        in_specs=[seq_spec(SQUARE)] + [layer_seq(layer, s) for s in (TALL, TALL, SQUARE, SQUARE)] + [
            layer_once(layer, s) for s in ((DIM, DIM), WIDE, (FFN, DIM), COLS)],
        out_specs=[seq_spec(SQUARE)] * TWO + [once((DIM, DIM)), once(WIDE), once((FFN, DIM)), once(COLS)],
        scratch_shapes=[pltpu.VMEM(SQUARE, BF16), pltpu.VMEM(TALL, BF16), pltpu.VMEM(SQUARE, BF16), pltpu.VMEM(SQUARE, F32),
                        pltpu.VMEM((EIGHT, DIM, LANES), F32)],
        compiler_params=PARAMS, name="mlp_bwd")(dy, slope, act, mid, ctx, wo, up, down, c)


def attn_bwd(layer, first, dctx, ctx, probs, q, k, v, x, dmid, w, c, tables):
    return pl.pallas_call(
        functools.partial(attn_bwd_kernel, first), grid=(SEQS,),
        out_shape=[act_shape(DIM, BF16), jax.ShapeDtypeStruct((THREE, DIM, DIM), F32), jax.ShapeDtypeStruct(COLS, F32)],
        in_specs=[seq_spec(SQUARE)] + [layer_seq(layer, s) for s in (SQUARE, (HEADS, TOK, TOK), SQUARE, SQUARE, SQUARE, SQUARE)] + [
            seq_spec(SQUARE), layer_once(layer, (THREE, DIM, DIM)), layer_once(layer, COLS), once((HALF, TOK)), once((HALF, TOK))],
        out_specs=[seq_spec(SQUARE), once((THREE, DIM, DIM)), once(COLS)],
        scratch_shapes=[pltpu.VMEM(SQUARE, F32)] * TWO + [pltpu.VMEM((THREE, *SQUARE), BF16), pltpu.VMEM(SQUARE, BF16),
                        pltpu.VMEM(SQUARE, F32), pltpu.VMEM((5, DIM, LANES), F32)],
        compiler_params=PARAMS, name="attn_bwd")(dctx, ctx, probs, q, k, v, x, dmid, w, c, *tables)


def rotary_tables():
    inv_freq = 1.0 / (THETA ** (jnp.arange(HALF, dtype=F32) * (2.0 / HEAD)))
    angles = inv_freq[:, None] * jnp.arange(TOK, dtype=F32)[None, :]
    return jnp.cos(angles), jnp.sin(angles)


MESH = pl.DeviceIdType.MESH
AXIS = "fsdp"
ORDERS = ((TWO, ONE, ZERO), (ONE, ZERO, TWO), (ZERO, TWO, ONE))


class Place:
    def __init__(self):
        me = lax.axis_index(AXIS)
        self.me = me
        self.core = lax.rem(me, TWO)
        self.pos = (me // 32, lax.rem(me // EIGHT, FOUR), lax.rem(me // TWO, FOUR))
        self.partner = me + ONE - TWO * self.core

    def coord(self, dim, delta):
        return lax.rem(self.pos[dim] + (delta + FOUR), FOUR)

    def device(self, dim, delta):
        pos = list(self.pos)
        pos[dim] = self.coord(dim, delta)
        return pos[ZERO] * 32 + pos[ONE] * EIGHT + pos[TWO] * TWO + self.core

    def greet(self, reach=(ONE, -ONE)):
        self.greeted = THREE * len(reach) + ONE
        barrier = pltpu.get_barrier_semaphore()
        for dim in range(THREE):
            for delta in reach:
                pl.semaphore_signal(barrier, inc=ONE, device_id=(self.device(dim, delta),), device_id_type=MESH)
        pl.semaphore_signal(barrier, inc=ONE, device_id=(self.partner,), device_id_type=MESH)

    def met(self):
        pl.semaphore_wait(pltpu.get_barrier_semaphore(), self.greeted)


def remote(src, dst, send_sem, recv_sem, device):
    return pltpu.make_async_remote_copy(src_ref=src, dst_ref=dst, send_sem=send_sem, recv_sem=recv_sem,
                                        device_id=(device,), device_id_type=MESH)


class Gather:
    def __init__(self, place, buf, order, send, recv):
        self.place, self.buf, self.order, self.send, self.recv = place, buf, order, send, recv
        self.units = buf.shape[FOUR]

    def where(self, stage, at, half=None):
        dim = self.order[stage]
        index = list(self.place.pos)
        index[dim] = at
        for done in self.order[:stage]:
            index[done] = slice(ZERO, FOUR)
        unit = slice(ZERO, self.units)
        if half is not None:
            if stage > ZERO:
                index[self.order[ZERO]] = pl.ds(TWO * half, TWO)
            else:
                cut = (self.units + ONE) // TWO
                unit = slice(ZERO, cut) if half == ZERO else slice(cut, self.units)
        index = [pl.ds(i, ONE) if not isinstance(i, (slice, pl.Slice)) else i for i in index]
        return self.buf.at[index[ZERO], index[ONE], index[TWO], pl.ds(self.place.core, ONE), unit]

    def copies(self, stage, step, way):
        place, dim = self.place, self.order[stage]
        delta = ONE if way == ZERO else -ONE
        key = (stage * TWO + step) * TWO + way
        if step == ZERO:
            mine = self.where(stage, place.pos[dim])
            came = self.where(stage, place.coord(dim, -delta))
        else:
            if stage == ZERO and self.units == ONE and way == ONE:
                return None, None
            mine = self.where(stage, place.coord(dim, -delta), way)
            came = self.where(stage, place.coord(dim, -TWO * delta), way)
        def build(ref):
            return remote(ref, ref, self.send.at[key], self.recv.at[key], place.device(dim, delta))

        return lambda: build(mine), lambda: build(came)

    def step_a(self, stage):
        for way in (ZERO, ONE):
            self.copies(stage, ZERO, way)[ZERO]().start()

    def step_b(self, stage):
        for way in (ZERO, ONE):
            self.copies(stage, ZERO, way)[ONE]().wait_recv()
            out = self.copies(stage, ONE, way)[ZERO]
            if out is not None:
                out().start()

    def step_c(self, stage):
        for way in (ZERO, ONE):
            inc = self.copies(stage, ONE, way)[ONE]
            if inc is not None:
                inc().wait_recv()

    def share(self):
        half = self.buf.at[:, :, :, pl.ds(self.place.core, ONE)]
        return remote(half, half, self.send.at[12], self.recv.at[12], self.place.partner)

    def shared(self):
        half = self.buf.at[:, :, :, pl.ds(ONE - self.place.core, ONE)]
        remote(half, half, self.send.at[12], self.recv.at[12], self.place.partner).wait_recv()

    def drain(self):
        for stage in range(THREE):
            for step in range(TWO):
                for way in (ZERO, ONE):
                    out = self.copies(stage, step, way)[ZERO]
                    if out is not None:
                        out().wait_send()
        self.share().wait_send()


def gather_all(gathers):
    for stage in range(THREE):
        for g in gathers:
            g.step_a(stage)
        for g in gathers:
            g.step_b(stage)
        for g in gathers:
            g.step_c(stage)
    for g in gathers:
        g.share().start()
    for g in gathers:
        g.shared()
    for g in gathers:
        g.drain()


class Scatter:
    def __init__(self, place, grads, acc, got_a, got_b, order, send, recv):
        self.place, self.grads, self.acc, self.order = place, grads, acc, order
        self.got_a, self.got_b, self.send, self.recv = got_a, got_b, send, recv
        self.units = acc.shape[ZERO]

    def columns(self, core):
        return pl.ds(pl.multiple_of(core * WIDTH, WIDTH), WIDTH)

    def swap(self):
        place = self.place
        for u in range(self.units):
            remote(self.grads(u).at[:, :, :, :, self.columns(ONE - place.core)], self.acc.at[u],
                   self.send.at[20 + u], self.recv.at[20 + u], place.partner).start()

    def swapped(self):
        place = self.place
        for u in range(self.units):
            copy = remote(self.grads(u).at[:, :, :, :, self.columns(ONE - place.core)], self.acc.at[u],
                          self.send.at[20 + u], self.recv.at[20 + u], place.partner)
            copy.wait_recv()
            grad, acc = self.grads(u), self.acc

            @pl.loop(ZERO, SIXTEEN)
            def _(i):
                z, y = i // FOUR, lax.rem(i, FOUR)
                acc[u, z, y] = acc[u, z, y] + grad[z, y, :, :, self.columns(place.core)]

    def index(self, stage, at):
        index = [slice(ZERO, FOUR)] * THREE
        for done in self.order[:stage]:
            index[done] = pl.ds(self.place.pos[done], ONE)
        index[self.order[stage]] = pl.ds(at, ONE)
        return index

    def part(self, stage, at, half=None):
        columns = slice(ZERO, WIDTH) if half is None else slice(128 * half, 128 * half + 128)
        return self.acc.at[(slice(ZERO, self.units), *self.index(stage, at), slice(ZERO, EIGHT), columns)]

    def copy(self, stage, step, way):
        place, dim = self.place, self.order[stage]
        delta = ONE if way == ZERO else -ONE
        key = (stage * TWO + step) * TWO + way
        if step == ZERO:
            src, ref, half = self.part(stage, place.coord(dim, TWO), way), self.got_a, way
        else:
            src, ref, half = self.part(stage, place.coord(dim, delta)), self.got_b, None
        return src, ref, half, key, place.device(dim, delta)

    def start(self, stage, step, way):
        src, ref, half, key, device = self.copy(stage, step, way)
        remote(src, self.cast(ref, stage, way, half, src), self.send.at[key], self.recv.at[key], device).start()

    def wait(self, stage, step, way):
        src, ref, half, key, device = self.copy(stage, step, way)
        remote(src, self.cast(ref, stage, way, half, src), self.send.at[key], self.recv.at[key], device).wait_recv()

    def cast(self, ref, stage, way, half, src):
        columns = slice(ZERO, WIDTH) if half is None else slice(128 * half, 128 * half + 128)
        return ref[stage].at[(ZERO if half is not None else way, slice(ZERO, self.units), *([slice(None)] * THREE), slice(ZERO, EIGHT), columns)]

    def add(self, stage, at, refs, half):
        units = self.units
        shape = self.got_b[stage].shape[TWO:5]
        total = units * shape[ZERO] * shape[ONE] * shape[TWO]
        columns = slice(ZERO, WIDTH) if half is None else slice(128 * half, 128 * half + 128)
        base = [ZERO, ZERO, ZERO]
        for done in self.order[:stage]:
            base[done] = self.place.pos[done]
        base[self.order[stage]] = at
        acc = self.acc
        bunch = FOUR if total % FOUR == ZERO else ONE

        @pl.loop(ZERO, total // bunch)
        def _(k):
            for j in range(bunch):
                i = k * bunch + j
                u = i // (shape[ZERO] * shape[ONE] * shape[TWO])
                a = lax.rem(i // (shape[ONE] * shape[TWO]), shape[ZERO])
                b = lax.rem(i // shape[TWO], shape[ONE])
                c = lax.rem(i, shape[TWO])
                here = (u, base[ZERO] + a, base[ONE] + b, base[TWO] + c, slice(ZERO, EIGHT), columns)
                value = acc[here]
                for ref, way in refs:
                    value = value + ref[stage][ZERO if half is not None else way, u, a, b, c, :, columns]
                acc[here] = value

    def step_a(self, stage):
        for way in (ZERO, ONE):
            self.start(stage, ZERO, way)

    def step_b(self, stage):
        dim = self.order[stage]
        for way in (ZERO, ONE):
            delta = ONE if way == ZERO else -ONE
            self.wait(stage, ZERO, way)
            self.add(stage, self.place.coord(dim, delta), [(self.got_a, way)], way)
            self.start(stage, ONE, way)

    def step_c(self, stage):
        dim = self.order[stage]
        for way in (ZERO, ONE):
            self.wait(stage, ONE, way)
        self.add(stage, self.place.pos[dim], [(self.got_b, ZERO), (self.got_b, ONE)], None)

    def last(self, own, other):
        place = self.place
        z, y, x = place.pos
        src = self.acc.at[:, z, y, x]
        return remote(src, other, self.send.at[12], self.recv.at[12], place.partner)

    def drain(self, other):
        for stage in range(THREE):
            for step in range(TWO):
                for way in (ZERO, ONE):
                    src, ref, half, key, device = self.copy(stage, step, way)
                    remote(src, self.cast(ref, stage, way, half, src), self.send.at[key], self.recv.at[key], device).wait_send()
        for u in range(self.units):
            remote(self.grads(u).at[:, :, :, :, self.columns(ONE - self.place.core)], self.acc.at[u],
                   self.send.at[20 + u], self.recv.at[20 + u], self.place.partner).wait_send()
        self.last(None, other).wait_send()

    def result(self, unit, other):
        z, y, x = self.place.pos
        own, came = self.acc[unit, z, y, x], other[unit]
        first = self.place.core == ZERO
        return jnp.concatenate([jnp.where(first, own, came), jnp.where(first, came, own)], axis=ONE)


def landing_shapes(order, units, ways):
    shapes = []
    for stage in range(THREE):
        size = [FOUR, FOUR, FOUR]
        for done in order[:stage + ONE]:
            size[done] = ONE
        shapes.append((ways, units, *size, EIGHT, WIDTH))
    return shapes


class Small:
    def __init__(self, place, value, slots, send, recv):
        self.place, self.value, self.slots, self.send, self.recv = place, value, slots, send, recv

    def copies(self, stage):
        if stage == THREE:
            return [remote(self.value, self.slots.at[9], self.send.at[9], self.recv.at[9], self.place.partner)]
        return [remote(self.value, self.slots.at[stage * THREE + k], self.send.at[stage * THREE + k], self.recv.at[stage * THREE + k],
                       self.place.device(stage, delta)) for k, delta in enumerate((ONE, -ONE, TWO))]

    def start(self, stage):
        for copy in self.copies(stage):
            copy.start()

    def finish(self, stage):
        copies = self.copies(stage)
        for copy in copies:
            copy.wait()
        value = self.value[...]
        for k in range(len(copies)):
            value = value + self.slots[stage * THREE + k]
        self.value[...] = value


KEYS = 28
THIRDS = ((ZERO, THREE, FOUR, 5), (ONE, 6, 7, EIGHT), (TWO, 9, 10, 11))


def each_unit():
    for colour in range(THREE):
        for layer in range(TWO):
            for slot, unit in enumerate(THIRDS[colour]):
                yield colour, layer, layer * FOUR + slot, unit


VMEM = pl.BlockSpec(memory_space=pltpu.VMEM)
HBM = pl.BlockSpec(memory_space=pl.ANY)
DMA = pltpu.SemaphoreType.DMA


def scatter_kernel(*refs):
    place = Place()
    place.greet((ONE, -ONE, TWO))
    weights, refs = (refs[:FOUR], refs[FOUR:EIGHT]), refs[EIGHT:]
    small, attn_out, up_out, down_out, small_out = refs[:5]
    grads, accs, others, (sm, slots), refs = refs[5:EIGHT], refs[EIGHT:11], refs[11:14], refs[14:SIXTEEN], refs[SIXTEEN:]
    got_a = [refs[THREE * k:THREE * k + THREE] for k in range(THREE)]
    got_b = [refs[9 + THREE * k:9 + THREE * k + THREE] for k in range(THREE)]
    send, recv, ssend, srecv, local = refs[18:]
    copies = []
    for colour, layer, u, unit in each_unit():
        qkv, out, up, down = weights[layer]
        if unit < THREE:
            src = qkv.at[unit]
        elif unit == THREE:
            src = out
        elif unit < EIGHT:
            src = up.at[:, :, :, :, pl.ds(DIM * (unit - FOUR), DIM)]
        else:
            src = down.at[:, :, :, unit - EIGHT]
        copies.append(pltpu.make_async_copy(src, grads[colour].at[u], local.at[colour]))
    copies.append(pltpu.make_async_copy(small, sm, local.at[THREE]))
    for copy in copies:
        copy.start()
    for copy in copies:
        copy.wait()
    place.met()
    scatters = [Scatter(place, (lambda u, k=k: grads[k].at[u]), accs[k], got_a[k], got_b[k], ORDERS[k], send.at[k], recv.at[k])
                for k in range(THREE)]
    tiny = Small(place, sm, slots, ssend, srecv)
    for s in scatters:
        s.swap()
    tiny.start(ZERO)
    for s in scatters:
        s.swapped()
        s.step_a(ZERO)
    for stage in range(THREE):
        if stage:
            for s in scatters:
                s.step_a(stage)
        for s in scatters:
            s.step_b(stage)
        tiny.finish(stage)
        tiny.start(stage + ONE)
        for s in scatters:
            s.step_c(stage)
    for s, other in zip(scatters, others):
        s.last(None, other).start()
    tiny.finish(THREE)
    for s, other in zip(scatters, others):
        s.last(None, other).wait_recv()
    small_out[...] = sm[...]
    first = place.core == ZERO
    for colour, layer, u, unit in each_unit():
        full = scatters[colour].result(u, others[colour])
        if unit < EIGHT:
            mine = jnp.where(first, full[:FOUR], full[FOUR:])
            if unit < FOUR:
                attn_out[layer, unit] = mine
            else:
                up_out[layer, :, DIM * (unit - FOUR):DIM * (unit - THREE)] = mine
        else:
            at = EIGHT * (unit % TWO)

            @pl.when(place.core == (unit - EIGHT) // TWO)
            def _():
                down_out[layer, at:at + EIGHT] = full
    for s, other in zip(scatters, others):
        s.drain(other)


def scatter_grads(weights, small):
    acc, tiny = (EIGHT, FOUR, FOUR, FOUR, EIGHT, WIDTH), (32, DIM)
    scratch = [pltpu.VMEM((EIGHT, FOUR, FOUR, FOUR, EIGHT, DIM), F32)] * THREE + [pltpu.VMEM(acc, F32)] * THREE + [pltpu.VMEM((EIGHT, EIGHT, WIDTH), F32)] * THREE
    scratch += [pltpu.VMEM(tiny, F32), pltpu.VMEM((10, *tiny), F32)]
    for ways in (ONE, TWO):
        for order in ORDERS:
            scratch += [pltpu.VMEM(s, F32) for s in landing_shapes(order, EIGHT, ways)]
    scratch += [DMA((THREE, KEYS)), DMA((THREE, KEYS)), DMA((10,)), DMA((10,)), DMA((FOUR,))]
    grid = (FOUR, FOUR, FOUR)
    flat = []
    for qkv, out, up, down in weights:
        flat += [qkv.reshape(THREE, *grid, EIGHT, DIM), out.reshape(*grid, EIGHT, DIM), up.reshape(*grid, EIGHT, FFN), down.reshape(*grid, FOUR, EIGHT, DIM)]
    return pl.pallas_call(
        scatter_kernel,
        out_shape=[jax.ShapeDtypeStruct(s, F32) for s in ((TWO, FOUR, FOUR, DIM), (TWO, FOUR, FFN), (TWO, SIXTEEN, DIM), tiny)],
        in_specs=[HBM] * 9,
        out_specs=[VMEM] * FOUR,
        scratch_shapes=scratch,
        compiler_params=pltpu.CompilerParams(collective_id=ONE, has_side_effects=True, vmem_limit_bytes=63 << 20),
        name="scatter_grads")(*flat, small)


COLOURS = ((THREE, FOUR, 5), (6, 7, EIGHT), (9, 10, 11))
SLOTS = EIGHT


def at_slot(slot, plan):
    for when, step in plan:
        pl.when(slot == when)(step)


def gather_plan(gathers, after, slots):
    def each(name, *args):
        def step():
            for g in gathers:
                getattr(g, name)(*args)
        return step

    def turn(stage):
        def step():
            each("step_c", stage)()
            each("step_a", stage + ONE)()
        return step

    def swap():
        each("step_c", TWO)()
        for g in gathers:
            g.share().start()

    def end():
        each("shared")()
        each("drain")()
        after()

    steps = [each("step_a", ZERO), each("step_b", ZERO), turn(ZERO), each("step_b", ONE), turn(ONE), each("step_b", TWO), swap, end]
    return list(zip(slots, steps))


def spread(buf, u, out_ref, column_base):
    @pl.loop(ZERO, EIGHT)
    def _(block):
        for part in range(FOUR):
            g = block * FOUR + part
            tiles = [buf[block // TWO, lax.rem(block, TWO) * TWO + part // TWO, part % TWO * TWO + k // TWO, k % TWO, u].astype(F32) for k in range(FOUR)]
            rows = pl.ds(pl.multiple_of(g * SIXTEEN, SIXTEEN), SIXTEEN)
            for j, cols in enumerate(lane_tiles()):
                value = jnp.concatenate([t[FOUR * j:FOUR * j + FOUR] for t in tiles], axis=ZERO).astype(BF16)
                out_ref[rows, column_base + cols.start:column_base + cols.stop] = value


def spread_down(buf, u, out_ref, cols):
    @pl.loop(ZERO, SIXTEEN)
    def _(i):
        for k in range(EIGHT):
            d = i * EIGHT + k
            out_ref[pl.ds(pl.multiple_of(d * SIXTEEN, SIXTEEN), SIXTEEN), cols] = buf[i // FOUR, lax.rem(i, FOUR), k // TWO, k % TWO, u]


def same(shape, test):
    row = lax.broadcasted_iota(jnp.int32, shape, ZERO)
    col = lax.broadcasted_iota(jnp.int32, shape, ONE)
    return jnp.where(test(row, col), 1.0, 0.0)


def small_columns(small_ref, c_ref):
    rows = [small_ref[z, y, x, c, ZERO] for z in range(FOUR) for y in range(FOUR) for x in range(FOUR) for c in range(TWO)]
    table = jnp.concatenate(rows, axis=ZERO).astype(BF16)
    quads = nn(same((DIM, LANES), lambda r, c: r // FOUR == c).astype(BF16), table)
    quads = (quads * same((DIM, LANES), lambda r, c: r % FOUR == c % FOUR)).astype(BF16)
    mask = same((DIM, LANES), lambda r, c: r % SIXTEEN == c % SIXTEEN)
    pick = same((DIM, 32), lambda r, c: r // SIXTEEN == c).astype(BF16)
    ups = [(nn(pick, table[32 * k:32 * k + 32]) * mask).astype(BF16) for k in range(FOUR)]
    for layer in range(TWO):
        def is_up(r):
            return (r // SIXTEEN == layer * FOUR + TWO)

        value = nn(quads, same((LANES, LANES), lambda r, c: (r // 64 == layer) & (r % 64 // FOUR == c) & ~is_up(r)).astype(BF16))
        for k in range(FOUR):
            value = value + nn(ups[k], same((LANES, LANES), lambda r, c: is_up(r) & (c == B_UP + k)).astype(BF16))
        c_ref[layer] = value


def forward_kernel(len_ref, x_ref, cos_ref, sin_ref, pack_qkv, pack_mo, small_ref,
                   xs_out, q_ref, k_ref, v_ref, p_hbm, ctx_ref, mid_ref, act_ref, slope_ref, c_ref,
                   nat_qkv, nat_wo, nat_up, nat_down,
                   xs, ctxb, wqkv, wo, up, down, n_qkv, n_wo, n_up, n_down, p_buf, h_ref, acc_ref,
                   sbuf, q0, q1, q2, r0, r1, r2, m0, m1, m2, n0, n1, n2, send, recv, local, p_sem, nat_sem):
    step = pl.program_id(ZERO)
    phase, seq, layer = step // FOUR, lax.rem(step, FOUR), step // EIGHT
    place = Place()
    z, y, x = place.pos
    bufs = ((q0, q1, q2), (m0, m1, m2), (r0, r1, r2), (n0, n1, n2))
    groups = [[Gather(place, b, ORDERS[k], send.at[i * THREE + k], recv.at[i * THREE + k]) for k, b in enumerate(group)] for i, group in enumerate(bufs)]
    little = Gather(place, sbuf, ORDERS[ZERO], send.at[12], recv.at[12])

    def own_copies():
        copies = [pltpu.make_async_copy(small_ref, sbuf.at[z, y, x, place.core], local.at[12])]
        for i, group in enumerate(bufs):
            source = (pack_qkv, pack_mo)[i % TWO]
            copies += [pltpu.make_async_copy(source.at[i // TWO, k], b.at[z, y, x, place.core], local.at[i * THREE + k]) for k, b in enumerate(group)]
        return copies

    def nat_copies(which, l):
        if which == ZERO:
            return [pltpu.make_async_copy(n_qkv, nat_qkv.at[l], nat_sem.at[ZERO])]
        return [pltpu.make_async_copy(src, dst.at[l], nat_sem.at[ONE + i]) for i, (src, dst) in enumerate(((n_wo, nat_wo), (n_up, nat_up), (n_down, nat_down)))]

    def take_qkv(l):
        if l:
            for copy in nat_copies(ZERO, ZERO):
                copy.wait()
        for m in range(THREE):
            spread(bufs[TWO * l][m], ZERO, n_qkv.at[m], ZERO)
            wqkv[m] = n_qkv[m].T
        for copy in nat_copies(ZERO, l):
            copy.start()

    def take_mo(l):
        if l:
            for copy in nat_copies(ONE, ZERO):
                copy.wait()
        for colour in range(THREE):
            for u, unit in enumerate(COLOURS[colour]):
                buf = bufs[TWO * l + ONE][colour]
                if unit == THREE:
                    spread(buf, u, n_wo, ZERO)
                    wo[...] = n_wo[...].T
                elif unit < EIGHT:
                    part = slice(DIM * (unit - FOUR), DIM * (unit - THREE))
                    spread(buf, u, n_up, part.start)
                    up[part, :] = n_up[:, part].T
                else:
                    spread_down(buf, u, n_down, lane_tiles()[unit - EIGHT])
        for k in range(FOUR):
            part = slice(DIM * k, DIM * k + DIM)
            down[:, part] = n_down[part, :].T
        for copy in nat_copies(ONE, l):
            copy.start()

    @pl.when(step == ZERO)
    def _():
        place.greet()
        for copy in own_copies():
            copy.start()
        for copy in own_copies():
            copy.wait()
        place.met()
        gather_all(groups[ZERO] + [little])
        small_columns(sbuf, c_ref)
        take_qkv(ZERO)

    attn_plan = gather_plan(groups[ONE], lambda: None, (ZERO, TWO, 5, EIGHT, 11, SIXTEEN, 24, 31)) + gather_plan(groups[THREE], lambda: None, (64, 66, 69, 72, 75, 80, 88, 95))
    mlp_plan = gather_plan(groups[TWO], lambda: None, (32, 34, 36, 40, 44, 48, 52, 60))

    @pl.when(phase % TWO == ZERO)
    def _():
        @pl.when(step < FOUR)
        def _():
            xs[seq] = x_ref[ZERO].T
            xs_out[ZERO, ZERO] = xs[seq]

        @pl.when(step == EIGHT)
        def _():
            take_qkv(ONE)

        attn_forward(len_ref[seq], layer, seq, step, xs.at[seq], wqkv, c_ref.at[layer], cos_ref, sin_ref, q_ref.at[ZERO, ZERO], k_ref.at[ZERO, ZERO],
                     v_ref.at[ZERO, ZERO], p_hbm, p_buf, p_sem, ctx_ref.at[ZERO, ZERO], ctxb.at[seq], h_ref, acc_ref, attn_plan)

    @pl.when(phase % TWO == ONE)
    def _():
        for l in range(TWO):
            pl.when(step == EIGHT * l + FOUR)(functools.partial(take_mo, l))
        mlp_forward(layer, step, ctxb.at[seq], xs.at[seq], wo, up, down, c_ref.at[layer], mid_ref.at[ZERO, ZERO], act_ref.at[ZERO, ZERO], slope_ref.at[ZERO, ZERO],
                    h_ref, mlp_plan)

        @pl.when(layer == ZERO)
        def _():
            xs_out[ZERO, ZERO] = xs[seq]

    @pl.when(step == 15)
    def _():
        for which in range(TWO):
            for copy in nat_copies(which, ONE):
                copy.wait()


def attn_forward(length, layer, seq, step, xt, w, c_ref, cos_ref, sin_ref, q_ref, k_ref, v_ref, p_hbm, p_buf, p_sem, ctx_ref, ctxb, h_ref, acc_ref, plan):
    norm_to(xt, c_ref, LN_PAR, h_ref)
    for m, out in enumerate((q_ref, k_ref, v_ref)):
        acc_ref[...] = nn(w[m], h_ref[...])
        bias = column(c_ref, B_ATTN + m)
        if m < TWO:
            scale = HEAD ** -0.5 if m == ZERO else 1.0
            for cols in lane_tiles():
                for head in range(HEADS):
                    one, two = slice(HEAD * head, HEAD * head + HALF), slice(HEAD * head + HALF, HEAD * head + HEAD)
                    a = (acc_ref[one, cols] + bias[one]) * scale
                    b = (acc_ref[two, cols] + bias[two]) * scale
                    cos, sin = cos_ref[:, cols], sin_ref[:, cols]
                    out[one, cols] = (a * cos - b * sin).astype(BF16)
                    out[two, cols] = (b * cos + a * sin).astype(BF16)
        else:
            for cols in lane_tiles():
                out[:, cols] = (acc_ref[:, cols] + bias).astype(BF16)

    key = lax.broadcasted_iota(jnp.int32, (SIXTEEN, TOK), ONE)
    row = lax.broadcasted_iota(jnp.int32, (SIXTEEN, TOK), ZERO)
    bias_rows = jnp.where((row == ZERO) & (key >= length), NEG_BIG, 0.0).astype(BF16)
    one_rows = jnp.where(row == ZERO, 1.0, 0.0).astype(BF16)

    @pl.loop(ZERO, HEADS)
    def _(head):
        at_slot(step * SLOTS + head, plan)
        rows = pl.ds(pl.multiple_of(head * HEAD, HEAD), HEAD)
        slot = lax.rem(head, TWO)
        copy = pltpu.make_async_copy(p_buf.at[slot], p_hbm.at[layer, seq, head], p_sem.at[slot])

        @pl.when((step > ZERO) | (head > ONE))
        def _():
            copy.wait()

        keys = jnp.concatenate([k_ref[rows, :], bias_rows], axis=ZERO)
        for cols in lane_tiles(TOK, WIDTH):
            queries = jnp.concatenate([q_ref[rows, cols], one_rows[:, cols]], axis=ZERO)
            scores = tn(keys, queries)
            weight = jnp.exp(scores - jnp.max(scores, axis=ZERO, keepdims=True))
            probs = (weight * (1.0 / total(weight))).astype(BF16)
            p_buf[slot, :, cols] = probs
            ctx = nn(v_ref[rows, :], probs)
            ctx_ref[rows, cols] = ctx
            ctxb[rows, cols] = ctx.astype(BF16)
        copy.start()

    @pl.when(step == 11)
    def _():
        for slot in range(TWO):
            pltpu.make_async_copy(p_buf.at[slot], p_hbm.at[layer, seq, slot], p_sem.at[slot]).wait()


def mlp_forward(layer, step, ctxb, xt, wo, up, down, c_ref, mid_ref, act_ref, slope_ref, h_ref, plan):
    attn = nn(wo[...], ctxb[...])
    for cols in lane_tiles():
        mid_ref[:, cols] = (xt[:, cols].astype(F32) + attn[:, cols] + column(c_ref, B_ATTN + THREE)).astype(BF16)
    norm_to(mid_ref, c_ref, LN_PAR + TWO, h_ref)
    for part in range(FFN // DIM):
        at_slot(step * SLOTS + TWO * part, plan)
        rows = slice(DIM * part, DIM * part + DIM)
        pre = nn(up[rows, :], h_ref[...])
        for cols in lane_tiles():
            value = pre[:, cols] + column(c_ref, B_UP + part)
            cdf = 0.5 * (1.0 + lax.erf(value * (1.0 / math.sqrt(2.0))))
            density = jnp.exp(-0.5 * value * value) * (1.0 / math.sqrt(2.0 * math.pi))
            act_ref[rows, cols] = (value * cdf).astype(BF16)
            slope_ref[rows, cols] = cdf + value * density

    @pl.when(layer == ZERO)
    def _():
        out = nn(down[...], act_ref[...])
        for cols in lane_tiles():
            xt[:, cols] = (mid_ref[:, cols].astype(F32) + out[:, cols] + column(c_ref, B_DOWN)).astype(BF16)


def forward(lengths, x, tables, pack_qkv, pack_mo, small):
    def saved(index, rows, dtype):
        return jax.ShapeDtypeStruct((TWO, SEQS, rows, TOK), dtype), pl.BlockSpec((ONE, ONE, rows, TOK), index)

    def attn_at(s):
        return s // EIGHT, jnp.where(s // FOUR % TWO == ZERO, s % FOUR, THREE), ZERO, ZERO

    def mlp_at(s):
        odd = s // FOUR % TWO == ONE
        return jnp.where(s < 12, ZERO, ONE), jnp.where(odd, s % FOUR, jnp.where(s < FOUR, ZERO, THREE)), ZERO, ZERO

    def xs_at(s):
        return jnp.where(s < FOUR, ZERO, ONE), jnp.where(s < EIGHT, s % FOUR, THREE), ZERO, ZERO

    outs = [saved(xs_at, DIM, BF16)] + [saved(attn_at, DIM, BF16)] * THREE
    outs += [(jax.ShapeDtypeStruct((TWO, SEQS, HEADS, TOK, TOK), BF16), HBM), saved(attn_at, DIM, F32)]
    outs += [saved(mlp_at, DIM, BF16), saved(mlp_at, FFN, BF16), saved(mlp_at, FFN, F32)]
    outs += [(jax.ShapeDtypeStruct((TWO, *COLS), F32), pl.BlockSpec((TWO, *COLS), lambda s: (ZERO, ZERO, ZERO), pipeline_mode=pl.Buffered(ONE)))]
    weights = ((THREE, DIM, DIM), (DIM, DIM), (DIM, FFN), (FFN, DIM))
    outs += [(jax.ShapeDtypeStruct((TWO, *w), BF16), HBM) for w in weights]
    grid = (FOUR, FOUR, FOUR, TWO)
    scratch = [(SEQS, *SQUARE), (SEQS, *SQUARE), weights[ZERO], weights[ONE], weights[THREE], weights[TWO], *weights, (TWO, TOK, TOK), SQUARE]
    scratch = [pltpu.VMEM(s, BF16) for s in scratch] + [pltpu.VMEM(SQUARE, F32), pltpu.VMEM((*grid, ONE, ONE, LANES), F32)]
    scratch += [pltpu.VMEM((*grid, n, SIXTEEN, LANES), BF16) for n in (ONE, ONE, ONE, ONE, ONE, ONE, THREE, THREE, THREE, THREE, THREE, THREE)]
    scratch += [DMA((13, 13)), DMA((13, 13)), DMA((13,)), DMA((TWO,)), DMA((FOUR,))]
    return pl.pallas_call(
        forward_kernel, grid=(SIXTEEN,),
        out_shape=[o[ZERO] for o in outs], out_specs=[o[ONE] for o in outs],
        in_specs=[pl.BlockSpec(memory_space=pltpu.SMEM), pl.BlockSpec((ONE, *SQUARE), lambda s: (jnp.minimum(s, THREE), ZERO, ZERO)),
                  once((HALF, TOK)), once((HALF, TOK)), HBM, HBM, HBM],
        scratch_shapes=scratch,
        compiler_params=pltpu.CompilerParams(collective_id=ZERO, has_side_effects=True, vmem_limit_bytes=63 << 20,
                                             dimension_semantics=("arbitrary",)),
        name="forward")(lengths, x, *tables, pack_qkv, pack_mo, small)


def pack_shards(w_attn, w_up, w_down):
    attn = w_attn.reshape(TWO, FOUR, FOUR, FOUR, LANES).transpose(ZERO, ONE, THREE, TWO, FOUR).reshape(TWO, FOUR, SIXTEEN, LANES)
    up = w_up.reshape(TWO, FOUR, FOUR, FOUR, LANES).transpose(ZERO, TWO, THREE, ONE, FOUR).reshape(TWO, FOUR, SIXTEEN, LANES)
    down = w_down.reshape(TWO, SIXTEEN, FOUR, LANES).transpose(ZERO, TWO, ONE, THREE)
    return attn[:, :THREE, None], jnp.concatenate([attn[:, THREE:], up, down], axis=ONE).reshape(TWO, THREE, THREE, SIXTEEN, LANES)


def pack_small(b_attn, ln_par, b_up, b_down):
    row = jnp.concatenate([b_attn.reshape(TWO, SIXTEEN), ln_par.reshape(TWO, SIXTEEN), b_up, b_down, jnp.zeros((TWO, 12), b_up.dtype)], axis=ONE)
    return row.reshape(ONE, ONE, LANES).astype(F32)


def solution(mesh):
    batch_spec = P(AXIS)
    weight_specs = (P(None, None, AXIS, None), P(None, None, AXIS), P(None, None, AXIS),
                    P(None, AXIS, None), P(None, AXIS), P(None, AXIS, None), P(None, AXIS))

    def device_step(x, lengths, d_y, w_attn, b_attn, ln_par, w_up, b_up, w_down, b_down):
        tables = rotary_tables()
        pack_qkv, pack_mo = pack_shards(w_attn, w_up, w_down)
        xs, q, k, v, probs, ctx, mid, act, slope, c, w_qkv, w_o, w_up, w_down = forward(
            lengths, x, tables, pack_qkv, pack_mo, pack_small(b_attn, ln_par, b_up, b_down))
        grad, weights, rows = d_y, [None] * TWO, [None] * TWO
        for l in (ONE, ZERO):
            dmid, dctx, gwo, gup, gdown, gc_mlp = mlp_bwd(l, l == ONE, grad, slope, act, mid, ctx, w_o, w_up, w_down, c)
            grad, gw, gc_attn = attn_bwd(l, l == ZERO, dctx, ctx, probs, q, k, v, xs, dmid, w_qkv, c, tables)
            weights[l] = (gw, gwo, gup, gdown)
            rows[l] = (gc_mlp + gc_attn)[:, :SIXTEEN].T
        attn, up, down, small = scatter_grads(weights, jnp.concatenate(rows))
        me = lax.axis_index(AXIS)
        small = small.reshape(TWO, SIXTEEN, DIM)
        mine = lax.dynamic_slice(small, (ZERO, ZERO, FOUR * me), (TWO, SIXTEEN, FOUR))
        b_up_grad = lax.dynamic_slice(small[:, B_UP:B_DOWN].reshape(TWO, FFN), (ZERO, SIXTEEN * me), (TWO, SIXTEEN))
        return grad, attn, mine[:, :FOUR], mine[:, FOUR:EIGHT], up, b_up_grad, down, mine[:, 12]

    return jax.shard_map(device_step, mesh=mesh,
                         in_specs=(batch_spec, batch_spec, batch_spec) + weight_specs,
                         out_specs=(batch_spec,) + weight_specs,
                         check_vma=False)
```

```python
import math
import functools
import jax
import jax.numpy as jnp
from jax import lax
from jax.experimental import pallas as pl
from jax.experimental.pallas import tpu as pltpu
from jax.sharding import PartitionSpec as P

ZERO, ONE, TWO, THREE, FOUR = range(5)
EIGHT, SIXTEEN, WIDTH = 8, 16, 256

F32, BF16 = jnp.float32, jnp.bfloat16
SEQS, TOK, DIM, FFN, HEADS, HEAD, LANES = FOUR, 512, 512, 2048, EIGHT, 64, 128
HALF = HEAD // TWO
EPS = 1e-5
THETA = 10000.0
NEG_BIG = -1e30
B_ATTN, LN_PAR, B_UP, B_DOWN = ZERO, FOUR, EIGHT, 12


def nn(a, b):
    return lax.dot_general(a, b, (((ONE,), (ZERO,)), ((), ())), preferred_element_type=F32)


def nt(a, b):
    return lax.dot_general(a, b, (((ONE,), (ONE,)), ((), ())), preferred_element_type=F32)


def tn(a, b):
    return lax.dot_general(a, b, (((ZERO,), (ZERO,)), ((), ())), preferred_element_type=F32)


def lane_tiles(width=TOK, size=LANES):
    return [slice(i, i + size) for i in range(ZERO, width, size)]


def column(c_ref, lane, width=LANES):
    return jnp.broadcast_to(c_ref[:, lane:lane + ONE], (c_ref.shape[ZERO], width))


def total(value):
    return jnp.sum(value, axis=ZERO, keepdims=True)


def normed(x):
    centred = x - total(x) * (1.0 / DIM)
    rstd = lax.rsqrt(total(centred * centred) * (1.0 / DIM) + EPS)
    return centred * rstd, rstd


def norm_to(x_ref, c_ref, lane, h_ref):
    gain, shift = column(c_ref, lane), column(c_ref, lane + ONE)
    for cols in lane_tiles():
        h_ref[:, cols] = (normed(x_ref[:, cols].astype(F32))[ZERO] * gain + shift).astype(BF16)


def fold(value):
    parts = [value[:, cols] for cols in lane_tiles(value.shape[ONE])]
    return functools.reduce(jnp.add, parts)


def seq_spec(shape):
    return pl.BlockSpec((ONE, *shape), lambda s: (s,) + (ZERO,) * len(shape))


def once(shape):
    return pl.BlockSpec(shape, lambda s: (ZERO,) * len(shape), pipeline_mode=pl.Buffered(ONE))


def act_shape(rows, dtype):
    return jax.ShapeDtypeStruct((SEQS, rows, TOK), dtype)


PARAMS = pltpu.CompilerParams(vmem_limit_bytes=60 << 20, dimension_semantics=("arbitrary",))
SQUARE, TALL, WIDE, COLS = (DIM, TOK), (FFN, TOK), (DIM, FFN), (DIM, LANES)


def rotary_tables():
    inv_freq = 1.0 / (THETA ** (jnp.arange(HALF, dtype=F32) * (2.0 / HEAD)))
    angles = inv_freq[:, None] * jnp.arange(TOK, dtype=F32)[None, :]
    return jnp.cos(angles), jnp.sin(angles)


MESH = pl.DeviceIdType.MESH
AXIS = "fsdp"
ORDERS = ((TWO, ONE, ZERO), (ONE, ZERO, TWO), (ZERO, TWO, ONE))


class Place:
    def __init__(self):
        me = lax.axis_index(AXIS)
        self.me = me
        self.core = lax.rem(me, TWO)
        self.pos = (me // 32, lax.rem(me // EIGHT, FOUR), lax.rem(me // TWO, FOUR))
        self.partner = me + ONE - TWO * self.core

    def coord(self, dim, delta):
        return lax.rem(self.pos[dim] + (delta + FOUR), FOUR)

    def device(self, dim, delta):
        pos = list(self.pos)
        pos[dim] = self.coord(dim, delta)
        return pos[ZERO] * 32 + pos[ONE] * EIGHT + pos[TWO] * TWO + self.core

    def greet(self, reach=(ONE, -ONE)):
        self.greeted = THREE * len(reach) + ONE
        barrier = pltpu.get_barrier_semaphore()
        for dim in range(THREE):
            for delta in reach:
                pl.semaphore_signal(barrier, inc=ONE, device_id=(self.device(dim, delta),), device_id_type=MESH)
        pl.semaphore_signal(barrier, inc=ONE, device_id=(self.partner,), device_id_type=MESH)

    def met(self):
        pl.semaphore_wait(pltpu.get_barrier_semaphore(), self.greeted)


def remote(src, dst, send_sem, recv_sem, device):
    return pltpu.make_async_remote_copy(src_ref=src, dst_ref=dst, send_sem=send_sem, recv_sem=recv_sem,
                                        device_id=(device,), device_id_type=MESH)


class Gather:
    def __init__(self, place, buf, order, send, recv):
        self.place, self.buf, self.order, self.send, self.recv = place, buf, order, send, recv
        self.units = buf.shape[FOUR]

    def where(self, stage, at, half=None):
        dim = self.order[stage]
        index = list(self.place.pos)
        index[dim] = at
        for done in self.order[:stage]:
            index[done] = slice(ZERO, FOUR)
        unit = slice(ZERO, self.units)
        if half is not None:
            if stage > ZERO:
                index[self.order[ZERO]] = pl.ds(TWO * half, TWO)
            else:
                cut = (self.units + ONE) // TWO
                unit = slice(ZERO, cut) if half == ZERO else slice(cut, self.units)
        index = [pl.ds(i, ONE) if not isinstance(i, (slice, pl.Slice)) else i for i in index]
        return self.buf.at[index[ZERO], index[ONE], index[TWO], pl.ds(self.place.core, ONE), unit]

    def copies(self, stage, step, way):
        place, dim = self.place, self.order[stage]
        delta = ONE if way == ZERO else -ONE
        key = (stage * TWO + step) * TWO + way
        if step == ZERO:
            mine = self.where(stage, place.pos[dim])
            came = self.where(stage, place.coord(dim, -delta))
        else:
            if stage == ZERO and self.units == ONE and way == ONE:
                return None, None
            mine = self.where(stage, place.coord(dim, -delta), way)
            came = self.where(stage, place.coord(dim, -TWO * delta), way)
        def build(ref):
            return remote(ref, ref, self.send.at[key], self.recv.at[key], place.device(dim, delta))

        return lambda: build(mine), lambda: build(came)

    def step_a(self, stage):
        for way in (ZERO, ONE):
            self.copies(stage, ZERO, way)[ZERO]().start()

    def step_b(self, stage):
        for way in (ZERO, ONE):
            self.copies(stage, ZERO, way)[ONE]().wait_recv()
            out = self.copies(stage, ONE, way)[ZERO]
            if out is not None:
                out().start()

    def step_c(self, stage):
        for way in (ZERO, ONE):
            inc = self.copies(stage, ONE, way)[ONE]
            if inc is not None:
                inc().wait_recv()

    def share(self):
        half = self.buf.at[:, :, :, pl.ds(self.place.core, ONE)]
        return remote(half, half, self.send.at[12], self.recv.at[12], self.place.partner)

    def shared(self):
        half = self.buf.at[:, :, :, pl.ds(ONE - self.place.core, ONE)]
        remote(half, half, self.send.at[12], self.recv.at[12], self.place.partner).wait_recv()

    def drain(self):
        for stage in range(THREE):
            for step in range(TWO):
                for way in (ZERO, ONE):
                    out = self.copies(stage, step, way)[ZERO]
                    if out is not None:
                        out().wait_send()
        self.share().wait_send()


def gather_all(gathers):
    for stage in range(THREE):
        for g in gathers:
            g.step_a(stage)
        for g in gathers:
            g.step_b(stage)
        for g in gathers:
            g.step_c(stage)
    for g in gathers:
        g.share().start()
    for g in gathers:
        g.shared()
    for g in gathers:
        g.drain()


class Scatter:
    def __init__(self, place, grads, acc, got_a, got_b, order, send, recv):
        self.place, self.grads, self.acc, self.order = place, grads, acc, order
        self.got_a, self.got_b, self.send, self.recv = got_a, got_b, send, recv
        self.units = acc.shape[ZERO]

    def columns(self, core):
        return pl.ds(pl.multiple_of(core * WIDTH, WIDTH), WIDTH)

    def swap(self):
        place = self.place
        for u in range(self.units):
            remote(self.grads(u).at[:, :, :, :, self.columns(ONE - place.core)], self.acc.at[u],
                   self.send.at[20 + u], self.recv.at[20 + u], place.partner).start()

    def swapped(self):
        place = self.place
        for u in range(self.units):
            copy = remote(self.grads(u).at[:, :, :, :, self.columns(ONE - place.core)], self.acc.at[u],
                          self.send.at[20 + u], self.recv.at[20 + u], place.partner)
            copy.wait_recv()
            grad, acc = self.grads(u), self.acc

            @pl.loop(ZERO, SIXTEEN)
            def _(i):
                z, y = i // FOUR, lax.rem(i, FOUR)
                acc[u, z, y] = acc[u, z, y] + grad[z, y, :, :, self.columns(place.core)]

    def index(self, stage, at):
        index = [slice(ZERO, FOUR)] * THREE
        for done in self.order[:stage]:
            index[done] = pl.ds(self.place.pos[done], ONE)
        index[self.order[stage]] = pl.ds(at, ONE)
        return index

    def part(self, stage, at, half=None):
        columns = slice(ZERO, WIDTH) if half is None else slice(128 * half, 128 * half + 128)
        return self.acc.at[(slice(ZERO, self.units), *self.index(stage, at), slice(ZERO, EIGHT), columns)]

    def copy(self, stage, step, way):
        place, dim = self.place, self.order[stage]
        delta = ONE if way == ZERO else -ONE
        key = (stage * TWO + step) * TWO + way
        if step == ZERO:
            src, ref, half = self.part(stage, place.coord(dim, TWO), way), self.got_a, way
        else:
            src, ref, half = self.part(stage, place.coord(dim, delta)), self.got_b, None
        return src, ref, half, key, place.device(dim, delta)

    def start(self, stage, step, way):
        src, ref, half, key, device = self.copy(stage, step, way)
        remote(src, self.cast(ref, stage, way, half, src), self.send.at[key], self.recv.at[key], device).start()

    def wait(self, stage, step, way):
        src, ref, half, key, device = self.copy(stage, step, way)
        remote(src, self.cast(ref, stage, way, half, src), self.send.at[key], self.recv.at[key], device).wait_recv()

    def cast(self, ref, stage, way, half, src):
        columns = slice(ZERO, WIDTH) if half is None else slice(128 * half, 128 * half + 128)
        return ref[stage].at[(ZERO if half is not None else way, slice(ZERO, self.units), *([slice(None)] * THREE), slice(ZERO, EIGHT), columns)]

    def add(self, stage, at, refs, half):
        units = self.units
        shape = self.got_b[stage].shape[TWO:5]
        total = units * shape[ZERO] * shape[ONE] * shape[TWO]
        columns = slice(ZERO, WIDTH) if half is None else slice(128 * half, 128 * half + 128)
        base = [ZERO, ZERO, ZERO]
        for done in self.order[:stage]:
            base[done] = self.place.pos[done]
        base[self.order[stage]] = at
        acc = self.acc
        bunch = FOUR if total % FOUR == ZERO else ONE

        @pl.loop(ZERO, total // bunch)
        def _(k):
            for j in range(bunch):
                i = k * bunch + j
                u = i // (shape[ZERO] * shape[ONE] * shape[TWO])
                a = lax.rem(i // (shape[ONE] * shape[TWO]), shape[ZERO])
                b = lax.rem(i // shape[TWO], shape[ONE])
                c = lax.rem(i, shape[TWO])
                here = (u, base[ZERO] + a, base[ONE] + b, base[TWO] + c, slice(ZERO, EIGHT), columns)
                value = acc[here]
                for ref, way in refs:
                    value = value + ref[stage][ZERO if half is not None else way, u, a, b, c, :, columns]
                acc[here] = value

    def step_a(self, stage):
        for way in (ZERO, ONE):
            self.start(stage, ZERO, way)

    def step_b(self, stage):
        dim = self.order[stage]
        for way in (ZERO, ONE):
            delta = ONE if way == ZERO else -ONE
            self.wait(stage, ZERO, way)
            self.add(stage, self.place.coord(dim, delta), [(self.got_a, way)], way)
            self.start(stage, ONE, way)

    def step_c(self, stage):
        dim = self.order[stage]
        for way in (ZERO, ONE):
            self.wait(stage, ONE, way)
        self.add(stage, self.place.pos[dim], [(self.got_b, ZERO), (self.got_b, ONE)], None)

    def last(self, own, other):
        place = self.place
        z, y, x = place.pos
        src = self.acc.at[:, z, y, x]
        return remote(src, other, self.send.at[12], self.recv.at[12], place.partner)

    def drain(self, other):
        for stage in range(THREE):
            for step in range(TWO):
                for way in (ZERO, ONE):
                    src, ref, half, key, device = self.copy(stage, step, way)
                    remote(src, self.cast(ref, stage, way, half, src), self.send.at[key], self.recv.at[key], device).wait_send()
        for u in range(self.units):
            remote(self.grads(u).at[:, :, :, :, self.columns(ONE - self.place.core)], self.acc.at[u],
                   self.send.at[20 + u], self.recv.at[20 + u], self.place.partner).wait_send()
        self.last(None, other).wait_send()

    def result(self, unit, other):
        z, y, x = self.place.pos
        own, came = self.acc[unit, z, y, x], other[unit]
        first = self.place.core == ZERO
        return jnp.concatenate([jnp.where(first, own, came), jnp.where(first, came, own)], axis=ONE)


def landing_shapes(order, units, ways):
    shapes = []
    for stage in range(THREE):
        size = [FOUR, FOUR, FOUR]
        for done in order[:stage + ONE]:
            size[done] = ONE
        shapes.append((ways, units, *size, EIGHT, WIDTH))
    return shapes


class Small:
    def __init__(self, place, value, slots, send, recv):
        self.place, self.value, self.slots, self.send, self.recv = place, value, slots, send, recv

    def copies(self, stage):
        if stage == THREE:
            return [remote(self.value, self.slots.at[9], self.send.at[9], self.recv.at[9], self.place.partner)]
        return [remote(self.value, self.slots.at[stage * THREE + k], self.send.at[stage * THREE + k], self.recv.at[stage * THREE + k],
                       self.place.device(stage, delta)) for k, delta in enumerate((ONE, -ONE, TWO))]

    def start(self, stage):
        for copy in self.copies(stage):
            copy.start()

    def finish(self, stage):
        copies = self.copies(stage)
        for copy in copies:
            copy.wait()
        value = self.value[...]
        for k in range(len(copies)):
            value = value + self.slots[stage * THREE + k]
        self.value[...] = value

    def steps(self):
        def turn(stage):
            def step():
                self.finish(stage)
                self.start(stage + ONE)
            return step

        return [lambda: self.start(ZERO), turn(ZERO), turn(ONE), turn(TWO), lambda: self.finish(THREE)]


VMEM = pl.BlockSpec(memory_space=pltpu.VMEM)
HBM = pl.BlockSpec(memory_space=pl.ANY)
DMA = pltpu.SemaphoreType.DMA


COLOURS = ((THREE, FOUR, 5), (6, 7, EIGHT), (9, 10, 11))
SLOTS = EIGHT


def at_slot(slot, plan):
    for when, step in plan:
        pl.when(slot == when)(step)


def gather_plan(gathers, after, slots):
    def each(name, *args):
        def step():
            for g in gathers:
                getattr(g, name)(*args)
        return step

    def turn(stage):
        def step():
            each("step_c", stage)()
            each("step_a", stage + ONE)()
        return step

    def swap():
        each("step_c", TWO)()
        for g in gathers:
            g.share().start()

    def end():
        each("shared")()
        each("drain")()
        after()

    steps = [each("step_a", ZERO), each("step_b", ZERO), turn(ZERO), each("step_b", ONE), turn(ONE), each("step_b", TWO), swap, end]
    return list(zip(slots, steps))


def spread(buf, u, out_ref, column_base):
    @pl.loop(ZERO, EIGHT)
    def _(block):
        for part in range(FOUR):
            g = block * FOUR + part
            tiles = [buf[block // TWO, lax.rem(block, TWO) * TWO + part // TWO, part % TWO * TWO + k // TWO, k % TWO, u].astype(F32) for k in range(FOUR)]
            rows = pl.ds(pl.multiple_of(g * SIXTEEN, SIXTEEN), SIXTEEN)
            for j, cols in enumerate(lane_tiles()):
                value = jnp.concatenate([t[FOUR * j:FOUR * j + FOUR] for t in tiles], axis=ZERO).astype(BF16)
                out_ref[rows, column_base + cols.start:column_base + cols.stop] = value


def spread_down(buf, u, out_ref, cols):
    @pl.loop(ZERO, SIXTEEN)
    def _(i):
        for k in range(EIGHT):
            d = i * EIGHT + k
            out_ref[pl.ds(pl.multiple_of(d * SIXTEEN, SIXTEEN), SIXTEEN), cols] = buf[i // FOUR, lax.rem(i, FOUR), k // TWO, k % TWO, u]


def same(shape, test):
    row = lax.broadcasted_iota(jnp.int32, shape, ZERO)
    col = lax.broadcasted_iota(jnp.int32, shape, ONE)
    return jnp.where(test(row, col), 1.0, 0.0)


def small_columns(small_ref, c_ref):
    rows = [small_ref[z, y, x, c, ZERO] for z in range(FOUR) for y in range(FOUR) for x in range(FOUR) for c in range(TWO)]
    table = jnp.concatenate(rows, axis=ZERO).astype(BF16)
    quads = nn(same((DIM, LANES), lambda r, c: r // FOUR == c).astype(BF16), table)
    quads = (quads * same((DIM, LANES), lambda r, c: r % FOUR == c % FOUR)).astype(BF16)
    mask = same((DIM, LANES), lambda r, c: r % SIXTEEN == c % SIXTEEN)
    pick = same((DIM, 32), lambda r, c: r // SIXTEEN == c).astype(BF16)
    ups = [(nn(pick, table[32 * k:32 * k + 32]) * mask).astype(BF16) for k in range(FOUR)]
    for layer in range(TWO):
        def is_up(r):
            return (r // SIXTEEN == layer * FOUR + TWO)

        value = nn(quads, same((LANES, LANES), lambda r, c: (r // 64 == layer) & (r % 64 // FOUR == c) & ~is_up(r)).astype(BF16))
        for k in range(FOUR):
            value = value + nn(ups[k], same((LANES, LANES), lambda r, c: is_up(r) & (c == B_UP + k)).astype(BF16))
        c_ref[layer] = value


def forward_kernel(len_ref, x_ref, cos_ref, sin_ref, pack_qkv, pack_mo, small_ref,
                   xs_out, q_ref, k_ref, v_ref, p_hbm, ctx_ref, mid_ref, act_ref, slope_ref, c_ref,
                   nat_qkv, nat_wo, nat_up, nat_down,
                   xs, ctxb, wqkv, wo, up, down, n_qkv, n_wo, n_up, n_down, p_buf, h_ref, acc_ref,
                   sbuf, q0, q1, q2, r0, r1, r2, m0, m1, m2, n0, n1, n2, send, recv, local, p_sem, nat_sem):
    step = pl.program_id(ZERO)
    phase, seq, layer = step // FOUR, lax.rem(step, FOUR), step // EIGHT
    place = Place()
    z, y, x = place.pos
    bufs = ((q0, q1, q2), (m0, m1, m2), (r0, r1, r2), (n0, n1, n2))
    groups = [[Gather(place, b, ORDERS[k], send.at[i * THREE + k], recv.at[i * THREE + k]) for k, b in enumerate(group)] for i, group in enumerate(bufs)]
    little = Gather(place, sbuf, ORDERS[ZERO], send.at[12], recv.at[12])

    def own_copies():
        copies = [pltpu.make_async_copy(small_ref, sbuf.at[z, y, x, place.core], local.at[12])]
        for i, group in enumerate(bufs):
            source = (pack_qkv, pack_mo)[i % TWO]
            copies += [pltpu.make_async_copy(source.at[i // TWO, k], b.at[z, y, x, place.core], local.at[i * THREE + k]) for k, b in enumerate(group)]
        return copies

    def nat_copies(which, l):
        if which == ZERO:
            return [pltpu.make_async_copy(n_qkv, nat_qkv.at[l], nat_sem.at[ZERO])]
        return [pltpu.make_async_copy(src, dst.at[l], nat_sem.at[ONE + i]) for i, (src, dst) in enumerate(((n_wo, nat_wo), (n_up, nat_up), (n_down, nat_down)))]

    def take_qkv(l):
        if l:
            for copy in nat_copies(ZERO, ZERO):
                copy.wait()
        for m in range(THREE):
            spread(bufs[TWO * l][m], ZERO, n_qkv.at[m], ZERO)
            wqkv[m] = n_qkv[m].T
        for copy in nat_copies(ZERO, l):
            copy.start()

    def take_mo(l):
        if l:
            for copy in nat_copies(ONE, ZERO):
                copy.wait()
        for colour in range(THREE):
            for u, unit in enumerate(COLOURS[colour]):
                buf = bufs[TWO * l + ONE][colour]
                if unit == THREE:
                    spread(buf, u, n_wo, ZERO)
                    wo[...] = n_wo[...].T
                elif unit < EIGHT:
                    part = slice(DIM * (unit - FOUR), DIM * (unit - THREE))
                    spread(buf, u, n_up, part.start)
                    up[part, :] = n_up[:, part].T
                else:
                    spread_down(buf, u, n_down, lane_tiles()[unit - EIGHT])
        for k in range(FOUR):
            part = slice(DIM * k, DIM * k + DIM)
            down[:, part] = n_down[part, :].T
        for copy in nat_copies(ONE, l):
            copy.start()

    @pl.when(step == ZERO)
    def _():
        place.greet()
        for copy in own_copies():
            copy.start()
        for copy in own_copies():
            copy.wait()
        place.met()
        gather_all(groups[ZERO] + [little])
        small_columns(sbuf, c_ref)
        take_qkv(ZERO)

    attn_plan = gather_plan(groups[ONE], lambda: None, (ZERO, TWO, 5, EIGHT, 11, SIXTEEN, 24, 31)) + gather_plan(groups[THREE], lambda: None, (64, 66, 69, 72, 75, 80, 88, 95))
    mlp_plan = gather_plan(groups[TWO], lambda: None, (32, 34, 36, 40, 44, 48, 52, 60))

    @pl.when(phase % TWO == ZERO)
    def _():
        @pl.when(step < FOUR)
        def _():
            xs[seq] = x_ref[ZERO].T
            xs_out[ZERO, ZERO] = xs[seq]

        @pl.when(step == EIGHT)
        def _():
            take_qkv(ONE)

        attn_forward(len_ref[seq], layer, seq, step, xs.at[seq], wqkv, c_ref.at[layer], cos_ref, sin_ref, q_ref.at[ZERO, ZERO], k_ref.at[ZERO, ZERO],
                     v_ref.at[ZERO, ZERO], p_hbm, p_buf, p_sem, ctx_ref.at[ZERO, ZERO], ctxb.at[seq], h_ref, acc_ref, attn_plan)

    @pl.when(phase % TWO == ONE)
    def _():
        for l in range(TWO):
            pl.when(step == EIGHT * l + FOUR)(functools.partial(take_mo, l))
        mlp_forward(layer, step, ctxb.at[seq], xs.at[seq], wo, up, down, c_ref.at[layer], mid_ref.at[ZERO, ZERO], act_ref.at[ZERO, ZERO], slope_ref.at[ZERO, ZERO],
                    h_ref, mlp_plan)

        @pl.when(layer == ZERO)
        def _():
            xs_out[ZERO, ZERO] = xs[seq]

    @pl.when(step == 15)
    def _():
        for which in range(TWO):
            for copy in nat_copies(which, ONE):
                copy.wait()


def attn_forward(length, layer, seq, step, xt, w, c_ref, cos_ref, sin_ref, q_ref, k_ref, v_ref, p_hbm, p_buf, p_sem, ctx_ref, ctxb, h_ref, acc_ref, plan):
    norm_to(xt, c_ref, LN_PAR, h_ref)
    for m, out in enumerate((q_ref, k_ref, v_ref)):
        acc_ref[...] = nn(w[m], h_ref[...])
        bias = column(c_ref, B_ATTN + m)
        if m < TWO:
            scale = HEAD ** -0.5 if m == ZERO else 1.0
            for cols in lane_tiles():
                for head in range(HEADS):
                    one, two = slice(HEAD * head, HEAD * head + HALF), slice(HEAD * head + HALF, HEAD * head + HEAD)
                    a = (acc_ref[one, cols] + bias[one]) * scale
                    b = (acc_ref[two, cols] + bias[two]) * scale
                    cos, sin = cos_ref[:, cols], sin_ref[:, cols]
                    out[one, cols] = (a * cos - b * sin).astype(BF16)
                    out[two, cols] = (b * cos + a * sin).astype(BF16)
        else:
            for cols in lane_tiles():
                out[:, cols] = (acc_ref[:, cols] + bias).astype(BF16)

    key = lax.broadcasted_iota(jnp.int32, (SIXTEEN, TOK), ONE)
    row = lax.broadcasted_iota(jnp.int32, (SIXTEEN, TOK), ZERO)
    bias_rows = jnp.where((row == ZERO) & (key >= length), NEG_BIG, 0.0).astype(BF16)
    one_rows = jnp.where(row == ZERO, 1.0, 0.0).astype(BF16)

    @pl.loop(ZERO, HEADS)
    def _(head):
        at_slot(step * SLOTS + head, plan)
        rows = pl.ds(pl.multiple_of(head * HEAD, HEAD), HEAD)
        slot = lax.rem(head, TWO)
        copy = pltpu.make_async_copy(p_buf.at[slot], p_hbm.at[layer, seq, head], p_sem.at[slot])

        @pl.when((step > ZERO) | (head > ONE))
        def _():
            copy.wait()

        keys = jnp.concatenate([k_ref[rows, :], bias_rows], axis=ZERO)
        for cols in lane_tiles(TOK, WIDTH):
            queries = jnp.concatenate([q_ref[rows, cols], one_rows[:, cols]], axis=ZERO)
            scores = tn(keys, queries)
            weight = jnp.exp(scores - jnp.max(scores, axis=ZERO, keepdims=True))
            probs = (weight * (1.0 / total(weight))).astype(BF16)
            p_buf[slot, :, cols] = probs
            ctx = nn(v_ref[rows, :], probs)
            ctx_ref[rows, cols] = ctx
            ctxb[rows, cols] = ctx.astype(BF16)
        copy.start()

    @pl.when(step == 11)
    def _():
        for slot in range(TWO):
            pltpu.make_async_copy(p_buf.at[slot], p_hbm.at[layer, seq, slot], p_sem.at[slot]).wait()


def mlp_forward(layer, step, ctxb, xt, wo, up, down, c_ref, mid_ref, act_ref, slope_ref, h_ref, plan):
    attn = nn(wo[...], ctxb[...])
    for cols in lane_tiles():
        mid_ref[:, cols] = (xt[:, cols].astype(F32) + attn[:, cols] + column(c_ref, B_ATTN + THREE)).astype(BF16)
    norm_to(mid_ref, c_ref, LN_PAR + TWO, h_ref)
    for part in range(FFN // DIM):
        at_slot(step * SLOTS + TWO * part, plan)
        rows = slice(DIM * part, DIM * part + DIM)
        pre = nn(up[rows, :], h_ref[...])
        for cols in lane_tiles():
            value = pre[:, cols] + column(c_ref, B_UP + part)
            cdf = 0.5 * (1.0 + lax.erf(value * (1.0 / math.sqrt(2.0))))
            density = jnp.exp(-0.5 * value * value) * (1.0 / math.sqrt(2.0 * math.pi))
            act_ref[rows, cols] = (value * cdf).astype(BF16)
            slope_ref[rows, cols] = cdf + value * density

    @pl.when(layer == ZERO)
    def _():
        out = nn(down[...], act_ref[...])
        for cols in lane_tiles():
            xt[:, cols] = (mid_ref[:, cols].astype(F32) + out[:, cols] + column(c_ref, B_DOWN)).astype(BF16)


def forward(lengths, x, tables, pack_qkv, pack_mo, small):
    def saved(index, rows, dtype):
        return jax.ShapeDtypeStruct((TWO, SEQS, rows, TOK), dtype), pl.BlockSpec((ONE, ONE, rows, TOK), index)

    def attn_at(s):
        return s // EIGHT, jnp.where(s // FOUR % TWO == ZERO, s % FOUR, THREE), ZERO, ZERO

    def mlp_at(s):
        odd = s // FOUR % TWO == ONE
        return jnp.where(s < 12, ZERO, ONE), jnp.where(odd, s % FOUR, jnp.where(s < FOUR, ZERO, THREE)), ZERO, ZERO

    def xs_at(s):
        return jnp.where(s < FOUR, ZERO, ONE), jnp.where(s < EIGHT, s % FOUR, THREE), ZERO, ZERO

    outs = [saved(xs_at, DIM, BF16)] + [saved(attn_at, DIM, BF16)] * THREE
    outs += [(jax.ShapeDtypeStruct((TWO, SEQS, HEADS, TOK, TOK), BF16), HBM), saved(attn_at, DIM, F32)]
    outs += [saved(mlp_at, DIM, BF16), saved(mlp_at, FFN, BF16), saved(mlp_at, FFN, F32)]
    outs += [(jax.ShapeDtypeStruct((TWO, *COLS), F32), pl.BlockSpec((TWO, *COLS), lambda s: (ZERO, ZERO, ZERO), pipeline_mode=pl.Buffered(ONE)))]
    weights = ((THREE, DIM, DIM), (DIM, DIM), (DIM, FFN), (FFN, DIM))
    outs += [(jax.ShapeDtypeStruct((TWO, *w), BF16), HBM) for w in weights]
    grid = (FOUR, FOUR, FOUR, TWO)
    scratch = [(SEQS, *SQUARE), (SEQS, *SQUARE), weights[ZERO], weights[ONE], weights[THREE], weights[TWO], *weights, (TWO, TOK, TOK), SQUARE]
    scratch = [pltpu.VMEM(s, BF16) for s in scratch] + [pltpu.VMEM(SQUARE, F32), pltpu.VMEM((*grid, ONE, ONE, LANES), F32)]
    scratch += [pltpu.VMEM((*grid, n, SIXTEEN, LANES), BF16) for n in (ONE, ONE, ONE, ONE, ONE, ONE, THREE, THREE, THREE, THREE, THREE, THREE)]
    scratch += [DMA((13, 13)), DMA((13, 13)), DMA((13,)), DMA((TWO,)), DMA((FOUR,))]
    return pl.pallas_call(
        forward_kernel, grid=(SIXTEEN,),
        out_shape=[o[ZERO] for o in outs], out_specs=[o[ONE] for o in outs],
        in_specs=[pl.BlockSpec(memory_space=pltpu.SMEM), pl.BlockSpec((ONE, *SQUARE), lambda s: (jnp.minimum(s, THREE), ZERO, ZERO)),
                  once((HALF, TOK)), once((HALF, TOK)), HBM, HBM, HBM],
        scratch_shapes=scratch,
        compiler_params=pltpu.CompilerParams(collective_id=ZERO, has_side_effects=True, vmem_limit_bytes=63 << 20,
                                             dimension_semantics=("arbitrary",)),
        name="forward")(lengths, x, *tables, pack_qkv, pack_mo, small)


def norm_back(dh, x, gain):
    xhat, rstd = normed(x)
    dxhat = dh * gain
    mean_one = total(dxhat) * (1.0 / DIM)
    mean_two = total(dxhat * xhat) * (1.0 / DIM)
    return rstd * (dxhat - mean_one - xhat * mean_two), xhat


def columns_of(pairs):
    lane = lax.broadcasted_iota(jnp.int32, COLS, ONE)
    value = jnp.zeros(COLS, F32)
    for at, partial in pairs:
        value = jnp.where(lane == at, jnp.sum(partial, axis=ONE, keepdims=True), value)
    return value


def head_rows(head):
    return slice(HEAD * head, HEAD * head + HEAD), slice(HEAD * head, HEAD * head + HALF), slice(HEAD * head + HALF, HEAD * head + HEAD)


GRID = (FOUR, FOUR, FOUR)


class Reduce:
    def __init__(self, place, units, grads, accs, got_a, got_b, others, send, recv):
        self.scatters = [Scatter(place, (lambda u, k=k: grads(units[k][u])), accs[k], got_a[k], got_b[k], ORDERS[k], send.at[k], recv.at[k])
                         for k in range(THREE)]
        self.others, self.units, self.place = others, units, place

    def each(self, name, *args):
        for s in self.scatters:
            getattr(s, name)(*args)

    def first(self):
        for s in self.scatters:
            s.swapped()
            s.step_a(ZERO)

    def turn(self, stage):
        for s in self.scatters:
            s.step_c(stage)
            s.step_a(stage + ONE)

    def last(self):
        for s, other in zip(self.scatters, self.others):
            s.step_c(TWO)
            s.last(None, other).start()

    def finish(self, store):
        for k, (s, other) in enumerate(zip(self.scatters, self.others)):
            s.last(None, other).wait_recv()
            for u, unit in enumerate(self.units[k]):
                store(unit, s.result(u, other))
            s.drain(other)

    def plan(self, slots, store):
        steps = [lambda: self.each("swap"), self.first, lambda: self.each("step_b", ZERO), lambda: self.turn(ZERO), lambda: self.each("step_b", ONE),
                 lambda: self.turn(ONE), lambda: self.each("step_b", TWO), self.last, lambda: self.finish(store)]
        return list(zip(slots, steps))


def backward_kernel(dy_ref, mid_ref, ctx_ref, q_ref, k_ref, v_ref, x_ref, cos_ref, sin_ref, c_ref, p_hbm, slope_hbm, act_hbm,
                    qkv_hbm, wo_hbm, up_hbm, down_hbm,
                    dx_ref, attn_out, up_out, down_out, small_out, *refs):
    (grad, dctx, delta, big, wqkv, wo, slope, act, dpre, h_ref, s_a, s_b, d_a, d_b, sums,
     g_qkv, g_wo, g_up, g_down, rows_ref, slots_ref), refs = refs[:21], refs[21:]
    accs, others, got_a, got_b, refs = refs[:6], refs[6:12], refs[12:30], refs[30:48], refs[48:]
    send, recv, ssend, srecv, big_sem, w_sem, mlp_sem = refs
    step = pl.program_id(ZERO)
    phase, seq = step // FOUR, lax.rem(step, FOUR)
    layer = ONE - step // EIGHT
    place = Place()

    def grads(unit):
        if unit < THREE:
            return g_qkv.at[unit]
        if unit == THREE:
            return g_wo
        if unit < EIGHT:
            return g_up.at[unit - FOUR]
        return g_down.at[:, :, :, unit - EIGHT]

    def got(refs, i):
        return [refs[9 * i + THREE * k:9 * i + THREE * k + THREE] for k in range(THREE)]

    qkv_sums = Reduce(place, ((ZERO,), (ONE,), (TWO,)), grads, accs[:THREE], got(got_a, ZERO), got(got_b, ZERO), others[:THREE], send.at[ZERO], recv.at[ZERO])
    mo_sums = Reduce(place, COLOURS, grads, accs[THREE:], got(got_a, ONE), got(got_b, ONE), others[THREE:], send.at[ONE], recv.at[ONE])
    tiny = Small(place, rows_ref, slots_ref, ssend, srecv)
    first_core = place.core == ZERO

    def store(l):
        def put(unit, full):
            if unit < EIGHT:
                mine = jnp.where(first_core, full[:FOUR], full[FOUR:])
                if unit < FOUR:
                    attn_out[l, unit] = mine
                else:
                    up_out[l, :, DIM * (unit - FOUR):DIM * (unit - THREE)] = mine
            else:
                at = EIGHT * (unit % TWO)

                @pl.when(place.core == (unit - EIGHT) // TWO)
                def _():
                    down_out[l, at:at + EIGHT] = full
        return put

    def mlp_weights(l):
        copies = [pltpu.make_async_copy(wo_hbm.at[l], wo, w_sem.at[ZERO])]
        for k in range(FOUR):
            part = pl.ds(DIM * k, DIM)
            copies.append(pltpu.make_async_copy(down_hbm.at[l, part], big.at[k], big_sem.at[k]))
            copies.append(pltpu.make_async_copy(up_hbm.at[l, :, part], big.at[FOUR + k], big_sem.at[FOUR + k]))
        return copies

    def attn_weights(l):
        return [pltpu.make_async_copy(qkv_hbm.at[l], wqkv, w_sem.at[ONE])]

    def probs(l, s):
        return [pltpu.make_async_copy(p_hbm.at[l, s, k], big.at[k], big_sem.at[k]) for k in range(HEADS)]

    def saved_mlp(l, s):
        return [pltpu.make_async_copy(slope_hbm.at[l, s], slope, mlp_sem.at[ZERO]), pltpu.make_async_copy(act_hbm.at[l, s], act, mlp_sem.at[ONE])]

    def start(copies):
        for copy in copies:
            copy.start()

    def wait(copies):
        for copy in copies:
            copy.wait()

    @pl.when(step == ZERO)
    def _():
        place.greet((ONE, -ONE, TWO))
        start(mlp_weights(ONE) + saved_mlp(ONE, ZERO) + attn_weights(ONE))

    pl.when(step == ONE)(place.met)
    live = step < SIXTEEN
    attn_plan = [((when, when + 32), run) for when, run in mo_sums.plan((SIXTEEN, 20, 22, 25, 26, 28, 29, 30, 31), store(layer))]
    late = range(64, 73)
    mlp_plan = list(zip(zip((32, 34, 36, 38, 40, 42, 44, 46, 47), late), [run for _, run in qkv_sums.plan(late, store(jnp.where(live, ONE, ZERO)))]))
    mlp_plan += [((when,), run) for when, run in zip((64, 66, 68, 70, 71), tiny.steps())]

    def hook(at, plan):
        for slots, run in plan:
            for when in slots:
                if when % FOUR == at:
                    others = [w for w in slots if w % FOUR == at]
                    if when == others[ZERO]:
                        pl.when(functools.reduce(jnp.logical_or, [step * FOUR + at == w for w in others]))(run)

    @pl.when(phase % TWO == ZERO)
    def _():
        @pl.when((seq == ZERO) & live)
        def _():
            for ref in (g_wo, g_up, g_down, sums):
                ref[...] = jnp.zeros_like(ref)

        @pl.when(step < FOUR)
        def _():
            grad[seq] = dy_ref[ZERO].T

        @pl.when((seq == ZERO) & live)
        def _():
            wait(mlp_weights(layer))

        hook(ZERO, mlp_plan)
        pl.when(live)(lambda: wait(saved_mlp(layer, seq)))
        mlp_backward(grad.at[seq], slope, act, mid_ref, ctx_ref, wo, big, c_ref, dctx.at[seq], delta.at[seq], g_wo, g_up, g_down,
                     dpre, h_ref, s_a, s_b, sums, pl.when(live), lambda at: hook(at, mlp_plan),
                     lambda: pl.when(seq < THREE)(lambda: start(saved_mlp(layer, seq + ONE))))

        @pl.when((seq == THREE) & live)
        def _():
            value = columns_of([(B_UP + i, sums[i]) for i in range(FOUR)] + [
                (LN_PAR + TWO, sums[FOUR]), (LN_PAR + THREE, sums[5]), (B_DOWN, sums[6]), (B_ATTN + THREE, sums[7])])
            rows_ref[pl.ds(pl.multiple_of(layer * SIXTEEN, SIXTEEN), SIXTEEN), :] = value.T[:SIXTEEN]

        hook(THREE, mlp_plan)

    @pl.when(phase % TWO == ONE)
    def _():
        @pl.when(seq == ZERO)
        def _():
            start(probs(layer, ZERO))
            wait(attn_weights(layer))
            for ref in (g_qkv, sums):
                ref[...] = jnp.zeros_like(ref)

        @pl.when(step == FOUR)
        def _():
            start(saved_mlp(ZERO, ZERO))
        hook(ZERO, attn_plan)
        wait(probs(layer, seq))
        attn_backward(dctx.at[seq], delta.at[seq], big, q_ref, k_ref, v_ref, x_ref, grad.at[seq], wqkv, c_ref, cos_ref, sin_ref,
                      g_qkv, dpre, h_ref, s_a, s_b, d_a, d_b, sums, lambda at: hook(at, attn_plan),
                      lambda: pl.when(seq < THREE)(lambda: start(probs(layer, seq + ONE))))

        @pl.when(seq == THREE)
        def _():
            value = columns_of([(B_ATTN + i, sums[i]) for i in range(THREE)] + [(LN_PAR, sums[THREE]), (LN_PAR + ONE, sums[FOUR])])
            rows = pl.ds(pl.multiple_of(layer * SIXTEEN, SIXTEEN), SIXTEEN)
            rows_ref[rows, :] = rows_ref[rows, :] + value.T[:SIXTEEN]

        @pl.when(step == 7)
        def _():
            start(mlp_weights(ZERO) + attn_weights(ZERO))

        @pl.when(step > 11)
        def _():
            dx_ref[ZERO] = grad[seq].T
        hook(THREE, attn_plan)

    @pl.when(step == 18)
    def _():
        small_out[...] = rows_ref[...]


def add_to(ref, value):
    ref[...] = ref[...] + value.reshape(ref.shape)


def mlp_backward(grad, slope, act, mid_ref, ctx_ref, wo, big, c_ref, dctx, delta, g_wo, g_up, g_down, dpre, h_ref, s_a, s_b, sums, when, hook, prefetch):
    parts = [slice(DIM * k, DIM * k + DIM) for k in range(FOUR)]
    pre = (s_a, s_b)

    def dact(k):
        pre[k % TWO][...] = nn(big[k], grad[...])

    @when
    def _():
        norm_to(mid_ref.at[ZERO], c_ref, LN_PAR + TWO, h_ref)
        dact(ZERO)
        for k, rows in enumerate(parts):
            if k < THREE:
                dact(k + ONE)
            if k:
                add_to(g_down.at[k - ONE], nt(act[parts[k - ONE], :], grad[...]))
            for cols in lane_tiles():
                value = pre[k % TWO][:, cols] * slope[rows, cols]
                sums[k] += value
                dpre[rows, cols] = value.astype(BF16)
        add_to(g_down.at[THREE], nt(act[parts[THREE], :], grad[...]))
        prefetch()
    hook(ONE)

    @when
    def _():
        s_a[...] = functools.reduce(jnp.add, [nn(big[FOUR + k], dpre[rows, :]) for k, rows in enumerate(parts)])
    hook(TWO)

    @when
    def _():
        for k, rows in enumerate(parts):
            add_to(g_up.at[k], nt(h_ref[...], dpre[rows, :]))
        gain = column(c_ref, LN_PAR + TWO)
        for cols in lane_tiles():
            dh, dy = s_a[:, cols], grad[:, cols].astype(F32)
            dx, xhat = norm_back(dh, mid_ref[ZERO, :, cols].astype(F32), gain)
            dmid = (dy + dx).astype(BF16)
            grad[:, cols] = dmid
            sums[FOUR] += dh * xhat
            sums[5] += dh
            sums[6] += dy
            sums[7] += dmid.astype(F32)
        add_to(g_wo, nt(ctx_ref[ZERO].astype(BF16), grad[...]))
        s_b[...] = nn(wo[...], grad[...])
        for head in range(HEADS):
            rows = head_rows(head)[ZERO]
            value = s_b[rows, :].astype(BF16)
            dctx[rows, :] = value
            delta[head:head + ONE, :] = total(value.astype(F32) * ctx_ref[ZERO, rows, :])


def attn_backward(dctx, delta, probs, q_ref, k_ref, v_ref, x_ref, grad, wqkv, c_ref, cos_ref, sin_ref, g_qkv, dproj, h_ref, s_a, s_b, d_a, d_b,
                  sums, hook, prefetch):
    scores, dscores = (s_a, s_b), (d_a, d_b)
    q, k, v = q_ref.at[ZERO], k_ref.at[ZERO], v_ref.at[ZERO]

    def open_head(head):
        rows = head_rows(head)[ZERO]
        scores[head % TWO][...] = tn(v[rows, :], dctx[rows, :])

    def weigh(head):
        dscores[head % TWO][...] = (probs[head].astype(F32) * (scores[head % TWO][...] - delta[head:head + ONE, :])).astype(BF16)

    def values(head):
        rows = head_rows(head)[ZERO]
        dv = nt(dctx[rows, :], probs[head])
        sums[TWO, rows, :] += fold(dv)
        dproj[TWO * DIM + rows.start:TWO * DIM + rows.stop, :] = dv.astype(BF16)

    def close_head(head):
        rows, one, two = head_rows(head)
        ds = dscores[head % TWO][...]
        for m, value in enumerate((nn(k[rows, :], ds) * HEAD ** -0.5, nt(q[rows, :], ds))):
            cos, sin = cos_ref[...], sin_ref[...]
            a, b = value[:HALF], value[HALF:]
            for at, out in ((one, a * cos + b * sin), (two, b * cos - a * sin)):
                dproj[m * DIM + at.start:m * DIM + at.stop, :] = out.astype(BF16)
                sums[m, at, :] += fold(out)

    open_head(ZERO)
    for head in range(HEADS):
        if head + ONE < HEADS:
            open_head(head + ONE)
        if head:
            close_head(head - ONE)
        values(head)
        weigh(head)
        if head == THREE:
            hook(ONE)
    close_head(HEADS - ONE)
    prefetch()
    hook(TWO)
    norm_to(x_ref.at[ZERO], c_ref, LN_PAR, h_ref)
    parts = [slice(DIM * m, DIM * m + DIM) for m in range(THREE)]
    s_a[...] = functools.reduce(jnp.add, [nn(wqkv[m], dproj[rows, :]) for m, rows in enumerate(parts)])
    for m, rows in enumerate(parts):
        add_to(g_qkv.at[m], nt(h_ref[...], dproj[rows, :]))
    gain = column(c_ref, LN_PAR)
    for cols in lane_tiles():
        dh = s_a[:, cols]
        dx, xhat = norm_back(dh, x_ref[ZERO, :, cols].astype(F32), gain)
        grad[:, cols] = (grad[:, cols].astype(F32) + dx).astype(BF16)
        sums[THREE] += dh * xhat
        sums[FOUR] += dh


def backward(dy, xs, q, k, v, probs, ctx, mid, act, slope, c, tables, w_qkv, w_o, w_up, w_down):
    def mlp_at(s):
        s = jnp.minimum(s, 15)
        odd = s // FOUR % TWO == ONE
        return ONE - s // EIGHT, jnp.where(odd, THREE, s % FOUR), ZERO, ZERO

    def attn_at(s):
        s = jnp.minimum(s, 15)
        odd = s // FOUR % TWO == ONE
        return jnp.where(s < EIGHT, ONE, ZERO) + jnp.where((s > 7) & (s < 12), ONE, ZERO), jnp.where(odd, s % FOUR, jnp.where(s < FOUR, ZERO, THREE)), ZERO, ZERO

    per_mlp = pl.BlockSpec((None, ONE, *SQUARE), mlp_at)
    per_attn = pl.BlockSpec((None, ONE, *SQUARE), attn_at)
    acc = [(*GRID, EIGHT, WIDTH)]
    scratch = [pltpu.VMEM((SEQS, *SQUARE), BF16), pltpu.VMEM((SEQS, *SQUARE), BF16), pltpu.VMEM((SEQS, HEADS, TOK), F32),
               pltpu.VMEM((HEADS, TOK, TOK), BF16), pltpu.VMEM((THREE, DIM, DIM), BF16), pltpu.VMEM((DIM, DIM), BF16),
               pltpu.VMEM(TALL, F32), pltpu.VMEM(TALL, BF16), pltpu.VMEM(TALL, BF16), pltpu.VMEM(SQUARE, BF16),
               pltpu.VMEM(SQUARE, F32), pltpu.VMEM(SQUARE, F32), pltpu.VMEM((TOK, TOK), BF16), pltpu.VMEM((TOK, TOK), BF16),
               pltpu.VMEM((EIGHT, *COLS), F32), pltpu.VMEM((THREE, *GRID, EIGHT, DIM), F32), pltpu.VMEM((*GRID, EIGHT, DIM), F32),
               pltpu.VMEM((FOUR, *GRID, EIGHT, DIM), F32), pltpu.VMEM((*GRID, FOUR, EIGHT, DIM), F32), pltpu.VMEM((32, DIM), F32), pltpu.VMEM((10, 32, DIM), F32)]
    counts = (ONE, THREE)
    scratch += [pltpu.VMEM((n, *GRID, EIGHT, WIDTH), F32) for n in counts for _ in range(THREE)]
    scratch += [pltpu.VMEM((n, EIGHT, WIDTH), F32) for n in counts for _ in range(THREE)]
    for ways in (ONE, TWO):
        for n in counts:
            for order in ORDERS:
                scratch += [pltpu.VMEM(s, F32) for s in landing_shapes(order, n, ways)]
    scratch += [DMA((TWO, THREE, 28)), DMA((TWO, THREE, 28)), DMA((10,)), DMA((10,)), DMA((EIGHT,)), DMA((TWO,)), DMA((TWO,))]
    outs = ((TWO, FOUR, FOUR, DIM), (TWO, FOUR, FFN), (TWO, SIXTEEN, DIM), (32, DIM))
    whole = [pl.BlockSpec(s, lambda i, n=len(s): (ZERO,) * n, pipeline_mode=pl.Buffered(ONE)) for s in outs]
    dx_at = lambda s: (jnp.clip(s - 12, ZERO, THREE), ZERO, ZERO)
    return pl.pallas_call(
        backward_kernel, grid=(19,),
        out_shape=[jax.ShapeDtypeStruct((SEQS, TOK, DIM), BF16)] + [jax.ShapeDtypeStruct(s, F32) for s in outs],
        out_specs=[pl.BlockSpec((ONE, TOK, DIM), dx_at)] + whole,
        in_specs=[pl.BlockSpec((ONE, TOK, DIM), lambda s: (jnp.minimum(s, THREE), ZERO, ZERO)), per_mlp, per_mlp, per_attn, per_attn, per_attn, per_attn,
                  once((HALF, TOK)), once((HALF, TOK)), pl.BlockSpec((None, *COLS), lambda s: (ONE - jnp.minimum(s, 15) // EIGHT, ZERO, ZERO))] + [HBM] * 7,
        scratch_shapes=scratch,
        compiler_params=pltpu.CompilerParams(collective_id=ONE, has_side_effects=True, vmem_limit_bytes=67043328,
                                             dimension_semantics=("arbitrary",)),
        name="backward")(dy, mid, ctx, q, k, v, xs, *tables, c, probs, slope, act, w_qkv, w_o, w_up, w_down)


def pack_shards(w_attn, w_up, w_down):
    attn = w_attn.reshape(TWO, FOUR, FOUR, FOUR, LANES).transpose(ZERO, ONE, THREE, TWO, FOUR).reshape(TWO, FOUR, SIXTEEN, LANES)
    up = w_up.reshape(TWO, FOUR, FOUR, FOUR, LANES).transpose(ZERO, TWO, THREE, ONE, FOUR).reshape(TWO, FOUR, SIXTEEN, LANES)
    down = w_down.reshape(TWO, SIXTEEN, FOUR, LANES).transpose(ZERO, TWO, ONE, THREE)
    return attn[:, :THREE, None], jnp.concatenate([attn[:, THREE:], up, down], axis=ONE).reshape(TWO, THREE, THREE, SIXTEEN, LANES)


def pack_small(b_attn, ln_par, b_up, b_down):
    row = jnp.concatenate([b_attn.reshape(TWO, SIXTEEN), ln_par.reshape(TWO, SIXTEEN), b_up, b_down, jnp.zeros((TWO, 12), b_up.dtype)], axis=ONE)
    return row.reshape(ONE, ONE, LANES).astype(F32)


def solution(mesh):
    batch_spec = P(AXIS)
    weight_specs = (P(None, None, AXIS, None), P(None, None, AXIS), P(None, None, AXIS),
                    P(None, AXIS, None), P(None, AXIS), P(None, AXIS, None), P(None, AXIS))

    def device_step(x, lengths, d_y, w_attn, b_attn, ln_par, w_up, b_up, w_down, b_down):
        tables = rotary_tables()
        pack_qkv, pack_mo = pack_shards(w_attn, w_up, w_down)
        xs, q, k, v, probs, ctx, mid, act, slope, c, w_qkv, w_o, w_up, w_down = forward(
            lengths, x, tables, pack_qkv, pack_mo, pack_small(b_attn, ln_par, b_up, b_down))
        grad, attn, up, down, small = backward(d_y, xs, q, k, v, probs, ctx, mid, act, slope, c, tables, w_qkv, w_o, w_up, w_down)
        me = lax.axis_index(AXIS)
        small = small.reshape(TWO, SIXTEEN, DIM)
        mine = lax.dynamic_slice(small, (ZERO, ZERO, FOUR * me), (TWO, SIXTEEN, FOUR))
        b_up_grad = lax.dynamic_slice(small[:, B_UP:B_DOWN].reshape(TWO, FFN), (ZERO, SIXTEEN * me), (TWO, SIXTEEN))
        return grad, attn, mine[:, :FOUR], mine[:, FOUR:EIGHT], up, b_up_grad, down, mine[:, 12]

    return jax.shard_map(device_step, mesh=mesh,
                         in_specs=(batch_spec, batch_spec, batch_spec) + weight_specs,
                         out_specs=(batch_spec,) + weight_specs,
                         check_vma=False)
```

```python
import math
import functools
import jax
import jax.numpy as jnp
from jax import lax
from jax.experimental import pallas as pl
from jax.experimental.pallas import tpu as pltpu
from jax.sharding import PartitionSpec as P

ZERO, ONE, TWO, THREE, FOUR = range(5)
EIGHT, SIXTEEN, WIDTH = 8, 16, 256

F32, BF16 = jnp.float32, jnp.bfloat16
SEQS, TOK, DIM, FFN, HEADS, HEAD, LANES = FOUR, 512, 512, 2048, EIGHT, 64, 128
HALF = HEAD // TWO
EPS = 1e-5
THETA = 10000.0
NEG_BIG = -1e30
B_ATTN, LN_PAR, B_UP, B_DOWN = ZERO, FOUR, EIGHT, 12


def nn(a, b):
    return lax.dot_general(a, b, (((ONE,), (ZERO,)), ((), ())), preferred_element_type=F32)


def nt(a, b):
    return lax.dot_general(a, b, (((ONE,), (ONE,)), ((), ())), preferred_element_type=F32)


def tn(a, b):
    return lax.dot_general(a, b, (((ZERO,), (ZERO,)), ((), ())), preferred_element_type=F32)


def lane_tiles(width=TOK, size=LANES):
    return [slice(i, i + size) for i in range(ZERO, width, size)]


def column(c_ref, lane, width=LANES):
    return jnp.broadcast_to(c_ref[:, lane:lane + ONE], (c_ref.shape[ZERO], width))


def total(value):
    return jnp.sum(value, axis=ZERO, keepdims=True)


def normed(x):
    centred = x - total(x) * (1.0 / DIM)
    rstd = lax.rsqrt(total(centred * centred) * (1.0 / DIM) + EPS)
    return centred * rstd, rstd


def norm_to(x_ref, c_ref, lane, h_ref):
    gain, shift = column(c_ref, lane), column(c_ref, lane + ONE)
    for cols in lane_tiles():
        h_ref[:, cols] = (normed(x_ref[:, cols].astype(F32))[ZERO] * gain + shift).astype(BF16)


def fold(value):
    parts = [value[:, cols] for cols in lane_tiles(value.shape[ONE])]
    return functools.reduce(jnp.add, parts)


def seq_spec(shape):
    return pl.BlockSpec((ONE, *shape), lambda s: (s,) + (ZERO,) * len(shape))


def once(shape):
    return pl.BlockSpec(shape, lambda s: (ZERO,) * len(shape), pipeline_mode=pl.Buffered(ONE))


def act_shape(rows, dtype):
    return jax.ShapeDtypeStruct((SEQS, rows, TOK), dtype)


PARAMS = pltpu.CompilerParams(vmem_limit_bytes=60 << 20, dimension_semantics=("arbitrary",))
SQUARE, TALL, WIDE, COLS = (DIM, TOK), (FFN, TOK), (DIM, FFN), (DIM, LANES)


def rotary_tables():
    inv_freq = 1.0 / (THETA ** (jnp.arange(HALF, dtype=F32) * (2.0 / HEAD)))
    angles = inv_freq[:, None] * jnp.arange(TOK, dtype=F32)[None, :]
    return jnp.cos(angles), jnp.sin(angles)


MESH = pl.DeviceIdType.MESH
AXIS = "fsdp"
ORDERS = ((TWO, ONE, ZERO), (ONE, ZERO, TWO), (ZERO, TWO, ONE))


class Place:
    def __init__(self):
        me = lax.axis_index(AXIS)
        self.core = lax.rem(me, TWO)
        self.pos = (me // 32, lax.rem(me // EIGHT, FOUR), lax.rem(me // TWO, FOUR))
        self.partner = me + ONE - TWO * self.core

    def coord(self, dim, delta):
        return lax.rem(self.pos[dim] + (delta + FOUR), FOUR)

    def device(self, offsets):
        pos = [self.coord(dim, offsets.get(dim, ZERO)) for dim in range(THREE)]
        return pos[ZERO] * 32 + pos[ONE] * EIGHT + pos[TWO] * TWO + self.core

    def greet(self):
        barrier = pltpu.get_barrier_semaphore()

        @pl.loop(ONE, 64)
        def _(i):
            offsets = {ZERO: i // SIXTEEN, ONE: lax.rem(i // FOUR, FOUR), TWO: lax.rem(i, FOUR)}

            @pl.when(offsets[ZERO] * offsets[ONE] * offsets[TWO] == ZERO)
            def _():
                pl.semaphore_signal(barrier, inc=ONE, device_id=(self.device(offsets),), device_id_type=MESH)
        pl.semaphore_signal(barrier, inc=ONE, device_id=(self.partner,), device_id_type=MESH)

    def met(self):
        pl.semaphore_wait(pltpu.get_barrier_semaphore(), 37)


def remote(src, dst, send_sem, recv_sem, device):
    return pltpu.make_async_remote_copy(src_ref=src, dst_ref=dst, send_sem=send_sem, recv_sem=recv_sem,
                                        device_id=(device,), device_id_type=MESH)


LINE = (ONE, -ONE, TWO)


def plane_offsets(order, k, sign=ONE):
    return {order[ONE]: sign * (k // FOUR), order[TWO]: sign * lax.rem(k, FOUR)}


class Gather:
    def __init__(self, place, buf, order, send, recv):
        self.place, self.buf, self.order, self.send, self.recv = place, buf, order, send, recv

    def block(self, offsets, whole=()):
        index = [slice(ZERO, FOUR) if dim in whole else pl.ds(self.place.coord(dim, offsets.get(dim, ZERO)), ONE) for dim in range(THREE)]
        return self.buf.at[index[ZERO], index[ONE], index[TWO], pl.ds(self.place.core, ONE)]

    def copy(self, ref, key, device):
        return remote(ref, ref, self.send.at[key], self.recv.at[key], device)

    def plane_start(self):
        @pl.loop(ONE, SIXTEEN)
        def _(k):
            self.copy(self.block({}), k, self.place.device(plane_offsets(self.order, k))).start()

    def plane_wait(self):
        @pl.loop(ONE, SIXTEEN)
        def _(k):
            self.copy(self.block(plane_offsets(self.order, k, -ONE)), k, self.place.partner).wait_recv()

    def line(self, i, sign):
        offsets = {self.order[ZERO]: sign * LINE[i]}
        return self.block(offsets, self.order[ONE:])

    def line_start(self):
        for i, delta in enumerate(LINE):
            self.copy(self.line(i, ZERO), SIXTEEN + i, self.place.device({self.order[ZERO]: delta})).start()

    def line_wait(self):
        for i in range(THREE):
            self.copy(self.line(i, -ONE), SIXTEEN + i, self.place.partner).wait_recv()

    def share(self, core):
        return self.copy(self.buf.at[:, :, :, pl.ds(core, ONE)], 19, self.place.partner)

    def share_start(self):
        self.share(self.place.core).start()

    def end(self):
        self.share(ONE - self.place.core).wait_recv()

        @pl.loop(ONE, SIXTEEN)
        def _(k):
            self.copy(self.block({}), k, self.place.partner).wait_send()
        for i in range(THREE):
            self.copy(self.line(i, ZERO), SIXTEEN + i, self.place.partner).wait_send()
        self.share(self.place.core).wait_send()


def gather_steps(gathers):
    def each(*names):
        def step():
            for name in names:
                for g in gathers:
                    getattr(g, name)()
        return step

    return [each("plane_start"), each("plane_wait", "line_start"), each("line_wait", "share_start"), each("end")]


class Scatter:
    def __init__(self, place, grads, acc, got_a, got_b, got_p, other, order, send, recv):
        self.place, self.grads, self.acc, self.order = place, grads, acc, order
        self.got_a, self.got_b, self.got_p, self.other, self.send, self.recv = got_a, got_b, got_p, other, send, recv
        self.units = acc.shape[ZERO]

    def columns(self, core):
        return pl.ds(pl.multiple_of(core * WIDTH, WIDTH), WIDTH)

    def swap_copy(self, u):
        place = self.place
        return remote(self.grads(u).at[:, :, :, :, self.columns(ONE - place.core)], self.acc.at[u], self.send.at[20 + u], self.recv.at[20 + u], place.partner)

    def swap(self):
        for u in range(self.units):
            self.swap_copy(u).start()

    def swapped(self):
        for u in range(self.units):
            self.swap_copy(u).wait()
            grad, acc = self.grads(u), self.acc

            @pl.loop(ZERO, FOUR)
            def _(z):
                acc[u, z] = acc[u, z] + grad[z, :, :, :, self.columns(self.place.core)]

    def part(self, delta, half=None):
        index = [slice(ZERO, FOUR)] * THREE
        index[self.order[ZERO]] = pl.ds(self.place.coord(self.order[ZERO], delta), ONE)
        return self.acc.at[:, index[ZERO], index[ONE], index[TWO], :, slice(ZERO, WIDTH) if half is None else lane_tiles()[half]]

    def ring(self, step, way):
        delta = (ONE, -ONE)[way]
        device = self.place.device({self.order[ZERO]: delta})
        if step == ZERO:
            src, dst = self.part(TWO, way), self.got_a.at[:, :, :, :, :, lane_tiles()[way]]
        else:
            src, dst = self.part(delta), self.got_b.at[way]
        key = SIXTEEN + TWO * step + way
        return remote(src, dst, self.send.at[key], self.recv.at[key], device)

    def ring_start(self):
        for way in range(TWO):
            self.ring(ZERO, way).start()

    def ring_turn(self):
        for way in range(TWO):
            self.ring(ZERO, way).wait_recv()
            self.add((ONE, -ONE)[way], way, self.got_a)
            self.ring(ONE, way).start()

    def add(self, delta, half, *refs):
        dim, acc = self.order[ZERO], self.acc
        at = self.place.coord(dim, delta)
        columns = slice(ZERO, WIDTH) if half is None else lane_tiles()[half]

        @pl.loop(ZERO, FOUR)
        def _(i):
            index = [i if d == self.order[ONE] else slice(ZERO, FOUR) for d in range(THREE)]
            there = [slice(None), *index, slice(None), columns]
            here = list(there)
            here[ONE + dim] = pl.ds(at, ONE)
            there[ONE + dim] = slice(ZERO, ONE)
            value = acc[tuple(here)]
            for ref in refs:
                value = value + ref[tuple(there)]
            acc[tuple(here)] = value

    def plane_copy(self, k):
        offsets = plane_offsets(self.order, k)
        index = [pl.ds(self.place.coord(dim, offsets.get(dim, ZERO)), ONE) for dim in range(THREE)]
        src = self.acc.at[:, index[ZERO], index[ONE], index[TWO]]
        return remote(src, self.got_p.at[k], self.send.at[k], self.recv.at[k], self.place.device(offsets))

    def plane_start(self):
        for way in range(TWO):
            self.ring(ONE, way).wait_recv()
        self.add(ZERO, None, self.got_b.at[ZERO], self.got_b.at[ONE])

        @pl.loop(ONE, SIXTEEN)
        def _(k):
            self.plane_copy(k).start()

    def own(self):
        z, y, x = [pl.ds(p, ONE) for p in self.place.pos]
        return self.acc.at[:, z, y, x]

    def last_copy(self):
        return remote(self.own(), self.other, self.send.at[23], self.recv.at[23], self.place.partner)

    def last(self):
        @pl.loop(ONE, SIXTEEN)
        def _(k):
            self.plane_copy(k).wait_recv()
        own = self.own()
        own[...] = functools.reduce(jnp.add, [self.got_p[k] for k in range(ONE, SIXTEEN)], own[...])
        self.last_copy().start()

    def finish(self, store):
        self.last_copy().wait_recv()
        first = self.place.core == ZERO
        for u in range(self.units):
            own, came = self.own()[u, ZERO, ZERO, ZERO], self.other[u, ZERO, ZERO, ZERO]
            store(u, jnp.concatenate([jnp.where(first, own, came), jnp.where(first, came, own)], axis=ONE))
        for step in range(TWO):
            for way in range(TWO):
                self.ring(step, way).wait_send()

        @pl.loop(ONE, SIXTEEN)
        def _(k):
            self.plane_copy(k).wait_send()
        self.last_copy().wait_send()


def landing_shapes(order, units):
    size = [FOUR, FOUR, FOUR]
    size[order[ZERO]] = ONE
    return (units, *size, EIGHT, WIDTH), (TWO, units, *size, EIGHT, WIDTH), (SIXTEEN, units, ONE, ONE, ONE, EIGHT, WIDTH), (units, ONE, ONE, ONE, EIGHT, WIDTH)


class Small:
    def __init__(self, place, value, slots, send, recv):
        self.place, self.value, self.slots, self.send, self.recv = place, value, slots, send, recv

    def copies(self, stage):
        if stage == THREE:
            return [remote(self.value, self.slots.at[9], self.send.at[9], self.recv.at[9], self.place.partner)]
        return [remote(self.value, self.slots.at[stage * THREE + k], self.send.at[stage * THREE + k], self.recv.at[stage * THREE + k],
                       self.place.device({stage: delta})) for k, delta in enumerate((ONE, -ONE, TWO))]

    def start(self, stage):
        for copy in self.copies(stage):
            copy.start()

    def finish(self, stage):
        copies = self.copies(stage)
        for copy in copies:
            copy.wait()
        value = self.value[...]
        for k in range(len(copies)):
            value = value + self.slots[stage * THREE + k]
        self.value[...] = value

    def steps(self):
        def turn(stage):
            def step():
                self.finish(stage)
                self.start(stage + ONE)
            return step

        return [lambda: self.start(ZERO), turn(ZERO), turn(ONE), turn(TWO), lambda: self.finish(THREE)]


VMEM = pl.BlockSpec(memory_space=pltpu.VMEM)
HBM = pl.BlockSpec(memory_space=pl.ANY)
DMA = pltpu.SemaphoreType.DMA


COLOURS = ((THREE, FOUR, 5), (6, 7, EIGHT), (9, 10, 11))
GRID = (FOUR, FOUR, FOUR)


def spread(buf, u, out_ref, column_base):
    @pl.loop(ZERO, EIGHT)
    def _(block):
        for part in range(FOUR):
            g = block * FOUR + part
            tiles = [buf[block // TWO, lax.rem(block, TWO) * TWO + part // TWO, part % TWO * TWO + k // TWO, k % TWO, u].astype(F32) for k in range(FOUR)]
            rows = pl.ds(pl.multiple_of(g * SIXTEEN, SIXTEEN), SIXTEEN)
            for j, cols in enumerate(lane_tiles()):
                value = jnp.concatenate([t[FOUR * j:FOUR * j + FOUR] for t in tiles], axis=ZERO).astype(BF16)
                out_ref[rows, column_base + cols.start:column_base + cols.stop] = value


def spread_down(buf, u, out_ref, cols):
    @pl.loop(ZERO, SIXTEEN)
    def _(i):
        for k in range(EIGHT):
            d = i * EIGHT + k
            out_ref[pl.ds(pl.multiple_of(d * SIXTEEN, SIXTEEN), SIXTEEN), cols] = buf[i // FOUR, lax.rem(i, FOUR), k // TWO, k % TWO, u]


def same(shape, test):
    row = lax.broadcasted_iota(jnp.int32, shape, ZERO)
    col = lax.broadcasted_iota(jnp.int32, shape, ONE)
    return jnp.where(test(row, col), 1.0, 0.0)


def small_columns(small_ref, c_ref):
    rows = [small_ref[z, y, x, c, ZERO] for z in range(FOUR) for y in range(FOUR) for x in range(FOUR) for c in range(TWO)]
    table = jnp.concatenate(rows, axis=ZERO).astype(BF16)
    quads = nn(same((DIM, LANES), lambda r, c: r // FOUR == c).astype(BF16), table)
    quads = (quads * same((DIM, LANES), lambda r, c: r % FOUR == c % FOUR)).astype(BF16)
    mask = same((DIM, LANES), lambda r, c: r % SIXTEEN == c % SIXTEEN)
    pick = same((DIM, 32), lambda r, c: r // SIXTEEN == c).astype(BF16)
    ups = [(nn(pick, table[32 * k:32 * k + 32]) * mask).astype(BF16) for k in range(FOUR)]
    for layer in range(TWO):
        def is_up(r):
            return r // SIXTEEN == layer * FOUR + TWO

        value = nn(quads, same((LANES, LANES), lambda r, c: (r // 64 == layer) & (r % 64 // FOUR == c) & ~is_up(r)).astype(BF16))
        for k in range(FOUR):
            value = value + nn(ups[k], same((LANES, LANES), lambda r, c: is_up(r) & (c == B_UP + k)).astype(BF16))
        c_ref[layer] = value


def tile_of(rows):
    rows = rows.astype(F32)
    return jnp.concatenate([rows[:, cols] for cols in lane_tiles()], axis=ZERO).astype(BF16)


def small_row(b_attn, ln_par, b_up, b_down):
    lane = lax.broadcasted_iota(jnp.int32, (ONE, LANES), ONE)
    row = jnp.zeros((ONE, LANES), F32)
    pieces = []
    for l in range(TWO):
        for m in range(FOUR):
            pieces += [(b_attn[l, m:m + ONE, :], 64 * l + FOUR * m), (ln_par[l, m:m + ONE, :], 64 * l + FOUR * m + SIXTEEN)]
        pieces += [(b_up[l:l + ONE, :], 64 * l + 32), (b_down[l:l + ONE, :], 64 * l + 48)]
    for piece, at in pieces:
        n = piece.shape[ONE]
        wide = jnp.concatenate([piece.astype(F32), jnp.zeros((ONE, LANES - n), F32)], axis=ONE)
        wide = pltpu.roll(wide, at, ONE) if at else wide
        row = jnp.where((lane >= at) & (lane < at + n), wide, row)
    return row


def hooks(slot, plan):
    def hook(at):
        for slots, run in plan:
            mine = [when for when in slots if when % FOUR == at]
            if mine:
                pl.when(functools.reduce(jnp.logical_or, [slot + at == when for when in mine]))(run)
    return hook


def forward_kernel(len_ref, x_ref, cos_ref, sin_ref, w_attn, b_attn, ln_par, w_up, b_up, w_down, b_down,
                   xs_out, q_ref, k_ref, v_ref, p_hbm, ctx_ref, mid_ref, act_ref, slope_ref, c_ref,
                   nat_qkv, nat_wo, nat_up, nat_down,
                   xs, ctxb, wqkv, wo, up, down, n_qkv, n_wo, n_up, n_down, p_buf, h_ref, s_a, s_b, s_c,
                   sbuf, q0, q1, q2, m0, m1, m2, send, recv, p_sem, nat_sem):
    step = pl.program_id(ZERO)
    phase, seq, layer = step // FOUR, lax.rem(step, FOUR), step // EIGHT
    place = Place()
    z, y, x = place.pos
    qkv_bufs, mo_bufs = (q0, q1, q2), (m0, m1, m2)

    def group(bufs, base, l):
        return [Gather(place, b.at[l], ORDERS[k], send.at[base + k, l], recv.at[base + k, l]) for k, b in enumerate(bufs)]

    little = Gather(place, sbuf, ORDERS[ZERO], send.at[6, ZERO], recv.at[6, ZERO])

    def nat_copies(which, l):
        if which == ZERO:
            return [pltpu.make_async_copy(n_qkv, nat_qkv.at[l], nat_sem.at[ZERO])]
        return [pltpu.make_async_copy(src, dst.at[l], nat_sem.at[ONE + i]) for i, (src, dst) in enumerate(((n_wo, nat_wo), (n_up, nat_up), (n_down, nat_down)))]

    def wait(copies):
        for copy in copies:
            copy.wait()

    def start(copies):
        for copy in copies:
            copy.start()

    def take_qkv():
        pl.when(step > ZERO)(lambda: wait(nat_copies(ZERO, layer)))
        for m in range(THREE):
            spread(qkv_bufs[m].at[layer], ZERO, n_qkv.at[m], ZERO)
            wqkv[m] = n_qkv[m].T
        start(nat_copies(ZERO, layer))

    def take_mo():
        pl.when(step > EIGHT)(lambda: wait(nat_copies(ONE, layer)))
        for colour in range(THREE):
            for u, unit in enumerate(COLOURS[colour]):
                buf = mo_bufs[colour].at[layer]
                if unit == THREE:
                    spread(buf, u, n_wo, ZERO)
                    wo[...] = n_wo[...].T
                elif unit < EIGHT:
                    part = slice(DIM * (unit - FOUR), DIM * (unit - THREE))
                    spread(buf, u, n_up, part.start)
                    up[part, :] = n_up[:, part].T
                else:
                    spread_down(buf, u, n_down, lane_tiles()[unit - EIGHT])
        for k in range(FOUR):
            part = slice(DIM * k, DIM * k + DIM)
            down[:, part] = n_down[part, :].T
        start(nat_copies(ONE, layer))

    @pl.when(step == ZERO)
    def _():
        place.greet()
        for l in range(TWO):
            for unit in range(12):
                if unit < FOUR:
                    tile = tile_of(w_attn[l, unit])
                elif unit < EIGHT:
                    tile = tile_of(w_up[l, :, DIM * (unit - FOUR):DIM * (unit - THREE)])
                else:
                    tile = w_down[l, :, lane_tiles()[unit - EIGHT]]
                if unit < THREE:
                    qkv_bufs[unit][l, z, y, x, place.core, ZERO] = tile
                else:
                    mo_bufs[(unit - THREE) // THREE][l, z, y, x, place.core, (unit - THREE) % THREE] = tile
        sbuf[z, y, x, place.core, ZERO] = small_row(b_attn, ln_par, b_up, b_down)
        place.met()
        for run in gather_steps(group(qkv_bufs, ZERO, ZERO) + [little]):
            run()
        small_columns(sbuf, c_ref)

    attn_hook = hooks(step * FOUR, [((when, when + 32), run) for when, run in zip(MO_SLOTS, gather_steps(group(mo_bufs, THREE, layer)))])
    mlp_hook = hooks(step * FOUR, [((when,), run) for when, run in zip(QKV_SLOTS, gather_steps(group(qkv_bufs, ZERO, ONE)))])

    @pl.when(phase % TWO == ZERO)
    def _():
        pl.when(seq == ZERO)(take_qkv)

        @pl.when(step < FOUR)
        def _():
            xs[seq] = x_ref[ZERO].T
            xs_out[ZERO, ZERO] = xs[seq]

        attn_hook(ZERO)
        copies = [pltpu.make_async_copy(p_buf.at[head], p_hbm.at[layer, seq, head], p_sem.at[head]) for head in range(HEADS)]
        attn_forward(len_ref[seq], xs.at[seq], wqkv, c_ref.at[layer], cos_ref, sin_ref, q_ref.at[ZERO, ZERO], k_ref.at[ZERO, ZERO],
                     v_ref.at[ZERO, ZERO], p_buf, ctx_ref.at[ZERO, ZERO], ctxb.at[seq], h_ref, s_a, s_b, s_c, attn_hook,
                     lambda: pl.when(step > ZERO)(lambda: wait(copies)))
        start(copies)
        pl.when(step == 11)(lambda: wait(copies))
        attn_hook(THREE)

    @pl.when(phase % TWO == ONE)
    def _():
        pl.when(seq == ZERO)(take_mo)
        mlp_hook(ZERO)
        mlp_forward(layer, ctxb.at[seq], xs.at[seq], wo, up, down, c_ref.at[layer], mid_ref.at[ZERO, ZERO], act_ref.at[ZERO, ZERO], slope_ref.at[ZERO, ZERO],
                    h_ref, s_a, s_b, mlp_hook)

        @pl.when(layer == ZERO)
        def _():
            xs_out[ZERO, ZERO] = xs[seq]
        mlp_hook(THREE)

    @pl.when(step == 15)
    def _():
        for which in range(TWO):
            wait(nat_copies(which, ONE))


def attn_forward(length, xt, w, c_ref, cos_ref, sin_ref, q_ref, k_ref, v_ref, p_buf, ctx_ref, ctxb, h_ref, s_a, s_b, s_c, hook, free):
    norm_to(xt, c_ref, LN_PAR, h_ref)
    for m, acc in enumerate((s_a, s_b, s_c)):
        acc[...] = nn(w[m], h_ref[...])
    for m, (acc, out) in enumerate(((s_a, q_ref), (s_b, k_ref), (s_c, v_ref))):
        bias = column(c_ref, B_ATTN + m)
        for cols in lane_tiles():
            if m == TWO:
                out[:, cols] = (acc[:, cols] + bias).astype(BF16)
                continue
            cos, sin = cos_ref[:, cols], sin_ref[:, cols]
            for head in range(HEADS):
                _, one, two = head_rows(head)
                a, b = acc[one, cols] + bias[one], acc[two, cols] + bias[two]
                if m == ZERO:
                    a, b = a * HEAD ** -0.5, b * HEAD ** -0.5
                out[one, cols] = (a * cos - b * sin).astype(BF16)
                out[two, cols] = (b * cos + a * sin).astype(BF16)
    hook(ONE)
    free()
    key = lax.broadcasted_iota(jnp.int32, (SIXTEEN, TOK), ONE)
    row = lax.broadcasted_iota(jnp.int32, (SIXTEEN, TOK), ZERO)
    bias_rows = jnp.where((row == ZERO) & (key >= length), NEG_BIG, 0.0).astype(BF16)
    one_rows = jnp.where(row == ZERO, 1.0, 0.0).astype(BF16)
    scores = (s_a, s_b)

    def open_head(head):
        rows = head_rows(head)[ZERO]
        keys = jnp.concatenate([k_ref[rows, :], bias_rows], axis=ZERO)
        queries = jnp.concatenate([q_ref[rows, :], one_rows], axis=ZERO)
        scores[head % TWO][...] = tn(keys, queries)

    def weigh(head):
        value = scores[head % TWO][...]
        weight = jnp.exp(value - jnp.max(value, axis=ZERO, keepdims=True))
        p_buf[head] = (weight * (1.0 / total(weight))).astype(BF16)

    def close_head(head):
        rows = head_rows(head)[ZERO]
        ctx = nn(v_ref[rows, :], p_buf[head])
        ctx_ref[rows, :] = ctx
        ctxb[rows, :] = ctx.astype(BF16)

    open_head(ZERO)
    for head in range(HEADS):
        if head + ONE < HEADS:
            open_head(head + ONE)
        if head:
            close_head(head - ONE)
        weigh(head)
        if head == THREE:
            hook(TWO)
    close_head(HEADS - ONE)


def mlp_forward(layer, ctxb, xt, wo, up, down, c_ref, mid_ref, act_ref, slope_ref, h_ref, s_a, s_b, hook):
    s_a[...] = nn(wo[...], ctxb[...])
    for cols in lane_tiles():
        mid_ref[:, cols] = (xt[:, cols].astype(F32) + s_a[:, cols] + column(c_ref, B_ATTN + THREE)).astype(BF16)
    norm_to(mid_ref, c_ref, LN_PAR + TWO, h_ref)
    hook(ONE)
    pre = (s_a, s_b)
    parts = [slice(DIM * k, DIM * k + DIM) for k in range(FOUR)]

    def open_part(k):
        pre[k % TWO][...] = nn(up[parts[k], :], h_ref[...])

    open_part(ZERO)
    for k, rows in enumerate(parts):
        if k < THREE:
            open_part(k + ONE)
        for cols in lane_tiles():
            value = pre[k % TWO][:, cols] + column(c_ref, B_UP + k)
            scaled = value * math.sqrt(0.5)
            cdf = 0.5 + 0.5 * lax.erf(scaled)
            density = jnp.exp2(scaled * scaled * -math.log2(math.e) - 0.5 * math.log2(2.0 * math.pi))
            act_ref[rows, cols] = (value * cdf).astype(BF16)
            slope_ref[rows, cols] = cdf + value * density
        if k == ONE:
            hook(TWO)

    @pl.when(layer == ZERO)
    def _():
        out = nn(down[...], act_ref[...])
        for cols in lane_tiles():
            xt[:, cols] = (mid_ref[:, cols].astype(F32) + out[:, cols] + column(c_ref, B_DOWN)).astype(BF16)


MO_SLOTS = (ZERO, 5, 13, 15)
QKV_SLOTS = (SIXTEEN, 22, 26, 28)


def forward(lengths, x, tables, params):
    def saved(index, rows, dtype):
        return jax.ShapeDtypeStruct((TWO, SEQS, rows, TOK), dtype), pl.BlockSpec((ONE, ONE, rows, TOK), index)

    def attn_at(s):
        return s // EIGHT, jnp.where(s // FOUR % TWO == ZERO, s % FOUR, THREE), ZERO, ZERO

    def mlp_at(s):
        odd = s // FOUR % TWO == ONE
        return jnp.where(s < 12, ZERO, ONE), jnp.where(odd, s % FOUR, jnp.where(s < FOUR, ZERO, THREE)), ZERO, ZERO

    def xs_at(s):
        return jnp.where(s < FOUR, ZERO, ONE), jnp.where(s < EIGHT, s % FOUR, THREE), ZERO, ZERO

    outs = [saved(xs_at, DIM, BF16)] + [saved(attn_at, DIM, BF16)] * THREE
    outs += [(jax.ShapeDtypeStruct((TWO, SEQS, HEADS, TOK, TOK), BF16), HBM), saved(attn_at, DIM, F32)]
    outs += [saved(mlp_at, DIM, BF16), saved(mlp_at, FFN, BF16), saved(mlp_at, FFN, F32)]
    outs += [(jax.ShapeDtypeStruct((TWO, *COLS), F32), once((TWO, *COLS)))]
    weights = ((THREE, DIM, DIM), (DIM, DIM), (DIM, FFN), (FFN, DIM))
    outs += [(jax.ShapeDtypeStruct((TWO, *w), BF16), HBM) for w in weights]
    scratch = [(SEQS, *SQUARE), (SEQS, *SQUARE), weights[ZERO], weights[ONE], weights[THREE], weights[TWO], *weights, (HEADS, TOK, TOK), SQUARE]
    scratch = [pltpu.VMEM(s, BF16) for s in scratch] + [pltpu.VMEM(SQUARE, F32)] * THREE + [pltpu.VMEM((*GRID, TWO, ONE, ONE, LANES), F32)]
    scratch += [pltpu.VMEM((TWO, *GRID, TWO, n, SIXTEEN, LANES), BF16) for n in (ONE, THREE) for _ in range(THREE)]
    scratch += [DMA((7, TWO, 20)), DMA((7, TWO, 20)), DMA((HEADS,)), DMA((FOUR,))]
    return pl.pallas_call(
        forward_kernel, grid=(SIXTEEN,),
        out_shape=[o[ZERO] for o in outs], out_specs=[o[ONE] for o in outs],
        in_specs=[pl.BlockSpec(memory_space=pltpu.SMEM), pl.BlockSpec((ONE, *SQUARE), lambda s: (jnp.minimum(s, THREE), ZERO, ZERO)),
                  once((HALF, TOK)), once((HALF, TOK))] + [once(p.shape) for p in params],
        scratch_shapes=scratch,
        compiler_params=pltpu.CompilerParams(collective_id=ZERO, has_side_effects=True, vmem_limit_bytes=67043328,
                                             dimension_semantics=("arbitrary",)),
        name="forward")(lengths, x, *tables, *params)


def norm_back(dh, x, gain):
    xhat, rstd = normed(x)
    dxhat = dh * gain
    mean_one = total(dxhat) * (1.0 / DIM)
    mean_two = total(dxhat * xhat) * (1.0 / DIM)
    return rstd * (dxhat - mean_one - xhat * mean_two), xhat


def columns_of(pairs):
    lane = lax.broadcasted_iota(jnp.int32, COLS, ONE)
    value = jnp.zeros(COLS, F32)
    for at, partial in pairs:
        value = jnp.where(lane == at, jnp.sum(partial, axis=ONE, keepdims=True), value)
    return value


def head_rows(head):
    return slice(HEAD * head, HEAD * head + HEAD), slice(HEAD * head, HEAD * head + HALF), slice(HEAD * head + HALF, HEAD * head + HEAD)


class Reduce:
    def __init__(self, place, units, grads, buffers, send, recv):
        self.units = units
        self.scatters = [Scatter(place, (lambda u, k=k: grads(units[k][u])), *buffers[k], ORDERS[k], send.at[k], recv.at[k]) for k in range(THREE)]

    def steps(self, store):
        def each(*names):
            def step():
                for name in names:
                    for s in self.scatters:
                        getattr(s, name)()
            return step

        def finish():
            for units, s in zip(self.units, self.scatters):
                s.finish(lambda u, full, units=units: store(units[u], full))

        return [each("swap"), each("swapped", "ring_start"), each("ring_turn"), each("plane_start"), each("last"), finish]


def backward_kernel(dy_ref, mid_ref, ctx_ref, q_ref, k_ref, v_ref, x_ref, cos_ref, sin_ref, c_ref, p_hbm, slope_hbm, act_hbm,
                    qkv_hbm, wo_hbm, up_hbm, down_hbm,
                    dx_ref, attn_out, up_out, down_out, small_out, *refs):
    (grad, dctx, delta, big, wqkv, wo, slope, act, dpre, h_ref, s_a, s_b, d_a, d_b, sums,
     g_qkv, g_wo, g_up, g_down, rows_ref, slots_ref), refs = refs[:21], refs[21:]
    qkv_bufs, mo_bufs, refs = [refs[5 * k:5 * k + 5] for k in range(THREE)], [refs[5 * k + 15:5 * k + 20] for k in range(THREE)], refs[30:]
    send, recv, ssend, srecv, big_sem, w_sem, mlp_sem = refs
    step = pl.program_id(ZERO)
    phase, seq = step // FOUR, lax.rem(step, FOUR)
    layer = ONE - step // EIGHT
    place = Place()

    def grads(unit):
        if unit < THREE:
            return g_qkv.at[unit]
        if unit == THREE:
            return g_wo
        if unit < EIGHT:
            return g_up.at[unit - FOUR]
        return g_down.at[:, :, :, unit - EIGHT]

    live = step < SIXTEEN
    turn = jnp.where(live, ZERO, ONE)
    qkv_sums = Reduce(place, ((ZERO,), (ONE,), (TWO,)), grads, [(a, ra, rb, rp.at[turn], o) for a, ra, rb, rp, o in qkv_bufs], send.at[turn], recv.at[turn])
    mo_sums = Reduce(place, COLOURS, grads, mo_bufs, send.at[TWO], recv.at[TWO])
    tiny = Small(place, rows_ref, slots_ref, ssend, srecv)
    first_core = place.core == ZERO

    def store(l):
        def put(unit, full):
            if unit < EIGHT:
                mine = jnp.where(first_core, full[:FOUR], full[FOUR:])
                if unit < FOUR:
                    attn_out[l, unit] = mine
                else:
                    up_out[l, :, DIM * (unit - FOUR):DIM * (unit - THREE)] = mine
            else:
                at = EIGHT * (unit % TWO)

                @pl.when(place.core == (unit - EIGHT) // TWO)
                def _():
                    down_out[l, at:at + EIGHT] = full
        return put

    def mlp_weights(l):
        copies = [pltpu.make_async_copy(wo_hbm.at[l], wo, w_sem.at[ZERO])]
        for k in range(FOUR):
            part = pl.ds(DIM * k, DIM)
            copies.append(pltpu.make_async_copy(down_hbm.at[l, part], big.at[k], big_sem.at[k]))
            copies.append(pltpu.make_async_copy(up_hbm.at[l, :, part], big.at[FOUR + k], big_sem.at[FOUR + k]))
        return copies

    def attn_weights(l):
        return [pltpu.make_async_copy(qkv_hbm.at[l], wqkv, w_sem.at[ONE])]

    def probs(l, s):
        return [pltpu.make_async_copy(p_hbm.at[l, s, k], big.at[k], big_sem.at[k]) for k in range(HEADS)]

    def saved_mlp(l, s):
        return [pltpu.make_async_copy(slope_hbm.at[l, s], slope, mlp_sem.at[ZERO]), pltpu.make_async_copy(act_hbm.at[l, s], act, mlp_sem.at[ONE])]

    def start(copies):
        for copy in copies:
            copy.start()

    def wait(copies):
        for copy in copies:
            copy.wait()

    @pl.when(step == ZERO)
    def _():
        place.greet()
        start(mlp_weights(ONE) + saved_mlp(ONE, ZERO) + attn_weights(ONE))

    pl.when(step == ONE)(place.met)
    mo_steps, qkv_steps = mo_sums.steps(store(layer)), qkv_sums.steps(store(ONE - turn))
    late_steps = mo_sums.steps(store(ONE - turn))[FOUR:]
    attn_hook = hooks(step * FOUR, [((when, when + 32), run) for when, run in zip((SIXTEEN, 20, 24, 30), mo_steps)])
    mlp_plan = list(zip(((37, 69), (38, 70)), late_steps))
    mlp_plan += list(zip(((32, 64), (33, 65), (38, 66), (43, 67), (47, 71), (47, 71)), qkv_steps))
    mlp_plan += [((when,), run) for when, run in zip((64, 65, 66, 67, 71), tiny.steps())]
    mlp_hook = hooks(step * FOUR, mlp_plan)

    @pl.when(phase % TWO == ZERO)
    def _():
        @pl.when((seq == ZERO) & live)
        def _():
            for ref in (g_wo, g_up, g_down, sums):
                ref[...] = jnp.zeros_like(ref)

        @pl.when(step < FOUR)
        def _():
            grad[seq] = dy_ref[ZERO].T

        @pl.when((seq == ZERO) & live)
        def _():
            wait(mlp_weights(layer))

        mlp_hook(ZERO)
        pl.when(live)(lambda: wait(saved_mlp(layer, seq)))
        mlp_backward(grad.at[seq], slope, act, mid_ref, ctx_ref, wo, big, c_ref, dctx.at[seq], delta.at[seq], g_wo, g_up, g_down,
                     dpre, h_ref, s_a, s_b, sums, pl.when(live), mlp_hook,
                     lambda: pl.when(seq < THREE)(lambda: start(saved_mlp(layer, seq + ONE))))

        @pl.when((seq == THREE) & live)
        def _():
            value = columns_of([(B_UP + i, sums[i]) for i in range(FOUR)] + [
                (LN_PAR + TWO, sums[FOUR]), (LN_PAR + THREE, sums[5]), (B_DOWN, sums[6]), (B_ATTN + THREE, sums[7])])
            rows_ref[pl.ds(pl.multiple_of(layer * SIXTEEN, SIXTEEN), SIXTEEN), :] = value.T[:SIXTEEN]

        mlp_hook(THREE)

    @pl.when(phase % TWO == ONE)
    def _():
        @pl.when(seq == ZERO)
        def _():
            start(probs(layer, ZERO))
            wait(attn_weights(layer))
            for ref in (g_qkv, sums):
                ref[...] = jnp.zeros_like(ref)

        @pl.when(step == FOUR)
        def _():
            start(saved_mlp(ZERO, ZERO))
        attn_hook(ZERO)
        wait(probs(layer, seq))
        attn_backward(dctx.at[seq], delta.at[seq], big, q_ref, k_ref, v_ref, x_ref, grad.at[seq], wqkv, c_ref, cos_ref, sin_ref,
                      g_qkv, dpre, h_ref, s_a, s_b, d_a, d_b, sums, attn_hook,
                      lambda: pl.when(seq < THREE)(lambda: start(probs(layer, seq + ONE))))

        @pl.when(seq == THREE)
        def _():
            value = columns_of([(B_ATTN + i, sums[i]) for i in range(THREE)] + [(LN_PAR, sums[THREE]), (LN_PAR + ONE, sums[FOUR])])
            rows = pl.ds(pl.multiple_of(layer * SIXTEEN, SIXTEEN), SIXTEEN)
            rows_ref[rows, :] = rows_ref[rows, :] + value.T[:SIXTEEN]

        @pl.when(step == 7)
        def _():
            start(mlp_weights(ZERO) + attn_weights(ZERO))

        @pl.when(step > 11)
        def _():
            dx_ref[ZERO] = grad[seq].T
        attn_hook(THREE)

    @pl.when(step == 17)
    def _():
        small_out[...] = rows_ref[...]


def add_to(ref, value):
    ref[...] = ref[...] + value.reshape(ref.shape)


def mlp_backward(grad, slope, act, mid_ref, ctx_ref, wo, big, c_ref, dctx, delta, g_wo, g_up, g_down, dpre, h_ref, s_a, s_b, sums, when, hook, prefetch):
    parts = [slice(DIM * k, DIM * k + DIM) for k in range(FOUR)]
    pre = (s_a, s_b)

    def dact(k):
        pre[k % TWO][...] = nn(big[k], grad[...])

    @when
    def _():
        norm_to(mid_ref.at[ZERO], c_ref, LN_PAR + TWO, h_ref)
        dact(ZERO)
        for k, rows in enumerate(parts):
            if k < THREE:
                dact(k + ONE)
            if k:
                add_to(g_down.at[k - ONE], nt(act[parts[k - ONE], :], grad[...]))
            for cols in lane_tiles():
                value = pre[k % TWO][:, cols] * slope[rows, cols]
                sums[k] += value
                dpre[rows, cols] = value.astype(BF16)
        add_to(g_down.at[THREE], nt(act[parts[THREE], :], grad[...]))
        prefetch()
    hook(ONE)

    @when
    def _():
        s_a[...] = functools.reduce(jnp.add, [nn(big[FOUR + k], dpre[rows, :]) for k, rows in enumerate(parts)])
    hook(TWO)

    @when
    def _():
        for k, rows in enumerate(parts):
            add_to(g_up.at[k], nt(h_ref[...], dpre[rows, :]))
        gain = column(c_ref, LN_PAR + TWO)
        for cols in lane_tiles():
            dh, dy = s_a[:, cols], grad[:, cols].astype(F32)
            dx, xhat = norm_back(dh, mid_ref[ZERO, :, cols].astype(F32), gain)
            dmid = (dy + dx).astype(BF16)
            grad[:, cols] = dmid
            sums[FOUR] += dh * xhat
            sums[5] += dh
            sums[6] += dy
            sums[7] += dmid.astype(F32)
        add_to(g_wo, nt(ctx_ref[ZERO].astype(BF16), grad[...]))
        s_b[...] = nn(wo[...], grad[...])
        for head in range(HEADS):
            rows = head_rows(head)[ZERO]
            value = s_b[rows, :].astype(BF16)
            dctx[rows, :] = value
            delta[head:head + ONE, :] = total(value.astype(F32) * ctx_ref[ZERO, rows, :])


def attn_backward(dctx, delta, probs, q_ref, k_ref, v_ref, x_ref, grad, wqkv, c_ref, cos_ref, sin_ref, g_qkv, dproj, h_ref, s_a, s_b, d_a, d_b,
                  sums, hook, prefetch):
    scores, dscores = (s_a, s_b), (d_a, d_b)
    q, k, v = q_ref.at[ZERO], k_ref.at[ZERO], v_ref.at[ZERO]

    def open_head(head):
        rows = head_rows(head)[ZERO]
        scores[head % TWO][...] = tn(v[rows, :], dctx[rows, :])

    def weigh(head):
        dscores[head % TWO][...] = (probs[head].astype(F32) * (scores[head % TWO][...] - delta[head:head + ONE, :])).astype(BF16)

    def values(head):
        rows = head_rows(head)[ZERO]
        dv = nt(dctx[rows, :], probs[head])
        sums[TWO, rows, :] += fold(dv)
        dproj[TWO * DIM + rows.start:TWO * DIM + rows.stop, :] = dv.astype(BF16)

    def close_head(head):
        rows, one, two = head_rows(head)
        ds = dscores[head % TWO][...]
        for m, value in enumerate((nn(k[rows, :], ds) * HEAD ** -0.5, nt(q[rows, :], ds))):
            cos, sin = cos_ref[...], sin_ref[...]
            a, b = value[:HALF], value[HALF:]
            for at, out in ((one, a * cos + b * sin), (two, b * cos - a * sin)):
                dproj[m * DIM + at.start:m * DIM + at.stop, :] = out.astype(BF16)
                sums[m, at, :] += fold(out)

    open_head(ZERO)
    for head in range(HEADS):
        if head + ONE < HEADS:
            open_head(head + ONE)
        if head:
            close_head(head - ONE)
        values(head)
        weigh(head)
        if head == THREE:
            hook(ONE)
    close_head(HEADS - ONE)
    prefetch()
    hook(TWO)
    norm_to(x_ref.at[ZERO], c_ref, LN_PAR, h_ref)
    parts = [slice(DIM * m, DIM * m + DIM) for m in range(THREE)]
    s_a[...] = functools.reduce(jnp.add, [nn(wqkv[m], dproj[rows, :]) for m, rows in enumerate(parts)])
    for m, rows in enumerate(parts):
        add_to(g_qkv.at[m], nt(h_ref[...], dproj[rows, :]))
    gain = column(c_ref, LN_PAR)
    for cols in lane_tiles():
        dh = s_a[:, cols]
        dx, xhat = norm_back(dh, x_ref[ZERO, :, cols].astype(F32), gain)
        grad[:, cols] = (grad[:, cols].astype(F32) + dx).astype(BF16)
        sums[THREE] += dh * xhat
        sums[FOUR] += dh


def backward(dy, xs, q, k, v, probs, ctx, mid, act, slope, c, tables, w_qkv, w_o, w_up, w_down):
    def mlp_at(s):
        s = jnp.minimum(s, 15)
        odd = s // FOUR % TWO == ONE
        return ONE - s // EIGHT, jnp.where(odd, THREE, s % FOUR), ZERO, ZERO

    def attn_at(s):
        s = jnp.minimum(s, 15)
        odd = s // FOUR % TWO == ONE
        return jnp.where(s < EIGHT, ONE, ZERO) + jnp.where((s > 7) & (s < 12), ONE, ZERO), jnp.where(odd, s % FOUR, jnp.where(s < FOUR, ZERO, THREE)), ZERO, ZERO

    per_mlp = pl.BlockSpec((None, ONE, *SQUARE), mlp_at)
    per_attn = pl.BlockSpec((None, ONE, *SQUARE), attn_at)
    acc = [(*GRID, EIGHT, WIDTH)]
    scratch = [pltpu.VMEM((SEQS, *SQUARE), BF16), pltpu.VMEM((SEQS, *SQUARE), BF16), pltpu.VMEM((SEQS, HEADS, TOK), F32),
               pltpu.VMEM((HEADS, TOK, TOK), BF16), pltpu.VMEM((THREE, DIM, DIM), BF16), pltpu.VMEM((DIM, DIM), BF16),
               pltpu.VMEM(TALL, F32), pltpu.VMEM(TALL, BF16), pltpu.VMEM(TALL, BF16), pltpu.VMEM(SQUARE, BF16),
               pltpu.VMEM(SQUARE, F32), pltpu.VMEM(SQUARE, F32), pltpu.VMEM((TOK, TOK), BF16), pltpu.VMEM((TOK, TOK), BF16),
               pltpu.VMEM((EIGHT, *COLS), F32), pltpu.VMEM((THREE, *GRID, EIGHT, DIM), F32), pltpu.VMEM((*GRID, EIGHT, DIM), F32),
               pltpu.VMEM((FOUR, *GRID, EIGHT, DIM), F32), pltpu.VMEM((*GRID, FOUR, EIGHT, DIM), F32), pltpu.VMEM((32, DIM), F32), pltpu.VMEM((10, 32, DIM), F32)]
    for n in (ONE, THREE):
        for order in ORDERS:
            ring_a, ring_b, plane, other = landing_shapes(order, n)
            plane = (TWO, *plane) if n == ONE else plane
            scratch += [pltpu.VMEM(s, F32) for s in ((n, *GRID, EIGHT, WIDTH), ring_a, ring_b, plane, other)]
    scratch += [DMA((THREE, THREE, 24)), DMA((THREE, THREE, 24)), DMA((10,)), DMA((10,)), DMA((EIGHT,)), DMA((TWO,)), DMA((TWO,))]
    outs = ((TWO, FOUR, FOUR, DIM), (TWO, FOUR, FFN), (TWO, SIXTEEN, DIM), (32, DIM))
    whole = [pl.BlockSpec(s, lambda i, n=len(s): (ZERO,) * n, pipeline_mode=pl.Buffered(ONE)) for s in outs]
    dx_at = lambda s: (jnp.clip(s - 12, ZERO, THREE), ZERO, ZERO)
    return pl.pallas_call(
        backward_kernel, grid=(18,),
        out_shape=[jax.ShapeDtypeStruct((SEQS, TOK, DIM), BF16)] + [jax.ShapeDtypeStruct(s, F32) for s in outs],
        out_specs=[pl.BlockSpec((ONE, TOK, DIM), dx_at)] + whole,
        in_specs=[pl.BlockSpec((ONE, TOK, DIM), lambda s: (jnp.minimum(s, THREE), ZERO, ZERO)), per_mlp, per_mlp, per_attn, per_attn, per_attn, per_attn,
                  once((HALF, TOK)), once((HALF, TOK)), pl.BlockSpec((None, *COLS), lambda s: (ONE - jnp.minimum(s, 15) // EIGHT, ZERO, ZERO))] + [HBM] * 7,
        scratch_shapes=scratch,
        compiler_params=pltpu.CompilerParams(collective_id=ONE, has_side_effects=True, vmem_limit_bytes=67043328,
                                             dimension_semantics=("arbitrary",)),
        name="backward")(dy, mid, ctx, q, k, v, xs, *tables, c, probs, slope, act, w_qkv, w_o, w_up, w_down)


def solution(mesh):
    batch_spec = P(AXIS)
    weight_specs = (P(None, None, AXIS, None), P(None, None, AXIS), P(None, None, AXIS),
                    P(None, AXIS, None), P(None, AXIS), P(None, AXIS, None), P(None, AXIS))

    def device_step(x, lengths, d_y, w_attn, b_attn, ln_par, w_up, b_up, w_down, b_down):
        tables = rotary_tables()
        xs, q, k, v, probs, ctx, mid, act, slope, c, w_qkv, w_o, w_up, w_down = forward(
            lengths, x, tables, (w_attn, b_attn, ln_par, w_up, b_up, w_down, b_down))
        grad, attn, up, down, small = backward(d_y, xs, q, k, v, probs, ctx, mid, act, slope, c, tables, w_qkv, w_o, w_up, w_down)
        me = lax.axis_index(AXIS)
        small = small.reshape(TWO, SIXTEEN, DIM)
        mine = lax.dynamic_slice(small, (ZERO, ZERO, FOUR * me), (TWO, SIXTEEN, FOUR))
        b_up_grad = lax.dynamic_slice(small[:, B_UP:B_DOWN].reshape(TWO, FFN), (ZERO, SIXTEEN * me), (TWO, SIXTEEN))
        return grad, attn, mine[:, :FOUR], mine[:, FOUR:EIGHT], up, b_up_grad, down, mine[:, 12]

    return jax.shard_map(device_step, mesh=mesh,
                         in_specs=(batch_spec, batch_spec, batch_spec) + weight_specs,
                         out_specs=(batch_spec,) + weight_specs,
                         check_vma=False)
```

```python
import math
import functools
import jax
import jax.numpy as jnp
from jax import lax
from jax.experimental import pallas as pl
from jax.experimental.pallas import tpu as pltpu
from jax.sharding import PartitionSpec as P

ZERO, ONE, TWO, THREE, FOUR = range(5)
EIGHT, SIXTEEN, WIDTH = 8, 16, 256

F32, BF16 = jnp.float32, jnp.bfloat16
SEQS, TOK, DIM, FFN, HEADS, HEAD, LANES = FOUR, 512, 512, 2048, EIGHT, 64, 128
HALF = HEAD // TWO
EPS = 1e-5
THETA = 10000.0
NEG_BIG = -1e30
B_ATTN, LN_PAR, B_UP, B_DOWN = ZERO, FOUR, EIGHT, 12


def nn(a, b):
    return lax.dot_general(a, b, (((ONE,), (ZERO,)), ((), ())), preferred_element_type=F32)


def nt(a, b):
    return lax.dot_general(a, b, (((ONE,), (ONE,)), ((), ())), preferred_element_type=F32)


def tn(a, b):
    return lax.dot_general(a, b, (((ZERO,), (ZERO,)), ((), ())), preferred_element_type=F32)


def lane_tiles(width=TOK, size=LANES):
    return [slice(i, i + size) for i in range(ZERO, width, size)]


def row_chunks(rows=DIM, size=64):
    return [slice(i, i + size) for i in range(ZERO, rows, size)]


def column(c_ref, rows, lane):
    return jnp.broadcast_to(c_ref[rows, lane:lane + ONE], (rows.stop - rows.start, TOK))


def total(value):
    return jnp.sum(value, axis=ZERO, keepdims=True)


def norm_stats(x_ref):
    mean = functools.reduce(jnp.add, [total(x_ref[rows, :].astype(F32)) for rows in row_chunks()]) * (1.0 / DIM)
    squares = []
    for rows in row_chunks():
        centred = x_ref[rows, :].astype(F32) - mean
        squares.append(total(centred * centred))
    return mean, lax.rsqrt(functools.reduce(jnp.add, squares) * (1.0 / DIM) + EPS)


def norm_to(x_ref, stats, c_ref, lane, h_ref):
    mean, rstd = stats
    for rows in row_chunks():
        xhat = (x_ref[rows, :].astype(F32) - mean) * rstd
        h_ref[rows, :] = (xhat * column(c_ref, rows, lane) + column(c_ref, rows, lane + ONE)).astype(BF16)


def put_stats(ref, stats):
    ref[ZERO:ONE, :], ref[ONE:TWO, :] = stats


def get_stats(ref):
    return ref[ZERO:ONE, :], ref[ONE:TWO, :]


def woven(products, rest):
    done = ZERO
    for n, step in enumerate(rest):
        while done < len(products) and done * len(rest) <= n * len(products):
            products[done]()
            done += ONE
        step()
    for product in products[done:]:
        product()


def fold(value):
    parts = [value[:, cols] for cols in lane_tiles(value.shape[ONE])]
    return functools.reduce(jnp.add, parts)


def seq_spec(shape):
    return pl.BlockSpec((ONE, *shape), lambda s: (s,) + (ZERO,) * len(shape))


def once(shape):
    return pl.BlockSpec(shape, lambda s: (ZERO,) * len(shape), pipeline_mode=pl.Buffered(ONE))


def act_shape(rows, dtype):
    return jax.ShapeDtypeStruct((SEQS, rows, TOK), dtype)


PARAMS = pltpu.CompilerParams(vmem_limit_bytes=60 << 20, dimension_semantics=("arbitrary",))
SQUARE, TALL, WIDE, COLS = (DIM, TOK), (FFN, TOK), (DIM, FFN), (DIM, LANES)


def rotary_tables():
    inv_freq = 1.0 / (THETA ** (jnp.arange(HALF, dtype=F32) * (2.0 / HEAD)))
    angles = inv_freq[:, None] * jnp.arange(TOK, dtype=F32)[None, :]
    return jnp.cos(angles), jnp.sin(angles)


MESH = pl.DeviceIdType.MESH
AXIS = "fsdp"
ORDERS = ((TWO, ONE, ZERO), (ONE, ZERO, TWO), (ZERO, TWO, ONE))


class Place:
    def __init__(self):
        me = lax.axis_index(AXIS)
        self.core = lax.rem(me, TWO)
        self.pos = (me // 32, lax.rem(me // EIGHT, FOUR), lax.rem(me // TWO, FOUR))
        self.partner = me + ONE - TWO * self.core

    def coord(self, dim, delta):
        return lax.rem(self.pos[dim] + (delta + FOUR), FOUR)

    def device(self, offsets):
        pos = [self.coord(dim, offsets.get(dim, ZERO)) for dim in range(THREE)]
        return pos[ZERO] * 32 + pos[ONE] * EIGHT + pos[TWO] * TWO + self.core

    def greet(self):
        barrier = pltpu.get_barrier_semaphore()

        @pl.loop(ONE, 64)
        def _(i):
            offsets = {ZERO: i // SIXTEEN, ONE: lax.rem(i // FOUR, FOUR), TWO: lax.rem(i, FOUR)}

            @pl.when(offsets[ZERO] * offsets[ONE] * offsets[TWO] == ZERO)
            def _():
                pl.semaphore_signal(barrier, inc=ONE, device_id=(self.device(offsets),), device_id_type=MESH)
        pl.semaphore_signal(barrier, inc=ONE, device_id=(self.partner,), device_id_type=MESH)

    def met(self):
        pl.semaphore_wait(pltpu.get_barrier_semaphore(), 37)


def remote(src, dst, send_sem, recv_sem, device):
    return pltpu.make_async_remote_copy(src_ref=src, dst_ref=dst, send_sem=send_sem, recv_sem=recv_sem,
                                        device_id=(device,), device_id_type=MESH)


LINE = (ONE, -ONE, TWO)


def plane_offsets(order, k, sign=ONE):
    return {order[ONE]: sign * (k // FOUR), order[TWO]: sign * lax.rem(k, FOUR)}


class Gather:
    def __init__(self, place, buf, order, send, recv):
        self.place, self.buf, self.order, self.send, self.recv = place, buf, order, send, recv

    def block(self, offsets, whole=()):
        index = [slice(ZERO, FOUR) if dim in whole else pl.ds(self.place.coord(dim, offsets.get(dim, ZERO)), ONE) for dim in range(THREE)]
        return self.buf.at[index[ZERO], index[ONE], index[TWO], pl.ds(self.place.core, ONE)]

    def copy(self, ref, key, device):
        return remote(ref, ref, self.send.at[key], self.recv.at[key], device)

    def plane_start(self):
        @pl.loop(ONE, SIXTEEN)
        def _(k):
            self.copy(self.block({}), k, self.place.device(plane_offsets(self.order, k))).start()

    def plane_wait(self):
        @pl.loop(ONE, SIXTEEN)
        def _(k):
            self.copy(self.block(plane_offsets(self.order, k, -ONE)), k, self.place.partner).wait_recv()

    def line(self, i, sign):
        offsets = {self.order[ZERO]: sign * LINE[i]}
        return self.block(offsets, self.order[ONE:])

    def line_start(self):
        for i, delta in enumerate(LINE):
            self.copy(self.line(i, ZERO), SIXTEEN + i, self.place.device({self.order[ZERO]: delta})).start()

    def line_wait(self):
        for i in range(THREE):
            self.copy(self.line(i, -ONE), SIXTEEN + i, self.place.partner).wait_recv()

    def share(self, core):
        return self.copy(self.buf.at[:, :, :, pl.ds(core, ONE)], 19, self.place.partner)

    def share_start(self):
        self.share(self.place.core).start()

    def end(self):
        self.share(ONE - self.place.core).wait_recv()

        @pl.loop(ONE, SIXTEEN)
        def _(k):
            self.copy(self.block({}), k, self.place.partner).wait_send()
        for i in range(THREE):
            self.copy(self.line(i, ZERO), SIXTEEN + i, self.place.partner).wait_send()
        self.share(self.place.core).wait_send()


def gather_steps(gathers):
    def each(*names):
        def step():
            for name in names:
                for g in gathers:
                    getattr(g, name)()
        return step

    return [each("plane_start"), each("plane_wait", "line_start"), each("line_wait", "share_start"), each("end")]


class Scatter:
    def __init__(self, place, grads, acc, got_a, got_b, got_p, other, order, send, recv):
        self.place, self.grads, self.acc, self.order = place, grads, acc, order
        self.got_a, self.got_b, self.got_p, self.other, self.send, self.recv = got_a, got_b, got_p, other, send, recv
        self.units = acc.shape[ZERO]

    def columns(self, core):
        return pl.ds(pl.multiple_of(core * WIDTH, WIDTH), WIDTH)

    def swap_copy(self, u):
        place = self.place
        return remote(self.grads(u).at[:, :, :, :, self.columns(ONE - place.core)], self.acc.at[u], self.send.at[20 + u], self.recv.at[20 + u], place.partner)

    def swap(self):
        for u in range(self.units):
            self.swap_copy(u).start()

    def swapped(self):
        for u in range(self.units):
            self.swap_copy(u).wait()
            grad, acc = self.grads(u), self.acc

            @pl.loop(ZERO, FOUR)
            def _(z):
                acc[u, z] = acc[u, z] + grad[z, :, :, :, self.columns(self.place.core)]

    def part(self, delta, half=None):
        index = [slice(ZERO, FOUR)] * THREE
        index[self.order[ZERO]] = pl.ds(self.place.coord(self.order[ZERO], delta), ONE)
        return self.acc.at[:, index[ZERO], index[ONE], index[TWO], :, slice(ZERO, WIDTH) if half is None else lane_tiles()[half]]

    def ring(self, step, way):
        delta = (ONE, -ONE)[way]
        device = self.place.device({self.order[ZERO]: delta})
        if step == ZERO:
            src, dst = self.part(TWO, way), self.got_a.at[:, :, :, :, :, lane_tiles()[way]]
        else:
            src, dst = self.part(delta), self.got_b.at[way]
        key = SIXTEEN + TWO * step + way
        return remote(src, dst, self.send.at[key], self.recv.at[key], device)

    def ring_start(self):
        for way in range(TWO):
            self.ring(ZERO, way).start()

    def ring_turn(self):
        for way in range(TWO):
            self.ring(ZERO, way).wait_recv()
            self.add((ONE, -ONE)[way], way, self.got_a)
            self.ring(ONE, way).start()

    def add(self, delta, half, *refs):
        dim, acc = self.order[ZERO], self.acc
        at = self.place.coord(dim, delta)
        columns = slice(ZERO, WIDTH) if half is None else lane_tiles()[half]

        @pl.loop(ZERO, FOUR)
        def _(i):
            index = [i if d == self.order[ONE] else slice(ZERO, FOUR) for d in range(THREE)]
            there = [slice(None), *index, slice(None), columns]
            here = list(there)
            here[ONE + dim] = pl.ds(at, ONE)
            there[ONE + dim] = slice(ZERO, ONE)
            value = acc[tuple(here)]
            for ref in refs:
                value = value + ref[tuple(there)]
            acc[tuple(here)] = value

    def plane_copy(self, k):
        offsets = plane_offsets(self.order, k)
        index = [pl.ds(self.place.coord(dim, offsets.get(dim, ZERO)), ONE) for dim in range(THREE)]
        src = self.acc.at[:, index[ZERO], index[ONE], index[TWO]]
        return remote(src, self.got_p.at[k], self.send.at[k], self.recv.at[k], self.place.device(offsets))

    def plane_start(self):
        for way in range(TWO):
            self.ring(ONE, way).wait_recv()
        self.add(ZERO, None, self.got_b.at[ZERO], self.got_b.at[ONE])

        @pl.loop(ONE, SIXTEEN)
        def _(k):
            self.plane_copy(k).start()

    def own(self):
        z, y, x = [pl.ds(p, ONE) for p in self.place.pos]
        return self.acc.at[:, z, y, x]

    def last_copy(self):
        return remote(self.own(), self.other, self.send.at[23], self.recv.at[23], self.place.partner)

    def last(self):
        @pl.loop(ONE, SIXTEEN)
        def _(k):
            self.plane_copy(k).wait_recv()
        own = self.own()
        own[...] = functools.reduce(jnp.add, [self.got_p[k] for k in range(ONE, SIXTEEN)], own[...])
        self.last_copy().start()

    def finish(self, store):
        self.last_copy().wait_recv()
        first = self.place.core == ZERO
        for u in range(self.units):
            own, came = self.own()[u, ZERO, ZERO, ZERO], self.other[u, ZERO, ZERO, ZERO]
            store(u, jnp.concatenate([jnp.where(first, own, came), jnp.where(first, came, own)], axis=ONE))
        for step in range(TWO):
            for way in range(TWO):
                self.ring(step, way).wait_send()

        @pl.loop(ONE, SIXTEEN)
        def _(k):
            self.plane_copy(k).wait_send()
        self.last_copy().wait_send()


def landing_shapes(order, units):
    size = [FOUR, FOUR, FOUR]
    size[order[ZERO]] = ONE
    return (units, *size, EIGHT, WIDTH), (TWO, units, *size, EIGHT, WIDTH), (SIXTEEN, units, ONE, ONE, ONE, EIGHT, WIDTH), (units, ONE, ONE, ONE, EIGHT, WIDTH)


class Small:
    def __init__(self, place, value, slots, send, recv):
        self.place, self.value, self.slots, self.send, self.recv = place, value, slots, send, recv

    def copies(self, stage):
        if stage == THREE:
            return [remote(self.value, self.slots.at[9], self.send.at[9], self.recv.at[9], self.place.partner)]
        return [remote(self.value, self.slots.at[stage * THREE + k], self.send.at[stage * THREE + k], self.recv.at[stage * THREE + k],
                       self.place.device({stage: delta})) for k, delta in enumerate((ONE, -ONE, TWO))]

    def start(self, stage):
        for copy in self.copies(stage):
            copy.start()

    def finish(self, stage):
        copies = self.copies(stage)
        for copy in copies:
            copy.wait()
        value = self.value[...]
        for k in range(len(copies)):
            value = value + self.slots[stage * THREE + k]
        self.value[...] = value

    def steps(self):
        def turn(stage):
            def step():
                self.finish(stage)
                self.start(stage + ONE)
            return step

        return [lambda: self.start(ZERO), turn(ZERO), turn(ONE), turn(TWO), lambda: self.finish(THREE)]


VMEM = pl.BlockSpec(memory_space=pltpu.VMEM)
HBM = pl.BlockSpec(memory_space=pl.ANY)
DMA = pltpu.SemaphoreType.DMA


COLOURS = ((THREE, FOUR, 5), (6, 7, EIGHT), (9, 10, 11))
GRID = (FOUR, FOUR, FOUR)


def spread(buf, u, out_ref, column_base):
    @pl.loop(ZERO, EIGHT)
    def _(block):
        for part in range(FOUR):
            g = block * FOUR + part
            tiles = [buf[block // TWO, lax.rem(block, TWO) * TWO + part // TWO, part % TWO * TWO + k // TWO, k % TWO, u].astype(F32) for k in range(FOUR)]
            rows = pl.ds(pl.multiple_of(g * SIXTEEN, SIXTEEN), SIXTEEN)
            for j, cols in enumerate(lane_tiles()):
                value = jnp.concatenate([t[FOUR * j:FOUR * j + FOUR] for t in tiles], axis=ZERO).astype(BF16)
                out_ref[rows, column_base + cols.start:column_base + cols.stop] = value


def spread_down(buf, u, out_ref, cols):
    @pl.loop(ZERO, SIXTEEN)
    def _(i):
        for k in range(EIGHT):
            d = i * EIGHT + k
            out_ref[pl.ds(pl.multiple_of(d * SIXTEEN, SIXTEEN), SIXTEEN), cols] = buf[i // FOUR, lax.rem(i, FOUR), k // TWO, k % TWO, u]


def same(shape, test):
    row = lax.broadcasted_iota(jnp.int32, shape, ZERO)
    col = lax.broadcasted_iota(jnp.int32, shape, ONE)
    return jnp.where(test(row, col), 1.0, 0.0)


def small_columns(small_ref, c_ref):
    rows = [small_ref[z, y, x, c, ZERO] for z in range(FOUR) for y in range(FOUR) for x in range(FOUR) for c in range(TWO)]
    table = jnp.concatenate(rows, axis=ZERO).astype(BF16)
    quads = nn(same((DIM, LANES), lambda r, c: r // FOUR == c).astype(BF16), table)
    quads = (quads * same((DIM, LANES), lambda r, c: r % FOUR == c % FOUR)).astype(BF16)
    mask = same((DIM, LANES), lambda r, c: r % SIXTEEN == c % SIXTEEN)
    pick = same((DIM, 32), lambda r, c: r // SIXTEEN == c).astype(BF16)
    ups = [(nn(pick, table[32 * k:32 * k + 32]) * mask).astype(BF16) for k in range(FOUR)]
    for layer in range(TWO):
        def is_up(r):
            return r // SIXTEEN == layer * FOUR + TWO

        value = nn(quads, same((LANES, LANES), lambda r, c: (r // 64 == layer) & (r % 64 // FOUR == c) & ~is_up(r)).astype(BF16))
        for k in range(FOUR):
            value = value + nn(ups[k], same((LANES, LANES), lambda r, c: is_up(r) & (c == B_UP + k)).astype(BF16))
        c_ref[layer] = value


def tile_of(rows):
    rows = rows.astype(F32)
    return jnp.concatenate([rows[:, cols] for cols in lane_tiles()], axis=ZERO).astype(BF16)


def small_row(b_attn, ln_par, b_up, b_down):
    lane = lax.broadcasted_iota(jnp.int32, (ONE, LANES), ONE)
    row = jnp.zeros((ONE, LANES), F32)
    pieces = []
    for l in range(TWO):
        for m in range(FOUR):
            pieces += [(b_attn[l, m:m + ONE, :], 64 * l + FOUR * m), (ln_par[l, m:m + ONE, :], 64 * l + FOUR * m + SIXTEEN)]
        pieces += [(b_up[l:l + ONE, :], 64 * l + 32), (b_down[l:l + ONE, :], 64 * l + 48)]
    for piece, at in pieces:
        n = piece.shape[ONE]
        wide = jnp.concatenate([piece.astype(F32), jnp.zeros((ONE, LANES - n), F32)], axis=ONE)
        wide = pltpu.roll(wide, at, ONE) if at else wide
        row = jnp.where((lane >= at) & (lane < at + n), wide, row)
    return row


def hooks(slot, plan):
    def hook(at):
        for slots, run in plan:
            mine = [when for when in slots if when % FOUR == at]
            if mine:
                pl.when(functools.reduce(jnp.logical_or, [slot + at == when for when in mine]))(run)
    return hook


def forward_kernel(len_ref, x_ref, cos_ref, sin_ref, w_attn, b_attn, ln_par, w_up, b_up, w_down, b_down,
                   xs_out, q_ref, k_ref, v_ref, p_hbm, ctx_ref, mid_ref, act_ref, slope_ref, st1_ref, st2_ref, c_ref,
                   nat_qkv, nat_wo, nat_up, nat_down,
                   xs, ctxb, wqkv, wo, up, down, n_qkv, n_wo, n_up, n_down, p_buf, h_ref, s_a, s_b, s_c,
                   sbuf, q0, q1, q2, m0, m1, m2, send, recv, p_sem, nat_sem):
    step = pl.program_id(ZERO)
    phase, seq, layer = step // FOUR, lax.rem(step, FOUR), step // EIGHT
    place = Place()
    z, y, x = place.pos
    qkv_bufs, mo_bufs = (q0, q1, q2), (m0, m1, m2)

    def group(bufs, base, l):
        return [Gather(place, b.at[l], ORDERS[k], send.at[base + k, l], recv.at[base + k, l]) for k, b in enumerate(bufs)]

    little = Gather(place, sbuf, ORDERS[ZERO], send.at[6, ZERO], recv.at[6, ZERO])

    def nat_copies(which, l):
        if which == ZERO:
            return [pltpu.make_async_copy(n_qkv, nat_qkv.at[l], nat_sem.at[ZERO])]
        return [pltpu.make_async_copy(src, dst.at[l], nat_sem.at[ONE + i]) for i, (src, dst) in enumerate(((n_wo, nat_wo), (n_up, nat_up), (n_down, nat_down)))]

    def wait(copies):
        for copy in copies:
            copy.wait()

    def start(copies):
        for copy in copies:
            copy.start()

    def take_qkv():
        pl.when(step > ZERO)(lambda: wait(nat_copies(ZERO, layer)))
        for m in range(THREE):
            spread(qkv_bufs[m].at[layer], ZERO, n_qkv.at[m], ZERO)
            wqkv[m] = n_qkv[m].T
        start(nat_copies(ZERO, layer))

    def take_mo():
        pl.when(step > EIGHT)(lambda: wait(nat_copies(ONE, layer)))
        for colour in range(THREE):
            for u, unit in enumerate(COLOURS[colour]):
                buf = mo_bufs[colour].at[layer]
                if unit == THREE:
                    spread(buf, u, n_wo, ZERO)
                    wo[...] = n_wo[...].T
                elif unit < EIGHT:
                    part = slice(DIM * (unit - FOUR), DIM * (unit - THREE))
                    spread(buf, u, n_up, part.start)
                    up[part, :] = n_up[:, part].T
                else:
                    spread_down(buf, u, n_down, lane_tiles()[unit - EIGHT])
        for k in range(FOUR):
            part = slice(DIM * k, DIM * k + DIM)
            down[:, part] = n_down[part, :].T
        start(nat_copies(ONE, layer))

    @pl.when(step == ZERO)
    def _():
        place.greet()
        for l in range(TWO):
            for unit in range(12):
                if unit < FOUR:
                    tile = tile_of(w_attn[l, unit])
                elif unit < EIGHT:
                    tile = tile_of(w_up[l, :, DIM * (unit - FOUR):DIM * (unit - THREE)])
                else:
                    tile = w_down[l, :, lane_tiles()[unit - EIGHT]]
                if unit < THREE:
                    qkv_bufs[unit][l, z, y, x, place.core, ZERO] = tile
                else:
                    mo_bufs[(unit - THREE) // THREE][l, z, y, x, place.core, (unit - THREE) % THREE] = tile
        sbuf[z, y, x, place.core, ZERO] = small_row(b_attn, ln_par, b_up, b_down)
        place.met()
        for run in gather_steps(group(qkv_bufs, ZERO, ZERO) + [little]):
            run()
        small_columns(sbuf, c_ref)

    attn_hook = hooks(step * FOUR, [((when, when + 32), run) for when, run in zip(MO_SLOTS, gather_steps(group(mo_bufs, THREE, layer)))])
    mlp_hook = hooks(step * FOUR, [((when,), run) for when, run in zip(QKV_SLOTS, gather_steps(group(qkv_bufs, ZERO, ONE)))])

    @pl.when(phase % TWO == ZERO)
    def _():
        pl.when(seq == ZERO)(take_qkv)

        @pl.when(step < FOUR)
        def _():
            xs[seq] = x_ref[ZERO].T
            xs_out[ZERO, ZERO] = xs[seq]

        attn_hook(ZERO)
        copies = [pltpu.make_async_copy(p_buf.at[head], p_hbm.at[layer, seq, head], p_sem.at[head]) for head in range(HEADS)]
        attn_forward(len_ref[seq], xs.at[seq], wqkv, c_ref.at[layer], cos_ref, sin_ref, q_ref.at[ZERO, ZERO], k_ref.at[ZERO, ZERO],
                     v_ref.at[ZERO, ZERO], p_buf, ctx_ref.at[ZERO, ZERO], ctxb.at[seq], st1_ref.at[ZERO, ZERO], h_ref, s_a, s_b, s_c, attn_hook,
                     lambda heads: pl.when(step > ZERO)(lambda: wait(copies[heads])), lambda heads: start(copies[heads]))
        pl.when(step == 11)(lambda: wait(copies))
        attn_hook(THREE)

    @pl.when(phase % TWO == ONE)
    def _():
        pl.when(seq == ZERO)(take_mo)
        mlp_hook(ZERO)
        mlp_forward(layer, ctxb.at[seq], xs.at[seq], wo, up, down, c_ref.at[layer], mid_ref.at[ZERO, ZERO], act_ref.at[ZERO, ZERO], slope_ref.at[ZERO, ZERO],
                    st2_ref.at[ZERO, ZERO], h_ref, s_a, s_b, mlp_hook)

        @pl.when(layer == ZERO)
        def _():
            xs_out[ZERO, ZERO] = xs[seq]
        mlp_hook(THREE)

    @pl.when(step == 15)
    def _():
        for which in range(TWO):
            wait(nat_copies(which, ONE))


def attn_forward(length, xt, w, c_ref, cos_ref, sin_ref, q_ref, k_ref, v_ref, p_buf, ctx_ref, ctxb, stat_ref, h_ref, s_a, s_b, s_c, hook, free, ship):
    stats = norm_stats(xt)
    put_stats(stat_ref, stats)
    norm_to(xt, stats, c_ref, LN_PAR, h_ref)
    for m, acc in enumerate((s_a, s_b, s_c)):
        acc[...] = nn(w[m], h_ref[...])
    cos, sin = cos_ref[...], sin_ref[...]
    for m, (acc, out) in enumerate(((s_a, q_ref), (s_b, k_ref), (s_c, v_ref))):
        for head in range(HEADS):
            rows, one, two = head_rows(head)
            if m == TWO:
                out[rows, :] = (acc[rows, :] + column(c_ref, rows, B_ATTN + m)).astype(BF16)
                continue
            a, b = [acc[half, :] + column(c_ref, half, B_ATTN + m) for half in (one, two)]
            if m == ZERO:
                a, b = a * HEAD ** -0.5, b * HEAD ** -0.5
            out[one, :] = (a * cos - b * sin).astype(BF16)
            out[two, :] = (b * cos + a * sin).astype(BF16)
    hook(ONE)
    halves = slice(ZERO, FOUR), slice(FOUR, EIGHT)
    free(halves[ZERO])
    key = lax.broadcasted_iota(jnp.int32, (SIXTEEN, TOK), ONE)
    row = lax.broadcasted_iota(jnp.int32, (SIXTEEN, TOK), ZERO)
    bias_rows = jnp.where((row == ZERO) & (key >= length), NEG_BIG, 0.0).astype(BF16)
    one_rows = jnp.where(row == ZERO, 1.0, 0.0).astype(BF16)
    scores = (s_a, s_b)

    def open_head(head):
        rows = head_rows(head)[ZERO]
        keys = jnp.concatenate([k_ref[rows, :], bias_rows], axis=ZERO)
        queries = jnp.concatenate([q_ref[rows, :], one_rows], axis=ZERO)
        scores[head % TWO][...] = tn(keys, queries)

    def weigh(head):
        value, tops, sums = scores[head % TWO], [], []

        def top(rows):
            tops.append(jnp.max(value[rows, :], axis=ZERO, keepdims=True))
            if rows.stop == TOK:
                tops[:] = [functools.reduce(jnp.maximum, tops)]

        def power(rows):
            weight = jnp.exp(value[rows, :] - tops[ZERO])
            value[rows, :] = weight
            sums.append(total(weight))
            if rows.stop == TOK:
                sums[:] = [1.0 / functools.reduce(jnp.add, sums)]

        def share(rows):
            p_buf[head, rows, :] = (value[rows, :] * sums[ZERO]).astype(BF16)

        return [functools.partial(run, rows) for run in (top, power, share) for rows in row_chunks()]

    def close_head(head):
        rows = head_rows(head)[ZERO]
        ctx = nn(v_ref[rows, :], p_buf[head])
        ctx_ref[rows, :] = ctx
        ctxb[rows, :] = ctx.astype(BF16)

    open_head(ZERO)
    for head in range(HEADS):
        products = [functools.partial(open_head, head + ONE)] if head + ONE < HEADS else []
        if head:
            products.append(functools.partial(close_head, head - ONE))
        woven(products, weigh(head))
        if head == THREE:
            ship(halves[ZERO])
            hook(TWO)
            free(halves[ONE])
    ship(halves[ONE])
    close_head(HEADS - ONE)


def mlp_forward(layer, ctxb, xt, wo, up, down, c_ref, mid_ref, act_ref, slope_ref, stat_ref, h_ref, s_a, s_b, hook):
    s_a[...] = nn(wo[...], ctxb[...])
    for rows in row_chunks():
        mid_ref[rows, :] = (xt[rows, :].astype(F32) + s_a[rows, :] + column(c_ref, rows, B_ATTN + THREE)).astype(BF16)
    stats = norm_stats(mid_ref)
    put_stats(stat_ref, stats)
    norm_to(mid_ref, stats, c_ref, LN_PAR + TWO, h_ref)
    hook(ONE)
    pre = (s_a, s_b)
    parts = [slice(DIM * k, DIM * k + DIM) for k in range(FOUR)]

    def open_part(k):
        pre[k % TWO][...] = nn(up[parts[k], :], h_ref[...])

    open_part(ZERO)
    for k, part in enumerate(parts):
        if k < THREE:
            open_part(k + ONE)
        for rows in row_chunks():
            value = pre[k % TWO][rows, :] + column(c_ref, rows, B_UP + k)
            scaled = value * math.sqrt(0.5)
            cdf = 0.5 + 0.5 * lax.erf(scaled)
            density = jnp.exp2(scaled * scaled * -math.log2(math.e) - 0.5 * math.log2(2.0 * math.pi))
            there = slice(part.start + rows.start, part.start + rows.stop)
            act_ref[there, :] = (value * cdf).astype(BF16)
            slope_ref[there, :] = cdf + value * density
        if k == ONE:
            hook(TWO)

    @pl.when(layer == ZERO)
    def _():
        s_a[...] = nn(down[...], act_ref[...])
        for rows in row_chunks():
            xt[rows, :] = (mid_ref[rows, :].astype(F32) + s_a[rows, :] + column(c_ref, rows, B_DOWN)).astype(BF16)


MO_SLOTS = (ZERO, 5, 13, 15)
QKV_SLOTS = (SIXTEEN, 22, 26, 28)


def forward(lengths, x, tables, params):
    def saved(index, rows, dtype):
        return jax.ShapeDtypeStruct((TWO, SEQS, rows, TOK), dtype), pl.BlockSpec((ONE, ONE, rows, TOK), index)

    def attn_at(s):
        return s // EIGHT, jnp.where(s // FOUR % TWO == ZERO, s % FOUR, THREE), ZERO, ZERO

    def mlp_at(s):
        odd = s // FOUR % TWO == ONE
        return jnp.where(s < 12, ZERO, ONE), jnp.where(odd, s % FOUR, jnp.where(s < FOUR, ZERO, THREE)), ZERO, ZERO

    def xs_at(s):
        return jnp.where(s < FOUR, ZERO, ONE), jnp.where(s < EIGHT, s % FOUR, THREE), ZERO, ZERO

    outs = [saved(xs_at, DIM, BF16)] + [saved(attn_at, DIM, BF16)] * THREE
    outs += [(jax.ShapeDtypeStruct((TWO, SEQS, HEADS, TOK, TOK), BF16), HBM), saved(attn_at, DIM, F32)]
    outs += [saved(mlp_at, DIM, BF16), saved(mlp_at, FFN, BF16), saved(mlp_at, FFN, F32), saved(attn_at, EIGHT, F32), saved(mlp_at, EIGHT, F32)]
    outs += [(jax.ShapeDtypeStruct((TWO, *COLS), F32), once((TWO, *COLS)))]
    weights = ((THREE, DIM, DIM), (DIM, DIM), (DIM, FFN), (FFN, DIM))
    outs += [(jax.ShapeDtypeStruct((TWO, *w), BF16), HBM) for w in weights]
    scratch = [(SEQS, *SQUARE), (SEQS, *SQUARE), weights[ZERO], weights[ONE], weights[THREE], weights[TWO], *weights, (HEADS, TOK, TOK), SQUARE]
    scratch = [pltpu.VMEM(s, BF16) for s in scratch] + [pltpu.VMEM(SQUARE, F32)] * THREE + [pltpu.VMEM((*GRID, TWO, ONE, ONE, LANES), F32)]
    scratch += [pltpu.VMEM((TWO, *GRID, TWO, n, SIXTEEN, LANES), BF16) for n in (ONE, THREE) for _ in range(THREE)]
    scratch += [DMA((7, TWO, 20)), DMA((7, TWO, 20)), DMA((HEADS,)), DMA((FOUR,))]
    return pl.pallas_call(
        forward_kernel, grid=(SIXTEEN,),
        out_shape=[o[ZERO] for o in outs], out_specs=[o[ONE] for o in outs],
        in_specs=[pl.BlockSpec(memory_space=pltpu.SMEM), pl.BlockSpec((ONE, *SQUARE), lambda s: (jnp.minimum(s, THREE), ZERO, ZERO)),
                  once((HALF, TOK)), once((HALF, TOK))] + [once(p.shape) for p in params],
        scratch_shapes=scratch,
        compiler_params=pltpu.CompilerParams(collective_id=ZERO, has_side_effects=True, vmem_limit_bytes=67043328,
                                             dimension_semantics=("arbitrary",)),
        name="forward")(lengths, x, *tables, *params)


def norm_back(dh_ref, x_ref, stats, c_ref, lane, sums, at, write, beside):
    mean, rstd = stats
    means = [0.0, 0.0]

    def both(rows):
        dh = dh_ref[rows, :]
        return dh, dh * column(c_ref, rows, lane), (x_ref[rows, :].astype(F32) - mean) * rstd

    def first(rows):
        dh, dxhat, xhat = both(rows)
        means[ZERO], means[ONE] = means[ZERO] + total(dxhat), means[ONE] + total(dxhat * xhat)
        sums[at, rows, :] += fold(dh * xhat)
        sums[at + ONE, rows, :] += fold(dh)

    def second(rows):
        dh, dxhat, xhat = both(rows)
        write(rows, rstd * (dxhat - means[ZERO] * (1.0 / DIM) - xhat * (means[ONE] * (1.0 / DIM))))

    woven(beside, [functools.partial(run, rows) for run in (first, second) for rows in row_chunks()])


def columns_of(pairs):
    lane = lax.broadcasted_iota(jnp.int32, COLS, ONE)
    value = jnp.zeros(COLS, F32)
    for at, partial in pairs:
        value = jnp.where(lane == at, jnp.sum(partial, axis=ONE, keepdims=True), value)
    return value


def head_rows(head):
    return slice(HEAD * head, HEAD * head + HEAD), slice(HEAD * head, HEAD * head + HALF), slice(HEAD * head + HALF, HEAD * head + HEAD)


class Reduce:
    def __init__(self, place, units, grads, buffers, send, recv):
        self.units = units
        self.scatters = [Scatter(place, (lambda u, k=k: grads(units[k][u])), *buffers[k], ORDERS[k], send.at[k], recv.at[k]) for k in range(THREE)]

    def steps(self, store):
        def each(*names):
            def step():
                for name in names:
                    for s in self.scatters:
                        getattr(s, name)()
            return step

        def finish():
            for units, s in zip(self.units, self.scatters):
                s.finish(lambda u, full, units=units: store(units[u], full))

        return [each("swap"), each("swapped", "ring_start"), each("ring_turn"), each("plane_start"), each("last"), finish]


def backward_kernel(dy_ref, mid_ref, ctx_ref, st2_ref, q_ref, k_ref, v_ref, x_ref, st1_ref, cos_ref, sin_ref, c_ref, p_hbm, slope_hbm, act_hbm,
                    qkv_hbm, wo_hbm, up_hbm, down_hbm,
                    dx_ref, attn_out, up_out, down_out, small_out, *refs):
    (grad, dctx, delta, big, wqkv, wo, slope, act, dpre, h_ref, s_a, s_b, d_a, d_b, sums,
     g_qkv, g_wo, g_up, g_down, rows_ref, slots_ref), refs = refs[:21], refs[21:]
    qkv_bufs, mo_bufs, refs = [refs[5 * k:5 * k + 5] for k in range(THREE)], [refs[5 * k + 15:5 * k + 20] for k in range(THREE)], refs[30:]
    send, recv, ssend, srecv, big_sem, w_sem, mlp_sem = refs
    step = pl.program_id(ZERO)
    phase, seq = step // FOUR, lax.rem(step, FOUR)
    layer = ONE - step // EIGHT
    place = Place()

    def grads(unit):
        if unit < THREE:
            return g_qkv.at[unit]
        if unit == THREE:
            return g_wo
        if unit < EIGHT:
            return g_up.at[unit - FOUR]
        return g_down.at[:, :, :, unit - EIGHT]

    live = step < SIXTEEN
    turn = jnp.where(live, ZERO, ONE)
    qkv_sums = Reduce(place, ((ZERO,), (ONE,), (TWO,)), grads, [(a, ra, rb, rp.at[turn], o) for a, ra, rb, rp, o in qkv_bufs], send.at[turn], recv.at[turn])
    mo_sums = Reduce(place, COLOURS, grads, mo_bufs, send.at[TWO], recv.at[TWO])
    tiny = Small(place, rows_ref, slots_ref, ssend, srecv)
    first_core = place.core == ZERO

    def store(l):
        def put(unit, full):
            if unit < EIGHT:
                mine = jnp.where(first_core, full[:FOUR], full[FOUR:])
                if unit < FOUR:
                    attn_out[l, unit] = mine
                else:
                    up_out[l, :, DIM * (unit - FOUR):DIM * (unit - THREE)] = mine
            else:
                at = EIGHT * (unit % TWO)

                @pl.when(place.core == (unit - EIGHT) // TWO)
                def _():
                    down_out[l, at:at + EIGHT] = full
        return put

    def mlp_weights(l):
        parts = [pl.ds(DIM * k, DIM) for k in range(FOUR)]
        return ([pltpu.make_async_copy(down_hbm.at[l, part], big.at[k], big_sem.at[k]) for k, part in enumerate(parts)],
                [pltpu.make_async_copy(up_hbm.at[l, :, part], big.at[FOUR + k], big_sem.at[FOUR + k]) for k, part in enumerate(parts)] +
                [pltpu.make_async_copy(wo_hbm.at[l], wo, w_sem.at[ZERO])])

    def attn_weights(l):
        return [pltpu.make_async_copy(qkv_hbm.at[l], wqkv, w_sem.at[ONE])]

    def probs(l, s):
        return [pltpu.make_async_copy(p_hbm.at[l, s, k], big.at[k], big_sem.at[k]) for k in range(HEADS)]

    def saved_mlp(l, s):
        return [pltpu.make_async_copy(slope_hbm.at[l, s], slope, mlp_sem.at[ZERO]), pltpu.make_async_copy(act_hbm.at[l, s], act, mlp_sem.at[ONE])]

    def start(copies):
        for copy in copies:
            copy.start()

    def wait(copies):
        for copy in copies:
            copy.wait()

    @pl.when(step == ZERO)
    def _():
        place.greet()
        start(mlp_weights(ONE)[ZERO] + saved_mlp(ONE, ZERO) + mlp_weights(ONE)[ONE] + attn_weights(ONE))

    pl.when(step == ONE)(place.met)
    mo_steps, qkv_steps = mo_sums.steps(store(layer)), qkv_sums.steps(store(ONE - turn))
    late_steps = mo_sums.steps(store(ONE - turn))[FOUR:]
    attn_hook = hooks(step * FOUR, [((when, when + 32), run) for when, run in zip((SIXTEEN, 20, 24, 30), mo_steps)])
    mlp_plan = list(zip(((37, 69), (38, 70)), late_steps))
    mlp_plan += list(zip(((32, 64), (33, 65), (38, 66), (43, 67), (47, 71), (47, 71)), qkv_steps))
    mlp_plan += [((when,), run) for when, run in zip((64, 65, 66, 67, 71), tiny.steps())]
    mlp_hook = hooks(step * FOUR, mlp_plan)

    @pl.when(phase % TWO == ZERO)
    def _():
        @pl.when((seq == ZERO) & live)
        def _():
            for ref in (g_wo, g_up, g_down, sums):
                ref[...] = jnp.zeros_like(ref)

        @pl.when(step < FOUR)
        def _():
            grad[seq] = dy_ref[ZERO].T

        @pl.when((seq == ZERO) & live)
        def _():
            wait(mlp_weights(layer)[ZERO])

        mlp_hook(ZERO)

        def after_first():
            pl.when(seq < THREE)(lambda: start(saved_mlp(layer, seq + ONE)))
            pl.when(seq == THREE)(lambda: start(probs(layer, ZERO)[:FOUR]))

        def before_second():
            pl.when(seq == ZERO)(lambda: wait(mlp_weights(layer)[ONE]))

        def after_second():
            pl.when(seq == THREE)(lambda: start(probs(layer, ZERO)[FOUR:]))

        pl.when(live)(lambda: wait(saved_mlp(layer, seq)))
        mlp_backward(grad.at[seq], slope, act, mid_ref, ctx_ref, st2_ref.at[ZERO], wo, big, c_ref, dctx.at[seq], delta.at[seq], g_wo, g_up, g_down,
                     dpre, h_ref, s_a, s_b, sums, pl.when(live), mlp_hook,
                     after_first, after_second, before_second)

        @pl.when((seq == THREE) & live)
        def _():
            value = columns_of([(B_UP + i, sums[i]) for i in range(FOUR)] + [
                (LN_PAR + TWO, sums[FOUR]), (LN_PAR + THREE, sums[5]), (B_DOWN, sums[6]), (B_ATTN + THREE, sums[7])])
            rows_ref[pl.ds(pl.multiple_of(layer * SIXTEEN, SIXTEEN), SIXTEEN), :] = value.T[:SIXTEEN]

        mlp_hook(THREE)

    @pl.when(phase % TWO == ONE)
    def _():
        @pl.when(seq == ZERO)
        def _():
            wait(attn_weights(layer))
            for ref in (g_qkv, sums):
                ref[...] = jnp.zeros_like(ref)

        @pl.when(step == FOUR)
        def _():
            start(saved_mlp(ZERO, ZERO))
        attn_hook(ZERO)

        def after_heads():
            pl.when(seq < THREE)(lambda: start(probs(layer, seq + ONE)))
            pl.when(step == 7)(lambda: start(mlp_weights(ZERO)[ZERO] + mlp_weights(ZERO)[ONE]))

        wait(probs(layer, seq))
        attn_backward(dctx.at[seq], delta.at[seq], big, q_ref, k_ref, v_ref, x_ref, st1_ref.at[ZERO], grad.at[seq], wqkv, c_ref, cos_ref, sin_ref,
                      g_qkv, dpre, h_ref, s_a, s_b, d_a, d_b, sums, attn_hook,
                      after_heads)

        @pl.when(seq == THREE)
        def _():
            value = columns_of([(B_ATTN + i, sums[i]) for i in range(THREE)] + [(LN_PAR, sums[THREE]), (LN_PAR + ONE, sums[FOUR])])
            rows = pl.ds(pl.multiple_of(layer * SIXTEEN, SIXTEEN), SIXTEEN)
            rows_ref[rows, :] = rows_ref[rows, :] + value.T[:SIXTEEN]

        @pl.when(step == 7)
        def _():
            start(attn_weights(ZERO))

        @pl.when(step > 11)
        def _():
            dx_ref[ZERO] = grad[seq].T
        attn_hook(THREE)

    @pl.when(step == 17)
    def _():
        small_out[...] = rows_ref[...]


def add_to(ref, value):
    ref[...] = ref[...] + value.reshape(ref.shape)


def mlp_backward(grad, slope, act, mid_ref, ctx_ref, stat_ref, wo, big, c_ref, dctx, delta, g_wo, g_up, g_down, dpre, h_ref, s_a, s_b, sums, when, hook, after_first, after_second, before_second):
    parts = [slice(DIM * k, DIM * k + DIM) for k in range(FOUR)]
    pre = (s_a, s_b)

    def dact(k):
        pre[k % TWO][...] = nn(big[k], grad[...])

    @when
    def _():
        def scale(k, chunk):
            there = slice(parts[k].start + chunk.start, parts[k].start + chunk.stop)
            value = pre[k % TWO][chunk, :] * slope[there, :]
            sums[k, chunk, :] += fold(value)
            dpre[there, :] = value.astype(BF16)

        def down_product(k):
            add_to(g_down.at[k], nt(act[parts[k], :], grad[...]))

        dact(ZERO)
        norm_to(mid_ref.at[ZERO], get_stats(stat_ref), c_ref, LN_PAR + TWO, h_ref)
        for k in range(FOUR):
            products = [functools.partial(down_product, k)]
            if k < THREE:
                products = [functools.partial(dact, k + ONE)] + products
            woven(products, [functools.partial(scale, k, chunk) for chunk in row_chunks()])
        after_first()
    hook(ONE)

    @when
    def _():
        before_second()
        s_a[...] = functools.reduce(jnp.add, [nn(big[FOUR + k], dpre[rows, :]) for k, rows in enumerate(parts)])
        after_second()
    hook(TWO)

    @when
    def _():
        def write(rows, dx):
            dy = grad[rows, :].astype(F32)
            dmid = (dy + dx).astype(BF16)
            grad[rows, :] = dmid
            sums[6, rows, :] += fold(dy)
            sums[7, rows, :] += fold(dmid.astype(F32))

        norm_back(s_a, mid_ref.at[ZERO], get_stats(stat_ref), c_ref, LN_PAR + TWO, sums, FOUR, write,
                  [lambda k=k, rows=rows: add_to(g_up.at[k], nt(h_ref[...], dpre[rows, :])) for k, rows in enumerate(parts)])
        add_to(g_wo, nt(ctx_ref[ZERO].astype(BF16), grad[...]))
        s_b[...] = nn(wo[...], grad[...])
        for head in range(HEADS):
            rows = head_rows(head)[ZERO]
            value = s_b[rows, :].astype(BF16)
            dctx[rows, :] = value
            delta[head:head + ONE, :] = total(value.astype(F32) * ctx_ref[ZERO, rows, :])


def attn_backward(dctx, delta, probs, q_ref, k_ref, v_ref, x_ref, stat_ref, grad, wqkv, c_ref, cos_ref, sin_ref, g_qkv, dproj, h_ref, s_a, s_b, d_a, d_b,
                  sums, hook, prefetch):
    scores, dscores = (s_a, s_b), (d_a, d_b)
    q, k, v = q_ref.at[ZERO], k_ref.at[ZERO], v_ref.at[ZERO]

    def open_head(head):
        rows = head_rows(head)[ZERO]
        scores[head % TWO][...] = tn(v[rows, :], dctx[rows, :])

    def weigh(head, rows):
        dscores[head % TWO][rows, :] = (probs[head, rows, :].astype(F32) * (scores[head % TWO][rows, :] - delta[head:head + ONE, :])).astype(BF16)

    def values(head):
        rows = head_rows(head)[ZERO]
        dv = nt(dctx[rows, :], probs[head])
        sums[TWO, rows, :] += fold(dv)
        dproj[TWO * DIM + rows.start:TWO * DIM + rows.stop, :] = dv.astype(BF16)

    def close_head(head, m):
        rows, one, two = head_rows(head)
        ds = dscores[head % TWO][...]
        value = nn(k[rows, :], ds) * HEAD ** -0.5 if m == ZERO else nt(q[rows, :], ds)
        cos, sin = cos_ref[...], sin_ref[...]
        a, b = value[:HALF], value[HALF:]
        for at, out in ((one, a * cos + b * sin), (two, b * cos - a * sin)):
            dproj[m * DIM + at.start:m * DIM + at.stop, :] = out.astype(BF16)
            sums[m, at, :] += fold(out)

    open_head(ZERO)
    for head in range(HEADS):
        products = [functools.partial(values, head)]
        if head:
            products = [functools.partial(close_head, head - ONE, m) for m in range(TWO)] + products
        if head + ONE < HEADS:
            products = [functools.partial(open_head, head + ONE)] + products
        woven(products, [functools.partial(weigh, head, rows) for rows in row_chunks()])
        if head == THREE:
            hook(ONE)
    for m in range(TWO):
        close_head(HEADS - ONE, m)
    prefetch()
    hook(TWO)
    norm_to(x_ref.at[ZERO], get_stats(stat_ref), c_ref, LN_PAR, h_ref)
    parts = [slice(DIM * m, DIM * m + DIM) for m in range(THREE)]
    s_a[...] = functools.reduce(jnp.add, [nn(wqkv[m], dproj[rows, :]) for m, rows in enumerate(parts)])

    def write(rows, dx):
        grad[rows, :] = (grad[rows, :].astype(F32) + dx).astype(BF16)

    norm_back(s_a, x_ref.at[ZERO], get_stats(stat_ref), c_ref, LN_PAR, sums, THREE, write,
              [lambda m=m, rows=rows: add_to(g_qkv.at[m], nt(h_ref[...], dproj[rows, :])) for m, rows in enumerate(parts)])


def backward(dy, xs, q, k, v, probs, ctx, mid, act, slope, st1, st2, c, tables, w_qkv, w_o, w_up, w_down):
    def mlp_at(s):
        s = jnp.minimum(s, 15)
        odd = s // FOUR % TWO == ONE
        return ONE - s // EIGHT, jnp.where(odd, THREE, s % FOUR), ZERO, ZERO

    def attn_at(s):
        s = jnp.minimum(s, 15)
        odd = s // FOUR % TWO == ONE
        return jnp.where(s < EIGHT, ONE, ZERO) + jnp.where((s > 7) & (s < 12), ONE, ZERO), jnp.where(odd, s % FOUR, jnp.where(s < FOUR, ZERO, THREE)), ZERO, ZERO

    per_mlp = pl.BlockSpec((None, ONE, *SQUARE), mlp_at)
    per_attn = pl.BlockSpec((None, ONE, *SQUARE), attn_at)

    def stat(at):
        return pl.BlockSpec((None, ONE, EIGHT, TOK), at)

    acc = [(*GRID, EIGHT, WIDTH)]
    scratch = [pltpu.VMEM((SEQS, *SQUARE), BF16), pltpu.VMEM((SEQS, *SQUARE), BF16), pltpu.VMEM((SEQS, HEADS, TOK), F32),
               pltpu.VMEM((HEADS, TOK, TOK), BF16), pltpu.VMEM((THREE, DIM, DIM), BF16), pltpu.VMEM((DIM, DIM), BF16),
               pltpu.VMEM(TALL, F32), pltpu.VMEM(TALL, BF16), pltpu.VMEM(TALL, BF16), pltpu.VMEM(SQUARE, BF16),
               pltpu.VMEM(SQUARE, F32), pltpu.VMEM(SQUARE, F32), pltpu.VMEM((TOK, TOK), BF16), pltpu.VMEM((TOK, TOK), BF16),
               pltpu.VMEM((EIGHT, *COLS), F32), pltpu.VMEM((THREE, *GRID, EIGHT, DIM), F32), pltpu.VMEM((*GRID, EIGHT, DIM), F32),
               pltpu.VMEM((FOUR, *GRID, EIGHT, DIM), F32), pltpu.VMEM((*GRID, FOUR, EIGHT, DIM), F32), pltpu.VMEM((32, DIM), F32), pltpu.VMEM((10, 32, DIM), F32)]
    for n in (ONE, THREE):
        for order in ORDERS:
            ring_a, ring_b, plane, other = landing_shapes(order, n)
            plane = (TWO, *plane) if n == ONE else plane
            scratch += [pltpu.VMEM(s, F32) for s in ((n, *GRID, EIGHT, WIDTH), ring_a, ring_b, plane, other)]
    scratch += [DMA((THREE, THREE, 24)), DMA((THREE, THREE, 24)), DMA((10,)), DMA((10,)), DMA((EIGHT,)), DMA((TWO,)), DMA((TWO,))]
    outs = ((TWO, FOUR, FOUR, DIM), (TWO, FOUR, FFN), (TWO, SIXTEEN, DIM), (32, DIM))
    whole = [pl.BlockSpec(s, lambda i, n=len(s): (ZERO,) * n, pipeline_mode=pl.Buffered(ONE)) for s in outs]
    dx_at = lambda s: (jnp.clip(s - 12, ZERO, THREE), ZERO, ZERO)
    return pl.pallas_call(
        backward_kernel, grid=(18,),
        out_shape=[jax.ShapeDtypeStruct((SEQS, TOK, DIM), BF16)] + [jax.ShapeDtypeStruct(s, F32) for s in outs],
        out_specs=[pl.BlockSpec((ONE, TOK, DIM), dx_at)] + whole,
        in_specs=[pl.BlockSpec((ONE, TOK, DIM), lambda s: (jnp.minimum(s, THREE), ZERO, ZERO)), per_mlp, per_mlp, stat(mlp_at)] + [per_attn] * FOUR + [stat(attn_at),
                  once((HALF, TOK)), once((HALF, TOK)), pl.BlockSpec((None, *COLS), lambda s: (ONE - jnp.minimum(s, 15) // EIGHT, ZERO, ZERO))] + [HBM] * 7,
        scratch_shapes=scratch,
        compiler_params=pltpu.CompilerParams(collective_id=ONE, has_side_effects=True, vmem_limit_bytes=67043328,
                                             dimension_semantics=("arbitrary",)),
        name="backward")(dy, mid, ctx, st2, q, k, v, xs, st1, *tables, c, probs, slope, act, w_qkv, w_o, w_up, w_down)


def solution(mesh):
    batch_spec = P(AXIS)
    weight_specs = (P(None, None, AXIS, None), P(None, None, AXIS), P(None, None, AXIS),
                    P(None, AXIS, None), P(None, AXIS), P(None, AXIS, None), P(None, AXIS))

    def device_step(x, lengths, d_y, w_attn, b_attn, ln_par, w_up, b_up, w_down, b_down):
        tables = rotary_tables()
        xs, q, k, v, probs, ctx, mid, act, slope, st1, st2, c, w_qkv, w_o, w_up, w_down = forward(
            lengths, x, tables, (w_attn, b_attn, ln_par, w_up, b_up, w_down, b_down))
        grad, attn, up, down, small = backward(d_y, xs, q, k, v, probs, ctx, mid, act, slope, st1, st2, c, tables, w_qkv, w_o, w_up, w_down)
        me = lax.axis_index(AXIS)
        small = small.reshape(TWO, SIXTEEN, DIM)
        mine = lax.dynamic_slice(small, (ZERO, ZERO, FOUR * me), (TWO, SIXTEEN, FOUR))
        b_up_grad = lax.dynamic_slice(small[:, B_UP:B_DOWN].reshape(TWO, FFN), (ZERO, SIXTEEN * me), (TWO, SIXTEEN))
        return grad, attn, mine[:, :FOUR], mine[:, FOUR:EIGHT], up, b_up_grad, down, mine[:, 12]

    return jax.shard_map(device_step, mesh=mesh,
                         in_specs=(batch_spec, batch_spec, batch_spec) + weight_specs,
                         out_specs=(batch_spec,) + weight_specs,
                         check_vma=False)
```

```python
import math
import functools
import jax
import jax.numpy as jnp
from jax import lax
from jax.experimental import pallas as pl
from jax.experimental.pallas import tpu as pltpu
from jax.sharding import PartitionSpec as P

ZERO, ONE, TWO, THREE, FOUR = range(5)
EIGHT, SIXTEEN, WIDTH = 8, 16, 256

F32, BF16 = jnp.float32, jnp.bfloat16
SEQS, TOK, DIM, FFN, HEADS, HEAD, LANES = FOUR, 512, 512, 2048, EIGHT, 64, 128
HALF = HEAD // TWO
EPS = 1e-5
THETA = 10000.0
NEG_BIG = -1e30
B_ATTN, LN_PAR, B_UP, B_DOWN = ZERO, FOUR, EIGHT, 12


def nn(a, b):
    return lax.dot_general(a, b, (((ONE,), (ZERO,)), ((), ())), preferred_element_type=F32)


def nt(a, b):
    return lax.dot_general(a, b, (((ONE,), (ONE,)), ((), ())), preferred_element_type=F32)


def tn(a, b):
    return lax.dot_general(a, b, (((ZERO,), (ZERO,)), ((), ())), preferred_element_type=F32)


def lane_tiles(width=TOK, size=LANES):
    return [slice(i, i + size) for i in range(ZERO, width, size)]


def row_chunks(rows=DIM, size=64):
    return [slice(i, i + size) for i in range(ZERO, rows, size)]


def column(c_ref, rows, lane):
    return jnp.broadcast_to(c_ref[rows, lane:lane + ONE], (rows.stop - rows.start, TOK))


def total(value):
    return jnp.sum(value, axis=ZERO, keepdims=True)


def norm_stats(x_ref):
    mean = functools.reduce(jnp.add, [total(x_ref[rows, :].astype(F32)) for rows in row_chunks()]) * (1.0 / DIM)
    squares = []
    for rows in row_chunks():
        centred = x_ref[rows, :].astype(F32) - mean
        squares.append(total(centred * centred))
    return mean, lax.rsqrt(functools.reduce(jnp.add, squares) * (1.0 / DIM) + EPS)


def norm_to(x_ref, stats, c_ref, lane, h_ref):
    mean, rstd = stats
    for rows in row_chunks():
        xhat = (x_ref[rows, :].astype(F32) - mean) * rstd
        h_ref[rows, :] = (xhat * column(c_ref, rows, lane) + column(c_ref, rows, lane + ONE)).astype(BF16)


def put_stats(ref, stats):
    ref[ZERO:ONE, :], ref[ONE:TWO, :] = stats


def get_stats(ref):
    return ref[ZERO:ONE, :], ref[ONE:TWO, :]


def woven(products, rest):
    done = ZERO
    for n, step in enumerate(rest):
        while done < len(products) and done * len(rest) <= n * len(products):
            products[done]()
            done += ONE
        step()
    for product in products[done:]:
        product()


def fold(value):
    parts = [value[:, cols] for cols in lane_tiles(value.shape[ONE])]
    return functools.reduce(jnp.add, parts)


def seq_spec(shape):
    return pl.BlockSpec((ONE, *shape), lambda s: (s,) + (ZERO,) * len(shape))


def once(shape):
    return pl.BlockSpec(shape, lambda s: (ZERO,) * len(shape), pipeline_mode=pl.Buffered(ONE))


def act_shape(rows, dtype):
    return jax.ShapeDtypeStruct((SEQS, rows, TOK), dtype)


PARAMS = pltpu.CompilerParams(vmem_limit_bytes=60 << 20, dimension_semantics=("arbitrary",))
SQUARE, TALL, WIDE, COLS = (DIM, TOK), (FFN, TOK), (DIM, FFN), (DIM, LANES)


def rotary_tables():
    inv_freq = 1.0 / (THETA ** (jnp.arange(HALF, dtype=F32) * (2.0 / HEAD)))
    angles = inv_freq[:, None] * jnp.arange(TOK, dtype=F32)[None, :]
    return jnp.cos(angles), jnp.sin(angles)


MESH = pl.DeviceIdType.MESH
AXIS = "fsdp"
ORDERS = ((TWO, ONE, ZERO), (ONE, ZERO, TWO), (ZERO, TWO, ONE))


class Place:
    def __init__(self):
        me = lax.axis_index(AXIS)
        self.core = lax.rem(me, TWO)
        self.pos = (me // 32, lax.rem(me // EIGHT, FOUR), lax.rem(me // TWO, FOUR))
        self.partner = me + ONE - TWO * self.core

    def coord(self, dim, delta):
        return lax.rem(self.pos[dim] + (delta + FOUR), FOUR)

    def device(self, offsets):
        pos = [self.coord(dim, offsets.get(dim, ZERO)) for dim in range(THREE)]
        return pos[ZERO] * 32 + pos[ONE] * EIGHT + pos[TWO] * TWO + self.core

    def greet(self):
        barrier = pltpu.get_barrier_semaphore()

        @pl.loop(ONE, 64)
        def _(i):
            offsets = {ZERO: i // SIXTEEN, ONE: lax.rem(i // FOUR, FOUR), TWO: lax.rem(i, FOUR)}

            @pl.when(offsets[ZERO] * offsets[ONE] * offsets[TWO] == ZERO)
            def _():
                pl.semaphore_signal(barrier, inc=ONE, device_id=(self.device(offsets),), device_id_type=MESH)
        pl.semaphore_signal(barrier, inc=ONE, device_id=(self.partner,), device_id_type=MESH)

    def met(self):
        pl.semaphore_wait(pltpu.get_barrier_semaphore(), 37)


def remote(src, dst, send_sem, recv_sem, device):
    return pltpu.make_async_remote_copy(src_ref=src, dst_ref=dst, send_sem=send_sem, recv_sem=recv_sem,
                                        device_id=(device,), device_id_type=MESH)


LINE = (ONE, -ONE, TWO)


def plane_offsets(order, k, sign=ONE):
    return {order[ONE]: sign * (k // FOUR), order[TWO]: sign * lax.rem(k, FOUR)}


class Gather:
    def __init__(self, place, buf, order, send, recv):
        self.place, self.buf, self.order, self.send, self.recv = place, buf, order, send, recv

    def block(self, offsets, whole=()):
        index = [slice(ZERO, FOUR) if dim in whole else pl.ds(self.place.coord(dim, offsets.get(dim, ZERO)), ONE) for dim in range(THREE)]
        return self.buf.at[index[ZERO], index[ONE], index[TWO], pl.ds(self.place.core, ONE)]

    def copy(self, ref, key, device):
        return remote(ref, ref, self.send.at[key], self.recv.at[key], device)

    def plane_start(self):
        @pl.loop(ONE, SIXTEEN)
        def _(k):
            self.copy(self.block({}), k, self.place.device(plane_offsets(self.order, k))).start()

    def plane_wait(self):
        @pl.loop(ONE, SIXTEEN)
        def _(k):
            self.copy(self.block(plane_offsets(self.order, k, -ONE)), k, self.place.partner).wait_recv()

    def line(self, i, sign):
        offsets = {self.order[ZERO]: sign * LINE[i]}
        return self.block(offsets, self.order[ONE:])

    def line_start(self):
        for i, delta in enumerate(LINE):
            self.copy(self.line(i, ZERO), SIXTEEN + i, self.place.device({self.order[ZERO]: delta})).start()

    def line_wait(self):
        for i in range(THREE):
            self.copy(self.line(i, -ONE), SIXTEEN + i, self.place.partner).wait_recv()

    def share(self, core):
        return self.copy(self.buf.at[:, :, :, pl.ds(core, ONE)], 19, self.place.partner)

    def share_start(self):
        self.share(self.place.core).start()

    def end(self):
        self.share(ONE - self.place.core).wait_recv()

        @pl.loop(ONE, SIXTEEN)
        def _(k):
            self.copy(self.block({}), k, self.place.partner).wait_send()
        for i in range(THREE):
            self.copy(self.line(i, ZERO), SIXTEEN + i, self.place.partner).wait_send()
        self.share(self.place.core).wait_send()


def gather_steps(gathers):
    def each(*names):
        def step():
            for name in names:
                for g in gathers:
                    getattr(g, name)()
        return step

    return [each("plane_start"), each("plane_wait", "line_start"), each("line_wait", "share_start"), each("end")]


class Scatter:
    def __init__(self, place, grads, acc, got_a, got_b, got_p, other, order, send, recv):
        self.place, self.grads, self.acc, self.order = place, grads, acc, order
        self.got_a, self.got_b, self.got_p, self.other, self.send, self.recv = got_a, got_b, got_p, other, send, recv
        self.units = acc.shape[ZERO]

    def columns(self, core):
        return pl.ds(pl.multiple_of(core * WIDTH, WIDTH), WIDTH)

    def swap_copy(self, u):
        place = self.place
        return remote(self.grads(u).at[:, :, :, :, self.columns(ONE - place.core)], self.acc.at[u], self.send.at[20 + u], self.recv.at[20 + u], place.partner)

    def swap(self):
        for u in range(self.units):
            self.swap_copy(u).start()

    def swapped(self):
        for u in range(self.units):
            self.swap_copy(u).wait()
            grad, acc = self.grads(u), self.acc

            @pl.loop(ZERO, FOUR)
            def _(z):
                acc[u, z] = acc[u, z] + grad[z, :, :, :, self.columns(self.place.core)]

    def part(self, delta, half=None):
        index = [slice(ZERO, FOUR)] * THREE
        index[self.order[ZERO]] = pl.ds(self.place.coord(self.order[ZERO], delta), ONE)
        return self.acc.at[:, index[ZERO], index[ONE], index[TWO], :, slice(ZERO, WIDTH) if half is None else lane_tiles()[half]]

    def ring(self, step, way):
        delta = (ONE, -ONE)[way]
        device = self.place.device({self.order[ZERO]: delta})
        if step == ZERO:
            src, dst = self.part(TWO, way), self.got_a.at[:, :, :, :, :, lane_tiles()[way]]
        else:
            src, dst = self.part(delta), self.got_b.at[way]
        key = SIXTEEN + TWO * step + way
        return remote(src, dst, self.send.at[key], self.recv.at[key], device)

    def ring_start(self):
        for way in range(TWO):
            self.ring(ZERO, way).start()

    def ring_turn(self):
        for way in range(TWO):
            self.ring(ZERO, way).wait_recv()
            self.add((ONE, -ONE)[way], way, self.got_a)
            self.ring(ONE, way).start()

    def add(self, delta, half, *refs):
        dim, acc = self.order[ZERO], self.acc
        at = self.place.coord(dim, delta)
        columns = slice(ZERO, WIDTH) if half is None else lane_tiles()[half]

        @pl.loop(ZERO, FOUR)
        def _(i):
            index = [i if d == self.order[ONE] else slice(ZERO, FOUR) for d in range(THREE)]
            there = [slice(None), *index, slice(None), columns]
            here = list(there)
            here[ONE + dim] = pl.ds(at, ONE)
            there[ONE + dim] = slice(ZERO, ONE)
            value = acc[tuple(here)]
            for ref in refs:
                value = value + ref[tuple(there)]
            acc[tuple(here)] = value

    def plane_copy(self, k):
        offsets = plane_offsets(self.order, k)
        index = [pl.ds(self.place.coord(dim, offsets.get(dim, ZERO)), ONE) for dim in range(THREE)]
        src = self.acc.at[:, index[ZERO], index[ONE], index[TWO]]
        return remote(src, self.got_p.at[k], self.send.at[k], self.recv.at[k], self.place.device(offsets))

    def plane_start(self):
        for way in range(TWO):
            self.ring(ONE, way).wait_recv()
        self.add(ZERO, None, self.got_b.at[ZERO], self.got_b.at[ONE])

        @pl.loop(ONE, SIXTEEN)
        def _(k):
            self.plane_copy(k).start()

    def own(self):
        z, y, x = [pl.ds(p, ONE) for p in self.place.pos]
        return self.acc.at[:, z, y, x]

    def last_copy(self):
        return remote(self.own(), self.other, self.send.at[23], self.recv.at[23], self.place.partner)

    def last(self):
        @pl.loop(ONE, SIXTEEN)
        def _(k):
            self.plane_copy(k).wait_recv()
        own = self.own()
        own[...] = functools.reduce(jnp.add, [self.got_p[k] for k in range(ONE, SIXTEEN)], own[...])
        self.last_copy().start()

    def finish(self, store):
        self.last_copy().wait_recv()
        first = self.place.core == ZERO
        for u in range(self.units):
            own, came = self.own()[u, ZERO, ZERO, ZERO], self.other[u, ZERO, ZERO, ZERO]
            store(u, jnp.concatenate([jnp.where(first, own, came), jnp.where(first, came, own)], axis=ONE))
        for step in range(TWO):
            for way in range(TWO):
                self.ring(step, way).wait_send()

        @pl.loop(ONE, SIXTEEN)
        def _(k):
            self.plane_copy(k).wait_send()
        self.last_copy().wait_send()


def landing_shapes(order, units):
    size = [FOUR, FOUR, FOUR]
    size[order[ZERO]] = ONE
    return (units, *size, EIGHT, WIDTH), (TWO, units, *size, EIGHT, WIDTH), (SIXTEEN, units, ONE, ONE, ONE, EIGHT, WIDTH), (units, ONE, ONE, ONE, EIGHT, WIDTH)


class Small:
    def __init__(self, place, value, slots, send, recv):
        self.place, self.value, self.slots, self.send, self.recv = place, value, slots, send, recv

    def peers(self, stage):
        if stage == THREE:
            return [self.place.partner]
        return [self.place.device({stage: delta}) for delta in LINE]

    def copies(self, stage):
        return [remote(self.value, self.slots.at[THREE * stage + k], self.send.at[THREE * stage + k], self.recv.at[THREE * stage + k], peer)
                for k, peer in enumerate(self.peers(stage))]

    def start(self, stage):
        for copy in self.copies(stage):
            copy.start()

    def finish(self, stage):
        copies = self.copies(stage)
        for copy in copies:
            copy.wait()
        self.value[...] = functools.reduce(jnp.add, [self.slots[THREE * stage + k] for k in range(len(copies))], self.value[...])

    def turn(self, stage):
        def step():
            self.finish(stage)
            self.start(stage + ONE)
        return step

    def steps(self):
        return [lambda: self.start(ZERO), self.turn(ZERO), self.turn(ONE), self.turn(TWO), lambda: self.finish(THREE)]


class Late(Small):
    def __init__(self, place, value, slots, send, recv, planes, plane_send, plane_recv):
        super().__init__(place, value, slots, send, recv)
        self.planes, self.plane_send, self.plane_recv = planes, plane_send, plane_recv

    def peers(self, stage):
        return super().peers({ZERO: ORDERS[ZERO][ZERO], ONE: THREE}[stage])

    def plane(self, k):
        return remote(self.value, self.planes.at[k], self.plane_send.at[k], self.plane_recv.at[k], self.place.device(plane_offsets(ORDERS[ZERO], k)))

    def steps(self):
        def first():
            @pl.loop(ONE, SIXTEEN)
            def _(k):
                self.plane(k).start()

        def second():
            @pl.loop(ONE, SIXTEEN)
            def _(k):
                self.plane(k).wait()
            self.value[...] = functools.reduce(jnp.add, [self.planes[k] for k in range(ONE, SIXTEEN)], self.value[...])
            self.start(ZERO)

        return [first, second, self.turn(ZERO), lambda: self.finish(ONE)]


VMEM = pl.BlockSpec(memory_space=pltpu.VMEM)
HBM = pl.BlockSpec(memory_space=pl.ANY)
DMA = pltpu.SemaphoreType.DMA


COLOURS = ((THREE, FOUR, 5), (6, 7, EIGHT), (9, 10, 11))
GRID = (FOUR, FOUR, FOUR)


def spread(buf, u, out_ref, column_base):
    @pl.loop(ZERO, EIGHT)
    def _(block):
        for part in range(FOUR):
            g = block * FOUR + part
            tiles = [buf[block // TWO, lax.rem(block, TWO) * TWO + part // TWO, part % TWO * TWO + k // TWO, k % TWO, u].astype(F32) for k in range(FOUR)]
            rows = pl.ds(pl.multiple_of(g * SIXTEEN, SIXTEEN), SIXTEEN)
            for j, cols in enumerate(lane_tiles()):
                value = jnp.concatenate([t[FOUR * j:FOUR * j + FOUR] for t in tiles], axis=ZERO).astype(BF16)
                out_ref[rows, column_base + cols.start:column_base + cols.stop] = value


def spread_down(buf, u, out_ref, cols):
    @pl.loop(ZERO, SIXTEEN)
    def _(i):
        for k in range(EIGHT):
            d = i * EIGHT + k
            out_ref[pl.ds(pl.multiple_of(d * SIXTEEN, SIXTEEN), SIXTEEN), cols] = buf[i // FOUR, lax.rem(i, FOUR), k // TWO, k % TWO, u]


def same(shape, test):
    row = lax.broadcasted_iota(jnp.int32, shape, ZERO)
    col = lax.broadcasted_iota(jnp.int32, shape, ONE)
    return jnp.where(test(row, col), 1.0, 0.0)


def small_columns(small_ref, c_ref):
    rows = [small_ref[z, y, x, c, ZERO] for z in range(FOUR) for y in range(FOUR) for x in range(FOUR) for c in range(TWO)]
    table = jnp.concatenate(rows, axis=ZERO).astype(BF16)
    quads = nn(same((DIM, LANES), lambda r, c: r // FOUR == c).astype(BF16), table)
    quads = (quads * same((DIM, LANES), lambda r, c: r % FOUR == c % FOUR)).astype(BF16)
    mask = same((DIM, LANES), lambda r, c: r % SIXTEEN == c % SIXTEEN)
    pick = same((DIM, 32), lambda r, c: r // SIXTEEN == c).astype(BF16)
    ups = [(nn(pick, table[32 * k:32 * k + 32]) * mask).astype(BF16) for k in range(FOUR)]
    for layer in range(TWO):
        def is_up(r):
            return r // SIXTEEN == layer * FOUR + TWO

        value = nn(quads, same((LANES, LANES), lambda r, c: (r // 64 == layer) & (r % 64 // FOUR == c) & ~is_up(r)).astype(BF16))
        for k in range(FOUR):
            value = value + nn(ups[k], same((LANES, LANES), lambda r, c: is_up(r) & (c == B_UP + k)).astype(BF16))
        c_ref[layer] = value


def tile_of(rows):
    rows = rows.astype(F32)
    return jnp.concatenate([rows[:, cols] for cols in lane_tiles()], axis=ZERO).astype(BF16)


def small_row(b_attn, ln_par, b_up, b_down):
    lane = lax.broadcasted_iota(jnp.int32, (ONE, LANES), ONE)
    row = jnp.zeros((ONE, LANES), F32)
    pieces = []
    for l in range(TWO):
        for m in range(FOUR):
            pieces += [(b_attn[l, m:m + ONE, :], 64 * l + FOUR * m), (ln_par[l, m:m + ONE, :], 64 * l + FOUR * m + SIXTEEN)]
        pieces += [(b_up[l:l + ONE, :], 64 * l + 32), (b_down[l:l + ONE, :], 64 * l + 48)]
    for piece, at in pieces:
        n = piece.shape[ONE]
        wide = jnp.concatenate([piece.astype(F32), jnp.zeros((ONE, LANES - n), F32)], axis=ONE)
        wide = pltpu.roll(wide, at, ONE) if at else wide
        row = jnp.where((lane >= at) & (lane < at + n), wide, row)
    return row


def hooks(slot, plan):
    def hook(at):
        for slots, run in plan:
            mine = [when for when in slots if when % FOUR == at]
            if mine:
                pl.when(functools.reduce(jnp.logical_or, [slot + at == when for when in mine]))(run)
    return hook


def forward_kernel(len_ref, x_hbm, cos_ref, sin_ref, w_attn, b_attn, ln_par, w_up, b_up, w_down, b_down,
                   xs_out, q_ref, k_ref, v_ref, p_hbm, ctx_ref, mid_ref, act_ref, slope_ref, st1_ref, st2_ref, c_ref,
                   nat_qkv, nat_wo, nat_up, nat_down,
                   xs, ctxb, wqkv, wo, up, down, n_qkv, n_wo, n_up, n_down, p_buf, h_ref, s_a, s_b, s_c,
                   sbuf, q0, q1, q2, m0, m1, m2, stats, send, recv, p_sem, nat_sem, x_sem):
    step = pl.program_id(ZERO)
    phase, seq, layer = step // FOUR, lax.rem(step, FOUR), step // EIGHT
    place = Place()
    z, y, x = place.pos
    qkv_bufs, mo_bufs = (q0, q1, q2), (m0, m1, m2)

    def group(bufs, base, l):
        return [Gather(place, b.at[l], ORDERS[k], send.at[base + k, l], recv.at[base + k, l]) for k, b in enumerate(bufs)]

    little = Gather(place, sbuf, ORDERS[ZERO], send.at[6, ZERO], recv.at[6, ZERO])

    def nat_copies(which, l):
        if which == ZERO:
            return [pltpu.make_async_copy(n_qkv, nat_qkv.at[l], nat_sem.at[ZERO])]
        return [pltpu.make_async_copy(src, dst.at[l], nat_sem.at[ONE + i]) for i, (src, dst) in enumerate(((n_wo, nat_wo), (n_up, nat_up), (n_down, nat_down)))]

    def wait(copies):
        for copy in copies:
            copy.wait()

    def start(copies):
        for copy in copies:
            copy.start()

    def take_qkv():
        pl.when(step > ZERO)(lambda: wait(nat_copies(ZERO, layer)))
        for m in range(THREE):
            spread(qkv_bufs[m].at[layer], ZERO, n_qkv.at[m], ZERO)
            wqkv[m] = n_qkv[m].T
        start(nat_copies(ZERO, layer))

    def take_mo():
        pl.when(step > EIGHT)(lambda: wait(nat_copies(ONE, layer)))
        for colour in range(THREE):
            for u, unit in enumerate(COLOURS[colour]):
                buf = mo_bufs[colour].at[layer]
                if unit == THREE:
                    spread(buf, u, n_wo, ZERO)
                    wo[...] = n_wo[...].T
                elif unit < EIGHT:
                    part = slice(DIM * (unit - FOUR), DIM * (unit - THREE))
                    spread(buf, u, n_up, part.start)
                    up[part, :] = n_up[:, part].T
                else:
                    spread_down(buf, u, n_down, lane_tiles()[unit - EIGHT])
        for k in range(FOUR):
            part = slice(DIM * k, DIM * k + DIM)
            down[:, part] = n_down[part, :].T
        start(nat_copies(ONE, layer))

    x_copies = [pltpu.make_async_copy(x_hbm.at[s], ctxb.at[s], x_sem.at[s]) for s in range(SEQS)]

    @pl.when(step == ZERO)
    def _():
        place.greet()
        start(x_copies)
        for l in range(TWO):
            for unit in range(12):
                if unit < FOUR:
                    tile = tile_of(w_attn[l, unit])
                elif unit < EIGHT:
                    tile = tile_of(w_up[l, :, DIM * (unit - FOUR):DIM * (unit - THREE)])
                else:
                    tile = w_down[l, :, lane_tiles()[unit - EIGHT]]
                if unit < THREE:
                    qkv_bufs[unit][l, z, y, x, place.core, ZERO] = tile
                else:
                    mo_bufs[(unit - THREE) // THREE][l, z, y, x, place.core, (unit - THREE) % THREE] = tile
        sbuf[z, y, x, place.core, ZERO] = small_row(b_attn, ln_par, b_up, b_down)
        first, second = gather_steps(group(qkv_bufs, ZERO, ZERO) + [little]), gather_steps(group(mo_bufs, THREE, ZERO))

        def ready(s):
            x_copies[s].wait()
            xs[s] = ctxb[s].T
            put_stats(stats.at[s], norm_stats(xs.at[s]))

        place.met()
        first[ZERO]()
        second[ZERO]()
        ready(ZERO)
        ready(ONE)
        first[ONE]()
        ready(TWO)
        ready(THREE)
        first[TWO]()
        second[ONE]()
        first[THREE]()
        small_columns(sbuf, c_ref)

    attn_hook = hooks(step * FOUR, [((when, when + 32), run) for when, run in zip((9, 13), gather_steps(group(mo_bufs, THREE, layer))[TWO:])])
    mlp_steps = gather_steps(group(qkv_bufs, ZERO, ONE)) + gather_steps(group(mo_bufs, THREE, ONE))[:TWO]
    mlp_hook = hooks(step * FOUR, [((when,), run) for when, run in zip((SIXTEEN, 25, 30, 31, 17, 26), mlp_steps)])

    @pl.when(phase % TWO == ZERO)
    def _():
        pl.when(seq == ZERO)(take_qkv)

        @pl.when(step < FOUR)
        def _():
            xs_out[ZERO, ZERO] = xs[seq]

        @pl.when(step > 7)
        def _():
            put_stats(stats.at[seq], norm_stats(xs.at[seq]))

        attn_hook(ZERO)
        copies = [pltpu.make_async_copy(p_buf.at[head], p_hbm.at[layer, seq, head], p_sem.at[head]) for head in range(HEADS)]
        attn_forward(len_ref[seq], xs.at[seq], wqkv, c_ref.at[layer], cos_ref, sin_ref, q_ref.at[ZERO, ZERO], k_ref.at[ZERO, ZERO],
                     v_ref.at[ZERO, ZERO], p_buf, ctx_ref.at[ZERO, ZERO], ctxb.at[seq], get_stats(stats.at[seq]), st1_ref.at[ZERO, ZERO], h_ref, s_a, s_b, s_c, attn_hook,
                     lambda heads: pl.when(step > ZERO)(lambda: wait(copies[heads])), lambda heads: start(copies[heads]))
        pl.when(step == 11)(lambda: wait(copies))
        attn_hook(THREE)

    @pl.when(phase % TWO == ONE)
    def _():
        pl.when(seq == ZERO)(take_mo)
        mlp_hook(ZERO)
        mlp_forward(layer, ctxb.at[seq], xs.at[seq], wo, up, down, c_ref.at[layer], mid_ref.at[ZERO, ZERO], act_ref.at[ZERO, ZERO], slope_ref.at[ZERO, ZERO],
                    st2_ref.at[ZERO, ZERO], h_ref, s_a, s_b, mlp_hook)

        @pl.when(layer == ZERO)
        def _():
            xs_out[ZERO, ZERO] = xs[seq]
        mlp_hook(THREE)

    @pl.when(step == 15)
    def _():
        for which in range(TWO):
            wait(nat_copies(which, ONE))


def attn_forward(length, xt, w, c_ref, cos_ref, sin_ref, q_ref, k_ref, v_ref, p_buf, ctx_ref, ctxb, stats, stat_ref, h_ref, s_a, s_b, s_c, hook, free, ship):
    put_stats(stat_ref, stats)
    norm_to(xt, stats, c_ref, LN_PAR, h_ref)
    for m, acc in enumerate((s_a, s_b, s_c)):
        acc[...] = nn(w[m], h_ref[...])
    cos, sin = cos_ref[...], sin_ref[...]
    for m, (acc, out) in enumerate(((s_a, q_ref), (s_b, k_ref), (s_c, v_ref))):
        for head in range(HEADS):
            rows, one, two = head_rows(head)
            if m == TWO:
                out[rows, :] = (acc[rows, :] + column(c_ref, rows, B_ATTN + m)).astype(BF16)
                continue
            a, b = [acc[half, :] + column(c_ref, half, B_ATTN + m) for half in (one, two)]
            if m == ZERO:
                a, b = a * HEAD ** -0.5, b * HEAD ** -0.5
            out[one, :] = (a * cos - b * sin).astype(BF16)
            out[two, :] = (b * cos + a * sin).astype(BF16)
    hook(ONE)
    halves = slice(ZERO, FOUR), slice(FOUR, EIGHT)
    free(halves[ZERO])
    key = lax.broadcasted_iota(jnp.int32, (SIXTEEN, TOK), ONE)
    row = lax.broadcasted_iota(jnp.int32, (SIXTEEN, TOK), ZERO)
    bias_rows = jnp.where((row == ZERO) & (key >= length), NEG_BIG, 0.0).astype(BF16)
    one_rows = jnp.where(row == ZERO, 1.0, 0.0).astype(BF16)
    scores = (s_a, s_b)

    def open_head(head):
        rows = head_rows(head)[ZERO]
        keys = jnp.concatenate([k_ref[rows, :], bias_rows], axis=ZERO)
        queries = jnp.concatenate([q_ref[rows, :], one_rows], axis=ZERO)
        scores[head % TWO][...] = tn(keys, queries)

    def weigh(head):
        value, tops, sums = scores[head % TWO], [], []

        def top(rows):
            tops.append(jnp.max(value[rows, :], axis=ZERO, keepdims=True))
            if rows.stop == TOK:
                tops[:] = [functools.reduce(jnp.maximum, tops)]

        def power(rows):
            weight = jnp.exp(value[rows, :] - tops[ZERO])
            value[rows, :] = weight
            sums.append(total(weight))
            if rows.stop == TOK:
                sums[:] = [1.0 / functools.reduce(jnp.add, sums)]

        def share(rows):
            p_buf[head, rows, :] = (value[rows, :] * sums[ZERO]).astype(BF16)

        return [functools.partial(run, rows) for run in (top, power, share) for rows in row_chunks()]

    def close_head(head):
        rows = head_rows(head)[ZERO]
        ctx = nn(v_ref[rows, :], p_buf[head])
        ctx_ref[rows, :] = ctx
        ctxb[rows, :] = ctx.astype(BF16)

    open_head(ZERO)
    for head in range(HEADS):
        products = [functools.partial(open_head, head + ONE)] if head + ONE < HEADS else []
        if head:
            products.append(functools.partial(close_head, head - ONE))
        woven(products, weigh(head))
        if head == THREE:
            ship(halves[ZERO])
            hook(TWO)
            free(halves[ONE])
    ship(halves[ONE])
    close_head(HEADS - ONE)


def mlp_forward(layer, ctxb, xt, wo, up, down, c_ref, mid_ref, act_ref, slope_ref, stat_ref, h_ref, s_a, s_b, hook):
    s_a[...] = nn(wo[...], ctxb[...])
    for rows in row_chunks():
        mid_ref[rows, :] = (xt[rows, :].astype(F32) + s_a[rows, :] + column(c_ref, rows, B_ATTN + THREE)).astype(BF16)
    stats = norm_stats(mid_ref)
    put_stats(stat_ref, stats)
    norm_to(mid_ref, stats, c_ref, LN_PAR + TWO, h_ref)
    hook(ONE)
    pre = (s_a, s_b)
    parts = [slice(DIM * k, DIM * k + DIM) for k in range(FOUR)]

    def open_part(k):
        pre[k % TWO][...] = nn(up[parts[k], :], h_ref[...])

    open_part(ZERO)
    for k, part in enumerate(parts):
        if k < THREE:
            open_part(k + ONE)
        for rows in row_chunks():
            value = pre[k % TWO][rows, :] + column(c_ref, rows, B_UP + k)
            scaled = value * math.sqrt(0.5)
            cdf = 0.5 + 0.5 * lax.erf(scaled)
            density = jnp.exp2(scaled * scaled * -math.log2(math.e) - 0.5 * math.log2(2.0 * math.pi))
            there = slice(part.start + rows.start, part.start + rows.stop)
            act_ref[there, :] = (value * cdf).astype(BF16)
            slope_ref[there, :] = cdf + value * density
        if k == ONE:
            hook(TWO)

    @pl.when(layer == ZERO)
    def _():
        s_a[...] = nn(down[...], act_ref[...])
        for rows in row_chunks():
            xt[rows, :] = (mid_ref[rows, :].astype(F32) + s_a[rows, :] + column(c_ref, rows, B_DOWN)).astype(BF16)


def forward(lengths, x, tables, params):
    def saved(index, rows, dtype):
        return jax.ShapeDtypeStruct((TWO, SEQS, rows, TOK), dtype), pl.BlockSpec((ONE, ONE, rows, TOK), index)

    def attn_at(s):
        return s // EIGHT, jnp.where(s // FOUR % TWO == ZERO, s % FOUR, THREE), ZERO, ZERO

    def mlp_at(s):
        odd = s // FOUR % TWO == ONE
        return jnp.where(s < 12, ZERO, ONE), jnp.where(odd, s % FOUR, jnp.where(s < FOUR, ZERO, THREE)), ZERO, ZERO

    def xs_at(s):
        return jnp.where(s < FOUR, ZERO, ONE), jnp.where(s < EIGHT, s % FOUR, THREE), ZERO, ZERO

    outs = [saved(xs_at, DIM, BF16)] + [saved(attn_at, DIM, BF16)] * THREE
    outs += [(jax.ShapeDtypeStruct((TWO, SEQS, HEADS, TOK, TOK), BF16), HBM), saved(attn_at, DIM, F32)]
    outs += [saved(mlp_at, DIM, BF16), saved(mlp_at, FFN, BF16), saved(mlp_at, FFN, F32), saved(attn_at, EIGHT, F32), saved(mlp_at, EIGHT, F32)]
    outs += [(jax.ShapeDtypeStruct((TWO, *COLS), F32), once((TWO, *COLS)))]
    weights = ((THREE, DIM, DIM), (DIM, DIM), (DIM, FFN), (FFN, DIM))
    outs += [(jax.ShapeDtypeStruct((TWO, *w), BF16), HBM) for w in weights]
    scratch = [(SEQS, *SQUARE), (SEQS, *SQUARE), weights[ZERO], weights[ONE], weights[THREE], weights[TWO], *weights, (HEADS, TOK, TOK), SQUARE]
    scratch = [pltpu.VMEM(s, BF16) for s in scratch] + [pltpu.VMEM(SQUARE, F32)] * THREE + [pltpu.VMEM((*GRID, TWO, ONE, ONE, LANES), F32)]
    scratch += [pltpu.VMEM((TWO, *GRID, TWO, n, SIXTEEN, LANES), BF16) for n in (ONE, THREE) for _ in range(THREE)]
    scratch += [pltpu.VMEM((SEQS, EIGHT, TOK), F32), DMA((7, TWO, 20)), DMA((7, TWO, 20)), DMA((HEADS,)), DMA((FOUR,)), DMA((SEQS,))]
    return pl.pallas_call(
        forward_kernel, grid=(SIXTEEN,),
        out_shape=[o[ZERO] for o in outs], out_specs=[o[ONE] for o in outs],
        in_specs=[pl.BlockSpec(memory_space=pltpu.SMEM), HBM, once((HALF, TOK)), once((HALF, TOK))] + [once(p.shape) for p in params],
        scratch_shapes=scratch,
        compiler_params=pltpu.CompilerParams(collective_id=ZERO, has_side_effects=True, vmem_limit_bytes=67043328,
                                             dimension_semantics=("arbitrary",)),
        name="forward")(lengths, x, *tables, *params)


def norm_back(dh_ref, x_ref, stats, c_ref, lane, sums, at, write, beside):
    mean, rstd = stats
    means = [0.0, 0.0]

    def both(rows):
        dh = dh_ref[rows, :]
        return dh, dh * column(c_ref, rows, lane), (x_ref[rows, :].astype(F32) - mean) * rstd

    def first(rows):
        dh, dxhat, xhat = both(rows)
        means[ZERO], means[ONE] = means[ZERO] + total(dxhat), means[ONE] + total(dxhat * xhat)
        sums[at, rows, :] += fold(dh * xhat)
        sums[at + ONE, rows, :] += fold(dh)

    def second(rows):
        dh, dxhat, xhat = both(rows)
        write(rows, rstd * (dxhat - means[ZERO] * (1.0 / DIM) - xhat * (means[ONE] * (1.0 / DIM))))

    woven(beside, [functools.partial(run, rows) for run in (first, second) for rows in row_chunks()])


def columns_of(partials):
    lane = lax.broadcasted_iota(jnp.int32, COLS, ONE)
    value = jnp.zeros(COLS, F32)
    for at, partial in enumerate(partials):
        value = jnp.where(lane == at, jnp.sum(partial, axis=ONE, keepdims=True), value)
    return value.T[:EIGHT]


def head_rows(head):
    return slice(HEAD * head, HEAD * head + HEAD), slice(HEAD * head, HEAD * head + HALF), slice(HEAD * head + HALF, HEAD * head + HEAD)


class Reduce:
    def __init__(self, place, units, grads, buffers, send, recv):
        self.units = units
        self.scatters = [Scatter(place, (lambda u, k=k: grads(units[k][u])), *buffers[k], ORDERS[k], send.at[k], recv.at[k]) for k in range(THREE)]

    def steps(self, store):
        def each(*names):
            def step():
                for name in names:
                    for s in self.scatters:
                        getattr(s, name)()
            return step

        def finish():
            for units, s in zip(self.units, self.scatters):
                s.finish(lambda u, full, units=units: store(units[u], full))

        return [each("swap"), each("swapped", "ring_start"), each("ring_turn"), each("plane_start"), each("last"), finish]


def backward_kernel(dy_ref, mid_ref, ctx_ref, st2_ref, q_ref, k_ref, v_ref, x_ref, st1_ref, cos_ref, sin_ref, c_ref, p_hbm, slope_hbm, act_hbm,
                    qkv_hbm, wo_hbm, up_hbm, down_hbm,
                    dx_ref, attn_out, up_out, down_out, small_out, *refs):
    (grad, dctx, delta, big, wqkv, wo, slope, act, dpre, h_ref, s_a, s_b, d_a, d_b, sums,
     g_qkv, g_wo, g_up, g_down, rows_ref, slots_ref, late_ref, late_slots, planes_ref), refs = refs[:24], refs[24:]
    qkv_bufs, mo_bufs, refs = [refs[5 * k:5 * k + 5] for k in range(THREE)], [refs[5 * k + 15:5 * k + 20] for k in range(THREE)], refs[30:]
    send, recv, small_sem, late_sem, plane_sem, big_sem, w_sem, mlp_sem = refs
    step = pl.program_id(ZERO)
    phase, seq = step // FOUR, lax.rem(step, FOUR)
    layer = ONE - step // EIGHT
    place = Place()

    def grads(unit):
        if unit < THREE:
            return g_qkv.at[unit]
        if unit == THREE:
            return g_wo
        if unit < EIGHT:
            return g_up.at[unit - FOUR]
        return g_down.at[:, :, :, unit - EIGHT]

    live = step < SIXTEEN
    turn = jnp.where(live, ZERO, ONE)
    qkv_sums = Reduce(place, ((ZERO,), (ONE,), (TWO,)), grads, [(a, ra, rb, rp.at[turn], o) for a, ra, rb, rp, o in qkv_bufs], send.at[turn], recv.at[turn])
    mo_sums = Reduce(place, COLOURS, grads, mo_bufs, send.at[TWO], recv.at[TWO])
    tiny = Small(place, rows_ref, slots_ref, small_sem.at[ZERO], small_sem.at[ONE])
    late = Late(place, late_ref, late_slots, late_sem.at[ZERO], late_sem.at[ONE], planes_ref, plane_sem.at[ZERO], plane_sem.at[ONE])
    first_core = place.core == ZERO

    def store(l):
        def put(unit, full):
            if unit < EIGHT:
                mine = jnp.where(first_core, full[:FOUR], full[FOUR:])
                if unit < FOUR:
                    attn_out[l, unit] = mine
                else:
                    up_out[l, :, DIM * (unit - FOUR):DIM * (unit - THREE)] = mine
            else:
                at = EIGHT * (unit % TWO)

                @pl.when(place.core == (unit - EIGHT) // TWO)
                def _():
                    down_out[l, at:at + EIGHT] = full
        return put

    def mlp_weights(l):
        parts = [pl.ds(DIM * k, DIM) for k in range(FOUR)]
        return ([pltpu.make_async_copy(down_hbm.at[l, part], big.at[k], big_sem.at[k]) for k, part in enumerate(parts)],
                [pltpu.make_async_copy(up_hbm.at[l, :, part], big.at[FOUR + k], big_sem.at[FOUR + k]) for k, part in enumerate(parts)] +
                [pltpu.make_async_copy(wo_hbm.at[l], wo, w_sem.at[ZERO])])

    def attn_weights(l):
        return [pltpu.make_async_copy(qkv_hbm.at[l], wqkv, w_sem.at[ONE])]

    def probs(l, s):
        return [pltpu.make_async_copy(p_hbm.at[l, s, k], big.at[k], big_sem.at[k]) for k in range(HEADS)]

    def saved_mlp(l, s):
        return [pltpu.make_async_copy(slope_hbm.at[l, s], slope, mlp_sem.at[ZERO]), pltpu.make_async_copy(act_hbm.at[l, s], act, mlp_sem.at[ONE])]

    def start(copies):
        for copy in copies:
            copy.start()

    def wait(copies):
        for copy in copies:
            copy.wait()

    @pl.when(step == ZERO)
    def _():
        place.greet()
        start(mlp_weights(ONE)[ZERO] + saved_mlp(ONE, ZERO) + mlp_weights(ONE)[ONE] + attn_weights(ONE))

    pl.when(step == ONE)(place.met)
    mo_steps, qkv_steps = mo_sums.steps(store(layer)), qkv_sums.steps(store(ONE - turn))
    late_steps = mo_sums.steps(store(ONE - turn))[FOUR:]
    attn_hook = hooks(step * FOUR, [((when, when + 32), run) for when, run in zip((SIXTEEN, 20, 24, 30), mo_steps)] + [((when,), run) for when, run in zip((48, 53, 57, 61, 63), tiny.steps())])
    mlp_plan = list(zip(((37, 69), (38, 70)), late_steps))
    mlp_plan += list(zip(((32, 64), (33, 65), (38, 66), (43, 67), (47, 71), (47, 71)), qkv_steps))
    mlp_plan += [((when,), run) for when, run in zip((64, 66, 67, 70), late.steps())]
    mlp_hook = hooks(step * FOUR, mlp_plan)

    @pl.when(phase % TWO == ZERO)
    def _():
        @pl.when((seq == ZERO) & live)
        def _():
            for ref in (g_wo, g_up, g_down, sums):
                ref[...] = jnp.zeros_like(ref)

        @pl.when(step < FOUR)
        def _():
            grad[seq] = dy_ref[ZERO].T

        @pl.when((seq == ZERO) & live)
        def _():
            wait(mlp_weights(layer)[ZERO])

        mlp_hook(ZERO)

        def after_first():
            pl.when(seq < THREE)(lambda: start(saved_mlp(layer, seq + ONE)))
            pl.when(seq == THREE)(lambda: start(probs(layer, ZERO)[:FOUR]))

        def before_second():
            pl.when(seq == ZERO)(lambda: wait(mlp_weights(layer)[ONE]))

        def after_second():
            pl.when(seq == THREE)(lambda: start(probs(layer, ZERO)[FOUR:]))

        pl.when(live)(lambda: wait(saved_mlp(layer, seq)))
        mlp_backward(grad.at[seq], slope, act, mid_ref, ctx_ref, st2_ref.at[ZERO], wo, big, c_ref, dctx.at[seq], delta.at[seq], g_wo, g_up, g_down,
                     dpre, h_ref, s_a, s_b, sums, pl.when(live), mlp_hook,
                     after_first, after_second, before_second)

        @pl.when((seq == THREE) & live)
        def _():
            rows_ref[pl.ds(pl.multiple_of(SIXTEEN - SIXTEEN * layer, EIGHT), EIGHT), :] = columns_of([sums[i] for i in range(EIGHT)])

        mlp_hook(THREE)

    @pl.when(phase % TWO == ONE)
    def _():
        @pl.when(seq == ZERO)
        def _():
            wait(attn_weights(layer))
            for ref in (g_qkv, sums):
                ref[...] = jnp.zeros_like(ref)

        @pl.when(step == FOUR)
        def _():
            start(saved_mlp(ZERO, ZERO))
        attn_hook(ZERO)

        def after_heads():
            pl.when(seq < THREE)(lambda: start(probs(layer, seq + ONE)))
            pl.when(step == 7)(lambda: start(mlp_weights(ZERO)[ZERO] + mlp_weights(ZERO)[ONE]))

        wait(probs(layer, seq))
        attn_backward(dctx.at[seq], delta.at[seq], big, q_ref, k_ref, v_ref, x_ref, st1_ref.at[ZERO], grad.at[seq], wqkv, c_ref, cos_ref, sin_ref,
                      g_qkv, dpre, h_ref, s_a, s_b, d_a, d_b, sums, attn_hook,
                      after_heads)

        @pl.when(seq == THREE)
        def _():
            late_ref[...] = columns_of([sums[i] for i in range(5)])

        @pl.when(step == 7)
        def _():
            rows_ref[EIGHT:SIXTEEN, :] = late_ref[...]

        @pl.when(step == 7)
        def _():
            start(attn_weights(ZERO))

        @pl.when(step > 11)
        def _():
            dx_ref[ZERO] = grad[seq].T
        attn_hook(THREE)

    @pl.when(step == 17)
    def _():
        small_out[:24, :], small_out[24:, :] = rows_ref[...], late_ref[...]


def add_to(ref, value):
    ref[...] = ref[...] + value.reshape(ref.shape)


def mlp_backward(grad, slope, act, mid_ref, ctx_ref, stat_ref, wo, big, c_ref, dctx, delta, g_wo, g_up, g_down, dpre, h_ref, s_a, s_b, sums, when, hook, after_first, after_second, before_second):
    parts = [slice(DIM * k, DIM * k + DIM) for k in range(FOUR)]
    pre = (s_a, s_b)

    def dact(k):
        pre[k % TWO][...] = nn(big[k], grad[...])

    @when
    def _():
        def scale(k, chunk):
            there = slice(parts[k].start + chunk.start, parts[k].start + chunk.stop)
            value = pre[k % TWO][chunk, :] * slope[there, :]
            sums[k, chunk, :] += fold(value)
            dpre[there, :] = value.astype(BF16)

        def down_product(k):
            add_to(g_down.at[k], nt(act[parts[k], :], grad[...]))

        dact(ZERO)
        norm_to(mid_ref.at[ZERO], get_stats(stat_ref), c_ref, LN_PAR + TWO, h_ref)
        for k in range(FOUR):
            products = [functools.partial(down_product, k)]
            if k < THREE:
                products = [functools.partial(dact, k + ONE)] + products
            woven(products, [functools.partial(scale, k, chunk) for chunk in row_chunks()])
        after_first()
    hook(ONE)

    @when
    def _():
        before_second()
        s_a[...] = functools.reduce(jnp.add, [nn(big[FOUR + k], dpre[rows, :]) for k, rows in enumerate(parts)])
        after_second()
    hook(TWO)

    @when
    def _():
        def write(rows, dx):
            dy = grad[rows, :].astype(F32)
            dmid = (dy + dx).astype(BF16)
            grad[rows, :] = dmid
            sums[6, rows, :] += fold(dy)
            sums[7, rows, :] += fold(dmid.astype(F32))

        norm_back(s_a, mid_ref.at[ZERO], get_stats(stat_ref), c_ref, LN_PAR + TWO, sums, FOUR, write,
                  [lambda k=k, rows=rows: add_to(g_up.at[k], nt(h_ref[...], dpre[rows, :])) for k, rows in enumerate(parts)])
        add_to(g_wo, nt(ctx_ref[ZERO].astype(BF16), grad[...]))
        s_b[...] = nn(wo[...], grad[...])
        for head in range(HEADS):
            rows = head_rows(head)[ZERO]
            value = s_b[rows, :].astype(BF16)
            dctx[rows, :] = value
            delta[head:head + ONE, :] = total(value.astype(F32) * ctx_ref[ZERO, rows, :])


def attn_backward(dctx, delta, probs, q_ref, k_ref, v_ref, x_ref, stat_ref, grad, wqkv, c_ref, cos_ref, sin_ref, g_qkv, dproj, h_ref, s_a, s_b, d_a, d_b,
                  sums, hook, prefetch):
    scores, dscores = (s_a, s_b), (d_a, d_b)
    q, k, v = q_ref.at[ZERO], k_ref.at[ZERO], v_ref.at[ZERO]

    def open_head(head):
        rows = head_rows(head)[ZERO]
        scores[head % TWO][...] = tn(v[rows, :], dctx[rows, :])

    def weigh(head, rows):
        dscores[head % TWO][rows, :] = (probs[head, rows, :].astype(F32) * (scores[head % TWO][rows, :] - delta[head:head + ONE, :])).astype(BF16)

    def values(head):
        rows = head_rows(head)[ZERO]
        dv = nt(dctx[rows, :], probs[head])
        sums[TWO, rows, :] += fold(dv)
        dproj[TWO * DIM + rows.start:TWO * DIM + rows.stop, :] = dv.astype(BF16)

    def close_head(head, m):
        rows, one, two = head_rows(head)
        ds = dscores[head % TWO][...]
        value = nn(k[rows, :], ds) * HEAD ** -0.5 if m == ZERO else nt(q[rows, :], ds)
        cos, sin = cos_ref[...], sin_ref[...]
        a, b = value[:HALF], value[HALF:]
        for at, out in ((one, a * cos + b * sin), (two, b * cos - a * sin)):
            dproj[m * DIM + at.start:m * DIM + at.stop, :] = out.astype(BF16)
            sums[m, at, :] += fold(out)

    open_head(ZERO)
    for head in range(HEADS):
        products = [functools.partial(values, head)]
        if head:
            products = [functools.partial(close_head, head - ONE, m) for m in range(TWO)] + products
        if head + ONE < HEADS:
            products = [functools.partial(open_head, head + ONE)] + products
        woven(products, [functools.partial(weigh, head, rows) for rows in row_chunks()])
        if head == THREE:
            hook(ONE)
    for m in range(TWO):
        close_head(HEADS - ONE, m)
    prefetch()
    hook(TWO)
    norm_to(x_ref.at[ZERO], get_stats(stat_ref), c_ref, LN_PAR, h_ref)
    parts = [slice(DIM * m, DIM * m + DIM) for m in range(THREE)]
    s_a[...] = functools.reduce(jnp.add, [nn(wqkv[m], dproj[rows, :]) for m, rows in enumerate(parts)])

    def write(rows, dx):
        grad[rows, :] = (grad[rows, :].astype(F32) + dx).astype(BF16)

    norm_back(s_a, x_ref.at[ZERO], get_stats(stat_ref), c_ref, LN_PAR, sums, THREE, write,
              [lambda m=m, rows=rows: add_to(g_qkv.at[m], nt(h_ref[...], dproj[rows, :])) for m, rows in enumerate(parts)])


def backward(dy, xs, q, k, v, probs, ctx, mid, act, slope, st1, st2, c, tables, w_qkv, w_o, w_up, w_down):
    def mlp_at(s):
        s = jnp.minimum(s, 15)
        odd = s // FOUR % TWO == ONE
        return ONE - s // EIGHT, jnp.where(odd, THREE, s % FOUR), ZERO, ZERO

    def attn_at(s):
        s = jnp.minimum(s, 15)
        odd = s // FOUR % TWO == ONE
        return jnp.where(s < EIGHT, ONE, ZERO) + jnp.where((s > 7) & (s < 12), ONE, ZERO), jnp.where(odd, s % FOUR, jnp.where(s < FOUR, ZERO, THREE)), ZERO, ZERO

    per_mlp = pl.BlockSpec((None, ONE, *SQUARE), mlp_at)
    per_attn = pl.BlockSpec((None, ONE, *SQUARE), attn_at)

    def stat(at):
        return pl.BlockSpec((None, ONE, EIGHT, TOK), at)

    acc = [(*GRID, EIGHT, WIDTH)]
    scratch = [pltpu.VMEM((SEQS, *SQUARE), BF16), pltpu.VMEM((SEQS, *SQUARE), BF16), pltpu.VMEM((SEQS, HEADS, TOK), F32),
               pltpu.VMEM((HEADS, TOK, TOK), BF16), pltpu.VMEM((THREE, DIM, DIM), BF16), pltpu.VMEM((DIM, DIM), BF16),
               pltpu.VMEM(TALL, F32), pltpu.VMEM(TALL, BF16), pltpu.VMEM(TALL, BF16), pltpu.VMEM(SQUARE, BF16),
               pltpu.VMEM(SQUARE, F32), pltpu.VMEM(SQUARE, F32), pltpu.VMEM((TOK, TOK), BF16), pltpu.VMEM((TOK, TOK), BF16),
               pltpu.VMEM((EIGHT, *COLS), F32), pltpu.VMEM((THREE, *GRID, EIGHT, DIM), F32), pltpu.VMEM((*GRID, EIGHT, DIM), F32),
               pltpu.VMEM((FOUR, *GRID, EIGHT, DIM), F32), pltpu.VMEM((*GRID, FOUR, EIGHT, DIM), F32), pltpu.VMEM((24, DIM), F32), pltpu.VMEM((10, 24, DIM), F32),
               pltpu.VMEM((EIGHT, DIM), F32), pltpu.VMEM((6, EIGHT, DIM), F32), pltpu.VMEM((SIXTEEN, EIGHT, DIM), F32)]
    for n in (ONE, THREE):
        for order in ORDERS:
            ring_a, ring_b, plane, other = landing_shapes(order, n)
            plane = (TWO, *plane) if n == ONE else plane
            scratch += [pltpu.VMEM(s, F32) for s in ((n, *GRID, EIGHT, WIDTH), ring_a, ring_b, plane, other)]
    scratch += [DMA((THREE, THREE, 24)), DMA((THREE, THREE, 24)), DMA((TWO, 10)), DMA((TWO, 6)), DMA((TWO, SIXTEEN)), DMA((EIGHT,)), DMA((TWO,)), DMA((TWO,))]
    outs = ((TWO, FOUR, FOUR, DIM), (TWO, FOUR, FFN), (TWO, SIXTEEN, DIM), (32, DIM))
    whole = [pl.BlockSpec(s, lambda i, n=len(s): (ZERO,) * n, pipeline_mode=pl.Buffered(ONE)) for s in outs]
    dx_at = lambda s: (jnp.clip(s - 12, ZERO, THREE), ZERO, ZERO)
    return pl.pallas_call(
        backward_kernel, grid=(18,),
        out_shape=[jax.ShapeDtypeStruct((SEQS, TOK, DIM), BF16)] + [jax.ShapeDtypeStruct(s, F32) for s in outs],
        out_specs=[pl.BlockSpec((ONE, TOK, DIM), dx_at)] + whole,
        in_specs=[pl.BlockSpec((ONE, TOK, DIM), lambda s: (jnp.minimum(s, THREE), ZERO, ZERO)), per_mlp, per_mlp, stat(mlp_at)] + [per_attn] * FOUR + [stat(attn_at),
                  once((HALF, TOK)), once((HALF, TOK)), pl.BlockSpec((None, *COLS), lambda s: (ONE - jnp.minimum(s, 15) // EIGHT, ZERO, ZERO))] + [HBM] * 7,
        scratch_shapes=scratch,
        compiler_params=pltpu.CompilerParams(collective_id=ONE, has_side_effects=True, vmem_limit_bytes=67043328,
                                             dimension_semantics=("arbitrary",)),
        name="backward")(dy, mid, ctx, st2, q, k, v, xs, st1, *tables, c, probs, slope, act, w_qkv, w_o, w_up, w_down)


def results_kernel(dx_ref, attn_ref, up_ref, down_ref, small_ref, dx_out, attn_out, gb_attn, g_ln, up_out, gb_up, down_out, gb_down):
    dx_out[...] = dx_ref[...]

    @pl.when(pl.program_id(ZERO) == ZERO)
    def _():
        me = lax.axis_index(AXIS)
        attn_out[...], up_out[...], down_out[...] = attn_ref[...], up_ref[...], down_ref[...]
        mine = pltpu.roll(small_ref[...], lax.rem(DIM - FOUR * me + FOUR * LANES, DIM), ONE)
        for l in range(TWO):
            mlp = SIXTEEN - SIXTEEN * l
            attn = mlp + EIGHT
            gb_attn[l, :THREE], gb_attn[l, THREE:] = mine[attn:attn + THREE, :FOUR], mine[mlp + 7:mlp + EIGHT, :FOUR]
            g_ln[l, :TWO], g_ln[l, TWO:] = mine[attn + THREE:attn + 5, :FOUR], mine[mlp + FOUR:mlp + 6, :FOUR]
            gb_down[l:l + ONE, :] = mine[mlp + 6:mlp + 7, :FOUR]
            ups = small_ref[pl.ds(mlp + me // 32, ONE), :]
            gb_up[l:l + ONE, :] = pltpu.roll(ups, lax.rem(DIM - SIXTEEN * lax.rem(me, 32), DIM), ONE)[:, :SIXTEEN]


def results(dx, attn, up, down, small):
    shapes = [attn.shape, (TWO, FOUR, FOUR), (TWO, FOUR, FOUR), up.shape, (TWO, SIXTEEN), down.shape, (TWO, FOUR)]
    per = pl.BlockSpec((ONE, TOK, DIM), lambda s: (s, ZERO, ZERO))
    return pl.pallas_call(
        results_kernel, grid=(SEQS,), name="results",
        out_shape=[jax.ShapeDtypeStruct(dx.shape, BF16)] + [jax.ShapeDtypeStruct(s, F32) for s in shapes],
        in_specs=[per] + [once(a.shape) for a in (attn, up, down, small)],
        out_specs=[per] + [once(s) for s in shapes])(dx, attn, up, down, small)


def solution(mesh):
    batch_spec = P(AXIS)
    weight_specs = (P(None, None, AXIS, None), P(None, None, AXIS), P(None, None, AXIS),
                    P(None, AXIS, None), P(None, AXIS), P(None, AXIS, None), P(None, AXIS))

    def device_step(x, lengths, d_y, w_attn, b_attn, ln_par, w_up, b_up, w_down, b_down):
        tables = rotary_tables()
        xs, q, k, v, probs, ctx, mid, act, slope, st1, st2, c, w_qkv, w_o, w_up, w_down = forward(
            lengths, x, tables, (w_attn, b_attn, ln_par, w_up, b_up, w_down, b_down))
        return results(*backward(d_y, xs, q, k, v, probs, ctx, mid, act, slope, st1, st2, c, tables, w_qkv, w_o, w_up, w_down))

    return jax.shard_map(device_step, mesh=mesh,
                         in_specs=(batch_spec, batch_spec, batch_spec) + weight_specs,
                         out_specs=(batch_spec,) + weight_specs,
                         check_vma=False)
```

```python
import math
import functools
import jax
import jax.numpy as jnp
from jax import lax
from jax.experimental import pallas as pl
from jax.experimental.pallas import tpu as pltpu
from jax.sharding import PartitionSpec as P

ZERO, ONE, TWO, THREE, FOUR = range(5)
EIGHT, SIXTEEN, WIDTH = 8, 16, 256

F32, BF16 = jnp.float32, jnp.bfloat16
SEQS, TOK, DIM, FFN, HEADS, HEAD, LANES = FOUR, 512, 512, 2048, EIGHT, 64, 128
HALF = HEAD // TWO
EPS = 1e-5
THETA = 10000.0
NEG_BIG = -1e30
B_ATTN, LN_PAR, B_UP, B_DOWN = ZERO, FOUR, EIGHT, 12


def nn(a, b):
    return lax.dot_general(a, b, (((ONE,), (ZERO,)), ((), ())), preferred_element_type=F32)


def nt(a, b):
    return lax.dot_general(a, b, (((ONE,), (ONE,)), ((), ())), preferred_element_type=F32)


def tn(a, b):
    return lax.dot_general(a, b, (((ZERO,), (ZERO,)), ((), ())), preferred_element_type=F32)


def lane_tiles(width=TOK, size=LANES):
    return [slice(i, i + size) for i in range(ZERO, width, size)]


def row_chunks(rows=DIM, size=64):
    return [slice(i, i + size) for i in range(ZERO, rows, size)]


def column(c_ref, rows, lane):
    return jnp.broadcast_to(c_ref[rows, lane:lane + ONE], (rows.stop - rows.start, TOK))


def total(value):
    return jnp.sum(value, axis=ZERO, keepdims=True)


def norm_stats(x_ref):
    mean = functools.reduce(jnp.add, [total(x_ref[rows, :].astype(F32)) for rows in row_chunks()]) * (1.0 / DIM)
    squares = []
    for rows in row_chunks():
        centred = x_ref[rows, :].astype(F32) - mean
        squares.append(total(centred * centred))
    return mean, lax.rsqrt(functools.reduce(jnp.add, squares) * (1.0 / DIM) + EPS)


def norm_to(x_ref, stats, c_ref, lane, h_ref):
    mean, rstd = stats
    for rows in row_chunks():
        xhat = (x_ref[rows, :].astype(F32) - mean) * rstd
        h_ref[rows, :] = (xhat * column(c_ref, rows, lane) + column(c_ref, rows, lane + ONE)).astype(BF16)


def put_stats(ref, stats):
    ref[ZERO:ONE, :], ref[ONE:TWO, :] = stats


def get_stats(ref):
    return ref[ZERO:ONE, :], ref[ONE:TWO, :]


def woven(products, rest):
    done = ZERO
    for n, step in enumerate(rest):
        while done < len(products) and done * len(rest) <= n * len(products):
            products[done]()
            done += ONE
        step()
    for product in products[done:]:
        product()


def fold(value):
    parts = [value[:, cols] for cols in lane_tiles(value.shape[ONE])]
    return functools.reduce(jnp.add, parts)


def seq_spec(shape):
    return pl.BlockSpec((ONE, *shape), lambda s: (s,) + (ZERO,) * len(shape))


def once(shape):
    return pl.BlockSpec(shape, lambda s: (ZERO,) * len(shape), pipeline_mode=pl.Buffered(ONE))


def act_shape(rows, dtype):
    return jax.ShapeDtypeStruct((SEQS, rows, TOK), dtype)


PARAMS = pltpu.CompilerParams(vmem_limit_bytes=60 << 20, dimension_semantics=("arbitrary",))
SQUARE, TALL, WIDE, COLS = (DIM, TOK), (FFN, TOK), (DIM, FFN), (DIM, LANES)


def rotary_tables():
    inv_freq = 1.0 / (THETA ** (jnp.arange(HALF, dtype=F32) * (2.0 / HEAD)))
    angles = inv_freq[:, None] * jnp.arange(TOK, dtype=F32)[None, :]
    return jnp.cos(angles), jnp.sin(angles)


MESH = pl.DeviceIdType.MESH
AXIS = "fsdp"
ORDERS = ((TWO, ONE, ZERO), (ONE, ZERO, TWO), (ZERO, TWO, ONE))


class Place:
    def __init__(self):
        me = lax.axis_index(AXIS)
        self.core = lax.rem(me, TWO)
        self.pos = (me // 32, lax.rem(me // EIGHT, FOUR), lax.rem(me // TWO, FOUR))
        self.partner = me + ONE - TWO * self.core

    def coord(self, dim, delta):
        return lax.rem(self.pos[dim] + (delta + FOUR), FOUR)

    def device(self, offsets):
        pos = [self.coord(dim, offsets.get(dim, ZERO)) for dim in range(THREE)]
        return pos[ZERO] * 32 + pos[ONE] * EIGHT + pos[TWO] * TWO + self.core

    def greet(self):
        barrier = pltpu.get_barrier_semaphore()

        @pl.loop(ONE, 64)
        def _(i):
            offsets = {ZERO: i // SIXTEEN, ONE: lax.rem(i // FOUR, FOUR), TWO: lax.rem(i, FOUR)}

            @pl.when(offsets[ZERO] * offsets[ONE] * offsets[TWO] == ZERO)
            def _():
                pl.semaphore_signal(barrier, inc=ONE, device_id=(self.device(offsets),), device_id_type=MESH)
        pl.semaphore_signal(barrier, inc=ONE, device_id=(self.partner,), device_id_type=MESH)

    def met(self):
        pl.semaphore_wait(pltpu.get_barrier_semaphore(), 37)


def remote(src, dst, send_sem, recv_sem, device):
    return pltpu.make_async_remote_copy(src_ref=src, dst_ref=dst, send_sem=send_sem, recv_sem=recv_sem,
                                        device_id=(device,), device_id_type=MESH)


LINE = (ONE, -ONE, TWO)


def plane_offsets(order, k, sign=ONE):
    return {order[ONE]: sign * (k // FOUR), order[TWO]: sign * lax.rem(k, FOUR)}


class Gather:
    def __init__(self, place, buf, fifteen, order, send, recv):
        self.place, self.buf, self.fifteen, self.order, self.send, self.recv = place, buf, fifteen, order, send, recv

    def block(self, offsets, whole=()):
        index = [slice(ZERO, FOUR) if dim in whole else pl.ds(self.place.coord(dim, offsets.get(dim, ZERO)), ONE) for dim in range(THREE)]
        return self.buf.at[index[ZERO], index[ONE], index[TWO], pl.ds(self.place.core, ONE)]

    def copy(self, ref, key, device):
        return remote(ref, ref, self.send.at[key], self.recv.at[key], device)

    def plane_start(self):
        @pl.loop(ONE, SIXTEEN)
        def _(k):
            self.copy(self.block({}), ZERO, self.place.device(plane_offsets(self.order, k))).start()

    def plane_all(self):
        return self.copy(self.fifteen, ZERO, self.place.partner)

    def plane_wait(self):
        self.plane_all().wait_recv()

    def line(self, i, sign):
        offsets = {self.order[ZERO]: sign * LINE[i]}
        return self.block(offsets, self.order[ONE:])

    def line_start(self):
        for i, delta in enumerate(LINE):
            self.copy(self.line(i, ZERO), ONE + i, self.place.device({self.order[ZERO]: delta})).start()

    def line_wait(self):
        for i in range(THREE):
            self.copy(self.line(i, -ONE), ONE + i, self.place.partner).wait_recv()

    def share(self, core):
        return self.copy(self.buf.at[:, :, :, pl.ds(core, ONE)], FOUR, self.place.partner)

    def share_start(self):
        self.share(self.place.core).start()

    def end(self):
        self.share(ONE - self.place.core).wait_recv()
        self.plane_all().wait_send()
        for i in range(THREE):
            self.copy(self.line(i, ZERO), ONE + i, self.place.partner).wait_send()
        self.share(self.place.core).wait_send()


def gather_steps(gathers):
    def each(*names):
        def step():
            for name in names:
                for g in gathers:
                    getattr(g, name)()
        return step

    return [each("plane_start"), each("plane_wait", "line_start"), each("line_wait", "share_start"), each("end")]


class Scatter:
    def __init__(self, place, grads, acc, got_a, got_b, got_p, other, order, send, recv):
        self.place, self.grads, self.acc, self.order = place, grads, acc, order
        self.got_a, self.got_b, self.got_p, self.other, self.send, self.recv = got_a, got_b, got_p, other, send, recv
        self.units = acc.shape[ZERO]

    def columns(self, core):
        return pl.ds(pl.multiple_of(core * WIDTH, WIDTH), WIDTH)

    def swap_copy(self, u):
        place = self.place
        return remote(self.grads(u).at[:, :, :, :, self.columns(ONE - place.core)], self.acc.at[u], self.send.at[6 + u], self.recv.at[6 + u], place.partner)

    def swap(self):
        for u in range(self.units):
            self.swap_copy(u).start()

    def swapped(self):
        for u in range(self.units):
            self.swap_copy(u).wait()
            grad, acc = self.grads(u), self.acc

            @pl.loop(ZERO, FOUR)
            def _(z):
                acc[u, z] = acc[u, z] + grad[z, :, :, :, self.columns(self.place.core)]

    def part(self, delta, half=None):
        index = [slice(ZERO, FOUR)] * THREE
        index[self.order[ZERO]] = pl.ds(self.place.coord(self.order[ZERO], delta), ONE)
        return self.acc.at[:, index[ZERO], index[ONE], index[TWO], :, slice(ZERO, WIDTH) if half is None else lane_tiles()[half]]

    def ring(self, step, way):
        delta = (ONE, -ONE)[way]
        device = self.place.device({self.order[ZERO]: delta})
        if step == ZERO:
            src, dst = self.part(TWO, way), self.got_a.at[:, :, :, :, :, lane_tiles()[way]]
        else:
            src, dst = self.part(delta), self.got_b.at[way]
        key = TWO * step + way
        return remote(src, dst, self.send.at[key], self.recv.at[key], device)

    def ring_start(self):
        for way in range(TWO):
            self.ring(ZERO, way).start()

    def ring_turn(self):
        for way in range(TWO):
            self.ring(ZERO, way).wait_recv()
            self.add((ONE, -ONE)[way], way, self.got_a)
            self.ring(ONE, way).start()

    def add(self, delta, half, *refs):
        dim, acc = self.order[ZERO], self.acc
        at = self.place.coord(dim, delta)
        columns = slice(ZERO, WIDTH) if half is None else lane_tiles()[half]

        @pl.loop(ZERO, FOUR)
        def _(i):
            index = [i if d == self.order[ONE] else slice(ZERO, FOUR) for d in range(THREE)]
            there = [slice(None), *index, slice(None), columns]
            here = list(there)
            here[ONE + dim] = pl.ds(at, ONE)
            there[ONE + dim] = slice(ZERO, ONE)
            value = acc[tuple(here)]
            for ref in refs:
                value = value + ref[tuple(there)]
            acc[tuple(here)] = value

    def plane_copy(self, k):
        offsets = plane_offsets(self.order, k)
        index = [pl.ds(self.place.coord(dim, offsets.get(dim, ZERO)), ONE) for dim in range(THREE)]
        src = self.acc.at[:, index[ZERO], index[ONE], index[TWO]]
        return remote(src, self.got_p.at[k], self.send.at[FOUR], self.recv.at[FOUR], self.place.device(offsets))

    def plane_all(self):
        return remote(self.got_p.at[ONE:], self.got_p.at[ONE:], self.send.at[FOUR], self.recv.at[FOUR], self.place.partner)

    def plane_start(self):
        for way in range(TWO):
            self.ring(ONE, way).wait_recv()
        self.add(ZERO, None, self.got_b.at[ZERO], self.got_b.at[ONE])

        @pl.loop(ONE, SIXTEEN)
        def _(k):
            self.plane_copy(k).start()

    def own(self):
        z, y, x = [pl.ds(p, ONE) for p in self.place.pos]
        return self.acc.at[:, z, y, x]

    def last_copy(self):
        return remote(self.own(), self.other, self.send.at[5], self.recv.at[5], self.place.partner)

    def last(self):
        self.plane_all().wait_recv()
        own = self.own()
        own[...] = functools.reduce(jnp.add, [self.got_p[k] for k in range(ONE, SIXTEEN)], own[...])
        self.last_copy().start()

    def finish(self, store):
        self.last_copy().wait_recv()
        first = self.place.core == ZERO
        for u in range(self.units):
            own, came = self.own()[u, ZERO, ZERO, ZERO], self.other[u, ZERO, ZERO, ZERO]
            store(u, jnp.concatenate([jnp.where(first, own, came), jnp.where(first, came, own)], axis=ONE))
        for step in range(TWO):
            for way in range(TWO):
                self.ring(step, way).wait_send()
        self.plane_all().wait_send()
        self.last_copy().wait_send()


def landing_shapes(order, units):
    size = [FOUR, FOUR, FOUR]
    size[order[ZERO]] = ONE
    return (units, *size, EIGHT, WIDTH), (TWO, units, *size, EIGHT, WIDTH), (SIXTEEN, units, ONE, ONE, ONE, EIGHT, WIDTH), (units, ONE, ONE, ONE, EIGHT, WIDTH)


class Small:
    def __init__(self, place, value, slots, send, recv):
        self.place, self.value, self.slots, self.send, self.recv = place, value, slots, send, recv

    def peers(self, stage):
        if stage == THREE:
            return [self.place.partner]
        return [self.place.device({stage: delta}) for delta in LINE]

    def copies(self, stage):
        return [remote(self.value, self.slots.at[THREE * stage + k], self.send.at[THREE * stage + k], self.recv.at[THREE * stage + k], peer)
                for k, peer in enumerate(self.peers(stage))]

    def start(self, stage):
        for copy in self.copies(stage):
            copy.start()

    def finish(self, stage):
        copies = self.copies(stage)
        for copy in copies:
            copy.wait()
        self.value[...] = functools.reduce(jnp.add, [self.slots[THREE * stage + k] for k in range(len(copies))], self.value[...])

    def turn(self, stage):
        def step():
            self.finish(stage)
            self.start(stage + ONE)
        return step

    def steps(self):
        return [lambda: self.start(ZERO), self.turn(ZERO), self.turn(ONE), self.turn(TWO), lambda: self.finish(THREE)]


class Late(Small):
    def __init__(self, place, value, slots, send, recv, planes, plane_send, plane_recv):
        super().__init__(place, value, slots, send, recv)
        self.planes, self.plane_send, self.plane_recv = planes, plane_send, plane_recv

    def peers(self, stage):
        return super().peers({ZERO: ORDERS[ZERO][ZERO], ONE: THREE}[stage])

    def plane(self, k):
        return remote(self.value, self.planes.at[k], self.plane_send, self.plane_recv, self.place.device(plane_offsets(ORDERS[ZERO], k)))

    def steps(self):
        def first():
            @pl.loop(ONE, SIXTEEN)
            def _(k):
                self.plane(k).start()

        def second():
            remote(self.planes.at[ONE:], self.planes.at[ONE:], self.plane_send, self.plane_recv, self.place.partner).wait()
            self.value[...] = functools.reduce(jnp.add, [self.planes[k] for k in range(ONE, SIXTEEN)], self.value[...])
            self.start(ZERO)

        return [first, second, self.turn(ZERO), lambda: self.finish(ONE)]


VMEM = pl.BlockSpec(memory_space=pltpu.VMEM)
HBM = pl.BlockSpec(memory_space=pl.ANY)
DMA = pltpu.SemaphoreType.DMA


COLOURS = ((THREE, FOUR, 5), (6, 7, EIGHT), (9, 10, 11))
GRID = (FOUR, FOUR, FOUR)


def spread(buf, u, out_ref, column_base):
    @pl.loop(ZERO, EIGHT)
    def _(block):
        for part in range(FOUR):
            g = block * FOUR + part
            tiles = [buf[block // TWO, lax.rem(block, TWO) * TWO + part // TWO, part % TWO * TWO + k // TWO, k % TWO, u].astype(F32) for k in range(FOUR)]
            rows = pl.ds(pl.multiple_of(g * SIXTEEN, SIXTEEN), SIXTEEN)
            for j, cols in enumerate(lane_tiles()):
                value = jnp.concatenate([t[FOUR * j:FOUR * j + FOUR] for t in tiles], axis=ZERO).astype(BF16)
                out_ref[rows, column_base + cols.start:column_base + cols.stop] = value


def spread_down(buf, u, out_ref, cols):
    @pl.loop(ZERO, SIXTEEN)
    def _(i):
        for k in range(EIGHT):
            d = i * EIGHT + k
            out_ref[pl.ds(pl.multiple_of(d * SIXTEEN, SIXTEEN), SIXTEEN), cols] = buf[i // FOUR, lax.rem(i, FOUR), k // TWO, k % TWO, u]


def same(shape, test):
    row = lax.broadcasted_iota(jnp.int32, shape, ZERO)
    col = lax.broadcasted_iota(jnp.int32, shape, ONE)
    return jnp.where(test(row, col), 1.0, 0.0)


def small_columns(small_ref, c_ref):
    rows = [small_ref[z, y, x, c, ZERO] for z in range(FOUR) for y in range(FOUR) for x in range(FOUR) for c in range(TWO)]
    table = jnp.concatenate(rows, axis=ZERO).astype(BF16)
    quads = nn(same((DIM, LANES), lambda r, c: r // FOUR == c).astype(BF16), table)
    quads = (quads * same((DIM, LANES), lambda r, c: r % FOUR == c % FOUR)).astype(BF16)
    mask = same((DIM, LANES), lambda r, c: r % SIXTEEN == c % SIXTEEN)
    pick = same((DIM, 32), lambda r, c: r // SIXTEEN == c).astype(BF16)
    ups = [(nn(pick, table[32 * k:32 * k + 32]) * mask).astype(BF16) for k in range(FOUR)]
    for layer in range(TWO):
        def is_up(r):
            return r // SIXTEEN == layer * FOUR + TWO

        value = nn(quads, same((LANES, LANES), lambda r, c: (r // 64 == layer) & (r % 64 // FOUR == c) & ~is_up(r)).astype(BF16))
        for k in range(FOUR):
            value = value + nn(ups[k], same((LANES, LANES), lambda r, c: is_up(r) & (c == B_UP + k)).astype(BF16))
        c_ref[layer] = value


def tile_of(rows):
    rows = rows.astype(F32)
    return jnp.concatenate([rows[:, cols] for cols in lane_tiles()], axis=ZERO).astype(BF16)


def small_row(b_attn, ln_par, b_up, b_down):
    lane = lax.broadcasted_iota(jnp.int32, (ONE, LANES), ONE)
    row = jnp.zeros((ONE, LANES), F32)
    pieces = []
    for l in range(TWO):
        for m in range(FOUR):
            pieces += [(b_attn[l, m:m + ONE, :], 64 * l + FOUR * m), (ln_par[l, m:m + ONE, :], 64 * l + FOUR * m + SIXTEEN)]
        pieces += [(b_up[l:l + ONE, :], 64 * l + 32), (b_down[l:l + ONE, :], 64 * l + 48)]
    for piece, at in pieces:
        n = piece.shape[ONE]
        wide = jnp.concatenate([piece.astype(F32), jnp.zeros((ONE, LANES - n), F32)], axis=ONE)
        wide = pltpu.roll(wide, at, ONE) if at else wide
        row = jnp.where((lane >= at) & (lane < at + n), wide, row)
    return row


def hooks(slot, plan):
    def hook(at):
        for slots, run in plan:
            mine = [when for when in slots if when % FOUR == at]
            if mine:
                pl.when(functools.reduce(jnp.logical_or, [slot + at == when for when in mine]))(run)
    return hook


def forward_kernel(len_ref, x_hbm, cos_ref, sin_ref, w_attn, b_attn, ln_par, w_up, b_up, w_down, b_down,
                   xs_out, q_ref, k_ref, v_ref, p_hbm, ctx_ref, mid_ref, act_ref, slope_ref, st1_ref, st2_ref, c_ref,
                   nat_qkv, nat_wo, nat_up, nat_down,
                   xs, ctxb, wqkv, wo, up, down, n_qkv, n_wo, n_up, n_down, p_buf, h_ref, s_a, s_b, s_c,
                   sbuf, q0, q1, q2, m0, m1, m2, stats, f0, f1, f2, send, recv, p_sem, nat_sem, x_sem):
    step = pl.program_id(ZERO)
    phase, seq, layer = step // FOUR, lax.rem(step, FOUR), step // EIGHT
    place = Place()
    z, y, x = place.pos
    qkv_bufs, mo_bufs, fifteen = (q0, q1, q2), (m0, m1, m2), (f0, f1, f2)

    def group(bufs, base, l):
        return [Gather(place, b.at[l], fifteen[base // THREE], ORDERS[k], send.at[base + k, l], recv.at[base + k, l]) for k, b in enumerate(bufs)]

    little = Gather(place, sbuf, fifteen[TWO], ORDERS[ZERO], send.at[6, ZERO], recv.at[6, ZERO])

    def nat_copies(which, l):
        if which == ZERO:
            return [pltpu.make_async_copy(n_qkv, nat_qkv.at[l], nat_sem.at[ZERO])]
        return [pltpu.make_async_copy(src, dst.at[l], nat_sem.at[ONE + i]) for i, (src, dst) in enumerate(((n_wo, nat_wo), (n_up, nat_up), (n_down, nat_down)))]

    def wait(copies):
        for copy in copies:
            copy.wait()

    def start(copies):
        for copy in copies:
            copy.start()

    def take_qkv():
        pl.when(step > ZERO)(lambda: wait(nat_copies(ZERO, layer)))
        for m in range(THREE):
            spread(qkv_bufs[m].at[layer], ZERO, n_qkv.at[m], ZERO)
            wqkv[m] = n_qkv[m].T
        start(nat_copies(ZERO, layer))

    def take_mo():
        pl.when(step > EIGHT)(lambda: wait(nat_copies(ONE, layer)))
        for colour in range(THREE):
            for u, unit in enumerate(COLOURS[colour]):
                buf = mo_bufs[colour].at[layer]
                if unit == THREE:
                    spread(buf, u, n_wo, ZERO)
                    wo[...] = n_wo[...].T
                elif unit < EIGHT:
                    part = slice(DIM * (unit - FOUR), DIM * (unit - THREE))
                    spread(buf, u, n_up, part.start)
                    up[part, :] = n_up[:, part].T
                else:
                    spread_down(buf, u, n_down, lane_tiles()[unit - EIGHT])
        for k in range(FOUR):
            part = slice(DIM * k, DIM * k + DIM)
            down[:, part] = n_down[part, :].T
        start(nat_copies(ONE, layer))

    x_copies = [pltpu.make_async_copy(x_hbm.at[s], ctxb.at[s], x_sem.at[s]) for s in range(SEQS)]

    @pl.when(step == ZERO)
    def _():
        place.greet()
        start(x_copies)
        for l in range(TWO):
            for unit in range(12):
                if unit < FOUR:
                    tile = tile_of(w_attn[l, unit])
                elif unit < EIGHT:
                    tile = tile_of(w_up[l, :, DIM * (unit - FOUR):DIM * (unit - THREE)])
                else:
                    tile = w_down[l, :, lane_tiles()[unit - EIGHT]]
                if unit < THREE:
                    qkv_bufs[unit][l, z, y, x, place.core, ZERO] = tile
                else:
                    mo_bufs[(unit - THREE) // THREE][l, z, y, x, place.core, (unit - THREE) % THREE] = tile
        sbuf[z, y, x, place.core, ZERO] = small_row(b_attn, ln_par, b_up, b_down)
        first, second = gather_steps(group(qkv_bufs, ZERO, ZERO) + [little]), gather_steps(group(mo_bufs, THREE, ZERO))

        def ready(s):
            x_copies[s].wait()
            xs[s] = ctxb[s].T
            put_stats(stats.at[s], norm_stats(xs.at[s]))

        place.met()
        first[ZERO]()
        second[ZERO]()
        ready(ZERO)
        ready(ONE)
        first[ONE]()
        ready(TWO)
        ready(THREE)
        first[TWO]()
        second[ONE]()
        first[THREE]()
        small_columns(sbuf, c_ref)

    attn_hook = hooks(step * FOUR, [((when, when + 32), run) for when, run in zip((9, 13), gather_steps(group(mo_bufs, THREE, layer))[TWO:])])
    mlp_steps = gather_steps(group(qkv_bufs, ZERO, ONE)) + gather_steps(group(mo_bufs, THREE, ONE))[:TWO]
    mlp_hook = hooks(step * FOUR, [((when,), run) for when, run in zip((SIXTEEN, 25, 30, 31, 17, 26), mlp_steps)])

    @pl.when(phase % TWO == ZERO)
    def _():
        pl.when(seq == ZERO)(take_qkv)

        @pl.when(step < FOUR)
        def _():
            xs_out[ZERO, ZERO] = xs[seq]

        @pl.when(step > 7)
        def _():
            put_stats(stats.at[seq], norm_stats(xs.at[seq]))

        attn_hook(ZERO)
        copies = [pltpu.make_async_copy(p_buf.at[head], p_hbm.at[layer, seq, head], p_sem.at[head]) for head in range(HEADS)]
        attn_forward(len_ref[seq], xs.at[seq], wqkv, c_ref.at[layer], cos_ref, sin_ref, q_ref.at[ZERO, ZERO], k_ref.at[ZERO, ZERO],
                     v_ref.at[ZERO, ZERO], p_buf, ctx_ref.at[ZERO, ZERO], ctxb.at[seq], get_stats(stats.at[seq]), st1_ref.at[ZERO, ZERO], h_ref, s_a, s_b, s_c, attn_hook,
                     lambda heads: pl.when(step > ZERO)(lambda: wait(copies[heads])), lambda heads: start(copies[heads]))
        pl.when(step == 11)(lambda: wait(copies))
        attn_hook(THREE)

    @pl.when(phase % TWO == ONE)
    def _():
        pl.when(seq == ZERO)(take_mo)
        mlp_hook(ZERO)
        mlp_forward(layer, ctxb.at[seq], xs.at[seq], wo, up, down, c_ref.at[layer], mid_ref.at[ZERO, ZERO], act_ref.at[ZERO, ZERO], slope_ref.at[ZERO, ZERO],
                    st2_ref.at[ZERO, ZERO], h_ref, s_a, s_b, mlp_hook)

        @pl.when(layer == ZERO)
        def _():
            xs_out[ZERO, ZERO] = xs[seq]
        mlp_hook(THREE)

    @pl.when(step == 15)
    def _():
        for which in range(TWO):
            wait(nat_copies(which, ONE))


def attn_forward(length, xt, w, c_ref, cos_ref, sin_ref, q_ref, k_ref, v_ref, p_buf, ctx_ref, ctxb, stats, stat_ref, h_ref, s_a, s_b, s_c, hook, free, ship):
    put_stats(stat_ref, stats)
    norm_to(xt, stats, c_ref, LN_PAR, h_ref)
    for m, acc in enumerate((s_a, s_b, s_c)):
        acc[...] = nn(w[m], h_ref[...])
    cos, sin = cos_ref[...], sin_ref[...]
    for m, (acc, out) in enumerate(((s_a, q_ref), (s_b, k_ref), (s_c, v_ref))):
        for head in range(HEADS):
            rows, one, two = head_rows(head)
            if m == TWO:
                out[rows, :] = (acc[rows, :] + column(c_ref, rows, B_ATTN + m)).astype(BF16)
                continue
            a, b = [acc[half, :] + column(c_ref, half, B_ATTN + m) for half in (one, two)]
            if m == ZERO:
                a, b = a * HEAD ** -0.5, b * HEAD ** -0.5
            out[one, :] = (a * cos - b * sin).astype(BF16)
            out[two, :] = (b * cos + a * sin).astype(BF16)
    hook(ONE)
    halves = slice(ZERO, FOUR), slice(FOUR, EIGHT)
    free(halves[ZERO])
    key = lax.broadcasted_iota(jnp.int32, (SIXTEEN, TOK), ONE)
    row = lax.broadcasted_iota(jnp.int32, (SIXTEEN, TOK), ZERO)
    bias_rows = jnp.where((row == ZERO) & (key >= length), NEG_BIG, 0.0).astype(BF16)
    one_rows = jnp.where(row == ZERO, 1.0, 0.0).astype(BF16)
    scores = (s_a, s_b)

    def open_head(head):
        rows = head_rows(head)[ZERO]
        keys = jnp.concatenate([k_ref[rows, :], bias_rows], axis=ZERO)
        queries = jnp.concatenate([q_ref[rows, :], one_rows], axis=ZERO)
        scores[head % TWO][...] = tn(keys, queries)

    def weigh(head):
        value, tops, sums = scores[head % TWO], [], []

        def top(rows):
            tops.append(jnp.max(value[rows, :], axis=ZERO, keepdims=True))
            if rows.stop == TOK:
                tops[:] = [functools.reduce(jnp.maximum, tops)]

        def power(rows):
            weight = jnp.exp(value[rows, :] - tops[ZERO])
            value[rows, :] = weight
            sums.append(total(weight))
            if rows.stop == TOK:
                sums[:] = [1.0 / functools.reduce(jnp.add, sums)]

        def share(rows):
            p_buf[head, rows, :] = (value[rows, :] * sums[ZERO]).astype(BF16)

        return [functools.partial(run, rows) for run in (top, power, share) for rows in row_chunks()]

    def close_head(head):
        rows = head_rows(head)[ZERO]
        ctx = nn(v_ref[rows, :], p_buf[head])
        ctx_ref[rows, :] = ctx
        ctxb[rows, :] = ctx.astype(BF16)

    open_head(ZERO)
    for head in range(HEADS):
        products = [functools.partial(open_head, head + ONE)] if head + ONE < HEADS else []
        if head:
            products.append(functools.partial(close_head, head - ONE))
        woven(products, weigh(head))
        if head == THREE:
            ship(halves[ZERO])
            hook(TWO)
            free(halves[ONE])
    close_head(HEADS - ONE)
    ship(halves[ONE])


def mlp_forward(layer, ctxb, xt, wo, up, down, c_ref, mid_ref, act_ref, slope_ref, stat_ref, h_ref, s_a, s_b, hook):
    s_a[...] = nn(wo[...], ctxb[...])
    for rows in row_chunks():
        mid_ref[rows, :] = (xt[rows, :].astype(F32) + s_a[rows, :] + column(c_ref, rows, B_ATTN + THREE)).astype(BF16)
    stats = norm_stats(mid_ref)
    put_stats(stat_ref, stats)
    norm_to(mid_ref, stats, c_ref, LN_PAR + TWO, h_ref)
    hook(ONE)
    pre = (s_a, s_b)
    parts = [slice(DIM * k, DIM * k + DIM) for k in range(FOUR)]

    def open_part(k):
        pre[k % TWO][...] = nn(up[parts[k], :], h_ref[...])

    open_part(ZERO)
    for k, part in enumerate(parts):
        if k < THREE:
            open_part(k + ONE)
        for rows in row_chunks():
            value = pre[k % TWO][rows, :] + column(c_ref, rows, B_UP + k)
            scaled = value * math.sqrt(0.5)
            cdf = 0.5 + 0.5 * lax.erf(scaled)
            density = jnp.exp2(scaled * scaled * -math.log2(math.e) - 0.5 * math.log2(2.0 * math.pi))
            there = slice(part.start + rows.start, part.start + rows.stop)
            act_ref[there, :] = (value * cdf).astype(BF16)
            slope_ref[there, :] = cdf + value * density
        if k == ONE:
            hook(TWO)

    @pl.when(layer == ZERO)
    def _():
        s_a[...] = nn(down[...], act_ref[...])
        for rows in row_chunks():
            xt[rows, :] = (mid_ref[rows, :].astype(F32) + s_a[rows, :] + column(c_ref, rows, B_DOWN)).astype(BF16)


def forward(lengths, x, tables, params):
    def saved(index, rows, dtype):
        return jax.ShapeDtypeStruct((TWO, SEQS, rows, TOK), dtype), pl.BlockSpec((ONE, ONE, rows, TOK), index)

    def attn_at(s):
        return s // EIGHT, jnp.where(s // FOUR % TWO == ZERO, s % FOUR, THREE), ZERO, ZERO

    def mlp_at(s):
        odd = s // FOUR % TWO == ONE
        return jnp.where(s < 12, ZERO, ONE), jnp.where(odd, s % FOUR, jnp.where(s < FOUR, ZERO, THREE)), ZERO, ZERO

    def xs_at(s):
        return jnp.where(s < FOUR, ZERO, ONE), jnp.where(s < EIGHT, s % FOUR, THREE), ZERO, ZERO

    outs = [saved(xs_at, DIM, BF16)] + [saved(attn_at, DIM, BF16)] * THREE
    outs += [(jax.ShapeDtypeStruct((TWO, SEQS, HEADS, TOK, TOK), BF16), HBM), saved(attn_at, DIM, F32)]
    outs += [saved(mlp_at, DIM, BF16), saved(mlp_at, FFN, BF16), saved(mlp_at, FFN, F32), saved(attn_at, EIGHT, F32), saved(mlp_at, EIGHT, F32)]
    outs += [(jax.ShapeDtypeStruct((TWO, *COLS), F32), once((TWO, *COLS)))]
    weights = ((THREE, DIM, DIM), (DIM, DIM), (DIM, FFN), (FFN, DIM))
    outs += [(jax.ShapeDtypeStruct((TWO, *w), BF16), HBM) for w in weights]
    scratch = [(SEQS, *SQUARE), (SEQS, *SQUARE), weights[ZERO], weights[ONE], weights[THREE], weights[TWO], *weights, (HEADS, TOK, TOK), SQUARE]
    scratch = [pltpu.VMEM(s, BF16) for s in scratch] + [pltpu.VMEM(SQUARE, F32)] * THREE + [pltpu.VMEM((*GRID, TWO, ONE, ONE, LANES), F32)]
    scratch += [pltpu.VMEM((TWO, *GRID, TWO, n, SIXTEEN, LANES), BF16) for n in (ONE, THREE) for _ in range(THREE)]
    scratch += [pltpu.VMEM((SEQS, EIGHT, TOK), F32)] + [pltpu.VMEM((15, n, SIXTEEN, LANES), BF16) for n in (ONE, THREE)]
    scratch += [pltpu.VMEM((15, ONE, ONE, LANES), F32), DMA((7, TWO, 5)), DMA((7, TWO, 5)), DMA((HEADS,)), DMA((FOUR,)), DMA((SEQS,))]
    return pl.pallas_call(
        forward_kernel, grid=(SIXTEEN,),
        out_shape=[o[ZERO] for o in outs], out_specs=[o[ONE] for o in outs],
        in_specs=[pl.BlockSpec(memory_space=pltpu.SMEM), HBM, once((HALF, TOK)), once((HALF, TOK))] + [once(p.shape) for p in params],
        scratch_shapes=scratch,
        compiler_params=pltpu.CompilerParams(collective_id=ZERO, has_side_effects=True, vmem_limit_bytes=67043328,
                                             dimension_semantics=("arbitrary",)),
        name="forward")(lengths, x, *tables, *params)


def norm_back(dh_ref, x_ref, stats, c_ref, lane, sums, at, write, beside):
    mean, rstd = stats
    means = [0.0, 0.0]

    def both(rows):
        dh = dh_ref[rows, :]
        return dh, dh * column(c_ref, rows, lane), (x_ref[rows, :].astype(F32) - mean) * rstd

    def first(rows):
        dh, dxhat, xhat = both(rows)
        means[ZERO], means[ONE] = means[ZERO] + total(dxhat), means[ONE] + total(dxhat * xhat)
        sums[at, rows, :] += fold(dh * xhat)
        sums[at + ONE, rows, :] += fold(dh)

    def second(rows):
        dh, dxhat, xhat = both(rows)
        write(rows, rstd * (dxhat - means[ZERO] * (1.0 / DIM) - xhat * (means[ONE] * (1.0 / DIM))))

    woven(beside, [functools.partial(run, rows) for run in (first, second) for rows in row_chunks()])


def columns_of(partials):
    lane = lax.broadcasted_iota(jnp.int32, COLS, ONE)
    value = jnp.zeros(COLS, F32)
    for at, partial in enumerate(partials):
        value = jnp.where(lane == at, jnp.sum(partial, axis=ONE, keepdims=True), value)
    return value.T[:EIGHT]


def head_rows(head):
    return slice(HEAD * head, HEAD * head + HEAD), slice(HEAD * head, HEAD * head + HALF), slice(HEAD * head + HALF, HEAD * head + HEAD)


class Reduce:
    def __init__(self, place, units, grads, buffers, send, recv):
        self.units = units
        self.scatters = [Scatter(place, (lambda u, k=k: grads(units[k][u])), *buffers[k], ORDERS[k], send.at[k], recv.at[k]) for k in range(THREE)]

    def steps(self, store):
        def each(*names):
            def step():
                for name in names:
                    for s in self.scatters:
                        getattr(s, name)()
            return step

        def finish():
            for units, s in zip(self.units, self.scatters):
                s.finish(lambda u, full, units=units: store(units[u], full))

        return [each("swap"), each("swapped", "ring_start"), each("ring_turn"), each("plane_start"), each("last"), finish]


def backward_kernel(dy_ref, mid_ref, ctx_ref, st2_ref, q_ref, k_ref, v_ref, x_ref, st1_ref, cos_ref, sin_ref, c_ref, p_hbm, slope_hbm, act_hbm,
                    qkv_hbm, wo_hbm, up_hbm, down_hbm,
                    dx_ref, attn_out, up_out, down_out, small_out, *refs):
    (grad, dctx, delta, big, wqkv, wo, slope, act, dpre, h_ref, s_a, s_b, d_a, d_b, sums,
     g_qkv, g_wo, g_up, g_down, *small_bufs), refs = refs[:28], refs[28:]
    qkv_bufs, mo_bufs, refs = [refs[5 * k:5 * k + 5] for k in range(THREE)], [refs[5 * k + 15:5 * k + 20] for k in range(THREE)], refs[30:]
    send, recv, late_sem, plane_sem, big_sem, w_sem, mlp_sem = refs
    step = pl.program_id(ZERO)
    phase, seq = step // FOUR, lax.rem(step, FOUR)
    layer = ONE - step // EIGHT
    place = Place()

    def grads(unit):
        if unit < THREE:
            return g_qkv.at[unit]
        if unit == THREE:
            return g_wo
        if unit < EIGHT:
            return g_up.at[unit - FOUR]
        return g_down.at[:, :, :, unit - EIGHT]

    live = step < SIXTEEN
    turn = jnp.where(live, ZERO, ONE)
    qkv_sums = Reduce(place, ((ZERO,), (ONE,), (TWO,)), grads, [(a, ra, rb, rp.at[turn], o) for a, ra, rb, rp, o in qkv_bufs], send.at[turn], recv.at[turn])
    mo_sums = Reduce(place, COLOURS, grads, mo_bufs, send.at[TWO], recv.at[TWO])
    small_refs = small_bufs[::THREE]
    early, middle, late = [Late(place, small_refs[i], small_bufs[THREE * i + ONE], late_sem.at[i, ZERO], late_sem.at[i, ONE], small_bufs[THREE * i + TWO],
                                plane_sem.at[i, ZERO], plane_sem.at[i, ONE]).steps() for i in range(THREE)]
    first_core = place.core == ZERO

    def store(l):
        def put(unit, full):
            if unit < EIGHT:
                mine = jnp.where(first_core, full[:FOUR], full[FOUR:])
                if unit < FOUR:
                    attn_out[l, unit] = mine
                else:
                    up_out[l, :, DIM * (unit - FOUR):DIM * (unit - THREE)] = mine
            else:
                at = EIGHT * (unit % TWO)

                @pl.when(place.core == (unit - EIGHT) // TWO)
                def _():
                    down_out[l, at:at + EIGHT] = full
        return put

    def mlp_weights(l):
        parts = [pl.ds(DIM * k, DIM) for k in range(FOUR)]
        return ([pltpu.make_async_copy(down_hbm.at[l, part], big.at[k], big_sem.at[k]) for k, part in enumerate(parts)],
                [pltpu.make_async_copy(up_hbm.at[l, :, part], big.at[FOUR + k], big_sem.at[FOUR + k]) for k, part in enumerate(parts)] +
                [pltpu.make_async_copy(wo_hbm.at[l], wo, w_sem.at[ZERO])])

    def attn_weights(l):
        return [pltpu.make_async_copy(qkv_hbm.at[l], wqkv, w_sem.at[ONE])]

    def probs(l, s):
        return [pltpu.make_async_copy(p_hbm.at[l, s, k], big.at[k], big_sem.at[k]) for k in range(HEADS)]

    def saved_mlp(l, s):
        return [pltpu.make_async_copy(slope_hbm.at[l, s], slope, mlp_sem.at[ZERO]), pltpu.make_async_copy(act_hbm.at[l, s], act, mlp_sem.at[ONE])]

    def start(copies):
        for copy in copies:
            copy.start()

    def wait(copies):
        for copy in copies:
            copy.wait()

    @pl.when(step == ZERO)
    def _():
        place.greet()
        start(mlp_weights(ONE)[ZERO] + saved_mlp(ONE, ZERO) + mlp_weights(ONE)[ONE] + attn_weights(ONE))

    pl.when(step == ONE)(place.met)
    mo_steps, qkv_steps = mo_sums.steps(store(layer)), qkv_sums.steps(store(ONE - turn))
    late_steps = mo_sums.steps(store(ONE - turn))[FOUR:]
    attn_hook = hooks(step * FOUR, list(zip(((48,), (52,), (57,), (61,)), middle)) +
                      [((when, when + 32), run) for when, run in zip((SIXTEEN, 20, 24, 30), mo_steps)])
    mlp_plan = list(zip(((37, 69), (38, 70)), late_steps))
    mlp_plan += list(zip(((32, 64), (33, 65), (38, 66), (43, 67), (47, 71), (47, 71)), qkv_steps))
    mlp_plan += [((when,), run) for when, run in zip((64, 66, 67, 70), late)]
    mlp_plan += [((when,), run) for when, run in zip((34, 37, 41, 45), early)]
    mlp_hook = hooks(step * FOUR, mlp_plan)

    @pl.when(phase % TWO == ZERO)
    def _():
        @pl.when((seq == ZERO) & live)
        def _():
            for ref in (g_wo, g_up, g_down, sums):
                ref[...] = jnp.zeros_like(ref)

        @pl.when(step < FOUR)
        def _():
            grad[seq] = dy_ref[ZERO].T

        @pl.when((seq == ZERO) & live)
        def _():
            wait(mlp_weights(layer)[ZERO])

        mlp_hook(ZERO)

        def after_first():
            pl.when(seq < THREE)(lambda: start(saved_mlp(layer, seq + ONE)))
            pl.when(seq == THREE)(lambda: start(probs(layer, ZERO)[:FOUR]))

        def before_second():
            pl.when(seq == ZERO)(lambda: wait(mlp_weights(layer)[ONE]))

        def after_second():
            pl.when(seq == THREE)(lambda: start(probs(layer, ZERO)[FOUR:]))

        pl.when(live)(lambda: wait(saved_mlp(layer, seq)))
        mlp_backward(grad.at[seq], slope, act, mid_ref, ctx_ref, st2_ref.at[ZERO], wo, big, c_ref, dctx.at[seq], delta.at[seq], g_wo, g_up, g_down,
                     dpre, h_ref, s_a, s_b, sums, pl.when(live), mlp_hook,
                     after_first, after_second, before_second)

        @pl.when((seq == THREE) & live)
        def _():
            value = columns_of([sums[i] for i in range(EIGHT)])

            @pl.when(layer == ONE)
            def _():
                small_refs[ZERO][:EIGHT, :] = value

            @pl.when(layer == ZERO)
            def _():
                small_refs[ONE][...] = value

        mlp_hook(THREE)

    @pl.when(phase % TWO == ONE)
    def _():
        @pl.when(seq == ZERO)
        def _():
            wait(attn_weights(layer))
            for ref in (g_qkv, sums):
                ref[...] = jnp.zeros_like(ref)

        @pl.when(step == FOUR)
        def _():
            start(saved_mlp(ZERO, ZERO))
        attn_hook(ZERO)

        def after_heads():
            pl.when(seq < THREE)(lambda: start(probs(layer, seq + ONE)))
            pl.when(step == 7)(lambda: start(mlp_weights(ZERO)[ZERO] + mlp_weights(ZERO)[ONE]))

        wait(probs(layer, seq))
        attn_backward(dctx.at[seq], delta.at[seq], big, q_ref, k_ref, v_ref, x_ref, st1_ref.at[ZERO], grad.at[seq], wqkv, c_ref, cos_ref, sin_ref,
                      g_qkv, dpre, h_ref, s_a, s_b, d_a, d_b, sums, attn_hook,
                      after_heads)

        @pl.when(seq == THREE)
        def _():
            value = columns_of([sums[i] for i in range(5)])

            @pl.when(layer == ONE)
            def _():
                small_refs[ZERO][EIGHT:, :] = value

            @pl.when(layer == ZERO)
            def _():
                small_refs[TWO][...] = value

        @pl.when(step == 7)
        def _():
            start(attn_weights(ZERO))

        @pl.when(step > 11)
        def _():
            dx_ref[ZERO] = grad[seq].T
        attn_hook(THREE)

    @pl.when(step == 17)
    def _():
        small_out[:SIXTEEN, :], small_out[SIXTEEN:24, :], small_out[24:, :] = [ref[...] for ref in small_refs]


def add_to(ref, value):
    ref[...] = ref[...] + value.reshape(ref.shape)


def mlp_backward(grad, slope, act, mid_ref, ctx_ref, stat_ref, wo, big, c_ref, dctx, delta, g_wo, g_up, g_down, dpre, h_ref, s_a, s_b, sums, when, hook, after_first, after_second, before_second):
    parts = [slice(DIM * k, DIM * k + DIM) for k in range(FOUR)]
    pre = (s_a, s_b)

    def dact(k):
        pre[k % TWO][...] = nn(big[k], grad[...])

    @when
    def _():
        def scale(k, chunk):
            there = slice(parts[k].start + chunk.start, parts[k].start + chunk.stop)
            value = pre[k % TWO][chunk, :] * slope[there, :]
            sums[k, chunk, :] += fold(value)
            dpre[there, :] = value.astype(BF16)

        def down_product(k):
            add_to(g_down.at[k], nt(act[parts[k], :], grad[...]))

        dact(ZERO)
        norm_to(mid_ref.at[ZERO], get_stats(stat_ref), c_ref, LN_PAR + TWO, h_ref)
        for k in range(FOUR):
            products = [functools.partial(down_product, k)]
            if k < THREE:
                products = [functools.partial(dact, k + ONE)] + products
            woven(products, [functools.partial(scale, k, chunk) for chunk in row_chunks()])
        after_first()
    hook(ONE)

    @when
    def _():
        before_second()
        s_a[...] = functools.reduce(jnp.add, [nn(big[FOUR + k], dpre[rows, :]) for k, rows in enumerate(parts)])
        after_second()
    hook(TWO)

    @when
    def _():
        def write(rows, dx):
            dy = grad[rows, :].astype(F32)
            dmid = (dy + dx).astype(BF16)
            grad[rows, :] = dmid
            sums[6, rows, :] += fold(dy)
            sums[7, rows, :] += fold(dmid.astype(F32))

        norm_back(s_a, mid_ref.at[ZERO], get_stats(stat_ref), c_ref, LN_PAR + TWO, sums, FOUR, write,
                  [lambda k=k, rows=rows: add_to(g_up.at[k], nt(h_ref[...], dpre[rows, :])) for k, rows in enumerate(parts)])
        add_to(g_wo, nt(ctx_ref[ZERO].astype(BF16), grad[...]))
        s_b[...] = nn(wo[...], grad[...])
        for head in range(HEADS):
            rows = head_rows(head)[ZERO]
            value = s_b[rows, :].astype(BF16)
            dctx[rows, :] = value
            delta[head:head + ONE, :] = total(value.astype(F32) * ctx_ref[ZERO, rows, :])


def attn_backward(dctx, delta, probs, q_ref, k_ref, v_ref, x_ref, stat_ref, grad, wqkv, c_ref, cos_ref, sin_ref, g_qkv, dproj, h_ref, s_a, s_b, d_a, d_b,
                  sums, hook, prefetch):
    scores, dscores = (s_a, s_b), (d_a, d_b)
    q, k, v = q_ref.at[ZERO], k_ref.at[ZERO], v_ref.at[ZERO]

    def open_head(head):
        rows = head_rows(head)[ZERO]
        scores[head % TWO][...] = tn(v[rows, :], dctx[rows, :])

    def weigh(head, rows):
        dscores[head % TWO][rows, :] = (probs[head, rows, :].astype(F32) * (scores[head % TWO][rows, :] - delta[head:head + ONE, :])).astype(BF16)

    def values(head):
        rows = head_rows(head)[ZERO]
        dv = nt(dctx[rows, :], probs[head])
        sums[TWO, rows, :] += fold(dv)
        dproj[TWO * DIM + rows.start:TWO * DIM + rows.stop, :] = dv.astype(BF16)

    def close_head(head, m):
        rows, one, two = head_rows(head)
        ds = dscores[head % TWO][...]
        value = nn(k[rows, :], ds) * HEAD ** -0.5 if m == ZERO else nt(q[rows, :], ds)
        cos, sin = cos_ref[...], sin_ref[...]
        a, b = value[:HALF], value[HALF:]
        for at, out in ((one, a * cos + b * sin), (two, b * cos - a * sin)):
            dproj[m * DIM + at.start:m * DIM + at.stop, :] = out.astype(BF16)
            sums[m, at, :] += fold(out)

    open_head(ZERO)
    for head in range(HEADS):
        products = [functools.partial(values, head)]
        if head:
            products = [functools.partial(close_head, head - ONE, m) for m in range(TWO)] + products
        if head + ONE < HEADS:
            products = [functools.partial(open_head, head + ONE)] + products
        woven(products, [functools.partial(weigh, head, rows) for rows in row_chunks()])
        if head == THREE:
            hook(ONE)
    for m in range(TWO):
        close_head(HEADS - ONE, m)
    prefetch()
    hook(TWO)
    norm_to(x_ref.at[ZERO], get_stats(stat_ref), c_ref, LN_PAR, h_ref)
    parts = [slice(DIM * m, DIM * m + DIM) for m in range(THREE)]
    s_a[...] = functools.reduce(jnp.add, [nn(wqkv[m], dproj[rows, :]) for m, rows in enumerate(parts)])

    def write(rows, dx):
        grad[rows, :] = (grad[rows, :].astype(F32) + dx).astype(BF16)

    norm_back(s_a, x_ref.at[ZERO], get_stats(stat_ref), c_ref, LN_PAR, sums, THREE, write,
              [lambda m=m, rows=rows: add_to(g_qkv.at[m], nt(h_ref[...], dproj[rows, :])) for m, rows in enumerate(parts)])


def backward(dy, xs, q, k, v, probs, ctx, mid, act, slope, st1, st2, c, tables, w_qkv, w_o, w_up, w_down):
    def mlp_at(s):
        s = jnp.minimum(s, 15)
        odd = s // FOUR % TWO == ONE
        return ONE - s // EIGHT, jnp.where(odd, THREE, s % FOUR), ZERO, ZERO

    def attn_at(s):
        s = jnp.minimum(s, 15)
        odd = s // FOUR % TWO == ONE
        return jnp.where(s < EIGHT, ONE, ZERO) + jnp.where((s > 7) & (s < 12), ONE, ZERO), jnp.where(odd, s % FOUR, jnp.where(s < FOUR, ZERO, THREE)), ZERO, ZERO

    per_mlp = pl.BlockSpec((None, ONE, *SQUARE), mlp_at)
    per_attn = pl.BlockSpec((None, ONE, *SQUARE), attn_at)

    def stat(at):
        return pl.BlockSpec((None, ONE, EIGHT, TOK), at)

    acc = [(*GRID, EIGHT, WIDTH)]
    scratch = [pltpu.VMEM((SEQS, *SQUARE), BF16), pltpu.VMEM((SEQS, *SQUARE), BF16), pltpu.VMEM((SEQS, HEADS, TOK), F32),
               pltpu.VMEM((HEADS, TOK, TOK), BF16), pltpu.VMEM((THREE, DIM, DIM), BF16), pltpu.VMEM((DIM, DIM), BF16),
               pltpu.VMEM(TALL, F32), pltpu.VMEM(TALL, BF16), pltpu.VMEM(TALL, BF16), pltpu.VMEM(SQUARE, BF16),
               pltpu.VMEM(SQUARE, F32), pltpu.VMEM(SQUARE, F32), pltpu.VMEM((TOK, TOK), BF16), pltpu.VMEM((TOK, TOK), BF16),
               pltpu.VMEM((EIGHT, *COLS), F32), pltpu.VMEM((THREE, *GRID, EIGHT, DIM), F32), pltpu.VMEM((*GRID, EIGHT, DIM), F32),
               pltpu.VMEM((FOUR, *GRID, EIGHT, DIM), F32), pltpu.VMEM((*GRID, FOUR, EIGHT, DIM), F32), *[pltpu.VMEM((*lead, rows, DIM), F32) for rows in (SIXTEEN, EIGHT, EIGHT) for lead in ((), (6,), (SIXTEEN,))]]
    for n in (ONE, THREE):
        for order in ORDERS:
            ring_a, ring_b, plane, other = landing_shapes(order, n)
            plane = (TWO, *plane) if n == ONE else plane
            scratch += [pltpu.VMEM(s, F32) for s in ((n, *GRID, EIGHT, WIDTH), ring_a, ring_b, plane, other)]
    scratch += [DMA((THREE, THREE, 9)), DMA((THREE, THREE, 9)), DMA((THREE, TWO, 6)), DMA((THREE, TWO)), DMA((EIGHT,)), DMA((TWO,)), DMA((TWO,))]
    outs = ((TWO, FOUR, FOUR, DIM), (TWO, FOUR, FFN), (TWO, SIXTEEN, DIM), (32, DIM))
    whole = [pl.BlockSpec(s, lambda i, n=len(s): (ZERO,) * n, pipeline_mode=pl.Buffered(ONE)) for s in outs]
    dx_at = lambda s: (jnp.clip(s - 12, ZERO, THREE), ZERO, ZERO)
    return pl.pallas_call(
        backward_kernel, grid=(18,),
        out_shape=[jax.ShapeDtypeStruct((SEQS, TOK, DIM), BF16)] + [jax.ShapeDtypeStruct(s, F32) for s in outs],
        out_specs=[pl.BlockSpec((ONE, TOK, DIM), dx_at)] + whole,
        in_specs=[pl.BlockSpec((ONE, TOK, DIM), lambda s: (jnp.minimum(s, THREE), ZERO, ZERO)), per_mlp, per_mlp, stat(mlp_at)] + [per_attn] * FOUR + [stat(attn_at),
                  once((HALF, TOK)), once((HALF, TOK)), pl.BlockSpec((None, *COLS), lambda s: (ONE - jnp.minimum(s, 15) // EIGHT, ZERO, ZERO))] + [HBM] * 7,
        scratch_shapes=scratch,
        compiler_params=pltpu.CompilerParams(collective_id=ONE, has_side_effects=True, vmem_limit_bytes=67043328,
                                             dimension_semantics=("arbitrary",)),
        name="backward")(dy, mid, ctx, st2, q, k, v, xs, st1, *tables, c, probs, slope, act, w_qkv, w_o, w_up, w_down)


def results_kernel(dx_ref, attn_ref, up_ref, down_ref, small_ref, dx_out, attn_out, gb_attn, g_ln, up_out, gb_up, down_out, gb_down):
    dx_out[...] = dx_ref[...]

    @pl.when(pl.program_id(ZERO) == ZERO)
    def _():
        me = lax.axis_index(AXIS)
        attn_out[...], up_out[...], down_out[...] = attn_ref[...], up_ref[...], down_ref[...]
        mine = pltpu.roll(small_ref[...], lax.rem(DIM - FOUR * me + FOUR * LANES, DIM), ONE)
        for l in range(TWO):
            mlp = SIXTEEN - SIXTEEN * l
            attn = mlp + EIGHT
            gb_attn[l, :THREE], gb_attn[l, THREE:] = mine[attn:attn + THREE, :FOUR], mine[mlp + 7:mlp + EIGHT, :FOUR]
            g_ln[l, :TWO], g_ln[l, TWO:] = mine[attn + THREE:attn + 5, :FOUR], mine[mlp + FOUR:mlp + 6, :FOUR]
            gb_down[l:l + ONE, :] = mine[mlp + 6:mlp + 7, :FOUR]
            ups = small_ref[pl.ds(mlp + me // 32, ONE), :]
            gb_up[l:l + ONE, :] = pltpu.roll(ups, lax.rem(DIM - SIXTEEN * lax.rem(me, 32), DIM), ONE)[:, :SIXTEEN]


def results(dx, attn, up, down, small):
    shapes = [attn.shape, (TWO, FOUR, FOUR), (TWO, FOUR, FOUR), up.shape, (TWO, SIXTEEN), down.shape, (TWO, FOUR)]
    per = pl.BlockSpec((ONE, TOK, DIM), lambda s: (s, ZERO, ZERO))
    return pl.pallas_call(
        results_kernel, grid=(SEQS,), name="results",
        out_shape=[jax.ShapeDtypeStruct(dx.shape, BF16)] + [jax.ShapeDtypeStruct(s, F32) for s in shapes],
        in_specs=[per] + [once(a.shape) for a in (attn, up, down, small)],
        out_specs=[per] + [once(s) for s in shapes])(dx, attn, up, down, small)


def solution(mesh):
    batch_spec = P(AXIS)
    weight_specs = (P(None, None, AXIS, None), P(None, None, AXIS), P(None, None, AXIS),
                    P(None, AXIS, None), P(None, AXIS), P(None, AXIS, None), P(None, AXIS))

    def device_step(x, lengths, d_y, w_attn, b_attn, ln_par, w_up, b_up, w_down, b_down):
        tables = rotary_tables()
        xs, q, k, v, probs, ctx, mid, act, slope, st1, st2, c, w_qkv, w_o, w_up, w_down = forward(
            lengths, x, tables, (w_attn, b_attn, ln_par, w_up, b_up, w_down, b_down))
        return results(*backward(d_y, xs, q, k, v, probs, ctx, mid, act, slope, st1, st2, c, tables, w_qkv, w_o, w_up, w_down))

    return jax.shard_map(device_step, mesh=mesh,
                         in_specs=(batch_spec, batch_spec, batch_spec) + weight_specs,
                         out_specs=(batch_spec,) + weight_specs,
                         check_vma=False)
```

```python
import math
import functools
import jax
import jax.numpy as jnp
from jax import lax
from jax.experimental import pallas as pl
from jax.experimental.pallas import tpu as pltpu
from jax.sharding import PartitionSpec as P

ZERO, ONE, TWO, THREE, FOUR = range(5)
EIGHT, SIXTEEN, WIDTH = 8, 16, 256

F32, BF16 = jnp.float32, jnp.bfloat16
SEQS, TOK, DIM, FFN, HEADS, HEAD, LANES = FOUR, 512, 512, 2048, EIGHT, 64, 128
HALF = HEAD // TWO
EPS = 1e-5
THETA = 10000.0
NEG_BIG = -1e30
B_ATTN, LN_PAR, B_UP, B_DOWN = ZERO, FOUR, EIGHT, 12


def nn(a, b):
    return lax.dot_general(a, b, (((ONE,), (ZERO,)), ((), ())), preferred_element_type=F32)


def nt(a, b):
    return lax.dot_general(a, b, (((ONE,), (ONE,)), ((), ())), preferred_element_type=F32)


def tn(a, b):
    return lax.dot_general(a, b, (((ZERO,), (ZERO,)), ((), ())), preferred_element_type=F32)


def lane_tiles(width=TOK, size=LANES):
    return [slice(i, i + size) for i in range(ZERO, width, size)]


def row_chunks(rows=DIM, size=64):
    return [slice(i, i + size) for i in range(ZERO, rows, size)]


def column(c_ref, rows, lane):
    return jnp.broadcast_to(c_ref[rows, lane:lane + ONE], (rows.stop - rows.start, TOK))


def total(value):
    return jnp.sum(value, axis=ZERO, keepdims=True)


def norm_stats(x_ref):
    mean = functools.reduce(jnp.add, [total(x_ref[rows, :].astype(F32)) for rows in row_chunks()]) * (1.0 / DIM)
    squares = []
    for rows in row_chunks():
        centred = x_ref[rows, :].astype(F32) - mean
        squares.append(total(centred * centred))
    return mean, lax.rsqrt(functools.reduce(jnp.add, squares) * (1.0 / DIM) + EPS)


def norm_to(x_ref, stats, c_ref, lane, h_ref):
    mean, rstd = stats
    for rows in row_chunks():
        xhat = (x_ref[rows, :].astype(F32) - mean) * rstd
        h_ref[rows, :] = (xhat * column(c_ref, rows, lane) + column(c_ref, rows, lane + ONE)).astype(BF16)


def put_stats(ref, stats):
    ref[ZERO:ONE, :], ref[ONE:TWO, :] = stats


def get_stats(ref):
    return ref[ZERO:ONE, :], ref[ONE:TWO, :]


def woven(products, rest):
    done = ZERO
    for n, step in enumerate(rest):
        while done < len(products) and done * len(rest) <= n * len(products):
            products[done]()
            done += ONE
        step()
    for product in products[done:]:
        product()


def fold(value):
    parts = [value[:, cols] for cols in lane_tiles(value.shape[ONE])]
    return functools.reduce(jnp.add, parts)


def seq_spec(shape):
    return pl.BlockSpec((ONE, *shape), lambda s: (s,) + (ZERO,) * len(shape))


def once(shape):
    return pl.BlockSpec(shape, lambda s: (ZERO,) * len(shape), pipeline_mode=pl.Buffered(ONE))


def act_shape(rows, dtype):
    return jax.ShapeDtypeStruct((SEQS, rows, TOK), dtype)


PARAMS = pltpu.CompilerParams(vmem_limit_bytes=60 << 20, dimension_semantics=("arbitrary",))
SQUARE, TALL, WIDE, COLS = (DIM, TOK), (FFN, TOK), (DIM, FFN), (DIM, LANES)


def rotary_tables():
    inv_freq = 1.0 / (THETA ** (jnp.arange(HALF, dtype=F32) * (2.0 / HEAD)))
    angles = inv_freq[:, None] * jnp.arange(TOK, dtype=F32)[None, :]
    return jnp.cos(angles), jnp.sin(angles)


MESH = pl.DeviceIdType.MESH
AXIS = "fsdp"
ORDERS = ((TWO, ONE, ZERO), (ONE, ZERO, TWO), (ZERO, TWO, ONE))


class Place:
    def __init__(self):
        me = lax.axis_index(AXIS)
        self.core = lax.rem(me, TWO)
        self.pos = (me // 32, lax.rem(me // EIGHT, FOUR), lax.rem(me // TWO, FOUR))
        self.partner = me + ONE - TWO * self.core
        self.near = [[lax.rem(at + delta, FOUR) if delta else at for delta in range(FOUR)] for at in self.pos]

    def coord(self, dim, delta):
        if isinstance(delta, int):
            return self.near[dim][delta % FOUR]
        return lax.rem(self.pos[dim] + delta, FOUR)

    def device(self, offsets):
        pos = [self.coord(dim, offsets.get(dim, ZERO)) for dim in range(THREE)]
        return pos[ZERO] * 32 + pos[ONE] * EIGHT + pos[TWO] * TWO + self.core

    def greet(self):
        barrier = pltpu.get_barrier_semaphore()
        for i in range(ONE, 64):
            offsets = {ZERO: i // SIXTEEN, ONE: i // FOUR % FOUR, TWO: i % FOUR}
            if min(offsets.values()) == ZERO:
                pl.semaphore_signal(barrier, inc=ONE, device_id=(self.device(offsets),), device_id_type=MESH)
        pl.semaphore_signal(barrier, inc=ONE, device_id=(self.partner,), device_id_type=MESH)

    def met(self):
        pl.semaphore_wait(pltpu.get_barrier_semaphore(), 37)


def remote(src, dst, send_sem, recv_sem, device):
    return pltpu.make_async_remote_copy(src_ref=src, dst_ref=dst, send_sem=send_sem, recv_sem=recv_sem,
                                        device_id=(device,), device_id_type=MESH)


LINE = (ONE, -ONE, TWO)


def each_of_plane(order, run):
    @pl.loop(ZERO, FOUR)
    def _(high):
        for low in range(FOUR):
            step = functools.partial(run, FOUR * high + low, {order[ONE]: high, order[TWO]: low})
            if low:
                step()
            else:
                pl.when(high > ZERO)(step)


class Gather:
    def __init__(self, place, buf, fifteen, order, send, recv):
        self.place, self.buf, self.fifteen, self.order, self.send, self.recv = place, buf, fifteen, order, send, recv

    def block(self, offsets, whole=()):
        index = [slice(ZERO, FOUR) if dim in whole else pl.ds(self.place.coord(dim, offsets.get(dim, ZERO)), ONE) for dim in range(THREE)]
        return self.buf.at[index[ZERO], index[ONE], index[TWO], pl.ds(self.place.core, ONE)]

    def copy(self, ref, key, device):
        return remote(ref, ref, self.send.at[key], self.recv.at[key], device)

    def plane_start(self):
        each_of_plane(self.order, lambda k, offsets: self.copy(self.block({}), ZERO, self.place.device(offsets)).start())

    def plane_all(self):
        return self.copy(self.fifteen, ZERO, self.place.partner)

    def plane_wait(self):
        self.plane_all().wait_recv()

    def line(self, i, sign):
        offsets = {self.order[ZERO]: sign * LINE[i]}
        return self.block(offsets, self.order[ONE:])

    def line_start(self):
        for i, delta in enumerate(LINE):
            self.copy(self.line(i, ZERO), ONE + i, self.place.device({self.order[ZERO]: delta})).start()

    def line_wait(self):
        for i in range(THREE):
            self.copy(self.line(i, -ONE), ONE + i, self.place.partner).wait_recv()

    def share(self, core):
        return self.copy(self.buf.at[:, :, :, pl.ds(core, ONE)], FOUR, self.place.partner)

    def share_start(self):
        self.share(self.place.core).start()

    def end(self):
        self.share(ONE - self.place.core).wait_recv()
        self.plane_all().wait_send()
        for i in range(THREE):
            self.copy(self.line(i, ZERO), ONE + i, self.place.partner).wait_send()
        self.share(self.place.core).wait_send()


def gather_steps(gathers):
    def each(*names):
        def step():
            for name in names:
                for g in gathers:
                    getattr(g, name)()
        return step

    return [each("plane_start"), each("plane_wait", "line_start"), each("line_wait", "share_start"), each("end")]


class Scatter:
    def __init__(self, place, grads, acc, got_a, got_b, got_p, mine, other, order, send, recv):
        self.place, self.grads, self.acc, self.order = place, grads, acc, order
        self.got_a, self.got_b, self.got_p, self.mine, self.other, self.send, self.recv = got_a, got_b, got_p, mine, other, send, recv
        self.units = acc.shape[ZERO]

    def columns(self, core):
        return pl.ds(pl.multiple_of(core * WIDTH, WIDTH), WIDTH)

    def swap_copy(self, u):
        place = self.place
        return remote(self.grads(u).at[:, :, :, :, self.columns(ONE - place.core)], self.acc.at[u], self.send.at[6 + u], self.recv.at[6 + u], place.partner)

    def swap(self):
        for u in range(self.units):
            self.swap_copy(u).start()

    def swapped(self):
        for u in range(self.units):
            self.swap_copy(u).wait()
            grad, acc = self.grads(u), self.acc

            @pl.loop(ZERO, FOUR)
            def _(z):
                acc[u, z] = acc[u, z] + grad[z, :, :, :, self.columns(self.place.core)]

    def part(self, delta, half=None):
        index = [slice(ZERO, FOUR)] * THREE
        index[self.order[ZERO]] = pl.ds(self.place.coord(self.order[ZERO], delta), ONE)
        return self.acc.at[:, index[ZERO], index[ONE], index[TWO], :, slice(ZERO, WIDTH) if half is None else lane_tiles()[half]]

    def ring(self, step, way):
        delta = (ONE, -ONE)[way]
        device = self.place.device({self.order[ZERO]: delta})
        if step == ZERO:
            src, dst = self.part(TWO, way), self.got_a.at[:, :, :, :, :, lane_tiles()[way]]
        else:
            src, dst = self.part(delta), self.got_b.at[way]
        key = TWO * step + way
        return remote(src, dst, self.send.at[key], self.recv.at[key], device)

    def ring_start(self):
        for way in range(TWO):
            self.ring(ZERO, way).start()

    def ring_turn(self):
        for way in range(TWO):
            self.ring(ZERO, way).wait_recv()
            self.add((ONE, -ONE)[way], way, self.got_a)
            self.ring(ONE, way).start()

    def add(self, delta, half, *refs):
        dim, acc = self.order[ZERO], self.acc
        at = self.place.coord(dim, delta)
        columns = slice(ZERO, WIDTH) if half is None else lane_tiles()[half]

        @pl.loop(ZERO, FOUR)
        def _(i):
            index = [i if d == self.order[ONE] else slice(ZERO, FOUR) for d in range(THREE)]
            there = [slice(None), *index, slice(None), columns]
            here = list(there)
            here[ONE + dim] = pl.ds(at, ONE)
            there[ONE + dim] = slice(ZERO, ONE)
            value = acc[tuple(here)]
            for ref in refs:
                value = value + ref[tuple(there)]
            acc[tuple(here)] = value

    def plane_copy(self, k, offsets):
        index = [pl.ds(self.place.coord(dim, offsets.get(dim, ZERO)), ONE) for dim in range(THREE)]
        src = self.acc.at[:, index[ZERO], index[ONE], index[TWO]]
        return remote(src, self.got_p.at[k], self.send.at[FOUR], self.recv.at[FOUR], self.place.device(offsets))

    def plane_all(self):
        return remote(self.got_p.at[ONE:], self.got_p.at[ONE:], self.send.at[FOUR], self.recv.at[FOUR], self.place.partner)

    def plane_start(self):
        for way in range(TWO):
            self.ring(ONE, way).wait_recv()
        self.add(ZERO, None, self.got_b.at[ZERO], self.got_b.at[ONE])

        each_of_plane(self.order, lambda k, offsets: self.plane_copy(k, offsets).start())

    def own(self):
        z, y, x = [pl.ds(p, ONE) for p in self.place.pos]
        return self.acc.at[:, z, y, x]

    def last_copy(self):
        return remote(self.mine, self.other, self.send.at[5], self.recv.at[5], self.place.partner)

    def last(self):
        self.plane_all().wait_recv()
        self.mine[...] = functools.reduce(jnp.add, [self.got_p[k] for k in range(ONE, SIXTEEN)], self.own()[...])
        for step in range(TWO):
            for way in range(TWO):
                self.ring(step, way).wait_send()
        self.plane_all().wait_send()
        self.last_copy().start()

    def finish(self, store):
        self.last_copy().wait_recv()
        first = self.place.core == ZERO
        for u in range(self.units):
            own, came = self.mine[u, ZERO, ZERO, ZERO], self.other[u, ZERO, ZERO, ZERO]
            store(u, jnp.concatenate([jnp.where(first, own, came), jnp.where(first, came, own)], axis=ONE))
        self.last_copy().wait_send()


def landing_shapes(order, units):
    size = [FOUR, FOUR, FOUR]
    size[order[ZERO]] = ONE
    return (units, *size, EIGHT, WIDTH), (TWO, units, *size, EIGHT, WIDTH), (SIXTEEN, units, ONE, ONE, ONE, EIGHT, WIDTH), (units, ONE, ONE, ONE, EIGHT, WIDTH), (units, ONE, ONE, ONE, EIGHT, WIDTH)


class Small:
    def __init__(self, place, value, slots, send, recv):
        self.place, self.value, self.slots, self.send, self.recv = place, value, slots, send, recv

    def peers(self, stage):
        if stage == THREE:
            return [self.place.partner]
        return [self.place.device({stage: delta}) for delta in LINE]

    def copies(self, stage):
        return [remote(self.value, self.slots.at[THREE * stage + k], self.send.at[THREE * stage + k], self.recv.at[THREE * stage + k], peer)
                for k, peer in enumerate(self.peers(stage))]

    def start(self, stage):
        for copy in self.copies(stage):
            copy.start()

    def finish(self, stage):
        copies = self.copies(stage)
        for copy in copies:
            copy.wait()
        self.value[...] = functools.reduce(jnp.add, [self.slots[THREE * stage + k] for k in range(len(copies))], self.value[...])

    def turn(self, stage):
        def step():
            self.finish(stage)
            self.start(stage + ONE)
        return step

    def steps(self):
        return [lambda: self.start(ZERO), self.turn(ZERO), self.turn(ONE), self.turn(TWO), lambda: self.finish(THREE)]


class Late(Small):
    def __init__(self, place, value, slots, send, recv, planes, plane_send, plane_recv):
        super().__init__(place, value, slots, send, recv)
        self.planes, self.plane_send, self.plane_recv = planes, plane_send, plane_recv

    def peers(self, stage):
        return super().peers({ZERO: ORDERS[ZERO][ZERO], ONE: THREE}[stage])

    def plane(self, k, offsets):
        return remote(self.value, self.planes.at[k], self.plane_send, self.plane_recv, self.place.device(offsets))

    def steps(self):
        def first():
            each_of_plane(ORDERS[ZERO], lambda k, offsets: self.plane(k, offsets).start())

        def second():
            remote(self.planes.at[ONE:], self.planes.at[ONE:], self.plane_send, self.plane_recv, self.place.partner).wait()
            self.value[...] = functools.reduce(jnp.add, [self.planes[k] for k in range(ONE, SIXTEEN)], self.value[...])
            self.start(ZERO)

        return [first, second, self.turn(ZERO), lambda: self.finish(ONE)]


VMEM = pl.BlockSpec(memory_space=pltpu.VMEM)
HBM = pl.BlockSpec(memory_space=pl.ANY)
DMA = pltpu.SemaphoreType.DMA


COLOURS = ((THREE, FOUR, 5), (6, 7, EIGHT), (9, 10, 11))
GRID = (FOUR, FOUR, FOUR)


def spread(buf, u, out_ref, column_base):
    @pl.loop(ZERO, EIGHT)
    def _(block):
        for part in range(FOUR):
            g = block * FOUR + part
            tiles = [buf[block // TWO, lax.rem(block, TWO) * TWO + part // TWO, part % TWO * TWO + k // TWO, k % TWO, u].astype(F32) for k in range(FOUR)]
            rows = pl.ds(pl.multiple_of(g * SIXTEEN, SIXTEEN), SIXTEEN)
            for j, cols in enumerate(lane_tiles()):
                value = jnp.concatenate([t[FOUR * j:FOUR * j + FOUR] for t in tiles], axis=ZERO).astype(BF16)
                out_ref[rows, column_base + cols.start:column_base + cols.stop] = value


def spread_down(buf, u, out_ref, cols):
    @pl.loop(ZERO, SIXTEEN)
    def _(i):
        for k in range(EIGHT):
            d = i * EIGHT + k
            out_ref[pl.ds(pl.multiple_of(d * SIXTEEN, SIXTEEN), SIXTEEN), cols] = buf[i // FOUR, lax.rem(i, FOUR), k // TWO, k % TWO, u]


def same(shape, test):
    row = lax.broadcasted_iota(jnp.int32, shape, ZERO)
    col = lax.broadcasted_iota(jnp.int32, shape, ONE)
    return jnp.where(test(row, col), 1.0, 0.0)


def small_columns(small_ref, c_ref):
    rows = [small_ref[z, y, x, c, ZERO] for z in range(FOUR) for y in range(FOUR) for x in range(FOUR) for c in range(TWO)]
    table = jnp.concatenate(rows, axis=ZERO).astype(BF16)
    quads = nn(same((DIM, LANES), lambda r, c: r // FOUR == c).astype(BF16), table)
    quads = (quads * same((DIM, LANES), lambda r, c: r % FOUR == c % FOUR)).astype(BF16)
    mask = same((DIM, LANES), lambda r, c: r % SIXTEEN == c % SIXTEEN)
    pick = same((DIM, 32), lambda r, c: r // SIXTEEN == c).astype(BF16)
    ups = [(nn(pick, table[32 * k:32 * k + 32]) * mask).astype(BF16) for k in range(FOUR)]
    for layer in range(TWO):
        def is_up(r):
            return r // SIXTEEN == layer * FOUR + TWO

        value = nn(quads, same((LANES, LANES), lambda r, c: (r // 64 == layer) & (r % 64 // FOUR == c) & ~is_up(r)).astype(BF16))
        for k in range(FOUR):
            value = value + nn(ups[k], same((LANES, LANES), lambda r, c: is_up(r) & (c == B_UP + k)).astype(BF16))
        c_ref[layer] = value


def tile_of(rows):
    rows = rows.astype(F32)
    return jnp.concatenate([rows[:, cols] for cols in lane_tiles()], axis=ZERO).astype(BF16)


def small_row(b_attn, ln_par, b_up, b_down):
    lane = lax.broadcasted_iota(jnp.int32, (ONE, LANES), ONE)
    row = jnp.zeros((ONE, LANES), F32)
    pieces = []
    for l in range(TWO):
        for m in range(FOUR):
            pieces += [(b_attn[l, m:m + ONE, :], 64 * l + FOUR * m), (ln_par[l, m:m + ONE, :], 64 * l + FOUR * m + SIXTEEN)]
        pieces += [(b_up[l:l + ONE, :], 64 * l + 32), (b_down[l:l + ONE, :], 64 * l + 48)]
    for piece, at in pieces:
        n = piece.shape[ONE]
        wide = jnp.concatenate([piece.astype(F32), jnp.zeros((ONE, LANES - n), F32)], axis=ONE)
        wide = pltpu.roll(wide, at, ONE) if at else wide
        row = jnp.where((lane >= at) & (lane < at + n), wide, row)
    return row


def hooks(slot, plan):
    def hook(at):
        for slots, run in plan:
            mine = [when for when in slots if when % FOUR == at]
            if mine:
                pl.when(functools.reduce(jnp.logical_or, [slot + at == when for when in mine]))(run)
    return hook


def forward_kernel(len_ref, x_hbm, cos_ref, sin_ref, w_attn, b_attn, ln_par, w_up, b_up, w_down, b_down,
                   xs_out, q_ref, k_ref, v_ref, p_hbm, ctx_ref, mid_ref, act_ref, slope_ref, st1_ref, st2_ref, c_ref,
                   nat_qkv, nat_wo, nat_up, nat_down,
                   xs, ctxb, wqkv, wo, up, down, n_qkv, n_wo, n_up, n_down, p_buf, h_ref, s_a, s_b, s_c,
                   sbuf, q0, q1, q2, m0, m1, m2, stats, f0, f1, f2, send, recv, p_sem, nat_sem, x_sem):
    step = pl.program_id(ZERO)
    phase, seq, layer = step // FOUR, lax.rem(step, FOUR), step // EIGHT
    place = Place()
    z, y, x = place.pos
    qkv_bufs, mo_bufs, fifteen = (q0, q1, q2), (m0, m1, m2), (f0, f1, f2)

    def group(bufs, base, l):
        return [Gather(place, b.at[l], fifteen[base // THREE], ORDERS[k], send.at[base + k, l], recv.at[base + k, l]) for k, b in enumerate(bufs)]

    little = Gather(place, sbuf, fifteen[TWO], ORDERS[ZERO], send.at[6, ZERO], recv.at[6, ZERO])

    def nat_copies(which, l):
        if which == ZERO:
            return [pltpu.make_async_copy(n_qkv, nat_qkv.at[l], nat_sem.at[ZERO])]
        return [pltpu.make_async_copy(src, dst.at[l], nat_sem.at[ONE + i]) for i, (src, dst) in enumerate(((n_wo, nat_wo), (n_up, nat_up), (n_down, nat_down)))]

    def wait(copies):
        for copy in copies:
            copy.wait()

    def start(copies):
        for copy in copies:
            copy.start()

    def take_qkv():
        pl.when(step > ZERO)(lambda: wait(nat_copies(ZERO, layer)))
        for m in range(THREE):
            spread(qkv_bufs[m].at[layer], ZERO, n_qkv.at[m], ZERO)
            wqkv[m] = n_qkv[m].T
        start(nat_copies(ZERO, layer))

    def take_mo():
        pl.when(step > EIGHT)(lambda: wait(nat_copies(ONE, layer)))
        for colour in range(THREE):
            for u, unit in enumerate(COLOURS[colour]):
                buf = mo_bufs[colour].at[layer]
                if unit == THREE:
                    spread(buf, u, n_wo, ZERO)
                    wo[...] = n_wo[...].T
                elif unit < EIGHT:
                    part = slice(DIM * (unit - FOUR), DIM * (unit - THREE))
                    spread(buf, u, n_up, part.start)
                    up[part, :] = n_up[:, part].T
                else:
                    spread_down(buf, u, n_down, lane_tiles()[unit - EIGHT])
        for k in range(FOUR):
            part = slice(DIM * k, DIM * k + DIM)
            down[:, part] = n_down[part, :].T
        start(nat_copies(ONE, layer))

    x_copies = [pltpu.make_async_copy(x_hbm.at[s], ctxb.at[s], x_sem.at[s]) for s in range(SEQS)]

    @pl.when(step == ZERO)
    def _():
        place.greet()
        start(x_copies)
        for l in range(TWO):
            for unit in range(12):
                if unit < FOUR:
                    tile = tile_of(w_attn[l, unit])
                elif unit < EIGHT:
                    tile = tile_of(w_up[l, :, DIM * (unit - FOUR):DIM * (unit - THREE)])
                else:
                    tile = w_down[l, :, lane_tiles()[unit - EIGHT]]
                if unit < THREE:
                    qkv_bufs[unit][l, z, y, x, place.core, ZERO] = tile
                else:
                    mo_bufs[(unit - THREE) // THREE][l, z, y, x, place.core, (unit - THREE) % THREE] = tile
        sbuf[z, y, x, place.core, ZERO] = small_row(b_attn, ln_par, b_up, b_down)
        first, second = gather_steps(group(qkv_bufs, ZERO, ZERO) + [little]), gather_steps(group(mo_bufs, THREE, ZERO))

        def ready(s):
            x_copies[s].wait()
            xs[s] = ctxb[s].T
            put_stats(stats.at[s], norm_stats(xs.at[s]))

        place.met()
        first[ZERO]()
        second[ZERO]()
        ready(ZERO)
        ready(ONE)
        first[ONE]()
        ready(TWO)
        ready(THREE)
        first[TWO]()
        second[ONE]()
        first[THREE]()
        small_columns(sbuf, c_ref)

    attn_hook = hooks(step * FOUR, [((when, when + 32), run) for when, run in zip((9, 13), gather_steps(group(mo_bufs, THREE, layer))[TWO:])])
    mlp_steps = gather_steps(group(qkv_bufs, ZERO, ONE)) + gather_steps(group(mo_bufs, THREE, ONE))[:TWO]
    mlp_hook = hooks(step * FOUR, [((when,), run) for when, run in zip((SIXTEEN, 25, 30, 31, 17, 26), mlp_steps)])

    @pl.when(phase % TWO == ZERO)
    def _():
        pl.when(seq == ZERO)(take_qkv)

        @pl.when(step < FOUR)
        def _():
            xs_out[ZERO, ZERO] = xs[seq]

        @pl.when(step > 7)
        def _():
            put_stats(stats.at[seq], norm_stats(xs.at[seq]))

        attn_hook(ZERO)
        copies = [pltpu.make_async_copy(p_buf.at[head], p_hbm.at[layer, seq, head], p_sem.at[head]) for head in range(HEADS)]
        attn_forward(len_ref[seq], xs.at[seq], wqkv, c_ref.at[layer], cos_ref, sin_ref, q_ref.at[ZERO, ZERO], k_ref.at[ZERO, ZERO],
                     v_ref.at[ZERO, ZERO], p_buf, ctx_ref.at[ZERO, ZERO], ctxb.at[seq], get_stats(stats.at[seq]), st1_ref.at[ZERO, ZERO], h_ref, s_a, s_b, s_c, attn_hook,
                     lambda heads: pl.when(step > ZERO)(lambda: wait(copies[heads])), lambda heads: start(copies[heads]))
        pl.when(step == 11)(lambda: wait(copies))
        attn_hook(THREE)

    @pl.when(phase % TWO == ONE)
    def _():
        pl.when(seq == ZERO)(take_mo)
        mlp_hook(ZERO)
        mlp_forward(layer, ctxb.at[seq], xs.at[seq], wo, up, down, c_ref.at[layer], mid_ref.at[ZERO, ZERO], act_ref.at[ZERO, ZERO], slope_ref.at[ZERO, ZERO],
                    st2_ref.at[ZERO, ZERO], h_ref, s_a, s_b, mlp_hook)

        @pl.when(layer == ZERO)
        def _():
            xs_out[ZERO, ZERO] = xs[seq]
        mlp_hook(THREE)

    @pl.when(step == 15)
    def _():
        for which in range(TWO):
            wait(nat_copies(which, ONE))


def attn_forward(length, xt, w, c_ref, cos_ref, sin_ref, q_ref, k_ref, v_ref, p_buf, ctx_ref, ctxb, stats, stat_ref, h_ref, s_a, s_b, s_c, hook, free, ship):
    put_stats(stat_ref, stats)
    norm_to(xt, stats, c_ref, LN_PAR, h_ref)
    for m, acc in enumerate((s_a, s_b, s_c)):
        acc[...] = nn(w[m], h_ref[...])
    cos, sin = cos_ref[...], sin_ref[...]
    for m, (acc, out) in enumerate(((s_a, q_ref), (s_b, k_ref), (s_c, v_ref))):
        for head in range(HEADS):
            rows, one, two = head_rows(head)
            if m == TWO:
                out[rows, :] = (acc[rows, :] + column(c_ref, rows, B_ATTN + m)).astype(BF16)
                continue
            a, b = [acc[half, :] + column(c_ref, half, B_ATTN + m) for half in (one, two)]
            if m == ZERO:
                a, b = a * HEAD ** -0.5, b * HEAD ** -0.5
            out[one, :] = (a * cos - b * sin).astype(BF16)
            out[two, :] = (b * cos + a * sin).astype(BF16)
    hook(ONE)
    halves = slice(ZERO, FOUR), slice(FOUR, EIGHT)
    free(halves[ZERO])
    key = lax.broadcasted_iota(jnp.int32, (SIXTEEN, TOK), ONE)
    row = lax.broadcasted_iota(jnp.int32, (SIXTEEN, TOK), ZERO)
    bias_rows = jnp.where((row == ZERO) & (key >= length), NEG_BIG, 0.0).astype(BF16)
    one_rows = jnp.where(row == ZERO, 1.0, 0.0).astype(BF16)
    scores = (s_a, s_b)

    def open_head(head):
        rows = head_rows(head)[ZERO]
        keys = jnp.concatenate([k_ref[rows, :], bias_rows], axis=ZERO)
        queries = jnp.concatenate([q_ref[rows, :], one_rows], axis=ZERO)
        scores[head % TWO][...] = tn(keys, queries)

    def weigh(head):
        value, tops, sums = scores[head % TWO], [], []

        def top(rows):
            tops.append(jnp.max(value[rows, :], axis=ZERO, keepdims=True))
            if rows.stop == TOK:
                tops[:] = [functools.reduce(jnp.maximum, tops)]

        def power(rows):
            weight = jnp.exp(value[rows, :] - tops[ZERO])
            value[rows, :] = weight
            sums.append(total(weight))
            if rows.stop == TOK:
                sums[:] = [1.0 / functools.reduce(jnp.add, sums)]

        def share(rows):
            p_buf[head, rows, :] = (value[rows, :] * sums[ZERO]).astype(BF16)

        return [functools.partial(run, rows) for run in (top, power, share) for rows in row_chunks()]

    def close_head(head):
        rows = head_rows(head)[ZERO]
        ctx = nn(v_ref[rows, :], p_buf[head])
        ctx_ref[rows, :] = ctx
        ctxb[rows, :] = ctx.astype(BF16)

    open_head(ZERO)
    for head in range(HEADS):
        products = [functools.partial(open_head, head + ONE)] if head + ONE < HEADS else []
        if head:
            products.append(functools.partial(close_head, head - ONE))
        woven(products, weigh(head))
        if head == THREE:
            ship(halves[ZERO])
            hook(TWO)
            free(halves[ONE])
    close_head(HEADS - ONE)
    ship(halves[ONE])


def mlp_forward(layer, ctxb, xt, wo, up, down, c_ref, mid_ref, act_ref, slope_ref, stat_ref, h_ref, s_a, s_b, hook):
    s_a[...] = nn(wo[...], ctxb[...])
    for rows in row_chunks():
        mid_ref[rows, :] = (xt[rows, :].astype(F32) + s_a[rows, :] + column(c_ref, rows, B_ATTN + THREE)).astype(BF16)
    stats = norm_stats(mid_ref)
    put_stats(stat_ref, stats)
    norm_to(mid_ref, stats, c_ref, LN_PAR + TWO, h_ref)
    hook(ONE)
    pre = (s_a, s_b)
    parts = [slice(DIM * k, DIM * k + DIM) for k in range(FOUR)]

    def open_part(k):
        pre[k % TWO][...] = nn(up[parts[k], :], h_ref[...])

    open_part(ZERO)
    for k, part in enumerate(parts):
        if k < THREE:
            open_part(k + ONE)
        for rows in row_chunks():
            value = pre[k % TWO][rows, :] + column(c_ref, rows, B_UP + k)
            scaled = value * math.sqrt(0.5)
            cdf = 0.5 + 0.5 * lax.erf(scaled)
            density = jnp.exp2(scaled * scaled * -math.log2(math.e) - 0.5 * math.log2(2.0 * math.pi))
            there = slice(part.start + rows.start, part.start + rows.stop)
            act_ref[there, :] = (value * cdf).astype(BF16)
            slope_ref[there, :] = cdf + value * density
        if k == ONE:
            hook(TWO)

    @pl.when(layer == ZERO)
    def _():
        s_a[...] = nn(down[...], act_ref[...])
        for rows in row_chunks():
            xt[rows, :] = (mid_ref[rows, :].astype(F32) + s_a[rows, :] + column(c_ref, rows, B_DOWN)).astype(BF16)


def forward(lengths, x, tables, params):
    def saved(index, rows, dtype):
        return jax.ShapeDtypeStruct((TWO, SEQS, rows, TOK), dtype), pl.BlockSpec((ONE, ONE, rows, TOK), index)

    def attn_at(s):
        return s // EIGHT, jnp.where(s // FOUR % TWO == ZERO, s % FOUR, THREE), ZERO, ZERO

    def mlp_at(s):
        odd = s // FOUR % TWO == ONE
        return jnp.where(s < 12, ZERO, ONE), jnp.where(odd, s % FOUR, jnp.where(s < FOUR, ZERO, THREE)), ZERO, ZERO

    def xs_at(s):
        return jnp.where(s < FOUR, ZERO, ONE), jnp.where(s < EIGHT, s % FOUR, THREE), ZERO, ZERO

    outs = [saved(xs_at, DIM, BF16)] + [saved(attn_at, DIM, BF16)] * THREE
    outs += [(jax.ShapeDtypeStruct((TWO, SEQS, HEADS, TOK, TOK), BF16), HBM), saved(attn_at, DIM, F32)]
    outs += [saved(mlp_at, DIM, BF16), saved(mlp_at, FFN, BF16), saved(mlp_at, FFN, F32), saved(attn_at, EIGHT, F32), saved(mlp_at, EIGHT, F32)]
    outs += [(jax.ShapeDtypeStruct((TWO, *COLS), F32), once((TWO, *COLS)))]
    weights = ((THREE, DIM, DIM), (DIM, DIM), (DIM, FFN), (FFN, DIM))
    outs += [(jax.ShapeDtypeStruct((TWO, *w), BF16), HBM) for w in weights]
    scratch = [(SEQS, *SQUARE), (SEQS, *SQUARE), weights[ZERO], weights[ONE], weights[THREE], weights[TWO], *weights, (HEADS, TOK, TOK), SQUARE]
    scratch = [pltpu.VMEM(s, BF16) for s in scratch] + [pltpu.VMEM(SQUARE, F32)] * THREE + [pltpu.VMEM((*GRID, TWO, ONE, ONE, LANES), F32)]
    scratch += [pltpu.VMEM((TWO, *GRID, TWO, n, SIXTEEN, LANES), BF16) for n in (ONE, THREE) for _ in range(THREE)]
    scratch += [pltpu.VMEM((SEQS, EIGHT, TOK), F32)] + [pltpu.VMEM((15, n, SIXTEEN, LANES), BF16) for n in (ONE, THREE)]
    scratch += [pltpu.VMEM((15, ONE, ONE, LANES), F32), DMA((7, TWO, 5)), DMA((7, TWO, 5)), DMA((HEADS,)), DMA((FOUR,)), DMA((SEQS,))]
    return pl.pallas_call(
        forward_kernel, grid=(SIXTEEN,),
        out_shape=[o[ZERO] for o in outs], out_specs=[o[ONE] for o in outs],
        in_specs=[pl.BlockSpec(memory_space=pltpu.SMEM), HBM, once((HALF, TOK)), once((HALF, TOK))] + [once(p.shape) for p in params],
        scratch_shapes=scratch,
        compiler_params=pltpu.CompilerParams(collective_id=ZERO, has_side_effects=True, vmem_limit_bytes=67043328,
                                             dimension_semantics=("arbitrary",)),
        name="forward")(lengths, x, *tables, *params)


def norm_back(dh_ref, x_ref, stats, c_ref, lane, sums, at, write, beside):
    mean, rstd = stats
    means = [0.0, 0.0]

    def both(rows):
        dh = dh_ref[rows, :]
        return dh, dh * column(c_ref, rows, lane), (x_ref[rows, :].astype(F32) - mean) * rstd

    def first(rows):
        dh, dxhat, xhat = both(rows)
        means[ZERO], means[ONE] = means[ZERO] + total(dxhat), means[ONE] + total(dxhat * xhat)
        sums[at, rows, :] += fold(dh * xhat)
        sums[at + ONE, rows, :] += fold(dh)

    def second(rows):
        dh, dxhat, xhat = both(rows)
        write(rows, rstd * (dxhat - means[ZERO] * (1.0 / DIM) - xhat * (means[ONE] * (1.0 / DIM))))

    woven(beside, [functools.partial(run, rows) for run in (first, second) for rows in row_chunks()])


def columns_of(partials):
    lane = lax.broadcasted_iota(jnp.int32, COLS, ONE)
    value = jnp.zeros(COLS, F32)
    for at, partial in enumerate(partials):
        value = jnp.where(lane == at, jnp.sum(partial, axis=ONE, keepdims=True), value)
    return value.T[:EIGHT]


def head_rows(head):
    return slice(HEAD * head, HEAD * head + HEAD), slice(HEAD * head, HEAD * head + HALF), slice(HEAD * head + HALF, HEAD * head + HEAD)


class Reduce:
    def __init__(self, place, units, grads, buffers, send, recv):
        self.units = units
        self.scatters = [Scatter(place, (lambda u, k=k: grads(units[k][u])), *buffers[k], ORDERS[k], send.at[k], recv.at[k]) for k in range(THREE)]

    def steps(self, store):
        def each(*names):
            def step():
                for name in names:
                    for s in self.scatters:
                        getattr(s, name)()
            return step

        def finish():
            for units, s in zip(self.units, self.scatters):
                s.finish(lambda u, full, units=units: store(units[u], full))

        return [each("swap"), each("swapped", "ring_start"), each("ring_turn"), each("plane_start"), each("last"), finish]


def backward_kernel(dy_ref, mid_ref, ctx_ref, st2_ref, q_ref, k_ref, v_ref, x_ref, st1_ref, cos_ref, sin_ref, c_ref, p_hbm, slope_hbm, act_hbm,
                    qkv_hbm, wo_hbm, up_hbm, down_hbm,
                    dx_ref, attn_out, up_out, down_out, small_out, *refs):
    (grad, dctx, delta, big, wqkv, wo, slope, act, dpre, h_ref, s_a, s_b, d_a, d_b, sums,
     g_qkv, g_wo, g_up, g_down, *small_bufs), refs = refs[:28], refs[28:]
    qkv_bufs, mo_bufs, refs = [refs[6 * k:6 * k + 6] for k in range(THREE)], [refs[6 * k + 18:6 * k + 24] for k in range(THREE)], refs[36:]
    send, recv, late_sem, plane_sem, big_sem, w_sem, mlp_sem = refs
    step = pl.program_id(ZERO)
    phase, seq = step // FOUR, lax.rem(step, FOUR)
    layer = ONE - step // EIGHT
    place = Place()

    def grads(unit):
        if unit < THREE:
            return g_qkv.at[unit]
        if unit == THREE:
            return g_wo
        if unit < EIGHT:
            return g_up.at[unit - FOUR]
        return g_down.at[:, :, :, unit - EIGHT]

    live = step < SIXTEEN
    turn = jnp.where(live, ZERO, ONE)
    qkv_sums = Reduce(place, ((ZERO,), (ONE,), (TWO,)), grads, [(a, ra, rb, rp.at[turn], *last) for a, ra, rb, rp, *last in qkv_bufs], send.at[turn], recv.at[turn])
    mo_sums = Reduce(place, COLOURS, grads, mo_bufs, send.at[TWO], recv.at[TWO])
    small_refs = small_bufs[::THREE]
    early, middle, late = [Late(place, small_refs[i], small_bufs[THREE * i + ONE], late_sem.at[i, ZERO], late_sem.at[i, ONE], small_bufs[THREE * i + TWO],
                                plane_sem.at[i, ZERO], plane_sem.at[i, ONE]).steps() for i in range(THREE)]
    first_core = place.core == ZERO

    def store(l):
        def put(unit, full):
            if unit < EIGHT:
                mine = jnp.where(first_core, full[:FOUR], full[FOUR:])
                if unit < FOUR:
                    attn_out[l, unit] = mine
                else:
                    up_out[l, :, DIM * (unit - FOUR):DIM * (unit - THREE)] = mine
            else:
                at = EIGHT * (unit % TWO)

                @pl.when(place.core == (unit - EIGHT) // TWO)
                def _():
                    down_out[l, at:at + EIGHT] = full
        return put

    def mlp_weights(l):
        parts = [pl.ds(DIM * k, DIM) for k in range(FOUR)]
        return ([pltpu.make_async_copy(down_hbm.at[l, part], big.at[k], big_sem.at[k]) for k, part in enumerate(parts)],
                [pltpu.make_async_copy(up_hbm.at[l, :, part], big.at[FOUR + k], big_sem.at[FOUR + k]) for k, part in enumerate(parts)] +
                [pltpu.make_async_copy(wo_hbm.at[l], wo, w_sem.at[ZERO])])

    def attn_weights(l):
        return [pltpu.make_async_copy(qkv_hbm.at[l], wqkv, w_sem.at[ONE])]

    def probs(l, s):
        return [pltpu.make_async_copy(p_hbm.at[l, s, k], big.at[k], big_sem.at[k]) for k in range(HEADS)]

    def saved_mlp(l, s):
        return [pltpu.make_async_copy(slope_hbm.at[l, s], slope, mlp_sem.at[ZERO]), pltpu.make_async_copy(act_hbm.at[l, s], act, mlp_sem.at[ONE])]

    def start(copies):
        for copy in copies:
            copy.start()

    def wait(copies):
        for copy in copies:
            copy.wait()

    @pl.when(step == ZERO)
    def _():
        place.greet()
        start(mlp_weights(ONE)[ZERO] + saved_mlp(ONE, ZERO) + mlp_weights(ONE)[ONE] + attn_weights(ONE))

    pl.when(step == ONE)(place.met)
    mo_steps, qkv_steps = mo_sums.steps(store(ONE - turn)), qkv_sums.steps(store(ONE - turn))

    def plan(slots, steps):
        return [((slot,), run) for slot, run in zip(slots, steps)]

    attn_hook = hooks(step * FOUR, plan((48, 57, 61, 63), middle) + plan((SIXTEEN, 24, 28), mo_steps) + plan((48, 53, 58), mo_steps) +
                      plan((53, 53), qkv_steps[FOUR:]))
    mlp_plan = plan((37, 45, 46), mo_steps[THREE:]) + plan((32, 36, 40, 47), qkv_steps) + plan((34, 41, 45, 47), early)
    mlp_hook = hooks(step * FOUR, mlp_plan + plan((64, 66, 70, 72, 75), qkv_steps) + plan((64, 72, 74, 75), late) + plan((65, 73, 74), mo_steps[THREE:]) +
                     plan((75,), qkv_steps[5:]))


    @pl.when(phase % TWO == ZERO)
    def _():
        @pl.when((seq == ZERO) & live)
        def _():
            for ref in (g_wo, g_up, g_down, sums):
                ref[...] = jnp.zeros_like(ref)

        @pl.when(step < FOUR)
        def _():
            grad[seq] = dy_ref[ZERO].T

        @pl.when((seq == ZERO) & live)
        def _():
            wait(mlp_weights(layer)[ZERO])

        mlp_hook(ZERO)

        def after_first():
            pl.when(seq < THREE)(lambda: start(saved_mlp(layer, seq + ONE)))
            pl.when(seq == THREE)(lambda: start(probs(layer, ZERO)[:FOUR]))

        def before_second():
            pl.when(seq == ZERO)(lambda: wait(mlp_weights(layer)[ONE]))

        def after_second():
            pl.when(seq == THREE)(lambda: start(probs(layer, ZERO)[FOUR:]))

        pl.when(live)(lambda: wait(saved_mlp(layer, seq)))
        mlp_backward(grad.at[seq], slope, act, mid_ref, ctx_ref, st2_ref.at[ZERO], wo, big, c_ref, dctx.at[seq], delta.at[seq], g_wo, g_up, g_down,
                     dpre, h_ref, s_a, s_b, sums, pl.when(live), mlp_hook,
                     after_first, after_second, before_second)

        @pl.when((seq == THREE) & live)
        def _():
            value = columns_of([sums[i] for i in range(EIGHT)])

            @pl.when(layer == ONE)
            def _():
                small_refs[ZERO][:EIGHT, :] = value

            @pl.when(layer == ZERO)
            def _():
                small_refs[ONE][...] = value

        mlp_hook(THREE)

    @pl.when(phase % TWO == ONE)
    def _():
        @pl.when(seq == ZERO)
        def _():
            wait(attn_weights(layer))
            for ref in (g_qkv, sums):
                ref[...] = jnp.zeros_like(ref)

        @pl.when(step == FOUR)
        def _():
            start(saved_mlp(ZERO, ZERO))
        attn_hook(ZERO)

        def after_heads():
            pl.when(seq < THREE)(lambda: start(probs(layer, seq + ONE)))
            pl.when(step == 7)(lambda: start(mlp_weights(ZERO)[ZERO] + mlp_weights(ZERO)[ONE]))

        wait(probs(layer, seq))
        attn_backward(dctx.at[seq], delta.at[seq], big, q_ref, k_ref, v_ref, x_ref, st1_ref.at[ZERO], grad.at[seq], wqkv, c_ref, cos_ref, sin_ref,
                      g_qkv, dpre, h_ref, s_a, s_b, d_a, d_b, sums, attn_hook,
                      after_heads)

        @pl.when(seq == THREE)
        def _():
            value = columns_of([sums[i] for i in range(5)])

            @pl.when(layer == ONE)
            def _():
                small_refs[ZERO][EIGHT:, :] = value

            @pl.when(layer == ZERO)
            def _():
                small_refs[TWO][...] = value

        @pl.when(step == 7)
        def _():
            start(attn_weights(ZERO))

        @pl.when(step > 11)
        def _():
            dx_ref[ZERO] = grad[seq].T
        attn_hook(THREE)

    @pl.when(step == 18)
    def _():
        small_out[:SIXTEEN, :], small_out[SIXTEEN:24, :], small_out[24:, :] = [ref[...] for ref in small_refs]


def add_to(ref, value):
    ref[...] = ref[...] + value.reshape(ref.shape)


def mlp_backward(grad, slope, act, mid_ref, ctx_ref, stat_ref, wo, big, c_ref, dctx, delta, g_wo, g_up, g_down, dpre, h_ref, s_a, s_b, sums, when, hook, after_first, after_second, before_second):
    parts = [slice(DIM * k, DIM * k + DIM) for k in range(FOUR)]
    pre = (s_a, s_b)

    def dact(k):
        pre[k % TWO][...] = nn(big[k], grad[...])

    @when
    def _():
        def scale(k, chunk):
            there = slice(parts[k].start + chunk.start, parts[k].start + chunk.stop)
            value = pre[k % TWO][chunk, :] * slope[there, :]
            sums[k, chunk, :] += fold(value)
            dpre[there, :] = value.astype(BF16)

        def down_product(k):
            add_to(g_down.at[k], nt(act[parts[k], :], grad[...]))

        dact(ZERO)
        norm_to(mid_ref.at[ZERO], get_stats(stat_ref), c_ref, LN_PAR + TWO, h_ref)
        for k in range(FOUR):
            products = [functools.partial(down_product, k)]
            if k < THREE:
                products = [functools.partial(dact, k + ONE)] + products
            woven(products, [functools.partial(scale, k, chunk) for chunk in row_chunks()])
        after_first()
    hook(ONE)

    @when
    def _():
        before_second()
        s_a[...] = functools.reduce(jnp.add, [nn(big[FOUR + k], dpre[rows, :]) for k, rows in enumerate(parts)])
        after_second()
    hook(TWO)

    @when
    def _():
        def write(rows, dx):
            dy = grad[rows, :].astype(F32)
            dmid = (dy + dx).astype(BF16)
            grad[rows, :] = dmid
            sums[6, rows, :] += fold(dy)
            sums[7, rows, :] += fold(dmid.astype(F32))

        norm_back(s_a, mid_ref.at[ZERO], get_stats(stat_ref), c_ref, LN_PAR + TWO, sums, FOUR, write,
                  [lambda k=k, rows=rows: add_to(g_up.at[k], nt(h_ref[...], dpre[rows, :])) for k, rows in enumerate(parts)])
        add_to(g_wo, nt(ctx_ref[ZERO].astype(BF16), grad[...]))
        s_b[...] = nn(wo[...], grad[...])
        for head in range(HEADS):
            rows = head_rows(head)[ZERO]
            value = s_b[rows, :].astype(BF16)
            dctx[rows, :] = value
            delta[head:head + ONE, :] = total(value.astype(F32) * ctx_ref[ZERO, rows, :])


def attn_backward(dctx, delta, probs, q_ref, k_ref, v_ref, x_ref, stat_ref, grad, wqkv, c_ref, cos_ref, sin_ref, g_qkv, dproj, h_ref, s_a, s_b, d_a, d_b,
                  sums, hook, prefetch):
    scores, dscores = (s_a, s_b), (d_a, d_b)
    q, k, v = q_ref.at[ZERO], k_ref.at[ZERO], v_ref.at[ZERO]

    def open_head(head):
        rows = head_rows(head)[ZERO]
        scores[head % TWO][...] = tn(v[rows, :], dctx[rows, :])

    def weigh(head, rows):
        dscores[head % TWO][rows, :] = (probs[head, rows, :].astype(F32) * (scores[head % TWO][rows, :] - delta[head:head + ONE, :])).astype(BF16)

    def values(head):
        rows = head_rows(head)[ZERO]
        dv = nt(dctx[rows, :], probs[head])
        sums[TWO, rows, :] += fold(dv)
        dproj[TWO * DIM + rows.start:TWO * DIM + rows.stop, :] = dv.astype(BF16)

    def close_head(head, m):
        rows, one, two = head_rows(head)
        ds = dscores[head % TWO][...]
        value = nn(k[rows, :], ds) * HEAD ** -0.5 if m == ZERO else nt(q[rows, :], ds)
        cos, sin = cos_ref[...], sin_ref[...]
        a, b = value[:HALF], value[HALF:]
        for at, out in ((one, a * cos + b * sin), (two, b * cos - a * sin)):
            dproj[m * DIM + at.start:m * DIM + at.stop, :] = out.astype(BF16)
            sums[m, at, :] += fold(out)

    open_head(ZERO)
    for head in range(HEADS):
        products = [functools.partial(values, head)]
        if head:
            products = [functools.partial(close_head, head - ONE, m) for m in range(TWO)] + products
        if head + ONE < HEADS:
            products = [functools.partial(open_head, head + ONE)] + products
        woven(products, [functools.partial(weigh, head, rows) for rows in row_chunks()])
        if head == THREE:
            hook(ONE)
    for m in range(TWO):
        close_head(HEADS - ONE, m)
    prefetch()
    hook(TWO)
    norm_to(x_ref.at[ZERO], get_stats(stat_ref), c_ref, LN_PAR, h_ref)
    parts = [slice(DIM * m, DIM * m + DIM) for m in range(THREE)]
    s_a[...] = functools.reduce(jnp.add, [nn(wqkv[m], dproj[rows, :]) for m, rows in enumerate(parts)])

    def write(rows, dx):
        grad[rows, :] = (grad[rows, :].astype(F32) + dx).astype(BF16)

    norm_back(s_a, x_ref.at[ZERO], get_stats(stat_ref), c_ref, LN_PAR, sums, THREE, write,
              [lambda m=m, rows=rows: add_to(g_qkv.at[m], nt(h_ref[...], dproj[rows, :])) for m, rows in enumerate(parts)])


def backward(dy, xs, q, k, v, probs, ctx, mid, act, slope, st1, st2, c, tables, w_qkv, w_o, w_up, w_down):
    def mlp_at(s):
        s = jnp.minimum(s, 15)
        odd = s // FOUR % TWO == ONE
        return ONE - s // EIGHT, jnp.where(odd, THREE, s % FOUR), ZERO, ZERO

    def attn_at(s):
        s = jnp.minimum(s, 15)
        odd = s // FOUR % TWO == ONE
        return jnp.where(s < EIGHT, ONE, ZERO) + jnp.where((s > 7) & (s < 12), ONE, ZERO), jnp.where(odd, s % FOUR, jnp.where(s < FOUR, ZERO, THREE)), ZERO, ZERO

    per_mlp = pl.BlockSpec((None, ONE, *SQUARE), mlp_at)
    per_attn = pl.BlockSpec((None, ONE, *SQUARE), attn_at)

    def stat(at):
        return pl.BlockSpec((None, ONE, EIGHT, TOK), at)

    acc = [(*GRID, EIGHT, WIDTH)]
    scratch = [pltpu.VMEM((SEQS, *SQUARE), BF16), pltpu.VMEM((SEQS, *SQUARE), BF16), pltpu.VMEM((SEQS, HEADS, TOK), F32),
               pltpu.VMEM((HEADS, TOK, TOK), BF16), pltpu.VMEM((THREE, DIM, DIM), BF16), pltpu.VMEM((DIM, DIM), BF16),
               pltpu.VMEM(TALL, F32), pltpu.VMEM(TALL, BF16), pltpu.VMEM(TALL, BF16), pltpu.VMEM(SQUARE, BF16),
               pltpu.VMEM(SQUARE, F32), pltpu.VMEM(SQUARE, F32), pltpu.VMEM((TOK, TOK), BF16), pltpu.VMEM((TOK, TOK), BF16),
               pltpu.VMEM((EIGHT, *COLS), F32), pltpu.VMEM((THREE, *GRID, EIGHT, DIM), F32), pltpu.VMEM((*GRID, EIGHT, DIM), F32),
               pltpu.VMEM((FOUR, *GRID, EIGHT, DIM), F32), pltpu.VMEM((*GRID, FOUR, EIGHT, DIM), F32), *[pltpu.VMEM((*lead, rows, DIM), F32) for rows in (SIXTEEN, EIGHT, EIGHT) for lead in ((), (6,), (SIXTEEN,))]]
    for n in (ONE, THREE):
        for order in ORDERS:
            ring_a, ring_b, plane, *last = landing_shapes(order, n)
            plane = (TWO, *plane) if n == ONE else plane
            scratch += [pltpu.VMEM(s, F32) for s in ((n, *GRID, EIGHT, WIDTH), ring_a, ring_b, plane, *last)]
    scratch += [DMA((THREE, THREE, 9)), DMA((THREE, THREE, 9)), DMA((THREE, TWO, 6)), DMA((THREE, TWO)), DMA((EIGHT,)), DMA((TWO,)), DMA((TWO,))]
    outs = ((TWO, FOUR, FOUR, DIM), (TWO, FOUR, FFN), (TWO, SIXTEEN, DIM), (32, DIM))
    whole = [pl.BlockSpec(s, lambda i, n=len(s): (ZERO,) * n, pipeline_mode=pl.Buffered(ONE)) for s in outs]
    dx_at = lambda s: (jnp.clip(s - 12, ZERO, THREE), ZERO, ZERO)
    return pl.pallas_call(
        backward_kernel, grid=(19,),
        out_shape=[jax.ShapeDtypeStruct((SEQS, TOK, DIM), BF16)] + [jax.ShapeDtypeStruct(s, F32) for s in outs],
        out_specs=[pl.BlockSpec((ONE, TOK, DIM), dx_at)] + whole,
        in_specs=[pl.BlockSpec((ONE, TOK, DIM), lambda s: (jnp.minimum(s, THREE), ZERO, ZERO)), per_mlp, per_mlp, stat(mlp_at)] + [per_attn] * FOUR + [stat(attn_at),
                  once((HALF, TOK)), once((HALF, TOK)), pl.BlockSpec((None, *COLS), lambda s: (ONE - jnp.minimum(s, 15) // EIGHT, ZERO, ZERO))] + [HBM] * 7,
        scratch_shapes=scratch,
        compiler_params=pltpu.CompilerParams(collective_id=ONE, has_side_effects=True, vmem_limit_bytes=67043328,
                                             dimension_semantics=("arbitrary",)),
        name="backward")(dy, mid, ctx, st2, q, k, v, xs, st1, *tables, c, probs, slope, act, w_qkv, w_o, w_up, w_down)


def results_kernel(dx_ref, attn_ref, up_ref, down_ref, small_ref, dx_out, attn_out, gb_attn, g_ln, up_out, gb_up, down_out, gb_down):
    dx_out[...] = dx_ref[...]

    @pl.when(pl.program_id(ZERO) == ZERO)
    def _():
        me = lax.axis_index(AXIS)
        attn_out[...], up_out[...], down_out[...] = attn_ref[...], up_ref[...], down_ref[...]
        mine = pltpu.roll(small_ref[...], lax.rem(DIM - FOUR * me + FOUR * LANES, DIM), ONE)
        for l in range(TWO):
            mlp = SIXTEEN - SIXTEEN * l
            attn = mlp + EIGHT
            gb_attn[l, :THREE], gb_attn[l, THREE:] = mine[attn:attn + THREE, :FOUR], mine[mlp + 7:mlp + EIGHT, :FOUR]
            g_ln[l, :TWO], g_ln[l, TWO:] = mine[attn + THREE:attn + 5, :FOUR], mine[mlp + FOUR:mlp + 6, :FOUR]
            gb_down[l:l + ONE, :] = mine[mlp + 6:mlp + 7, :FOUR]
            ups = small_ref[pl.ds(mlp + me // 32, ONE), :]
            gb_up[l:l + ONE, :] = pltpu.roll(ups, lax.rem(DIM - SIXTEEN * lax.rem(me, 32), DIM), ONE)[:, :SIXTEEN]


def results(dx, attn, up, down, small):
    shapes = [attn.shape, (TWO, FOUR, FOUR), (TWO, FOUR, FOUR), up.shape, (TWO, SIXTEEN), down.shape, (TWO, FOUR)]
    per = pl.BlockSpec((TWO, TOK, DIM), lambda s: (s, ZERO, ZERO))
    return pl.pallas_call(
        results_kernel, grid=(SEQS // TWO,), name="results",
        out_shape=[jax.ShapeDtypeStruct(dx.shape, BF16)] + [jax.ShapeDtypeStruct(s, F32) for s in shapes],
        in_specs=[per] + [once(a.shape) for a in (attn, up, down, small)],
        out_specs=[per] + [once(s) for s in shapes])(dx, attn, up, down, small)


def solution(mesh):
    batch_spec = P(AXIS)
    weight_specs = (P(None, None, AXIS, None), P(None, None, AXIS), P(None, None, AXIS),
                    P(None, AXIS, None), P(None, AXIS), P(None, AXIS, None), P(None, AXIS))

    def device_step(x, lengths, d_y, w_attn, b_attn, ln_par, w_up, b_up, w_down, b_down):
        tables = rotary_tables()
        xs, q, k, v, probs, ctx, mid, act, slope, st1, st2, c, w_qkv, w_o, w_up, w_down = forward(
            lengths, x, tables, (w_attn, b_attn, ln_par, w_up, b_up, w_down, b_down))
        return results(*backward(d_y, xs, q, k, v, probs, ctx, mid, act, slope, st1, st2, c, tables, w_qkv, w_o, w_up, w_down))

    return jax.shard_map(device_step, mesh=mesh,
                         in_specs=(batch_spec, batch_spec, batch_spec) + weight_specs,
                         out_specs=(batch_spec,) + weight_specs,
                         check_vma=False)
```

```python
import math
import functools
import jax
import jax.numpy as jnp
from jax import lax
from jax.experimental import pallas as pl
from jax.experimental.pallas import tpu as pltpu
from jax.sharding import PartitionSpec as P

ZERO, ONE, TWO, THREE, FOUR = range(5)
EIGHT, SIXTEEN, WIDTH = 8, 16, 256

F32, BF16 = jnp.float32, jnp.bfloat16
SEQS, TOK, DIM, FFN, HEADS, HEAD, LANES = FOUR, 512, 512, 2048, EIGHT, 64, 128
HALF = HEAD // TWO
EPS = 1e-5
THETA = 10000.0
NEG_BIG = -1e30
B_ATTN, LN_PAR, B_UP, B_DOWN = ZERO, FOUR, EIGHT, 12


def nn(a, b):
    return lax.dot_general(a, b, (((ONE,), (ZERO,)), ((), ())), preferred_element_type=F32)


def nt(a, b):
    return lax.dot_general(a, b, (((ONE,), (ONE,)), ((), ())), preferred_element_type=F32)


def tn(a, b):
    return lax.dot_general(a, b, (((ZERO,), (ZERO,)), ((), ())), preferred_element_type=F32)


def lane_tiles(width=TOK, size=LANES):
    return [slice(i, i + size) for i in range(ZERO, width, size)]


def row_chunks(rows=DIM, size=64):
    return [slice(i, i + size) for i in range(ZERO, rows, size)]


def column(c_ref, rows, lane):
    return jnp.broadcast_to(c_ref[rows, lane:lane + ONE], (rows.stop - rows.start, TOK))


def total(value):
    return jnp.sum(value, axis=ZERO, keepdims=True)


def norm_stats(x_ref):
    mean = functools.reduce(jnp.add, [total(x_ref[rows, :].astype(F32)) for rows in row_chunks()]) * (1.0 / DIM)
    squares = []
    for rows in row_chunks():
        centred = x_ref[rows, :].astype(F32) - mean
        squares.append(total(centred * centred))
    return mean, lax.rsqrt(functools.reduce(jnp.add, squares) * (1.0 / DIM) + EPS)


def norm_to(x_ref, stats, c_ref, lane, h_ref):
    mean, rstd = stats
    for rows in row_chunks():
        xhat = (x_ref[rows, :].astype(F32) - mean) * rstd
        h_ref[rows, :] = (xhat * column(c_ref, rows, lane) + column(c_ref, rows, lane + ONE)).astype(BF16)


def put_stats(ref, stats):
    ref[ZERO:ONE, :], ref[ONE:TWO, :] = stats


def get_stats(ref):
    return ref[ZERO:ONE, :], ref[ONE:TWO, :]


def woven(products, rest):
    done = ZERO
    for n, step in enumerate(rest):
        while done < len(products) and done * len(rest) <= n * len(products):
            products[done]()
            done += ONE
        step()
    for product in products[done:]:
        product()


def fold(value):
    parts = [value[:, cols] for cols in lane_tiles(value.shape[ONE])]
    return functools.reduce(jnp.add, parts)


def seq_spec(shape):
    return pl.BlockSpec((ONE, *shape), lambda s: (s,) + (ZERO,) * len(shape))


def once(shape):
    return pl.BlockSpec(shape, lambda s: (ZERO,) * len(shape), pipeline_mode=pl.Buffered(ONE))


def act_shape(rows, dtype):
    return jax.ShapeDtypeStruct((SEQS, rows, TOK), dtype)


PARAMS = pltpu.CompilerParams(vmem_limit_bytes=60 << 20, dimension_semantics=("arbitrary",))
SQUARE, TALL, WIDE, COLS = (DIM, TOK), (FFN, TOK), (DIM, FFN), (DIM, LANES)


def rotary_tables():
    inv_freq = 1.0 / (THETA ** (jnp.arange(HALF, dtype=F32) * (2.0 / HEAD)))
    angles = inv_freq[:, None] * jnp.arange(TOK, dtype=F32)[None, :]
    return jnp.cos(angles), jnp.sin(angles)


MESH = pl.DeviceIdType.MESH
AXIS = "fsdp"
ORDERS = ((TWO, ONE, ZERO), (ONE, ZERO, TWO), (ZERO, TWO, ONE))


class Place:
    def __init__(self):
        me = lax.axis_index(AXIS)
        self.core = lax.rem(me, TWO)
        self.pos = (me // 32, lax.rem(me // EIGHT, FOUR), lax.rem(me // TWO, FOUR))
        self.partner = me + ONE - TWO * self.core
        self.near = [[lax.rem(at + delta, FOUR) if delta else at for delta in range(FOUR)] for at in self.pos]

    def coord(self, dim, delta):
        if isinstance(delta, int):
            return self.near[dim][delta % FOUR]
        return lax.rem(self.pos[dim] + delta, FOUR)

    def device(self, offsets):
        pos = [self.coord(dim, offsets.get(dim, ZERO)) for dim in range(THREE)]
        return pos[ZERO] * 32 + pos[ONE] * EIGHT + pos[TWO] * TWO + self.core

    def greet(self):
        barrier = pltpu.get_barrier_semaphore()
        for i in range(ONE, 64):
            offsets = {ZERO: i // SIXTEEN, ONE: i // FOUR % FOUR, TWO: i % FOUR}
            if min(offsets.values()) == ZERO:
                pl.semaphore_signal(barrier, inc=ONE, device_id=(self.device(offsets),), device_id_type=MESH)
        pl.semaphore_signal(barrier, inc=ONE, device_id=(self.partner,), device_id_type=MESH)

    def met(self):
        pl.semaphore_wait(pltpu.get_barrier_semaphore(), 37)


def remote(src, dst, send_sem, recv_sem, device):
    return pltpu.make_async_remote_copy(src_ref=src, dst_ref=dst, send_sem=send_sem, recv_sem=recv_sem,
                                        device_id=(device,), device_id_type=MESH)


LINE = (ONE, -ONE, TWO)


def each_of_plane(order, run):
    @pl.loop(ZERO, FOUR)
    def _(high):
        for low in range(FOUR):
            step = functools.partial(run, FOUR * high + low, {order[ONE]: high, order[TWO]: low})
            if low:
                step()
            else:
                pl.when(high > ZERO)(step)


class Gather:
    def __init__(self, place, buf, fifteen, order, send, recv):
        self.place, self.buf, self.fifteen, self.order, self.send, self.recv = place, buf, fifteen, order, send, recv

    def block(self, offsets, whole=()):
        index = [slice(ZERO, FOUR) if dim in whole else pl.ds(self.place.coord(dim, offsets.get(dim, ZERO)), ONE) for dim in range(THREE)]
        return self.buf.at[index[ZERO], index[ONE], index[TWO], pl.ds(self.place.core, ONE)]

    def copy(self, ref, key, device):
        return remote(ref, ref, self.send.at[key], self.recv.at[key], device)

    def plane_start(self):
        each_of_plane(self.order, lambda k, offsets: self.copy(self.block({}), ZERO, self.place.device(offsets)).start())

    def plane_all(self):
        return self.copy(self.fifteen, ZERO, self.place.partner)

    def plane_wait(self):
        self.plane_all().wait_recv()

    def line(self, i, sign):
        offsets = {self.order[ZERO]: sign * LINE[i]}
        return self.block(offsets, self.order[ONE:])

    def line_start(self):
        for i, delta in enumerate(LINE):
            self.copy(self.line(i, ZERO), ONE + i, self.place.device({self.order[ZERO]: delta})).start()

    def line_wait(self):
        for i in range(THREE):
            self.copy(self.line(i, -ONE), ONE + i, self.place.partner).wait_recv()

    def share(self, core):
        return self.copy(self.buf.at[:, :, :, pl.ds(core, ONE)], FOUR, self.place.partner)

    def share_start(self):
        self.share(self.place.core).start()

    def end(self):
        self.share(ONE - self.place.core).wait_recv()
        self.plane_all().wait_send()
        for i in range(THREE):
            self.copy(self.line(i, ZERO), ONE + i, self.place.partner).wait_send()
        self.share(self.place.core).wait_send()


def gather_steps(gathers):
    def each(*names):
        def step():
            for name in names:
                for g in gathers:
                    getattr(g, name)()
        return step

    return [each("plane_start"), each("plane_wait", "line_start"), each("line_wait", "share_start"), each("end")]


class Scatter:
    def __init__(self, place, grads, acc, got_a, got_b, got_p, mine, other, order, send, recv):
        self.place, self.grads, self.acc, self.order = place, grads, acc, order
        self.got_a, self.got_b, self.got_p, self.mine, self.other, self.send, self.recv = got_a, got_b, got_p, mine, other, send, recv
        self.units = acc.shape[ZERO]

    def columns(self, core):
        return pl.ds(pl.multiple_of(core * WIDTH, WIDTH), WIDTH)

    def swap_copy(self, u):
        place = self.place
        return remote(self.grads(u).at[:, :, :, :, self.columns(ONE - place.core)], self.acc.at[u], self.send.at[6 + u], self.recv.at[6 + u], place.partner)

    def swap(self):
        for u in range(self.units):
            self.swap_copy(u).start()

    def swapped(self):
        for u in range(self.units):
            self.swap_copy(u).wait()
            grad, acc = self.grads(u), self.acc

            @pl.loop(ZERO, FOUR)
            def _(z):
                acc[u, z] = acc[u, z] + grad[z, :, :, :, self.columns(self.place.core)]

    def part(self, delta, half=None):
        index = [slice(ZERO, FOUR)] * THREE
        index[self.order[ZERO]] = pl.ds(self.place.coord(self.order[ZERO], delta), ONE)
        return self.acc.at[:, index[ZERO], index[ONE], index[TWO], :, slice(ZERO, WIDTH) if half is None else lane_tiles()[half]]

    def ring(self, step, way):
        delta = (ONE, -ONE)[way]
        device = self.place.device({self.order[ZERO]: delta})
        if step == ZERO:
            src, dst = self.part(TWO, way), self.got_a.at[:, :, :, :, :, lane_tiles()[way]]
        else:
            src, dst = self.part(delta), self.got_b.at[way]
        key = TWO * step + way
        return remote(src, dst, self.send.at[key], self.recv.at[key], device)

    def ring_start(self):
        for way in range(TWO):
            self.ring(ZERO, way).start()

    def ring_turn(self):
        for way in range(TWO):
            self.ring(ZERO, way).wait_recv()
            self.add((ONE, -ONE)[way], way, self.got_a)
            self.ring(ONE, way).start()

    def add(self, delta, half, *refs):
        dim, acc = self.order[ZERO], self.acc
        at = self.place.coord(dim, delta)
        columns = slice(ZERO, WIDTH) if half is None else lane_tiles()[half]

        @pl.loop(ZERO, FOUR)
        def _(i):
            index = [i if d == self.order[ONE] else slice(ZERO, FOUR) for d in range(THREE)]
            there = [slice(None), *index, slice(None), columns]
            here = list(there)
            here[ONE + dim] = pl.ds(at, ONE)
            there[ONE + dim] = slice(ZERO, ONE)
            value = acc[tuple(here)]
            for ref in refs:
                value = value + ref[tuple(there)]
            acc[tuple(here)] = value

    def plane_copy(self, k, offsets):
        index = [pl.ds(self.place.coord(dim, offsets.get(dim, ZERO)), ONE) for dim in range(THREE)]
        src = self.acc.at[:, index[ZERO], index[ONE], index[TWO]]
        return remote(src, self.got_p.at[k], self.send.at[FOUR], self.recv.at[FOUR], self.place.device(offsets))

    def plane_all(self):
        return remote(self.got_p.at[ONE:], self.got_p.at[ONE:], self.send.at[FOUR], self.recv.at[FOUR], self.place.partner)

    def plane_start(self):
        for way in range(TWO):
            self.ring(ONE, way).wait_recv()
        self.add(ZERO, None, self.got_b.at[ZERO], self.got_b.at[ONE])

        each_of_plane(self.order, lambda k, offsets: self.plane_copy(k, offsets).start())

    def own(self):
        z, y, x = [pl.ds(p, ONE) for p in self.place.pos]
        return self.acc.at[:, z, y, x]

    def last_copy(self):
        return remote(self.mine, self.other, self.send.at[5], self.recv.at[5], self.place.partner)

    def last(self):
        self.plane_all().wait_recv()
        self.mine[...] = functools.reduce(jnp.add, [self.got_p[k] for k in range(ONE, SIXTEEN)], self.own()[...])
        for step in range(TWO):
            for way in range(TWO):
                self.ring(step, way).wait_send()
        self.plane_all().wait_send()
        self.last_copy().start()

    def finish(self, store):
        self.last_copy().wait_recv()
        first = self.place.core == ZERO
        for u in range(self.units):
            own, came = self.mine[u, ZERO, ZERO, ZERO], self.other[u, ZERO, ZERO, ZERO]
            store(u, jnp.concatenate([jnp.where(first, own, came), jnp.where(first, came, own)], axis=ONE))
        self.last_copy().wait_send()


def landing_shapes(order, units):
    size = [FOUR, FOUR, FOUR]
    size[order[ZERO]] = ONE
    return (units, *size, EIGHT, WIDTH), (TWO, units, *size, EIGHT, WIDTH), (SIXTEEN, units, ONE, ONE, ONE, EIGHT, WIDTH), (units, ONE, ONE, ONE, EIGHT, WIDTH), (units, ONE, ONE, ONE, EIGHT, WIDTH)


class Small:
    def __init__(self, place, value, slots, send, recv):
        self.place, self.value, self.slots, self.send, self.recv = place, value, slots, send, recv

    def peers(self, stage):
        if stage == THREE:
            return [self.place.partner]
        return [self.place.device({stage: delta}) for delta in LINE]

    def copies(self, stage):
        return [remote(self.value, self.slots.at[THREE * stage + k], self.send.at[THREE * stage + k], self.recv.at[THREE * stage + k], peer)
                for k, peer in enumerate(self.peers(stage))]

    def start(self, stage):
        for copy in self.copies(stage):
            copy.start()

    def finish(self, stage):
        copies = self.copies(stage)
        for copy in copies:
            copy.wait()
        self.value[...] = functools.reduce(jnp.add, [self.slots[THREE * stage + k] for k in range(len(copies))], self.value[...])

    def turn(self, stage):
        def step():
            self.finish(stage)
            self.start(stage + ONE)
        return step

    def steps(self):
        return [lambda: self.start(ZERO), self.turn(ZERO), self.turn(ONE), self.turn(TWO), lambda: self.finish(THREE)]


class Late(Small):
    def __init__(self, place, value, slots, send, recv, planes, plane_send, plane_recv):
        super().__init__(place, value, slots, send, recv)
        self.planes, self.plane_send, self.plane_recv = planes, plane_send, plane_recv

    def peers(self, stage):
        return super().peers({ZERO: ORDERS[ZERO][ZERO], ONE: THREE}[stage])

    def plane(self, k, offsets):
        return remote(self.value, self.planes.at[k], self.plane_send, self.plane_recv, self.place.device(offsets))

    def steps(self):
        def first():
            each_of_plane(ORDERS[ZERO], lambda k, offsets: self.plane(k, offsets).start())

        def second():
            remote(self.planes.at[ONE:], self.planes.at[ONE:], self.plane_send, self.plane_recv, self.place.partner).wait()
            self.value[...] = functools.reduce(jnp.add, [self.planes[k] for k in range(ONE, SIXTEEN)], self.value[...])
            self.start(ZERO)

        return [first, second, self.turn(ZERO), lambda: self.finish(ONE)]


VMEM = pl.BlockSpec(memory_space=pltpu.VMEM)
HBM = pl.BlockSpec(memory_space=pl.ANY)
DMA = pltpu.SemaphoreType.DMA


COLOURS = ((THREE, FOUR, 5), (6, 7, EIGHT), (9, 10, 11))
GRID = (FOUR, FOUR, FOUR)


def spread(buf, u, out_ref, column_base):
    @pl.loop(ZERO, EIGHT)
    def _(block):
        for part in range(FOUR):
            g = block * FOUR + part
            tiles = [buf[block // TWO, lax.rem(block, TWO) * TWO + part // TWO, part % TWO * TWO + k // TWO, k % TWO, u].astype(F32) for k in range(FOUR)]
            rows = pl.ds(pl.multiple_of(g * SIXTEEN, SIXTEEN), SIXTEEN)
            for j, cols in enumerate(lane_tiles()):
                value = jnp.concatenate([t[FOUR * j:FOUR * j + FOUR] for t in tiles], axis=ZERO).astype(BF16)
                out_ref[rows, column_base + cols.start:column_base + cols.stop] = value


def spread_down(buf, u, out_ref, cols):
    @pl.loop(ZERO, SIXTEEN)
    def _(i):
        for k in range(EIGHT):
            d = i * EIGHT + k
            out_ref[pl.ds(pl.multiple_of(d * SIXTEEN, SIXTEEN), SIXTEEN), cols] = buf[i // FOUR, lax.rem(i, FOUR), k // TWO, k % TWO, u]


def same(shape, test):
    row = lax.broadcasted_iota(jnp.int32, shape, ZERO)
    col = lax.broadcasted_iota(jnp.int32, shape, ONE)
    return jnp.where(test(row, col), 1.0, 0.0)


def small_columns(small_ref, c_ref):
    rows = [small_ref[z, y, x, c, ZERO] for z in range(FOUR) for y in range(FOUR) for x in range(FOUR) for c in range(TWO)]
    table = jnp.concatenate(rows, axis=ZERO).astype(BF16)
    quads = nn(same((DIM, LANES), lambda r, c: r // FOUR == c).astype(BF16), table)
    quads = (quads * same((DIM, LANES), lambda r, c: r % FOUR == c % FOUR)).astype(BF16)
    mask = same((DIM, LANES), lambda r, c: r % SIXTEEN == c % SIXTEEN)
    pick = same((DIM, 32), lambda r, c: r // SIXTEEN == c).astype(BF16)
    ups = [(nn(pick, table[32 * k:32 * k + 32]) * mask).astype(BF16) for k in range(FOUR)]
    for layer in range(TWO):
        def is_up(r):
            return r // SIXTEEN == layer * FOUR + TWO

        value = nn(quads, same((LANES, LANES), lambda r, c: (r // 64 == layer) & (r % 64 // FOUR == c) & ~is_up(r)).astype(BF16))
        for k in range(FOUR):
            value = value + nn(ups[k], same((LANES, LANES), lambda r, c: is_up(r) & (c == B_UP + k)).astype(BF16))
        c_ref[layer] = value


def tile_of(rows):
    rows = rows.astype(F32)
    return jnp.concatenate([rows[:, cols] for cols in lane_tiles()], axis=ZERO).astype(BF16)


def small_row(b_attn, ln_par, b_up, b_down):
    lane = lax.broadcasted_iota(jnp.int32, (ONE, LANES), ONE)
    row = jnp.zeros((ONE, LANES), F32)
    pieces = []
    for l in range(TWO):
        for m in range(FOUR):
            pieces += [(b_attn[l, m:m + ONE, :], 64 * l + FOUR * m), (ln_par[l, m:m + ONE, :], 64 * l + FOUR * m + SIXTEEN)]
        pieces += [(b_up[l:l + ONE, :], 64 * l + 32), (b_down[l:l + ONE, :], 64 * l + 48)]
    for piece, at in pieces:
        n = piece.shape[ONE]
        wide = jnp.concatenate([piece.astype(F32), jnp.zeros((ONE, LANES - n), F32)], axis=ONE)
        wide = pltpu.roll(wide, at, ONE) if at else wide
        row = jnp.where((lane >= at) & (lane < at + n), wide, row)
    return row


def hooks(slot, plan):
    def hook(at):
        for slots, run in plan:
            mine = [when for when in slots if when % FOUR == at]
            if mine:
                pl.when(functools.reduce(jnp.logical_or, [slot + at == when for when in mine]))(run)
    return hook


def forward_kernel(len_ref, x_hbm, cos_ref, sin_ref, w_attn, b_attn, ln_par, w_up, b_up, w_down, b_down,
                   xs_out, q_ref, k_ref, v_ref, p_ref, ctx_ref, mid_ref, act_ref, slope_ref, st1_ref, st2_ref, c_ref,
                   nat_qkv, nat_wo, nat_up, nat_down,
                   xs, ctxb, n_qkv, n_wo, n_up, n_down, h_ref, s_a, s_b, s_c,
                   sbuf, q0, q1, q2, m0, m1, m2, stats, f0, f1, f2, send, recv, nat_sem, x_sem):
    step = pl.program_id(ZERO)
    phase, seq, layer = step // FOUR, lax.rem(step, FOUR), step // EIGHT
    place = Place()
    z, y, x = place.pos
    qkv_bufs, mo_bufs, fifteen = (q0, q1, q2), (m0, m1, m2), (f0, f1, f2)

    def group(bufs, base, l):
        return [Gather(place, b.at[l], fifteen[base // THREE], ORDERS[k], send.at[base + k, l], recv.at[base + k, l]) for k, b in enumerate(bufs)]

    little = Gather(place, sbuf, fifteen[TWO], ORDERS[ZERO], send.at[6, ZERO], recv.at[6, ZERO])

    def nat_copies(which, l):
        if which == ZERO:
            return [pltpu.make_async_copy(n_qkv, nat_qkv.at[l], nat_sem.at[ZERO])]
        return [pltpu.make_async_copy(src, dst.at[l], nat_sem.at[ONE + i]) for i, (src, dst) in enumerate(((n_wo, nat_wo), (n_up, nat_up), (n_down, nat_down)))]

    def wait(copies):
        for copy in copies:
            copy.wait()

    def start(copies):
        for copy in copies:
            copy.start()

    def take_qkv():
        pl.when(step > ZERO)(lambda: wait(nat_copies(ZERO, layer)))
        for m in range(THREE):
            spread(qkv_bufs[m].at[layer], ZERO, n_qkv.at[m], ZERO)
        start(nat_copies(ZERO, layer))

    def take_mo():
        pl.when(step > EIGHT)(lambda: wait(nat_copies(ONE, layer)))
        for colour in range(THREE):
            for u, unit in enumerate(COLOURS[colour]):
                buf = mo_bufs[colour].at[layer]
                if unit == THREE:
                    spread(buf, u, n_wo, ZERO)
                elif unit < EIGHT:
                    spread(buf, u, n_up, DIM * (unit - FOUR))
                else:
                    spread_down(buf, u, n_down, lane_tiles()[unit - EIGHT])
        start(nat_copies(ONE, layer))

    x_copies = [pltpu.make_async_copy(x_hbm.at[s], ctxb.at[s], x_sem.at[s]) for s in range(SEQS)]

    @pl.when(step == ZERO)
    def _():
        place.greet()
        start(x_copies)
        for l in range(TWO):
            for unit in range(12):
                if unit < FOUR:
                    tile = tile_of(w_attn[l, unit])
                elif unit < EIGHT:
                    tile = tile_of(w_up[l, :, DIM * (unit - FOUR):DIM * (unit - THREE)])
                else:
                    tile = w_down[l, :, lane_tiles()[unit - EIGHT]]
                if unit < THREE:
                    qkv_bufs[unit][l, z, y, x, place.core, ZERO] = tile
                else:
                    mo_bufs[(unit - THREE) // THREE][l, z, y, x, place.core, (unit - THREE) % THREE] = tile
        sbuf[z, y, x, place.core, ZERO] = small_row(b_attn, ln_par, b_up, b_down)
        first, second = gather_steps(group(qkv_bufs, ZERO, ZERO) + [little]), gather_steps(group(mo_bufs, THREE, ZERO))

        def ready(s):
            x_copies[s].wait()
            xs[s] = ctxb[s].T
            put_stats(stats.at[s], norm_stats(xs.at[s]))

        place.met()
        first[ZERO]()
        second[ZERO]()
        ready(ZERO)
        ready(ONE)
        first[ONE]()
        ready(TWO)
        ready(THREE)
        first[TWO]()
        second[ONE]()
        first[THREE]()
        small_columns(sbuf, c_ref)

    attn_hook = hooks(step * FOUR, [((when, when + 32), run) for when, run in zip((9, 13), gather_steps(group(mo_bufs, THREE, layer))[TWO:])])
    mlp_steps = gather_steps(group(qkv_bufs, ZERO, ONE)) + gather_steps(group(mo_bufs, THREE, ONE))[:TWO]
    mlp_hook = hooks(step * FOUR, [((when,), run) for when, run in zip((SIXTEEN, 25, 30, 31, 17, 26), mlp_steps)])

    @pl.when(phase % TWO == ZERO)
    def _():
        pl.when(seq == ZERO)(take_qkv)

        @pl.when(step < FOUR)
        def _():
            xs_out[ZERO, ZERO] = xs[seq]

        @pl.when(step > 7)
        def _():
            put_stats(stats.at[seq], norm_stats(xs.at[seq]))

        attn_hook(ZERO)
        attn_forward(len_ref[seq], xs.at[seq], n_qkv, c_ref.at[layer], cos_ref, sin_ref, q_ref.at[ZERO, ZERO], k_ref.at[ZERO, ZERO],
                     v_ref.at[ZERO, ZERO], p_ref.at[ZERO, ZERO], ctx_ref.at[ZERO, ZERO], ctxb.at[seq], get_stats(stats.at[seq]), st1_ref.at[ZERO, ZERO], h_ref, s_a, s_b, s_c, attn_hook)
        attn_hook(THREE)

    @pl.when(phase % TWO == ONE)
    def _():
        pl.when(seq == ZERO)(take_mo)
        mlp_hook(ZERO)
        mlp_forward(layer, ctxb.at[seq], xs.at[seq], n_wo, n_up, n_down, c_ref.at[layer], mid_ref.at[ZERO, ZERO], act_ref.at[ZERO, ZERO], slope_ref.at[ZERO, ZERO],
                    st2_ref.at[ZERO, ZERO], h_ref, s_a, s_b, mlp_hook)

        @pl.when(layer == ZERO)
        def _():
            xs_out[ZERO, ZERO] = xs[seq]
        mlp_hook(THREE)

    @pl.when(step == 15)
    def _():
        for which in range(TWO):
            wait(nat_copies(which, ONE))


def attn_forward(length, xt, w, c_ref, cos_ref, sin_ref, q_ref, k_ref, v_ref, p_buf, ctx_ref, ctxb, stats, stat_ref, h_ref, s_a, s_b, s_c, hook):
    put_stats(stat_ref, stats)
    norm_to(xt, stats, c_ref, LN_PAR, h_ref)
    for m, acc in enumerate((s_a, s_b, s_c)):
        acc[...] = tn(w[m], h_ref[...])
    cos, sin = cos_ref[...], sin_ref[...]
    for m, (acc, out) in enumerate(((s_a, q_ref), (s_b, k_ref), (s_c, v_ref))):
        for head in range(HEADS):
            rows, one, two = head_rows(head)
            if m == TWO:
                out[rows, :] = (acc[rows, :] + column(c_ref, rows, B_ATTN + m)).astype(BF16)
                continue
            a, b = [acc[half, :] + column(c_ref, half, B_ATTN + m) for half in (one, two)]
            if m == ZERO:
                a, b = a * HEAD ** -0.5, b * HEAD ** -0.5
            out[one, :] = (a * cos - b * sin).astype(BF16)
            out[two, :] = (b * cos + a * sin).astype(BF16)
    hook(ONE)
    key = lax.broadcasted_iota(jnp.int32, (SIXTEEN, TOK), ONE)
    row = lax.broadcasted_iota(jnp.int32, (SIXTEEN, TOK), ZERO)
    bias_rows = jnp.where((row == ZERO) & (key >= length), NEG_BIG, 0.0).astype(BF16)
    one_rows = jnp.where(row == ZERO, 1.0, 0.0).astype(BF16)
    scores = (s_a, s_b)

    def open_head(head):
        rows = head_rows(head)[ZERO]
        keys = jnp.concatenate([k_ref[rows, :], bias_rows], axis=ZERO)
        queries = jnp.concatenate([q_ref[rows, :], one_rows], axis=ZERO)
        scores[head % TWO][...] = tn(keys, queries)

    def weigh(head):
        value, tops, sums = scores[head % TWO], [], []

        def top(rows):
            tops.append(jnp.max(value[rows, :], axis=ZERO, keepdims=True))
            if rows.stop == TOK:
                tops[:] = [functools.reduce(jnp.maximum, tops)]

        def power(rows):
            weight = jnp.exp(value[rows, :] - tops[ZERO])
            value[rows, :] = weight
            sums.append(total(weight))
            if rows.stop == TOK:
                sums[:] = [1.0 / functools.reduce(jnp.add, sums)]

        def share(rows):
            p_buf[head, rows, :] = (value[rows, :] * sums[ZERO]).astype(BF16)

        return [functools.partial(run, rows) for run in (top, power, share) for rows in row_chunks()]

    def close_head(head):
        rows = head_rows(head)[ZERO]
        ctx = nn(v_ref[rows, :], p_buf[head])
        ctx_ref[rows, :] = ctx
        ctxb[rows, :] = ctx.astype(BF16)

    open_head(ZERO)
    for head in range(HEADS):
        products = [functools.partial(open_head, head + ONE)] if head + ONE < HEADS else []
        if head:
            products.append(functools.partial(close_head, head - ONE))
        woven(products, weigh(head))
        if head == THREE:
            hook(TWO)
    close_head(HEADS - ONE)


def mlp_forward(layer, ctxb, xt, wo, up, down, c_ref, mid_ref, act_ref, slope_ref, stat_ref, h_ref, s_a, s_b, hook):
    s_a[...] = tn(wo[...], ctxb[...])
    for rows in row_chunks():
        mid_ref[rows, :] = (xt[rows, :].astype(F32) + s_a[rows, :] + column(c_ref, rows, B_ATTN + THREE)).astype(BF16)
    stats = norm_stats(mid_ref)
    put_stats(stat_ref, stats)
    norm_to(mid_ref, stats, c_ref, LN_PAR + TWO, h_ref)
    hook(ONE)
    pre = (s_a, s_b)
    parts = [slice(DIM * k, DIM * k + DIM) for k in range(FOUR)]

    def open_part(k):
        pre[k % TWO][...] = tn(up[:, parts[k]], h_ref[...])

    open_part(ZERO)
    for k, part in enumerate(parts):
        if k < THREE:
            open_part(k + ONE)
        for rows in row_chunks():
            value = pre[k % TWO][rows, :] + column(c_ref, rows, B_UP + k)
            scaled = value * math.sqrt(0.5)
            cdf = 0.5 + 0.5 * lax.erf(scaled)
            density = jnp.exp2(scaled * scaled * -math.log2(math.e) - 0.5 * math.log2(2.0 * math.pi))
            there = slice(part.start + rows.start, part.start + rows.stop)
            act_ref[there, :] = (value * cdf).astype(BF16)
            slope_ref[there, :] = cdf + value * density
        if k == ONE:
            hook(TWO)

    @pl.when(layer == ZERO)
    def _():
        s_a[...] = tn(down[...], act_ref[...])
        for rows in row_chunks():
            xt[rows, :] = (mid_ref[rows, :].astype(F32) + s_a[rows, :] + column(c_ref, rows, B_DOWN)).astype(BF16)


def forward(lengths, x, tables, params):
    def saved(index, rows, dtype):
        return jax.ShapeDtypeStruct((TWO, SEQS, rows, TOK), dtype), pl.BlockSpec((ONE, ONE, rows, TOK), index)

    def attn_at(s):
        return s // EIGHT, jnp.where(s // FOUR % TWO == ZERO, s % FOUR, THREE), ZERO, ZERO

    def mlp_at(s):
        odd = s // FOUR % TWO == ONE
        return jnp.where(s < 12, ZERO, ONE), jnp.where(odd, s % FOUR, jnp.where(s < FOUR, ZERO, THREE)), ZERO, ZERO

    def xs_at(s):
        return jnp.where(s < FOUR, ZERO, ONE), jnp.where(s < EIGHT, s % FOUR, THREE), ZERO, ZERO

    outs = [saved(xs_at, DIM, BF16)] + [saved(attn_at, DIM, BF16)] * THREE
    outs += [(jax.ShapeDtypeStruct((TWO, SEQS, HEADS, TOK, TOK), BF16), pl.BlockSpec((ONE, ONE, HEADS, TOK, TOK), lambda s: (*attn_at(s), ZERO))), saved(attn_at, DIM, F32)]
    outs += [saved(mlp_at, DIM, BF16), saved(mlp_at, FFN, BF16), saved(mlp_at, FFN, F32), saved(attn_at, EIGHT, F32), saved(mlp_at, EIGHT, F32)]
    outs += [(jax.ShapeDtypeStruct((TWO, *COLS), F32), once((TWO, *COLS)))]
    weights = ((THREE, DIM, DIM), (DIM, DIM), (DIM, FFN), (FFN, DIM))
    outs += [(jax.ShapeDtypeStruct((TWO, *w), BF16), HBM) for w in weights]
    scratch = [(SEQS, *SQUARE), (SEQS, *SQUARE), *weights, SQUARE]
    scratch = [pltpu.VMEM(s, BF16) for s in scratch] + [pltpu.VMEM(SQUARE, F32)] * THREE + [pltpu.VMEM((*GRID, TWO, ONE, ONE, LANES), F32)]
    scratch += [pltpu.VMEM((TWO, *GRID, TWO, n, SIXTEEN, LANES), BF16) for n in (ONE, THREE) for _ in range(THREE)]
    scratch += [pltpu.VMEM((SEQS, EIGHT, TOK), F32)] + [pltpu.VMEM((15, n, SIXTEEN, LANES), BF16) for n in (ONE, THREE)]
    scratch += [pltpu.VMEM((15, ONE, ONE, LANES), F32), DMA((7, TWO, 5)), DMA((7, TWO, 5)), DMA((FOUR,)), DMA((SEQS,))]
    return pl.pallas_call(
        forward_kernel, grid=(SIXTEEN,),
        out_shape=[o[ZERO] for o in outs], out_specs=[o[ONE] for o in outs],
        in_specs=[pl.BlockSpec(memory_space=pltpu.SMEM), HBM, once((HALF, TOK)), once((HALF, TOK))] + [once(p.shape) for p in params],
        scratch_shapes=scratch,
        compiler_params=pltpu.CompilerParams(collective_id=ZERO, has_side_effects=True, vmem_limit_bytes=67043328,
                                             dimension_semantics=("arbitrary",)),
        name="forward")(lengths, x, *tables, *params)


def norm_back(dh_ref, x_ref, stats, c_ref, lane, sums, at, write, beside):
    mean, rstd = stats
    means = [0.0, 0.0]

    def both(rows):
        dh = dh_ref[rows, :]
        return dh, dh * column(c_ref, rows, lane), (x_ref[rows, :].astype(F32) - mean) * rstd

    def first(rows):
        dh, dxhat, xhat = both(rows)
        means[ZERO], means[ONE] = means[ZERO] + total(dxhat), means[ONE] + total(dxhat * xhat)
        sums[at, rows, :] += fold(dh * xhat)
        sums[at + ONE, rows, :] += fold(dh)

    def second(rows):
        dh, dxhat, xhat = both(rows)
        write(rows, rstd * (dxhat - means[ZERO] * (1.0 / DIM) - xhat * (means[ONE] * (1.0 / DIM))))

    woven(beside, [functools.partial(run, rows) for run in (first, second) for rows in row_chunks()])


def columns_of(partials):
    lane = lax.broadcasted_iota(jnp.int32, COLS, ONE)
    value = jnp.zeros(COLS, F32)
    for at, partial in enumerate(partials):
        value = jnp.where(lane == at, jnp.sum(partial, axis=ONE, keepdims=True), value)
    return value.T[:EIGHT]


def head_rows(head):
    return slice(HEAD * head, HEAD * head + HEAD), slice(HEAD * head, HEAD * head + HALF), slice(HEAD * head + HALF, HEAD * head + HEAD)


class Reduce:
    def __init__(self, place, units, grads, buffers, send, recv):
        self.units = units
        self.scatters = [Scatter(place, (lambda u, k=k: grads(units[k][u])), *buffers[k], ORDERS[k], send.at[k], recv.at[k]) for k in range(THREE)]

    def steps(self, store):
        def each(*names):
            def step():
                for name in names:
                    for s in self.scatters:
                        getattr(s, name)()
            return step

        def finish():
            for units, s in zip(self.units, self.scatters):
                s.finish(lambda u, full, units=units: store(units[u], full))

        return [each("swap"), each("swapped", "ring_start"), each("ring_turn"), each("plane_start"), each("last"), finish]


def backward_kernel(dy_ref, mid_ref, ctx_ref, st2_ref, q_ref, k_ref, v_ref, x_ref, st1_ref, cos_ref, sin_ref, c_ref, p_hbm, slope_hbm, act_hbm,
                    qkv_hbm, wo_hbm, up_hbm, down_hbm,
                    dx_ref, attn_out, up_out, down_out, small_out, *refs):
    (grad, dctx, delta, big, wqkv, wo, slope, act, dpre, h_ref, s_a, s_b, d_a, d_b, sums,
     g_qkv, g_wo, g_up, g_down, *small_bufs), refs = refs[:28], refs[28:]
    qkv_bufs, mo_bufs, refs = [refs[6 * k:6 * k + 6] for k in range(THREE)], [refs[6 * k + 18:6 * k + 24] for k in range(THREE)], refs[36:]
    send, recv, late_sem, plane_sem, big_sem, w_sem, mlp_sem = refs
    step = pl.program_id(ZERO)
    phase, seq = step // FOUR, lax.rem(step, FOUR)
    layer = ONE - step // EIGHT
    place = Place()

    def grads(unit):
        if unit < THREE:
            return g_qkv.at[unit]
        if unit == THREE:
            return g_wo
        if unit < EIGHT:
            return g_up.at[unit - FOUR]
        return g_down.at[:, :, :, unit - EIGHT]

    live = step < SIXTEEN
    turn = jnp.where(live, ZERO, ONE)
    qkv_sums = Reduce(place, ((ZERO,), (ONE,), (TWO,)), grads, [(a, ra, rb, rp.at[turn], *last) for a, ra, rb, rp, *last in qkv_bufs], send.at[turn], recv.at[turn])
    mo_sums = Reduce(place, COLOURS, grads, mo_bufs, send.at[TWO], recv.at[TWO])

    def third(i):
        one = pl.ds(i, ONE)
        bufs = [(a.at[one], ra.at[one], rb.at[:, one], rp.at[:, one], mine.at[one], other.at[one]) for a, ra, rb, rp, mine, other in mo_bufs]
        return Reduce(place, [units[i:i + ONE] for units in COLOURS], grads, bufs, send.at[THREE + i], recv.at[THREE + i]).steps(store(ONE - turn))

    small_refs = small_bufs[::THREE]
    early, middle, late = [Late(place, small_refs[i], small_bufs[THREE * i + ONE], late_sem.at[i, ZERO], late_sem.at[i, ONE], small_bufs[THREE * i + TWO],
                                plane_sem.at[i, ZERO], plane_sem.at[i, ONE]).steps() for i in range(THREE)]
    first_core = place.core == ZERO

    def store(l):
        def put(unit, full):
            if unit < EIGHT:
                mine = jnp.where(first_core, full[:FOUR], full[FOUR:])
                if unit < FOUR:
                    attn_out[l, unit] = mine
                else:
                    up_out[l, :, DIM * (unit - FOUR):DIM * (unit - THREE)] = mine
            else:
                at = EIGHT * (unit % TWO)

                @pl.when(place.core == (unit - EIGHT) // TWO)
                def _():
                    down_out[l, at:at + EIGHT] = full
        return put

    def mlp_weights(l):
        parts = [pl.ds(DIM * k, DIM) for k in range(FOUR)]
        return ([pltpu.make_async_copy(down_hbm.at[l, part], big.at[k], big_sem.at[k]) for k, part in enumerate(parts)],
                [pltpu.make_async_copy(up_hbm.at[l, :, part], big.at[FOUR + k], big_sem.at[FOUR + k]) for k, part in enumerate(parts)] +
                [pltpu.make_async_copy(wo_hbm.at[l], wo, w_sem.at[ZERO])])

    def attn_weights(l):
        return [pltpu.make_async_copy(qkv_hbm.at[l], wqkv, w_sem.at[ONE])]

    def probs(l, s):
        return [pltpu.make_async_copy(p_hbm.at[l, s, k], big.at[k], big_sem.at[k]) for k in range(HEADS)]

    def saved_mlp(l, s):
        return [pltpu.make_async_copy(slope_hbm.at[l, s], slope, mlp_sem.at[ZERO]), pltpu.make_async_copy(act_hbm.at[l, s], act, mlp_sem.at[ONE])]

    def start(copies):
        for copy in copies:
            copy.start()

    def wait(copies):
        for copy in copies:
            copy.wait()

    @pl.when(step == ZERO)
    def _():
        place.greet()
        start(mlp_weights(ONE)[ZERO] + saved_mlp(ONE, ZERO) + mlp_weights(ONE)[ONE] + attn_weights(ONE))

    pl.when(step == ONE)(place.met)
    mo_steps, qkv_steps = mo_sums.steps(store(ONE - turn)), qkv_sums.steps(store(ONE - turn))

    def plan(slots, steps):
        return [((slot,), run) for slot, run in zip(slots, steps)]

    thirds = [], []
    for i, slots in enumerate(((48, 50, 54, 59, 73, 74), (48, 51, 55, 62, 73, 74), (48, 53, 57, 63, 73, 74))):
        steps = plan(slots, third(i))
        thirds[ZERO].extend(steps[:FOUR])
        thirds[ONE].extend(steps[FOUR:])
    attn_hook = hooks(step * FOUR, plan((48, 57, 61, 63), middle) + plan((SIXTEEN, 24, 28), mo_steps) + thirds[ZERO] +
                      plan((53, 53), qkv_steps[FOUR:]))
    mlp_plan = plan((37, 45, 46), mo_steps[THREE:]) + plan((32, 36, 40, 47), qkv_steps) + plan((34, 41, 45, 47), early)
    mlp_hook = hooks(step * FOUR, mlp_plan + plan((64, 66, 70, 72, 75), qkv_steps) + plan((64, 72, 74, 75), late) + thirds[ONE] +
                     plan((75,), qkv_steps[5:]))


    @pl.when(phase % TWO == ZERO)
    def _():
        @pl.when((seq == ZERO) & live)
        def _():
            for ref in (g_wo, g_up, g_down, sums):
                ref[...] = jnp.zeros_like(ref)

        @pl.when(step < FOUR)
        def _():
            grad[seq] = dy_ref[ZERO].T

        @pl.when((seq == ZERO) & live)
        def _():
            wait(mlp_weights(layer)[ZERO])

        mlp_hook(ZERO)

        def after_first():
            pl.when(seq < THREE)(lambda: start(saved_mlp(layer, seq + ONE)))
            pl.when(seq == THREE)(lambda: start(probs(layer, ZERO)[:FOUR]))

        def before_second():
            pl.when(seq == ZERO)(lambda: wait(mlp_weights(layer)[ONE]))

        def after_second():
            pl.when(seq == THREE)(lambda: start(probs(layer, ZERO)[FOUR:]))

        pl.when(live)(lambda: wait(saved_mlp(layer, seq)))
        mlp_backward(grad.at[seq], slope, act, mid_ref, ctx_ref, st2_ref.at[ZERO], wo, big, c_ref, dctx.at[seq], delta.at[seq], g_wo, g_up, g_down,
                     dpre, h_ref, s_a, s_b, sums, pl.when(live), mlp_hook,
                     after_first, after_second, before_second)

        @pl.when((seq == THREE) & live)
        def _():
            value = columns_of([sums[i] for i in range(EIGHT)])

            @pl.when(layer == ONE)
            def _():
                small_refs[ZERO][:EIGHT, :] = value

            @pl.when(layer == ZERO)
            def _():
                small_refs[ONE][...] = value

        mlp_hook(THREE)

    @pl.when(phase % TWO == ONE)
    def _():
        @pl.when(seq == ZERO)
        def _():
            wait(attn_weights(layer))
            for ref in (g_qkv, sums):
                ref[...] = jnp.zeros_like(ref)

        @pl.when(step == FOUR)
        def _():
            start(saved_mlp(ZERO, ZERO))
        attn_hook(ZERO)

        def after_heads():
            pl.when(seq < THREE)(lambda: start(probs(layer, seq + ONE)))
            pl.when(step == 7)(lambda: start(mlp_weights(ZERO)[ZERO] + mlp_weights(ZERO)[ONE]))

        wait(probs(layer, seq))
        attn_backward(dctx.at[seq], delta.at[seq], big, q_ref, k_ref, v_ref, x_ref, st1_ref.at[ZERO], grad.at[seq], wqkv, c_ref, cos_ref, sin_ref,
                      g_qkv, dpre, h_ref, s_a, s_b, d_a, d_b, sums, attn_hook,
                      after_heads)

        @pl.when(seq == THREE)
        def _():
            value = columns_of([sums[i] for i in range(5)])

            @pl.when(layer == ONE)
            def _():
                small_refs[ZERO][EIGHT:, :] = value

            @pl.when(layer == ZERO)
            def _():
                small_refs[TWO][...] = value

        @pl.when(step == 7)
        def _():
            start(attn_weights(ZERO))

        @pl.when(step > 11)
        def _():
            dx_ref[ZERO] = grad[seq].T
        attn_hook(THREE)

    @pl.when(step == 18)
    def _():
        small_out[:SIXTEEN, :], small_out[SIXTEEN:24, :], small_out[24:, :] = [ref[...] for ref in small_refs]


def add_to(ref, value):
    ref[...] = ref[...] + value.reshape(ref.shape)


def mlp_backward(grad, slope, act, mid_ref, ctx_ref, stat_ref, wo, big, c_ref, dctx, delta, g_wo, g_up, g_down, dpre, h_ref, s_a, s_b, sums, when, hook, after_first, after_second, before_second):
    parts = [slice(DIM * k, DIM * k + DIM) for k in range(FOUR)]
    pre = (s_a, s_b)

    def dact(k):
        pre[k % TWO][...] = nn(big[k], grad[...])

    @when
    def _():
        def scale(k, chunk):
            there = slice(parts[k].start + chunk.start, parts[k].start + chunk.stop)
            value = pre[k % TWO][chunk, :] * slope[there, :]
            sums[k, chunk, :] += fold(value)
            dpre[there, :] = value.astype(BF16)

        def down_product(k):
            add_to(g_down.at[k], nt(act[parts[k], :], grad[...]))

        dact(ZERO)
        norm_to(mid_ref.at[ZERO], get_stats(stat_ref), c_ref, LN_PAR + TWO, h_ref)
        for k in range(FOUR):
            products = [functools.partial(down_product, k)]
            if k < THREE:
                products = [functools.partial(dact, k + ONE)] + products
            woven(products, [functools.partial(scale, k, chunk) for chunk in row_chunks()])
        after_first()
    hook(ONE)

    @when
    def _():
        before_second()
        s_a[...] = functools.reduce(jnp.add, [nn(big[FOUR + k], dpre[rows, :]) for k, rows in enumerate(parts)])
        after_second()
    hook(TWO)

    @when
    def _():
        def write(rows, dx):
            dy = grad[rows, :].astype(F32)
            dmid = (dy + dx).astype(BF16)
            grad[rows, :] = dmid
            sums[6, rows, :] += fold(dy)
            sums[7, rows, :] += fold(dmid.astype(F32))

        norm_back(s_a, mid_ref.at[ZERO], get_stats(stat_ref), c_ref, LN_PAR + TWO, sums, FOUR, write,
                  [lambda k=k, rows=rows: add_to(g_up.at[k], nt(h_ref[...], dpre[rows, :])) for k, rows in enumerate(parts)])
        add_to(g_wo, nt(ctx_ref[ZERO].astype(BF16), grad[...]))
        s_b[...] = nn(wo[...], grad[...])
        for head in range(HEADS):
            rows = head_rows(head)[ZERO]
            value = s_b[rows, :].astype(BF16)
            dctx[rows, :] = value
            delta[head:head + ONE, :] = total(value.astype(F32) * ctx_ref[ZERO, rows, :])


def attn_backward(dctx, delta, probs, q_ref, k_ref, v_ref, x_ref, stat_ref, grad, wqkv, c_ref, cos_ref, sin_ref, g_qkv, dproj, h_ref, s_a, s_b, d_a, d_b,
                  sums, hook, prefetch):
    scores, dscores = (s_a, s_b), (d_a, d_b)
    q, k, v = q_ref.at[ZERO], k_ref.at[ZERO], v_ref.at[ZERO]

    def open_head(head):
        rows = head_rows(head)[ZERO]
        scores[head % TWO][...] = tn(v[rows, :], dctx[rows, :])

    def weigh(head, rows):
        dscores[head % TWO][rows, :] = (probs[head, rows, :].astype(F32) * (scores[head % TWO][rows, :] - delta[head:head + ONE, :])).astype(BF16)

    def values(head):
        rows = head_rows(head)[ZERO]
        dv = nt(dctx[rows, :], probs[head])
        sums[TWO, rows, :] += fold(dv)
        dproj[TWO * DIM + rows.start:TWO * DIM + rows.stop, :] = dv.astype(BF16)

    def close_head(head, m):
        rows, one, two = head_rows(head)
        ds = dscores[head % TWO][...]
        value = nn(k[rows, :], ds) * HEAD ** -0.5 if m == ZERO else nt(q[rows, :], ds)
        cos, sin = cos_ref[...], sin_ref[...]
        a, b = value[:HALF], value[HALF:]
        for at, out in ((one, a * cos + b * sin), (two, b * cos - a * sin)):
            dproj[m * DIM + at.start:m * DIM + at.stop, :] = out.astype(BF16)
            sums[m, at, :] += fold(out)

    open_head(ZERO)
    for head in range(HEADS):
        products = [functools.partial(values, head)]
        if head:
            products = [functools.partial(close_head, head - ONE, m) for m in range(TWO)] + products
        if head + ONE < HEADS:
            products = [functools.partial(open_head, head + ONE)] + products
        woven(products, [functools.partial(weigh, head, rows) for rows in row_chunks()])
        if head == THREE:
            hook(ONE)
    for m in range(TWO):
        close_head(HEADS - ONE, m)
    prefetch()
    hook(TWO)
    norm_to(x_ref.at[ZERO], get_stats(stat_ref), c_ref, LN_PAR, h_ref)
    parts = [slice(DIM * m, DIM * m + DIM) for m in range(THREE)]
    s_a[...] = functools.reduce(jnp.add, [nn(wqkv[m], dproj[rows, :]) for m, rows in enumerate(parts)])

    def write(rows, dx):
        grad[rows, :] = (grad[rows, :].astype(F32) + dx).astype(BF16)

    norm_back(s_a, x_ref.at[ZERO], get_stats(stat_ref), c_ref, LN_PAR, sums, THREE, write,
              [lambda m=m, rows=rows: add_to(g_qkv.at[m], nt(h_ref[...], dproj[rows, :])) for m, rows in enumerate(parts)])


def backward(dy, xs, q, k, v, probs, ctx, mid, act, slope, st1, st2, c, tables, w_qkv, w_o, w_up, w_down):
    def mlp_at(s):
        s = jnp.minimum(s, 15)
        odd = s // FOUR % TWO == ONE
        return ONE - s // EIGHT, jnp.where(odd, THREE, s % FOUR), ZERO, ZERO

    def attn_at(s):
        s = jnp.minimum(s, 15)
        odd = s // FOUR % TWO == ONE
        return jnp.where(s < EIGHT, ONE, ZERO) + jnp.where((s > 7) & (s < 12), ONE, ZERO), jnp.where(odd, s % FOUR, jnp.where(s < FOUR, ZERO, THREE)), ZERO, ZERO

    per_mlp = pl.BlockSpec((None, ONE, *SQUARE), mlp_at)
    per_attn = pl.BlockSpec((None, ONE, *SQUARE), attn_at)

    def stat(at):
        return pl.BlockSpec((None, ONE, EIGHT, TOK), at)

    acc = [(*GRID, EIGHT, WIDTH)]
    scratch = [pltpu.VMEM((SEQS, *SQUARE), BF16), pltpu.VMEM((SEQS, *SQUARE), BF16), pltpu.VMEM((SEQS, HEADS, TOK), F32),
               pltpu.VMEM((HEADS, TOK, TOK), BF16), pltpu.VMEM((THREE, DIM, DIM), BF16), pltpu.VMEM((DIM, DIM), BF16),
               pltpu.VMEM(TALL, F32), pltpu.VMEM(TALL, BF16), pltpu.VMEM(TALL, BF16), pltpu.VMEM(SQUARE, BF16),
               pltpu.VMEM(SQUARE, F32), pltpu.VMEM(SQUARE, F32), pltpu.VMEM((TOK, TOK), BF16), pltpu.VMEM((TOK, TOK), BF16),
               pltpu.VMEM((EIGHT, *COLS), F32), pltpu.VMEM((THREE, *GRID, EIGHT, DIM), F32), pltpu.VMEM((*GRID, EIGHT, DIM), F32),
               pltpu.VMEM((FOUR, *GRID, EIGHT, DIM), F32), pltpu.VMEM((*GRID, FOUR, EIGHT, DIM), F32), *[pltpu.VMEM((*lead, rows, DIM), F32) for rows in (SIXTEEN, EIGHT, EIGHT) for lead in ((), (6,), (SIXTEEN,))]]
    for n in (ONE, THREE):
        for order in ORDERS:
            ring_a, ring_b, plane, *last = landing_shapes(order, n)
            plane = (TWO, *plane) if n == ONE else plane
            scratch += [pltpu.VMEM(s, F32) for s in ((n, *GRID, EIGHT, WIDTH), ring_a, ring_b, plane, *last)]
    scratch += [DMA((6, THREE, 9)), DMA((6, THREE, 9)), DMA((THREE, TWO, 6)), DMA((THREE, TWO)), DMA((EIGHT,)), DMA((TWO,)), DMA((TWO,))]
    outs = ((TWO, FOUR, FOUR, DIM), (TWO, FOUR, FFN), (TWO, SIXTEEN, DIM), (32, DIM))
    whole = [pl.BlockSpec(s, lambda i, n=len(s): (ZERO,) * n, pipeline_mode=pl.Buffered(ONE)) for s in outs]
    dx_at = lambda s: (jnp.clip(s - 12, ZERO, THREE), ZERO, ZERO)
    return pl.pallas_call(
        backward_kernel, grid=(19,),
        out_shape=[jax.ShapeDtypeStruct((SEQS, TOK, DIM), BF16)] + [jax.ShapeDtypeStruct(s, F32) for s in outs],
        out_specs=[pl.BlockSpec((ONE, TOK, DIM), dx_at)] + whole,
        in_specs=[pl.BlockSpec((ONE, TOK, DIM), lambda s: (jnp.minimum(s, THREE), ZERO, ZERO)), per_mlp, per_mlp, stat(mlp_at)] + [per_attn] * FOUR + [stat(attn_at),
                  once((HALF, TOK)), once((HALF, TOK)), pl.BlockSpec((None, *COLS), lambda s: (ONE - jnp.minimum(s, 15) // EIGHT, ZERO, ZERO))] + [HBM] * 7,
        scratch_shapes=scratch,
        compiler_params=pltpu.CompilerParams(collective_id=ONE, has_side_effects=True, vmem_limit_bytes=67043328,
                                             dimension_semantics=("arbitrary",)),
        name="backward")(dy, mid, ctx, st2, q, k, v, xs, st1, *tables, c, probs, slope, act, w_qkv, w_o, w_up, w_down)


def results_kernel(dx_ref, attn_ref, up_ref, down_ref, small_ref, dx_out, attn_out, gb_attn, g_ln, up_out, gb_up, down_out, gb_down):
    dx_out[...] = dx_ref[...]

    @pl.when(pl.program_id(ZERO) == ZERO)
    def _():
        me = lax.axis_index(AXIS)
        attn_out[...], up_out[...], down_out[...] = attn_ref[...], up_ref[...], down_ref[...]
        mine = pltpu.roll(small_ref[...], lax.rem(DIM - FOUR * me + FOUR * LANES, DIM), ONE)
        for l in range(TWO):
            mlp = SIXTEEN - SIXTEEN * l
            attn = mlp + EIGHT
            gb_attn[l, :THREE], gb_attn[l, THREE:] = mine[attn:attn + THREE, :FOUR], mine[mlp + 7:mlp + EIGHT, :FOUR]
            g_ln[l, :TWO], g_ln[l, TWO:] = mine[attn + THREE:attn + 5, :FOUR], mine[mlp + FOUR:mlp + 6, :FOUR]
            gb_down[l:l + ONE, :] = mine[mlp + 6:mlp + 7, :FOUR]
            ups = small_ref[pl.ds(mlp + me // 32, ONE), :]
            gb_up[l:l + ONE, :] = pltpu.roll(ups, lax.rem(DIM - SIXTEEN * lax.rem(me, 32), DIM), ONE)[:, :SIXTEEN]


def results(dx, attn, up, down, small):
    shapes = [attn.shape, (TWO, FOUR, FOUR), (TWO, FOUR, FOUR), up.shape, (TWO, SIXTEEN), down.shape, (TWO, FOUR)]
    per = pl.BlockSpec((TWO, TOK, DIM), lambda s: (s, ZERO, ZERO))
    return pl.pallas_call(
        results_kernel, grid=(SEQS // TWO,), name="results",
        out_shape=[jax.ShapeDtypeStruct(dx.shape, BF16)] + [jax.ShapeDtypeStruct(s, F32) for s in shapes],
        in_specs=[per] + [once(a.shape) for a in (attn, up, down, small)],
        out_specs=[per] + [once(s) for s in shapes])(dx, attn, up, down, small)


def solution(mesh):
    batch_spec = P(AXIS)
    weight_specs = (P(None, None, AXIS, None), P(None, None, AXIS), P(None, None, AXIS),
                    P(None, AXIS, None), P(None, AXIS), P(None, AXIS, None), P(None, AXIS))

    def device_step(x, lengths, d_y, w_attn, b_attn, ln_par, w_up, b_up, w_down, b_down):
        tables = rotary_tables()
        xs, q, k, v, probs, ctx, mid, act, slope, st1, st2, c, w_qkv, w_o, w_up, w_down = forward(
            lengths, x, tables, (w_attn, b_attn, ln_par, w_up, b_up, w_down, b_down))
        return results(*backward(d_y, xs, q, k, v, probs, ctx, mid, act, slope, st1, st2, c, tables, w_qkv, w_o, w_up, w_down))

    return jax.shard_map(device_step, mesh=mesh,
                         in_specs=(batch_spec, batch_spec, batch_spec) + weight_specs,
                         out_specs=(batch_spec,) + weight_specs,
                         check_vma=False)
```

```python
import math
import functools
import jax
import jax.numpy as jnp
from jax import lax
from jax.experimental import pallas as pl
from jax.experimental.pallas import tpu as pltpu
from jax.sharding import PartitionSpec as P

ZERO, ONE, TWO, THREE, FOUR = range(5)
EIGHT, SIXTEEN, WIDTH = 8, 16, 256

F32, BF16 = jnp.float32, jnp.bfloat16
SEQS, TOK, DIM, FFN, HEADS, HEAD, LANES = FOUR, 512, 512, 2048, EIGHT, 64, 128
HALF = HEAD // TWO
EPS = 1e-5
THETA = 10000.0
NEG_BIG = -1e30
B_ATTN, LN_PAR, B_UP, B_DOWN = ZERO, FOUR, EIGHT, 12


def nn(a, b):
    return lax.dot_general(a, b, (((ONE,), (ZERO,)), ((), ())), preferred_element_type=F32)


def nt(a, b):
    return lax.dot_general(a, b, (((ONE,), (ONE,)), ((), ())), preferred_element_type=F32)


def tn(a, b):
    return lax.dot_general(a, b, (((ZERO,), (ZERO,)), ((), ())), preferred_element_type=F32)


def lane_tiles(width=TOK, size=LANES):
    return [slice(i, i + size) for i in range(ZERO, width, size)]


def row_chunks(rows=DIM, size=64):
    return [slice(i, i + size) for i in range(ZERO, rows, size)]


def column(c_ref, rows, lane):
    return jnp.broadcast_to(c_ref[rows, lane:lane + ONE], (rows.stop - rows.start, TOK))


def total(value):
    return jnp.sum(value, axis=ZERO, keepdims=True)


def norm_stats(x_ref):
    mean = functools.reduce(jnp.add, [total(x_ref[rows, :].astype(F32)) for rows in row_chunks()]) * (1.0 / DIM)
    squares = []
    for rows in row_chunks():
        centred = x_ref[rows, :].astype(F32) - mean
        squares.append(total(centred * centred))
    return mean, lax.rsqrt(functools.reduce(jnp.add, squares) * (1.0 / DIM) + EPS)


def norm_to(x_ref, stats, c_ref, lane, h_ref):
    mean, rstd = stats
    for rows in row_chunks():
        xhat = (x_ref[rows, :].astype(F32) - mean) * rstd
        h_ref[rows, :] = (xhat * column(c_ref, rows, lane) + column(c_ref, rows, lane + ONE)).astype(BF16)


def put_stats(ref, stats):
    ref[ZERO:ONE, :], ref[ONE:TWO, :] = stats


def get_stats(ref):
    return ref[ZERO:ONE, :], ref[ONE:TWO, :]


def woven(products, rest):
    done = ZERO
    for n, step in enumerate(rest):
        while done < len(products) and done * len(rest) <= n * len(products):
            products[done]()
            done += ONE
        step()
    for product in products[done:]:
        product()


def fold(value):
    parts = [value[:, cols] for cols in lane_tiles(value.shape[ONE])]
    return functools.reduce(jnp.add, parts)


def seq_spec(shape):
    return pl.BlockSpec((ONE, *shape), lambda s: (s,) + (ZERO,) * len(shape))


def once(shape):
    return pl.BlockSpec(shape, lambda s: (ZERO,) * len(shape), pipeline_mode=pl.Buffered(ONE))


def act_shape(rows, dtype):
    return jax.ShapeDtypeStruct((SEQS, rows, TOK), dtype)


PARAMS = pltpu.CompilerParams(vmem_limit_bytes=60 << 20, dimension_semantics=("arbitrary",))
SQUARE, TALL, WIDE, COLS = (DIM, TOK), (FFN, TOK), (DIM, FFN), (DIM, LANES)


def rotary_tables():
    inv_freq = 1.0 / (THETA ** (jnp.arange(HALF, dtype=F32) * (2.0 / HEAD)))
    angles = inv_freq[:, None] * jnp.arange(TOK, dtype=F32)[None, :]
    return jnp.cos(angles), jnp.sin(angles)


MESH = pl.DeviceIdType.MESH
AXIS = "fsdp"
ORDERS = ((TWO, ONE, ZERO), (ONE, ZERO, TWO), (ZERO, TWO, ONE))


class Place:
    def __init__(self):
        me = lax.axis_index(AXIS)
        self.core = lax.rem(me, TWO)
        self.pos = (me // 32, lax.rem(me // EIGHT, FOUR), lax.rem(me // TWO, FOUR))
        self.partner = me + ONE - TWO * self.core
        self.near = [[lax.rem(at + delta, FOUR) if delta else at for delta in range(FOUR)] for at in self.pos]

    def coord(self, dim, delta):
        if isinstance(delta, int):
            return self.near[dim][delta % FOUR]
        return lax.rem(self.pos[dim] + delta, FOUR)

    def device(self, offsets):
        pos = [self.coord(dim, offsets.get(dim, ZERO)) for dim in range(THREE)]
        return pos[ZERO] * 32 + pos[ONE] * EIGHT + pos[TWO] * TWO + self.core

    def greet(self):
        barrier = pltpu.get_barrier_semaphore()
        for i in range(ONE, 64):
            offsets = {ZERO: i // SIXTEEN, ONE: i // FOUR % FOUR, TWO: i % FOUR}
            if min(offsets.values()) == ZERO:
                pl.semaphore_signal(barrier, inc=ONE, device_id=(self.device(offsets),), device_id_type=MESH)
        pl.semaphore_signal(barrier, inc=ONE, device_id=(self.partner,), device_id_type=MESH)

    def met(self):
        pl.semaphore_wait(pltpu.get_barrier_semaphore(), 37)


def remote(src, dst, send_sem, recv_sem, device):
    return pltpu.make_async_remote_copy(src_ref=src, dst_ref=dst, send_sem=send_sem, recv_sem=recv_sem,
                                        device_id=(device,), device_id_type=MESH)


LINE = (ONE, -ONE, TWO)


def each_of_plane(order, run):
    @pl.loop(ZERO, FOUR)
    def _(high):
        for low in range(FOUR):
            step = functools.partial(run, FOUR * high + low, {order[ONE]: high, order[TWO]: low})
            if low:
                step()
            else:
                pl.when(high > ZERO)(step)


class Gather:
    def __init__(self, place, buf, fifteen, order, send, recv):
        self.place, self.buf, self.fifteen, self.order, self.send, self.recv = place, buf, fifteen, order, send, recv

    def block(self, offsets, whole=()):
        index = [slice(ZERO, FOUR) if dim in whole else pl.ds(self.place.coord(dim, offsets.get(dim, ZERO)), ONE) for dim in range(THREE)]
        return self.buf.at[index[ZERO], index[ONE], index[TWO], pl.ds(self.place.core, ONE)]

    def copy(self, ref, key, device):
        return remote(ref, ref, self.send.at[key], self.recv.at[key], device)

    def plane_start(self):
        each_of_plane(self.order, lambda k, offsets: self.copy(self.block({}), ZERO, self.place.device(offsets)).start())

    def plane_all(self):
        return self.copy(self.fifteen, ZERO, self.place.partner)

    def plane_wait(self):
        self.plane_all().wait_recv()

    def line(self, i, sign):
        offsets = {self.order[ZERO]: sign * LINE[i]}
        return self.block(offsets, self.order[ONE:])

    def line_start(self):
        for i, delta in enumerate(LINE):
            self.copy(self.line(i, ZERO), ONE + i, self.place.device({self.order[ZERO]: delta})).start()

    def line_wait(self):
        for i in range(THREE):
            self.copy(self.line(i, -ONE), ONE + i, self.place.partner).wait_recv()

    def share(self, core):
        return self.copy(self.buf.at[:, :, :, pl.ds(core, ONE)], FOUR, self.place.partner)

    def share_start(self):
        self.share(self.place.core).start()

    def end(self):
        self.share(ONE - self.place.core).wait_recv()
        self.plane_all().wait_send()
        for i in range(THREE):
            self.copy(self.line(i, ZERO), ONE + i, self.place.partner).wait_send()
        self.share(self.place.core).wait_send()


def gather_steps(gathers):
    def each(*names):
        def step():
            for name in names:
                for g in gathers:
                    getattr(g, name)()
        return step

    return [each("plane_start"), each("plane_wait", "line_start"), each("line_wait", "share_start"), each("end")]


class Scatter:
    def __init__(self, place, grads, acc, got_a, got_b, got_p, mine, other, order, send, recv):
        self.place, self.grads, self.acc, self.order = place, grads, acc, order
        self.got_a, self.got_b, self.got_p, self.mine, self.other, self.send, self.recv = got_a, got_b, got_p, mine, other, send, recv
        self.units = acc.shape[ZERO]

    def columns(self, core):
        return pl.ds(pl.multiple_of(core * WIDTH, WIDTH), WIDTH)

    def swap_copy(self, u):
        place = self.place
        return remote(self.grads(u).at[:, :, :, :, self.columns(ONE - place.core)], self.acc.at[u], self.send.at[6 + u], self.recv.at[6 + u], place.partner)

    def swap(self):
        for u in range(self.units):
            self.swap_copy(u).start()

    def swapped(self):
        for u in range(self.units):
            self.swap_copy(u).wait()
            grad, acc = self.grads(u), self.acc

            @pl.loop(ZERO, FOUR)
            def _(z):
                acc[u, z] = acc[u, z] + grad[z, :, :, :, self.columns(self.place.core)]

    def part(self, delta, half=None):
        index = [slice(ZERO, FOUR)] * THREE
        index[self.order[ZERO]] = pl.ds(self.place.coord(self.order[ZERO], delta), ONE)
        return self.acc.at[:, index[ZERO], index[ONE], index[TWO], :, slice(ZERO, WIDTH) if half is None else lane_tiles()[half]]

    def ring(self, step, way):
        delta = (ONE, -ONE)[way]
        device = self.place.device({self.order[ZERO]: delta})
        if step == ZERO:
            src, dst = self.part(TWO, way), self.got_a.at[:, :, :, :, :, lane_tiles()[way]]
        else:
            src, dst = self.part(delta), self.got_b.at[way]
        key = TWO * step + way
        return remote(src, dst, self.send.at[key], self.recv.at[key], device)

    def ring_start(self):
        for way in range(TWO):
            self.ring(ZERO, way).start()

    def ring_turn(self):
        for way in range(TWO):
            self.ring(ZERO, way).wait_recv()
            self.add((ONE, -ONE)[way], way, self.got_a)
            self.ring(ONE, way).start()

    def add(self, delta, half, *refs):
        dim, acc = self.order[ZERO], self.acc
        at = self.place.coord(dim, delta)
        columns = slice(ZERO, WIDTH) if half is None else lane_tiles()[half]

        @pl.loop(ZERO, FOUR)
        def _(i):
            index = [i if d == self.order[ONE] else slice(ZERO, FOUR) for d in range(THREE)]
            there = [slice(None), *index, slice(None), columns]
            here = list(there)
            here[ONE + dim] = pl.ds(at, ONE)
            there[ONE + dim] = slice(ZERO, ONE)
            value = acc[tuple(here)]
            for ref in refs:
                value = value + ref[tuple(there)]
            acc[tuple(here)] = value

    def plane_copy(self, k, offsets):
        index = [pl.ds(self.place.coord(dim, offsets.get(dim, ZERO)), ONE) for dim in range(THREE)]
        src = self.acc.at[:, index[ZERO], index[ONE], index[TWO]]
        return remote(src, self.got_p.at[k], self.send.at[FOUR], self.recv.at[FOUR], self.place.device(offsets))

    def plane_all(self):
        return remote(self.got_p.at[ONE:], self.got_p.at[ONE:], self.send.at[FOUR], self.recv.at[FOUR], self.place.partner)

    def plane_start(self):
        for way in range(TWO):
            self.ring(ONE, way).wait_recv()
        self.add(ZERO, None, self.got_b.at[ZERO], self.got_b.at[ONE])

        each_of_plane(self.order, lambda k, offsets: self.plane_copy(k, offsets).start())

    def own(self):
        z, y, x = [pl.ds(p, ONE) for p in self.place.pos]
        return self.acc.at[:, z, y, x]

    def last_copy(self):
        return remote(self.mine, self.other, self.send.at[5], self.recv.at[5], self.place.partner)

    def last(self):
        self.plane_all().wait_recv()
        self.mine[...] = functools.reduce(jnp.add, [self.got_p[k] for k in range(ONE, SIXTEEN)], self.own()[...])
        for step in range(TWO):
            for way in range(TWO):
                self.ring(step, way).wait_send()
        self.plane_all().wait_send()
        self.last_copy().start()

    def finish(self, store):
        self.last_copy().wait_recv()
        first = self.place.core == ZERO
        for u in range(self.units):
            own, came = self.mine[u, ZERO, ZERO, ZERO], self.other[u, ZERO, ZERO, ZERO]
            store(u, jnp.concatenate([jnp.where(first, own, came), jnp.where(first, came, own)], axis=ONE))
        self.last_copy().wait_send()


def landing_shapes(order, units):
    size = [FOUR, FOUR, FOUR]
    size[order[ZERO]] = ONE
    return (units, *size, EIGHT, WIDTH), (TWO, units, *size, EIGHT, WIDTH), (SIXTEEN, units, ONE, ONE, ONE, EIGHT, WIDTH), (units, ONE, ONE, ONE, EIGHT, WIDTH), (units, ONE, ONE, ONE, EIGHT, WIDTH)


class Small:
    def __init__(self, place, value, slots, send, recv):
        self.place, self.value, self.slots, self.send, self.recv = place, value, slots, send, recv

    def peers(self, stage):
        if stage == THREE:
            return [self.place.partner]
        return [self.place.device({stage: delta}) for delta in LINE]

    def copies(self, stage):
        return [remote(self.value, self.slots.at[THREE * stage + k], self.send.at[THREE * stage + k], self.recv.at[THREE * stage + k], peer)
                for k, peer in enumerate(self.peers(stage))]

    def start(self, stage):
        for copy in self.copies(stage):
            copy.start()

    def finish(self, stage):
        copies = self.copies(stage)
        for copy in copies:
            copy.wait()
        self.value[...] = functools.reduce(jnp.add, [self.slots[THREE * stage + k] for k in range(len(copies))], self.value[...])

    def turn(self, stage):
        def step():
            self.finish(stage)
            self.start(stage + ONE)
        return step

    def steps(self):
        return [lambda: self.start(ZERO), self.turn(ZERO), self.turn(ONE), self.turn(TWO), lambda: self.finish(THREE)]


class Late(Small):
    def __init__(self, place, value, slots, send, recv, planes, plane_send, plane_recv):
        super().__init__(place, value, slots, send, recv)
        self.planes, self.plane_send, self.plane_recv = planes, plane_send, plane_recv

    def peers(self, stage):
        return super().peers({ZERO: ORDERS[ZERO][ZERO], ONE: THREE}[stage])

    def plane(self, k, offsets):
        return remote(self.value, self.planes.at[k], self.plane_send, self.plane_recv, self.place.device(offsets))

    def steps(self):
        def first():
            each_of_plane(ORDERS[ZERO], lambda k, offsets: self.plane(k, offsets).start())

        def second():
            remote(self.planes.at[ONE:], self.planes.at[ONE:], self.plane_send, self.plane_recv, self.place.partner).wait()
            self.value[...] = functools.reduce(jnp.add, [self.planes[k] for k in range(ONE, SIXTEEN)], self.value[...])
            self.start(ZERO)

        return [first, second, self.turn(ZERO), lambda: self.finish(ONE)]


VMEM = pl.BlockSpec(memory_space=pltpu.VMEM)
HBM = pl.BlockSpec(memory_space=pl.ANY)
DMA = pltpu.SemaphoreType.DMA


COLOURS = ((THREE, FOUR, 5), (6, 7, EIGHT), (9, 10, 11))
GRID = (FOUR, FOUR, FOUR)


def spread(buf, u, out_ref, column_base):
    @pl.loop(ZERO, FOUR)
    def _(z):
        for part in range(EIGHT):
            g = z * EIGHT + part
            tiles = [buf[z, part // TWO, part % TWO * TWO + k // TWO, k % TWO, u].astype(F32) for k in range(FOUR)]
            rows = pl.ds(pl.multiple_of(g * SIXTEEN, SIXTEEN), SIXTEEN)
            for j, cols in enumerate(lane_tiles()):
                value = jnp.concatenate([t[FOUR * j:FOUR * j + FOUR] for t in tiles], axis=ZERO).astype(BF16)
                out_ref[rows, column_base + cols.start:column_base + cols.stop] = value


def spread_down(buf, u, out_ref, cols):
    @pl.loop(ZERO, SIXTEEN)
    def _(i):
        for k in range(EIGHT):
            d = i * EIGHT + k
            out_ref[pl.ds(pl.multiple_of(d * SIXTEEN, SIXTEEN), SIXTEEN), cols] = buf[i // FOUR, lax.rem(i, FOUR), k // TWO, k % TWO, u]


def same(shape, test):
    row = lax.broadcasted_iota(jnp.int32, shape, ZERO)
    col = lax.broadcasted_iota(jnp.int32, shape, ONE)
    return jnp.where(test(row, col), 1.0, 0.0)


def small_columns(small_ref, c_ref):
    rows = [small_ref[z, y, x, c, ZERO] for z in range(FOUR) for y in range(FOUR) for x in range(FOUR) for c in range(TWO)]
    table = jnp.concatenate(rows, axis=ZERO).astype(BF16)
    quads = nn(same((DIM, LANES), lambda r, c: r // FOUR == c).astype(BF16), table)
    quads = (quads * same((DIM, LANES), lambda r, c: r % FOUR == c % FOUR)).astype(BF16)
    mask = same((DIM, LANES), lambda r, c: r % SIXTEEN == c % SIXTEEN)
    pick = same((DIM, 32), lambda r, c: r // SIXTEEN == c).astype(BF16)
    ups = [(nn(pick, table[32 * k:32 * k + 32]) * mask).astype(BF16) for k in range(FOUR)]
    for layer in range(TWO):
        def is_up(r):
            return r // SIXTEEN == layer * FOUR + TWO

        value = nn(quads, same((LANES, LANES), lambda r, c: (r // 64 == layer) & (r % 64 // FOUR == c) & ~is_up(r)).astype(BF16))
        for k in range(FOUR):
            value = value + nn(ups[k], same((LANES, LANES), lambda r, c: is_up(r) & (c == B_UP + k)).astype(BF16))
        c_ref[layer] = value


def tile_of(rows):
    rows = rows.astype(F32)
    return jnp.concatenate([rows[:, cols] for cols in lane_tiles()], axis=ZERO).astype(BF16)


def small_row(b_attn, ln_par, b_up, b_down):
    lane = lax.broadcasted_iota(jnp.int32, (ONE, LANES), ONE)
    row = jnp.zeros((ONE, LANES), F32)
    pieces = []
    for l in range(TWO):
        for m in range(FOUR):
            pieces += [(b_attn[l, m:m + ONE, :], 64 * l + FOUR * m), (ln_par[l, m:m + ONE, :], 64 * l + FOUR * m + SIXTEEN)]
        pieces += [(b_up[l:l + ONE, :], 64 * l + 32), (b_down[l:l + ONE, :], 64 * l + 48)]
    for piece, at in pieces:
        n = piece.shape[ONE]
        wide = jnp.concatenate([piece.astype(F32), jnp.zeros((ONE, LANES - n), F32)], axis=ONE)
        wide = pltpu.roll(wide, at, ONE) if at else wide
        row = jnp.where((lane >= at) & (lane < at + n), wide, row)
    return row


def hooks(slot, plan):
    def hook(at):
        for slots, run in plan:
            mine = [when for when in slots if when % FOUR == at]
            if mine:
                pl.when(functools.reduce(jnp.logical_or, [slot + at == when for when in mine]))(run)
    return hook


def forward_kernel(len_ref, x_hbm, cos_ref, sin_ref, w_attn, b_attn, ln_par, w_up, b_up, w_down, b_down,
                   xs_out, q_ref, k_ref, v_ref, p_ref, ctx_ref, mid_ref, act_ref, slope_ref, st1_ref, st2_ref, c_ref,
                   nat_qkv, nat_wo, nat_up, nat_down,
                   xs, ctxb, n_qkv, n_wo, n_up, n_down, h_ref, s_a, s_b, s_c,
                   sbuf, q0, q1, q2, m0, m1, m2, stats, f0, f1, f2, send, recv, nat_sem, x_sem):
    step = pl.program_id(ZERO)
    phase, seq, layer = step // FOUR, lax.rem(step, FOUR), step // EIGHT
    place = Place()
    z, y, x = place.pos
    qkv_bufs, mo_bufs, fifteen = (q0, q1, q2), (m0, m1, m2), (f0, f1, f2)

    def group(bufs, base, l):
        return [Gather(place, b.at[l], fifteen[base // THREE], ORDERS[k], send.at[base + k, l], recv.at[base + k, l]) for k, b in enumerate(bufs)]

    little = Gather(place, sbuf, fifteen[TWO], ORDERS[ZERO], send.at[6, ZERO], recv.at[6, ZERO])

    def nat_copies(which, l):
        if which == ZERO:
            return [pltpu.make_async_copy(n_qkv, nat_qkv.at[l], nat_sem.at[ZERO])]
        return [pltpu.make_async_copy(src, dst.at[l], nat_sem.at[ONE + i]) for i, (src, dst) in enumerate(((n_wo, nat_wo), (n_up, nat_up), (n_down, nat_down)))]

    def wait(copies):
        for copy in copies:
            copy.wait()

    def start(copies):
        for copy in copies:
            copy.start()

    def take_qkv():
        pl.when(step > ZERO)(lambda: wait(nat_copies(ZERO, layer)))
        for m in range(THREE):
            spread(qkv_bufs[m].at[layer], ZERO, n_qkv.at[m], ZERO)
        start(nat_copies(ZERO, layer))

    def take_mo():
        pl.when(step > EIGHT)(lambda: wait(nat_copies(ONE, layer)))
        for colour in range(THREE):
            for u, unit in enumerate(COLOURS[colour]):
                buf = mo_bufs[colour].at[layer]
                if unit == THREE:
                    spread(buf, u, n_wo, ZERO)
                elif unit < EIGHT:
                    spread(buf, u, n_up, DIM * (unit - FOUR))
                else:
                    spread_down(buf, u, n_down, lane_tiles()[unit - EIGHT])
        start(nat_copies(ONE, layer))

    x_copies = [pltpu.make_async_copy(x_hbm.at[s], ctxb.at[s], x_sem.at[s]) for s in range(SEQS)]

    @pl.when(step == ZERO)
    def _():
        place.greet()
        start(x_copies)
        for l in range(TWO):
            for unit in range(12):
                if unit < FOUR:
                    tile = tile_of(w_attn[l, unit])
                elif unit < EIGHT:
                    tile = tile_of(w_up[l, :, DIM * (unit - FOUR):DIM * (unit - THREE)])
                else:
                    tile = w_down[l, :, lane_tiles()[unit - EIGHT]]
                if unit < THREE:
                    qkv_bufs[unit][l, z, y, x, place.core, ZERO] = tile
                else:
                    mo_bufs[(unit - THREE) // THREE][l, z, y, x, place.core, (unit - THREE) % THREE] = tile
        sbuf[z, y, x, place.core, ZERO] = small_row(b_attn, ln_par, b_up, b_down)
        parts = group(qkv_bufs, ZERO, ZERO)
        first, second = gather_steps([little] + parts), gather_steps(group(mo_bufs, THREE, ZERO))

        def ready(s):
            x_copies[s].wait()
            xs[s] = ctxb[s].T
            put_stats(stats.at[s], norm_stats(xs.at[s]))

        place.met()
        first[ZERO]()
        second[ZERO]()
        ready(ZERO)
        ready(ONE)
        first[ONE]()
        ready(TWO)
        ready(THREE)
        first[TWO]()
        second[ONE]()
        little.end()
        small_columns(sbuf, c_ref)
        for part in parts:
            part.end()

    attn_hook = hooks(step * FOUR, [((when, when + 32), run) for when, run in zip((9, 13), gather_steps(group(mo_bufs, THREE, layer))[TWO:])])
    mlp_steps = gather_steps(group(qkv_bufs, ZERO, ONE)) + gather_steps(group(mo_bufs, THREE, ONE))[:TWO]
    mlp_hook = hooks(step * FOUR, [((when,), run) for when, run in zip((SIXTEEN, 25, 30, 31, 17, 26), mlp_steps)])

    @pl.when(phase % TWO == ZERO)
    def _():
        pl.when(seq == ZERO)(take_qkv)

        @pl.when(step < FOUR)
        def _():
            xs_out[ZERO, ZERO] = xs[seq]

        @pl.when(step > 7)
        def _():
            put_stats(stats.at[seq], norm_stats(xs.at[seq]))

        attn_hook(ZERO)
        attn_forward(len_ref[seq], xs.at[seq], n_qkv, c_ref.at[layer], cos_ref, sin_ref, q_ref.at[ZERO, ZERO], k_ref.at[ZERO, ZERO],
                     v_ref.at[ZERO, ZERO], p_ref.at[ZERO, ZERO], ctx_ref.at[ZERO, ZERO], ctxb.at[seq], get_stats(stats.at[seq]), st1_ref.at[ZERO, ZERO], h_ref, s_a, s_b, s_c, attn_hook)
        attn_hook(THREE)

    @pl.when(phase % TWO == ONE)
    def _():
        pl.when(seq == ZERO)(take_mo)
        mlp_hook(ZERO)
        mlp_forward(layer, ctxb.at[seq], xs.at[seq], n_wo, n_up, n_down, c_ref.at[layer], mid_ref.at[ZERO, ZERO], act_ref.at[ZERO, ZERO], slope_ref.at[ZERO, ZERO],
                    st2_ref.at[ZERO, ZERO], h_ref, s_a, s_b, mlp_hook)

        @pl.when(layer == ZERO)
        def _():
            xs_out[ZERO, ZERO] = xs[seq]
        mlp_hook(THREE)

    @pl.when(step == 15)
    def _():
        for which in range(TWO):
            wait(nat_copies(which, ONE))


def attn_forward(length, xt, w, c_ref, cos_ref, sin_ref, q_ref, k_ref, v_ref, p_buf, ctx_ref, ctxb, stats, stat_ref, h_ref, s_a, s_b, s_c, hook):
    put_stats(stat_ref, stats)
    norm_to(xt, stats, c_ref, LN_PAR, h_ref)
    for m, acc in enumerate((s_a, s_b, s_c)):
        acc[...] = tn(w[m], h_ref[...])
    cos, sin = cos_ref[...], sin_ref[...]
    for m, (acc, out) in enumerate(((s_a, q_ref), (s_b, k_ref), (s_c, v_ref))):
        for head in range(HEADS):
            rows, one, two = head_rows(head)
            if m == TWO:
                out[rows, :] = (acc[rows, :] + column(c_ref, rows, B_ATTN + m)).astype(BF16)
                continue
            a, b = [acc[half, :] + column(c_ref, half, B_ATTN + m) for half in (one, two)]
            if m == ZERO:
                a, b = a * HEAD ** -0.5, b * HEAD ** -0.5
            out[one, :] = (a * cos - b * sin).astype(BF16)
            out[two, :] = (b * cos + a * sin).astype(BF16)
    hook(ONE)
    key = lax.broadcasted_iota(jnp.int32, (SIXTEEN, TOK), ONE)
    row = lax.broadcasted_iota(jnp.int32, (SIXTEEN, TOK), ZERO)
    bias_rows = jnp.where((row == ZERO) & (key >= length), NEG_BIG, 0.0).astype(BF16)
    one_rows = jnp.where(row == ZERO, 1.0, 0.0).astype(BF16)
    scores = (s_a, s_b)

    def open_head(head):
        rows = head_rows(head)[ZERO]
        keys = jnp.concatenate([k_ref[rows, :], bias_rows], axis=ZERO)
        queries = jnp.concatenate([q_ref[rows, :], one_rows], axis=ZERO)
        scores[head % TWO][...] = tn(keys, queries)

    def weigh(head):
        value, tops, sums = scores[head % TWO], [], []

        def top(rows):
            tops.append(jnp.max(value[rows, :], axis=ZERO, keepdims=True))
            if rows.stop == TOK:
                tops[:] = [functools.reduce(jnp.maximum, tops)]

        def power(rows):
            weight = jnp.exp(value[rows, :] - tops[ZERO])
            value[rows, :] = weight
            sums.append(total(weight))
            if rows.stop == TOK:
                sums[:] = [1.0 / functools.reduce(jnp.add, sums)]

        def share(rows):
            p_buf[head, rows, :] = (value[rows, :] * sums[ZERO]).astype(BF16)

        return [functools.partial(run, rows) for run in (top, power, share) for rows in row_chunks()]

    def close_head(head):
        rows = head_rows(head)[ZERO]
        ctx = nn(v_ref[rows, :], p_buf[head])
        ctx_ref[rows, :] = ctx
        ctxb[rows, :] = ctx.astype(BF16)

    open_head(ZERO)
    for head in range(HEADS):
        products = [functools.partial(open_head, head + ONE)] if head + ONE < HEADS else []
        if head:
            products.append(functools.partial(close_head, head - ONE))
        woven(products, weigh(head))
        if head == THREE:
            hook(TWO)
    close_head(HEADS - ONE)


def mlp_forward(layer, ctxb, xt, wo, up, down, c_ref, mid_ref, act_ref, slope_ref, stat_ref, h_ref, s_a, s_b, hook):
    s_a[...] = tn(wo[...], ctxb[...])
    for rows in row_chunks():
        mid_ref[rows, :] = (xt[rows, :].astype(F32) + s_a[rows, :] + column(c_ref, rows, B_ATTN + THREE)).astype(BF16)
    stats = norm_stats(mid_ref)
    put_stats(stat_ref, stats)
    norm_to(mid_ref, stats, c_ref, LN_PAR + TWO, h_ref)
    hook(ONE)
    pre = (s_a, s_b)
    parts = [slice(DIM * k, DIM * k + DIM) for k in range(FOUR)]

    def open_part(k):
        pre[k % TWO][...] = tn(up[:, parts[k]], h_ref[...])

    open_part(ZERO)
    for k, part in enumerate(parts):
        if k < THREE:
            open_part(k + ONE)
        for rows in row_chunks():
            value = pre[k % TWO][rows, :] + column(c_ref, rows, B_UP + k)
            scaled = value * math.sqrt(0.5)
            cdf = 0.5 + 0.5 * lax.erf(scaled)
            density = jnp.exp2(scaled * scaled * -math.log2(math.e) - 0.5 * math.log2(2.0 * math.pi))
            there = slice(part.start + rows.start, part.start + rows.stop)
            act_ref[there, :] = (value * cdf).astype(BF16)
            slope_ref[there, :] = cdf + value * density
        if k == ONE:
            hook(TWO)

    @pl.when(layer == ZERO)
    def _():
        s_a[...] = tn(down[...], act_ref[...])
        for rows in row_chunks():
            xt[rows, :] = (mid_ref[rows, :].astype(F32) + s_a[rows, :] + column(c_ref, rows, B_DOWN)).astype(BF16)


def forward(lengths, x, tables, params):
    def saved(index, rows, dtype):
        return jax.ShapeDtypeStruct((TWO, SEQS, rows, TOK), dtype), pl.BlockSpec((ONE, ONE, rows, TOK), index)

    def attn_at(s):
        return s // EIGHT, jnp.where(s // FOUR % TWO == ZERO, s % FOUR, THREE), ZERO, ZERO

    def mlp_at(s):
        odd = s // FOUR % TWO == ONE
        return jnp.where(s < 12, ZERO, ONE), jnp.where(odd, s % FOUR, jnp.where(s < FOUR, ZERO, THREE)), ZERO, ZERO

    def xs_at(s):
        return jnp.where(s < FOUR, ZERO, ONE), jnp.where(s < EIGHT, s % FOUR, THREE), ZERO, ZERO

    outs = [saved(xs_at, DIM, BF16)] + [saved(attn_at, DIM, BF16)] * THREE
    outs += [(jax.ShapeDtypeStruct((TWO, SEQS, HEADS, TOK, TOK), BF16), pl.BlockSpec((ONE, ONE, HEADS, TOK, TOK), lambda s: (*attn_at(s), ZERO))), saved(attn_at, DIM, F32)]
    outs += [saved(mlp_at, DIM, BF16), saved(mlp_at, FFN, BF16), saved(mlp_at, FFN, F32), saved(attn_at, EIGHT, F32), saved(mlp_at, EIGHT, F32)]
    outs += [(jax.ShapeDtypeStruct((TWO, *COLS), F32), once((TWO, *COLS)))]
    weights = ((THREE, DIM, DIM), (DIM, DIM), (DIM, FFN), (FFN, DIM))
    outs += [(jax.ShapeDtypeStruct((TWO, *w), BF16), HBM) for w in weights]
    scratch = [(SEQS, *SQUARE), (SEQS, *SQUARE), *weights, SQUARE]
    scratch = [pltpu.VMEM(s, BF16) for s in scratch] + [pltpu.VMEM(SQUARE, F32)] * THREE + [pltpu.VMEM((*GRID, TWO, ONE, ONE, LANES), F32)]
    scratch += [pltpu.VMEM((TWO, *GRID, TWO, n, SIXTEEN, LANES), BF16) for n in (ONE, THREE) for _ in range(THREE)]
    scratch += [pltpu.VMEM((SEQS, EIGHT, TOK), F32)] + [pltpu.VMEM((15, n, SIXTEEN, LANES), BF16) for n in (ONE, THREE)]
    scratch += [pltpu.VMEM((15, ONE, ONE, LANES), F32), DMA((7, TWO, 5)), DMA((7, TWO, 5)), DMA((FOUR,)), DMA((SEQS,))]
    return pl.pallas_call(
        forward_kernel, grid=(SIXTEEN,),
        out_shape=[o[ZERO] for o in outs], out_specs=[o[ONE] for o in outs],
        in_specs=[pl.BlockSpec(memory_space=pltpu.SMEM), HBM, once((HALF, TOK)), once((HALF, TOK))] + [once(p.shape) for p in params],
        scratch_shapes=scratch,
        compiler_params=pltpu.CompilerParams(collective_id=ZERO, has_side_effects=True, vmem_limit_bytes=67043328,
                                             dimension_semantics=("arbitrary",)),
        name="forward")(lengths, x, *tables, *params)


def norm_back(dh_ref, x_ref, stats, c_ref, lane, sums, at, write, beside):
    mean, rstd = stats
    means = [0.0, 0.0]

    def both(rows):
        dh = dh_ref[rows, :]
        return dh, dh * column(c_ref, rows, lane), (x_ref[rows, :].astype(F32) - mean) * rstd

    def first(rows):
        dh, dxhat, xhat = both(rows)
        means[ZERO], means[ONE] = means[ZERO] + total(dxhat), means[ONE] + total(dxhat * xhat)
        sums[at, rows, :] += fold(dh * xhat)
        sums[at + ONE, rows, :] += fold(dh)

    def second(rows):
        dh, dxhat, xhat = both(rows)
        write(rows, rstd * (dxhat - means[ZERO] * (1.0 / DIM) - xhat * (means[ONE] * (1.0 / DIM))))

    woven(beside, [functools.partial(run, rows) for run in (first, second) for rows in row_chunks()])


def columns_of(partials):
    lane = lax.broadcasted_iota(jnp.int32, COLS, ONE)
    value = jnp.zeros(COLS, F32)
    for at, partial in enumerate(partials):
        value = jnp.where(lane == at, jnp.sum(partial, axis=ONE, keepdims=True), value)
    return value.T[:EIGHT]


def head_rows(head):
    return slice(HEAD * head, HEAD * head + HEAD), slice(HEAD * head, HEAD * head + HALF), slice(HEAD * head + HALF, HEAD * head + HEAD)


class Reduce:
    def __init__(self, place, units, grads, buffers, send, recv):
        self.units = units
        self.scatters = [Scatter(place, (lambda u, k=k: grads(units[k][u])), *buffers[k], ORDERS[k], send.at[k], recv.at[k]) for k in range(THREE)]

    def steps(self, store):
        def each(*names):
            def step():
                for name in names:
                    for s in self.scatters:
                        getattr(s, name)()
            return step

        def finish():
            for units, s in zip(self.units, self.scatters):
                s.finish(lambda u, full, units=units: store(units[u], full))

        return [each("swap"), each("swapped", "ring_start"), each("ring_turn"), each("plane_start"), each("last"), finish]


def backward_kernel(dy_ref, mid_ref, ctx_ref, st2_ref, q_ref, k_ref, v_ref, x_ref, st1_ref, cos_ref, sin_ref, c_ref, p_hbm, slope_hbm, act_hbm,
                    qkv_hbm, wo_hbm, up_hbm, down_hbm,
                    dx_ref, attn_out, up_out, down_out, small_out, *refs):
    (grad, dctx, delta, big, wqkv, wo, slope, act, dpre, h_ref, s_a, s_b, d_a, d_b, sums,
     g_qkv, g_wo, g_up, g_down, *small_bufs), refs = refs[:28], refs[28:]
    qkv_bufs, mo_bufs, refs = [refs[6 * k:6 * k + 6] for k in range(THREE)], [refs[6 * k + 18:6 * k + 24] for k in range(THREE)], refs[36:]
    send, recv, late_sem, plane_sem, big_sem, w_sem, mlp_sem = refs
    step = pl.program_id(ZERO)
    phase, seq = step // FOUR, lax.rem(step, FOUR)
    layer = ONE - step // EIGHT
    place = Place()

    def grads(unit):
        if unit < THREE:
            return g_qkv.at[unit]
        if unit == THREE:
            return g_wo
        if unit < EIGHT:
            return g_up.at[unit - FOUR]
        return g_down.at[:, :, :, unit - EIGHT]

    live = step < SIXTEEN
    turn = jnp.where(live, ZERO, ONE)
    qkv_sums = Reduce(place, ((ZERO,), (ONE,), (TWO,)), grads, [(a, ra, rb, rp.at[turn], *last) for a, ra, rb, rp, *last in qkv_bufs], send.at[turn], recv.at[turn])
    mo_sums = Reduce(place, COLOURS, grads, mo_bufs, send.at[TWO], recv.at[TWO])

    def third(i):
        one = pl.ds(i, ONE)
        bufs = [(a.at[one], ra.at[one], rb.at[:, one], rp.at[:, one], mine.at[one], other.at[one]) for a, ra, rb, rp, mine, other in mo_bufs]
        return Reduce(place, [units[i:i + ONE] for units in COLOURS], grads, bufs, send.at[THREE + i], recv.at[THREE + i]).steps(store(ONE - turn))

    small_refs = small_bufs[::THREE]
    early, middle, late = [Late(place, small_refs[i], small_bufs[THREE * i + ONE], late_sem.at[i, ZERO], late_sem.at[i, ONE], small_bufs[THREE * i + TWO],
                                plane_sem.at[i, ZERO], plane_sem.at[i, ONE]).steps() for i in range(THREE)]
    first_core = place.core == ZERO

    def store(l):
        def put(unit, full):
            if unit < EIGHT:
                mine = jnp.where(first_core, full[:FOUR], full[FOUR:])
                if unit < FOUR:
                    attn_out[l, unit] = mine
                else:
                    up_out[l, :, DIM * (unit - FOUR):DIM * (unit - THREE)] = mine
            else:
                at = EIGHT * (unit % TWO)

                @pl.when(place.core == (unit - EIGHT) // TWO)
                def _():
                    down_out[l, at:at + EIGHT] = full
        return put

    def mlp_weights(l):
        parts = [pl.ds(DIM * k, DIM) for k in range(FOUR)]
        return ([pltpu.make_async_copy(down_hbm.at[l, part], big.at[k], big_sem.at[k]) for k, part in enumerate(parts)],
                [pltpu.make_async_copy(up_hbm.at[l, :, part], big.at[FOUR + k], big_sem.at[FOUR + k]) for k, part in enumerate(parts)] +
                [pltpu.make_async_copy(wo_hbm.at[l], wo, w_sem.at[ZERO])])

    def attn_weights(l):
        return [pltpu.make_async_copy(qkv_hbm.at[l], wqkv, w_sem.at[ONE])]

    def probs(l, s):
        return [pltpu.make_async_copy(p_hbm.at[l, s, k], big.at[k], big_sem.at[k]) for k in range(HEADS)]

    def saved_mlp(l, s):
        return [pltpu.make_async_copy(slope_hbm.at[l, s], slope, mlp_sem.at[ZERO]), pltpu.make_async_copy(act_hbm.at[l, s], act, mlp_sem.at[ONE])]

    def start(copies):
        for copy in copies:
            copy.start()

    def wait(copies):
        for copy in copies:
            copy.wait()

    @pl.when(step == ZERO)
    def _():
        place.greet()
        start(mlp_weights(ONE)[ZERO] + saved_mlp(ONE, ZERO) + mlp_weights(ONE)[ONE] + attn_weights(ONE))

    pl.when(step == ONE)(place.met)
    mo_steps, qkv_steps = mo_sums.steps(store(ONE - turn)), qkv_sums.steps(store(ONE - turn))

    def plan(slots, steps):
        return [((slot,), run) for slot, run in zip(slots, steps)]

    thirds = [], []
    for i, slots in enumerate(((48, 50, 54, 59, 73, 74), (48, 51, 55, 62, 73, 74), (48, 53, 57, 63, 73, 74))):
        steps = plan(slots, third(i))
        thirds[ZERO].extend(steps[:FOUR])
        thirds[ONE].extend(steps[FOUR:])
    attn_hook = hooks(step * FOUR, plan((48, 57, 61, 63), middle) + plan((SIXTEEN, 24, 28), mo_steps) + thirds[ZERO] +
                      plan((53, 53), qkv_steps[FOUR:]))
    mlp_plan = plan((37, 45, 46), mo_steps[THREE:]) + plan((32, 36, 40, 47), qkv_steps) + plan((34, 41, 45, 47), early)
    mlp_hook = hooks(step * FOUR, mlp_plan + plan((64, 66, 70, 72, 75), qkv_steps) + plan((65, 72, 74, 75), late) + thirds[ONE] +
                     plan((75,), qkv_steps[5:]))


    @pl.when(phase % TWO == ZERO)
    def _():
        @pl.when((seq == ZERO) & live)
        def _():
            for ref in (g_wo, g_up, g_down, sums):
                ref[...] = jnp.zeros_like(ref)

        @pl.when(step < FOUR)
        def _():
            grad[seq] = dy_ref[ZERO].T

        @pl.when((seq == ZERO) & live)
        def _():
            wait(mlp_weights(layer)[ZERO])

        mlp_hook(ZERO)

        @pl.when(step == SIXTEEN)
        def _():
            small_refs[TWO][...] = columns_of([sums[i] for i in range(5)])

        def after_first():
            pl.when(seq < THREE)(lambda: start(saved_mlp(layer, seq + ONE)))
            pl.when(seq == THREE)(lambda: start(probs(layer, ZERO)[:FOUR]))

        def before_second():
            pl.when(seq == ZERO)(lambda: wait(mlp_weights(layer)[ONE]))

        def after_second():
            pl.when(seq == THREE)(lambda: start(probs(layer, ZERO)[FOUR:]))

        pl.when(live)(lambda: wait(saved_mlp(layer, seq)))
        mlp_backward(grad.at[seq], slope, act, mid_ref, ctx_ref, st2_ref.at[ZERO], wo, big, c_ref, dctx.at[seq], delta.at[seq], g_wo, g_up, g_down,
                     dpre, h_ref, s_a, s_b, sums, pl.when(live), mlp_hook,
                     after_first, after_second, before_second)

        @pl.when((seq == THREE) & live)
        def _():
            value = columns_of([sums[i] for i in range(EIGHT)])

            @pl.when(layer == ONE)
            def _():
                small_refs[ZERO][:EIGHT, :] = value

            @pl.when(layer == ZERO)
            def _():
                small_refs[ONE][...] = value

        mlp_hook(THREE)

    @pl.when(phase % TWO == ONE)
    def _():
        @pl.when(seq == ZERO)
        def _():
            wait(attn_weights(layer))
            for ref in (g_qkv, sums):
                ref[...] = jnp.zeros_like(ref)

        @pl.when(step == FOUR)
        def _():
            start(saved_mlp(ZERO, ZERO))
        attn_hook(ZERO)

        def after_heads():
            pl.when(seq < THREE)(lambda: start(probs(layer, seq + ONE)))
            pl.when(step == 7)(lambda: start(mlp_weights(ZERO)[ZERO] + mlp_weights(ZERO)[ONE]))

        wait(probs(layer, seq))
        attn_backward(dctx.at[seq], delta.at[seq], big, q_ref, k_ref, v_ref, x_ref, st1_ref.at[ZERO], grad.at[seq], wqkv, c_ref, cos_ref, sin_ref,
                      g_qkv, dpre, h_ref, s_a, s_b, d_a, d_b, sums, attn_hook,
                      after_heads)

        @pl.when(step == 7)
        def _():
            small_refs[ZERO][EIGHT:, :] = columns_of([sums[i] for i in range(5)])

        @pl.when(step == 7)
        def _():
            start(attn_weights(ZERO))

        @pl.when(step > 11)
        def _():
            dx_ref[ZERO] = grad[seq].T
        attn_hook(THREE)

    @pl.when(step == 18)
    def _():
        small_out[:SIXTEEN, :], small_out[SIXTEEN:24, :], small_out[24:, :] = [ref[...] for ref in small_refs]


def add_to(ref, value):
    ref[...] = ref[...] + value.reshape(ref.shape)


def mlp_backward(grad, slope, act, mid_ref, ctx_ref, stat_ref, wo, big, c_ref, dctx, delta, g_wo, g_up, g_down, dpre, h_ref, s_a, s_b, sums, when, hook, after_first, after_second, before_second):
    parts = [slice(DIM * k, DIM * k + DIM) for k in range(FOUR)]
    pre = (s_a, s_b)

    def dact(k):
        pre[k % TWO][...] = nn(big[k], grad[...])

    @when
    def _():
        def scale(k, chunk):
            there = slice(parts[k].start + chunk.start, parts[k].start + chunk.stop)
            value = pre[k % TWO][chunk, :] * slope[there, :]
            sums[k, chunk, :] += fold(value)
            dpre[there, :] = value.astype(BF16)

        def down_product(k):
            add_to(g_down.at[k], nt(act[parts[k], :], grad[...]))

        dact(ZERO)
        norm_to(mid_ref.at[ZERO], get_stats(stat_ref), c_ref, LN_PAR + TWO, h_ref)
        for k in range(FOUR):
            products = [functools.partial(down_product, k)]
            if k < THREE:
                products = [functools.partial(dact, k + ONE)] + products
            woven(products, [functools.partial(scale, k, chunk) for chunk in row_chunks()])
        after_first()
    hook(ONE)

    @when
    def _():
        before_second()
        s_a[...] = functools.reduce(jnp.add, [nn(big[FOUR + k], dpre[rows, :]) for k, rows in enumerate(parts)])
        after_second()
    hook(TWO)

    @when
    def _():
        def write(rows, dx):
            dy = grad[rows, :].astype(F32)
            dmid = (dy + dx).astype(BF16)
            grad[rows, :] = dmid
            sums[6, rows, :] += fold(dy)
            sums[7, rows, :] += fold(dmid.astype(F32))

        norm_back(s_a, mid_ref.at[ZERO], get_stats(stat_ref), c_ref, LN_PAR + TWO, sums, FOUR, write,
                  [lambda k=k, rows=rows: add_to(g_up.at[k], nt(h_ref[...], dpre[rows, :])) for k, rows in enumerate(parts)])
        add_to(g_wo, nt(ctx_ref[ZERO].astype(BF16), grad[...]))
        s_b[...] = nn(wo[...], grad[...])
        for head in range(HEADS):
            rows = head_rows(head)[ZERO]
            value = s_b[rows, :].astype(BF16)
            dctx[rows, :] = value
            delta[head:head + ONE, :] = total(value.astype(F32) * ctx_ref[ZERO, rows, :])


def attn_backward(dctx, delta, probs, q_ref, k_ref, v_ref, x_ref, stat_ref, grad, wqkv, c_ref, cos_ref, sin_ref, g_qkv, dproj, h_ref, s_a, s_b, d_a, d_b,
                  sums, hook, prefetch):
    scores, dscores = (s_a, s_b), (d_a, d_b)
    q, k, v = q_ref.at[ZERO], k_ref.at[ZERO], v_ref.at[ZERO]

    def open_head(head):
        rows = head_rows(head)[ZERO]
        scores[head % TWO][...] = tn(v[rows, :], dctx[rows, :])

    def weigh(head, rows):
        dscores[head % TWO][rows, :] = (probs[head, rows, :].astype(F32) * (scores[head % TWO][rows, :] - delta[head:head + ONE, :])).astype(BF16)

    def values(head):
        rows = head_rows(head)[ZERO]
        dv = nt(dctx[rows, :], probs[head])
        sums[TWO, rows, :] += fold(dv)
        dproj[TWO * DIM + rows.start:TWO * DIM + rows.stop, :] = dv.astype(BF16)

    def close_head(head, m):
        rows, one, two = head_rows(head)
        ds = dscores[head % TWO][...]
        value = nn(k[rows, :], ds) * HEAD ** -0.5 if m == ZERO else nt(q[rows, :], ds)
        cos, sin = cos_ref[...], sin_ref[...]
        a, b = value[:HALF], value[HALF:]
        for at, out in ((one, a * cos + b * sin), (two, b * cos - a * sin)):
            dproj[m * DIM + at.start:m * DIM + at.stop, :] = out.astype(BF16)
            sums[m, at, :] += fold(out)

    open_head(ZERO)
    for head in range(HEADS):
        products = [functools.partial(values, head)]
        if head:
            products = [functools.partial(close_head, head - ONE, m) for m in range(TWO)] + products
        if head + ONE < HEADS:
            products = [functools.partial(open_head, head + ONE)] + products
        woven(products, [functools.partial(weigh, head, rows) for rows in row_chunks()])
        if head == THREE:
            hook(ONE)
    for m in range(TWO):
        close_head(HEADS - ONE, m)
    prefetch()
    hook(TWO)
    norm_to(x_ref.at[ZERO], get_stats(stat_ref), c_ref, LN_PAR, h_ref)
    parts = [slice(DIM * m, DIM * m + DIM) for m in range(THREE)]
    s_a[...] = functools.reduce(jnp.add, [nn(wqkv[m], dproj[rows, :]) for m, rows in enumerate(parts)])

    def write(rows, dx):
        grad[rows, :] = (grad[rows, :].astype(F32) + dx).astype(BF16)

    norm_back(s_a, x_ref.at[ZERO], get_stats(stat_ref), c_ref, LN_PAR, sums, THREE, write,
              [lambda m=m, rows=rows: add_to(g_qkv.at[m], nt(h_ref[...], dproj[rows, :])) for m, rows in enumerate(parts)])


def backward(dy, xs, q, k, v, probs, ctx, mid, act, slope, st1, st2, c, tables, w_qkv, w_o, w_up, w_down):
    def mlp_at(s):
        s = jnp.minimum(s, 15)
        odd = s // FOUR % TWO == ONE
        return ONE - s // EIGHT, jnp.where(odd, THREE, s % FOUR), ZERO, ZERO

    def attn_at(s):
        s = jnp.minimum(s, 15)
        odd = s // FOUR % TWO == ONE
        return jnp.where(s < EIGHT, ONE, ZERO) + jnp.where((s > 7) & (s < 12), ONE, ZERO), jnp.where(odd, s % FOUR, jnp.where(s < FOUR, ZERO, THREE)), ZERO, ZERO

    per_mlp = pl.BlockSpec((None, ONE, *SQUARE), mlp_at)
    per_attn = pl.BlockSpec((None, ONE, *SQUARE), attn_at)

    def stat(at):
        return pl.BlockSpec((None, ONE, EIGHT, TOK), at)

    acc = [(*GRID, EIGHT, WIDTH)]
    scratch = [pltpu.VMEM((SEQS, *SQUARE), BF16), pltpu.VMEM((SEQS, *SQUARE), BF16), pltpu.VMEM((SEQS, HEADS, TOK), F32),
               pltpu.VMEM((HEADS, TOK, TOK), BF16), pltpu.VMEM((THREE, DIM, DIM), BF16), pltpu.VMEM((DIM, DIM), BF16),
               pltpu.VMEM(TALL, F32), pltpu.VMEM(TALL, BF16), pltpu.VMEM(TALL, BF16), pltpu.VMEM(SQUARE, BF16),
               pltpu.VMEM(SQUARE, F32), pltpu.VMEM(SQUARE, F32), pltpu.VMEM((TOK, TOK), BF16), pltpu.VMEM((TOK, TOK), BF16),
               pltpu.VMEM((EIGHT, *COLS), F32), pltpu.VMEM((THREE, *GRID, EIGHT, DIM), F32), pltpu.VMEM((*GRID, EIGHT, DIM), F32),
               pltpu.VMEM((FOUR, *GRID, EIGHT, DIM), F32), pltpu.VMEM((*GRID, FOUR, EIGHT, DIM), F32), *[pltpu.VMEM((*lead, rows, DIM), F32) for rows in (SIXTEEN, EIGHT, EIGHT) for lead in ((), (6,), (SIXTEEN,))]]
    for n in (ONE, THREE):
        for order in ORDERS:
            ring_a, ring_b, plane, *last = landing_shapes(order, n)
            plane = (TWO, *plane) if n == ONE else plane
            scratch += [pltpu.VMEM(s, F32) for s in ((n, *GRID, EIGHT, WIDTH), ring_a, ring_b, plane, *last)]
    scratch += [DMA((6, THREE, 9)), DMA((6, THREE, 9)), DMA((THREE, TWO, 6)), DMA((THREE, TWO)), DMA((EIGHT,)), DMA((TWO,)), DMA((TWO,))]
    outs = ((TWO, FOUR, FOUR, DIM), (TWO, FOUR, FFN), (TWO, SIXTEEN, DIM), (32, DIM))
    whole = [pl.BlockSpec(s, lambda i, n=len(s): (ZERO,) * n, pipeline_mode=pl.Buffered(ONE)) for s in outs]
    dx_at = lambda s: (jnp.clip(s - 12, ZERO, THREE), ZERO, ZERO)
    return pl.pallas_call(
        backward_kernel, grid=(19,),
        out_shape=[jax.ShapeDtypeStruct((SEQS, TOK, DIM), BF16)] + [jax.ShapeDtypeStruct(s, F32) for s in outs],
        out_specs=[pl.BlockSpec((ONE, TOK, DIM), dx_at)] + whole,
        in_specs=[pl.BlockSpec((ONE, TOK, DIM), lambda s: (jnp.minimum(s, THREE), ZERO, ZERO)), per_mlp, per_mlp, stat(mlp_at)] + [per_attn] * FOUR + [stat(attn_at),
                  once((HALF, TOK)), once((HALF, TOK)), pl.BlockSpec((None, *COLS), lambda s: (ONE - jnp.minimum(s, 15) // EIGHT, ZERO, ZERO))] + [HBM] * 7,
        scratch_shapes=scratch,
        compiler_params=pltpu.CompilerParams(collective_id=ONE, has_side_effects=True, vmem_limit_bytes=67043328,
                                             dimension_semantics=("arbitrary",)),
        name="backward")(dy, mid, ctx, st2, q, k, v, xs, st1, *tables, c, probs, slope, act, w_qkv, w_o, w_up, w_down)


def results_kernel(dx_ref, attn_ref, up_ref, down_ref, small_ref, dx_out, attn_out, gb_attn, g_ln, up_out, gb_up, down_out, gb_down):
    dx_out[...] = dx_ref[...]

    @pl.when(pl.program_id(ZERO) == ZERO)
    def _():
        me = lax.axis_index(AXIS)
        attn_out[...], up_out[...], down_out[...] = attn_ref[...], up_ref[...], down_ref[...]
        mine = pltpu.roll(small_ref[...], lax.rem(DIM - FOUR * me + FOUR * LANES, DIM), ONE)
        for l in range(TWO):
            mlp = SIXTEEN - SIXTEEN * l
            attn = mlp + EIGHT
            gb_attn[l, :THREE], gb_attn[l, THREE:] = mine[attn:attn + THREE, :FOUR], mine[mlp + 7:mlp + EIGHT, :FOUR]
            g_ln[l, :TWO], g_ln[l, TWO:] = mine[attn + THREE:attn + 5, :FOUR], mine[mlp + FOUR:mlp + 6, :FOUR]
            gb_down[l:l + ONE, :] = mine[mlp + 6:mlp + 7, :FOUR]
            ups = small_ref[pl.ds(mlp + me // 32, ONE), :]
            gb_up[l:l + ONE, :] = pltpu.roll(ups, lax.rem(DIM - SIXTEEN * lax.rem(me, 32), DIM), ONE)[:, :SIXTEEN]


def results(dx, attn, up, down, small):
    shapes = [attn.shape, (TWO, FOUR, FOUR), (TWO, FOUR, FOUR), up.shape, (TWO, SIXTEEN), down.shape, (TWO, FOUR)]
    per = pl.BlockSpec((TWO, TOK, DIM), lambda s: (s, ZERO, ZERO))
    return pl.pallas_call(
        results_kernel, grid=(SEQS // TWO,), name="results",
        out_shape=[jax.ShapeDtypeStruct(dx.shape, BF16)] + [jax.ShapeDtypeStruct(s, F32) for s in shapes],
        in_specs=[per] + [once(a.shape) for a in (attn, up, down, small)],
        out_specs=[per] + [once(s) for s in shapes])(dx, attn, up, down, small)


def solution(mesh):
    batch_spec = P(AXIS)
    weight_specs = (P(None, None, AXIS, None), P(None, None, AXIS), P(None, None, AXIS),
                    P(None, AXIS, None), P(None, AXIS), P(None, AXIS, None), P(None, AXIS))

    def device_step(x, lengths, d_y, w_attn, b_attn, ln_par, w_up, b_up, w_down, b_down):
        tables = rotary_tables()
        xs, q, k, v, probs, ctx, mid, act, slope, st1, st2, c, w_qkv, w_o, w_up, w_down = forward(
            lengths, x, tables, (w_attn, b_attn, ln_par, w_up, b_up, w_down, b_down))
        return results(*backward(d_y, xs, q, k, v, probs, ctx, mid, act, slope, st1, st2, c, tables, w_qkv, w_o, w_up, w_down))

    return jax.shard_map(device_step, mesh=mesh,
                         in_specs=(batch_spec, batch_spec, batch_spec) + weight_specs,
                         out_specs=(batch_spec,) + weight_specs,
                         check_vma=False)
```

```python
import math
import functools
import jax
import numpy as np
import jax.numpy as jnp
from jax import lax
from jax.experimental import pallas as pl
from jax.experimental.pallas import tpu as pltpu
from jax.sharding import PartitionSpec as P

ZERO, ONE, TWO, THREE, FOUR = range(5)
EIGHT, SIXTEEN, WIDTH = 8, 16, 256

F32, BF16 = jnp.float32, jnp.bfloat16
SEQS, TOK, DIM, FFN, HEADS, HEAD, LANES = FOUR, 512, 512, 2048, EIGHT, 64, 128
HALF = HEAD // TWO
EPS = 1e-5
THETA = 10000.0
NEG_BIG = -1e30
B_ATTN, LN_PAR, B_UP, B_DOWN = ZERO, FOUR, EIGHT, 12


def nn(a, b):
    return lax.dot_general(a, b, (((ONE,), (ZERO,)), ((), ())), preferred_element_type=F32)


def nt(a, b):
    return lax.dot_general(a, b, (((ONE,), (ONE,)), ((), ())), preferred_element_type=F32)


def tn(a, b):
    return lax.dot_general(a, b, (((ZERO,), (ZERO,)), ((), ())), preferred_element_type=F32)


def lane_tiles(width=TOK, size=LANES):
    return [slice(i, i + size) for i in range(ZERO, width, size)]


def row_chunks(rows=DIM, size=128):
    return [slice(i, i + size) for i in range(ZERO, rows, size)]


def column(c_ref, rows, lane):
    return jnp.broadcast_to(c_ref[rows, lane:lane + ONE], (rows.stop - rows.start, TOK))


def total(value):
    return jnp.sum(value, axis=ZERO, keepdims=True)


def norm_stats(x_ref):
    mean = functools.reduce(jnp.add, [total(x_ref[rows, :].astype(F32)) for rows in row_chunks()]) * (1.0 / DIM)
    squares = []
    for rows in row_chunks():
        centred = x_ref[rows, :].astype(F32) - mean
        squares.append(total(centred * centred))
    return mean, lax.rsqrt(functools.reduce(jnp.add, squares) * (1.0 / DIM) + EPS)


def norm_to(x_ref, stats, c_ref, lane, h_ref):
    mean, rstd = stats
    for rows in row_chunks():
        xhat = (x_ref[rows, :].astype(F32) - mean) * rstd
        h_ref[rows, :] = (xhat * column(c_ref, rows, lane) + column(c_ref, rows, lane + ONE)).astype(BF16)


def put_stats(ref, stats):
    ref[ZERO:ONE, :], ref[ONE:TWO, :] = stats


def get_stats(ref):
    return ref[ZERO:ONE, :], ref[ONE:TWO, :]


def woven(products, rest):
    done = ZERO
    for n, step in enumerate(rest):
        while done < len(products) and done * len(rest) <= n * len(products):
            products[done]()
            done += ONE
        step()
    for product in products[done:]:
        product()


def fold(value):
    parts = [value[:, cols] for cols in lane_tiles(value.shape[ONE])]
    return functools.reduce(jnp.add, parts)


def seq_spec(shape):
    return pl.BlockSpec((ONE, *shape), lambda s: (s,) + (ZERO,) * len(shape))


def once(shape):
    return pl.BlockSpec(shape, lambda s: (ZERO,) * len(shape), pipeline_mode=pl.Buffered(ONE))


def act_shape(rows, dtype):
    return jax.ShapeDtypeStruct((SEQS, rows, TOK), dtype)


PARAMS = pltpu.CompilerParams(vmem_limit_bytes=60 << 20, dimension_semantics=("arbitrary",))
SQUARE, TALL, WIDE, COLS = (DIM, TOK), (FFN, TOK), (DIM, FFN), (DIM, LANES)


def rotary_tables():
    inv_freq = np.float32(1.0) / np.float32(THETA) ** (np.arange(HALF, dtype=np.float32) * np.float32(2.0 / HEAD))
    angles = inv_freq[:, None] * np.arange(TOK, dtype=np.float32)[None, :]
    return np.cos(angles).astype(np.float32), np.sin(angles).astype(np.float32)


MESH = pl.DeviceIdType.MESH
AXIS = "fsdp"
ORDERS = ((TWO, ONE, ZERO), (ONE, ZERO, TWO), (ZERO, TWO, ONE))


class Place:
    def __init__(self):
        me = lax.axis_index(AXIS)
        self.core = lax.rem(me, TWO)
        self.pos = (me // 32, lax.rem(me // EIGHT, FOUR), lax.rem(me // TWO, FOUR))
        self.partner = me + ONE - TWO * self.core
        self.near = [[lax.rem(at + delta, FOUR) if delta else at for delta in range(FOUR)] for at in self.pos]

    def coord(self, dim, delta):
        if isinstance(delta, int):
            return self.near[dim][delta % FOUR]
        return lax.rem(self.pos[dim] + delta, FOUR)

    def device(self, offsets):
        pos = [self.coord(dim, offsets.get(dim, ZERO)) for dim in range(THREE)]
        return pos[ZERO] * 32 + pos[ONE] * EIGHT + pos[TWO] * TWO + self.core

    def greet(self):
        barrier = pltpu.get_barrier_semaphore()
        for i in range(ONE, 64):
            offsets = {ZERO: i // SIXTEEN, ONE: i // FOUR % FOUR, TWO: i % FOUR}
            if min(offsets.values()) == ZERO:
                pl.semaphore_signal(barrier, inc=ONE, device_id=(self.device(offsets),), device_id_type=MESH)
        pl.semaphore_signal(barrier, inc=ONE, device_id=(self.partner,), device_id_type=MESH)

    def met(self):
        pl.semaphore_wait(pltpu.get_barrier_semaphore(), 37)


def remote(src, dst, send_sem, recv_sem, device):
    return pltpu.make_async_remote_copy(src_ref=src, dst_ref=dst, send_sem=send_sem, recv_sem=recv_sem,
                                        device_id=(device,), device_id_type=MESH)


LINE = (ONE, -ONE, TWO)


def each_of_plane(order, run):
    @pl.loop(ZERO, FOUR)
    def _(high):
        for low in range(FOUR):
            step = functools.partial(run, FOUR * high + low, {order[ONE]: high, order[TWO]: low})
            if low:
                step()
            else:
                pl.when(high > ZERO)(step)


class Gather:
    def __init__(self, place, buf, fifteen, order, send, recv):
        self.place, self.buf, self.fifteen, self.order, self.send, self.recv = place, buf, fifteen, order, send, recv

    def block(self, offsets, whole=()):
        index = [slice(ZERO, FOUR) if dim in whole else pl.ds(self.place.coord(dim, offsets.get(dim, ZERO)), ONE) for dim in range(THREE)]
        return self.buf.at[index[ZERO], index[ONE], index[TWO], pl.ds(self.place.core, ONE)]

    def copy(self, ref, key, device):
        return remote(ref, ref, self.send.at[key], self.recv.at[key], device)

    def plane_start(self):
        each_of_plane(self.order, lambda k, offsets: self.copy(self.block({}), ZERO, self.place.device(offsets)).start())

    def plane_all(self):
        return self.copy(self.fifteen, ZERO, self.place.partner)

    def plane_wait(self):
        self.plane_all().wait_recv()

    def line(self, i, sign):
        offsets = {self.order[ZERO]: sign * LINE[i]}
        return self.block(offsets, self.order[ONE:])

    def line_start(self):
        for i, delta in enumerate(LINE):
            self.copy(self.line(i, ZERO), ONE + i, self.place.device({self.order[ZERO]: delta})).start()

    def line_wait(self):
        for i in range(THREE):
            self.copy(self.line(i, -ONE), ONE + i, self.place.partner).wait_recv()

    def share(self, core):
        return self.copy(self.buf.at[:, :, :, pl.ds(core, ONE)], FOUR, self.place.partner)

    def share_start(self):
        self.share(self.place.core).start()

    def end(self):
        self.share(ONE - self.place.core).wait_recv()
        self.plane_all().wait_send()
        for i in range(THREE):
            self.copy(self.line(i, ZERO), ONE + i, self.place.partner).wait_send()
        self.share(self.place.core).wait_send()


def gather_steps(gathers):
    def each(*names):
        def step():
            for name in names:
                for g in gathers:
                    getattr(g, name)()
        return step

    return [each("plane_start"), each("plane_wait", "line_start"), each("line_wait", "share_start"), each("end")]


class Scatter:
    def __init__(self, place, grads, acc, got_a, got_b, got_p, mine, other, order, send, recv):
        self.place, self.grads, self.acc, self.order = place, grads, acc, order
        self.got_a, self.got_b, self.got_p, self.mine, self.other, self.send, self.recv = got_a, got_b, got_p, mine, other, send, recv
        self.units = acc.shape[ZERO]

    def columns(self, core):
        return pl.ds(pl.multiple_of(core * WIDTH, WIDTH), WIDTH)

    def swap_copy(self, u):
        place = self.place
        return remote(self.grads(u).at[:, :, :, :, self.columns(ONE - place.core)], self.acc.at[u], self.send.at[6 + u], self.recv.at[6 + u], place.partner)

    def swap(self):
        for u in range(self.units):
            self.swap_copy(u).start()

    def swapped(self):
        for u in range(self.units):
            self.swap_copy(u).wait()
            grad, acc = self.grads(u), self.acc

            @pl.loop(ZERO, FOUR)
            def _(z):
                acc[u, z] = acc[u, z] + grad[z, :, :, :, self.columns(self.place.core)]

    def part(self, delta, half=None):
        index = [slice(ZERO, FOUR)] * THREE
        index[self.order[ZERO]] = pl.ds(self.place.coord(self.order[ZERO], delta), ONE)
        return self.acc.at[:, index[ZERO], index[ONE], index[TWO], :, slice(ZERO, WIDTH) if half is None else lane_tiles()[half]]

    def ring(self, step, way):
        delta = (ONE, -ONE)[way]
        device = self.place.device({self.order[ZERO]: delta})
        if step == ZERO:
            src, dst = self.part(TWO, way), self.got_a.at[:, :, :, :, :, lane_tiles()[way]]
        else:
            src, dst = self.part(delta), self.got_b.at[way]
        key = TWO * step + way
        return remote(src, dst, self.send.at[key], self.recv.at[key], device)

    def ring_start(self):
        for way in range(TWO):
            self.ring(ZERO, way).start()

    def ring_turn(self):
        for way in range(TWO):
            self.ring(ZERO, way).wait_recv()
            self.add((ONE, -ONE)[way], way, self.got_a)
            self.ring(ONE, way).start()

    def add(self, delta, half, *refs):
        dim, acc = self.order[ZERO], self.acc
        at = self.place.coord(dim, delta)
        columns = slice(ZERO, WIDTH) if half is None else lane_tiles()[half]

        @pl.loop(ZERO, FOUR)
        def _(i):
            index = [i if d == self.order[ONE] else slice(ZERO, FOUR) for d in range(THREE)]
            there = [slice(None), *index, slice(None), columns]
            here = list(there)
            here[ONE + dim] = pl.ds(at, ONE)
            there[ONE + dim] = slice(ZERO, ONE)
            value = acc[tuple(here)]
            for ref in refs:
                value = value + ref[tuple(there)]
            acc[tuple(here)] = value

    def plane_copy(self, k, offsets):
        index = [pl.ds(self.place.coord(dim, offsets.get(dim, ZERO)), ONE) for dim in range(THREE)]
        src = self.acc.at[:, index[ZERO], index[ONE], index[TWO]]
        return remote(src, self.got_p.at[k], self.send.at[FOUR], self.recv.at[FOUR], self.place.device(offsets))

    def plane_all(self):
        return remote(self.got_p.at[ONE:], self.got_p.at[ONE:], self.send.at[FOUR], self.recv.at[FOUR], self.place.partner)

    def plane_start(self):
        for way in range(TWO):
            self.ring(ONE, way).wait_recv()
        self.add(ZERO, None, self.got_b.at[ZERO], self.got_b.at[ONE])

        each_of_plane(self.order, lambda k, offsets: self.plane_copy(k, offsets).start())

    def own(self):
        z, y, x = [pl.ds(p, ONE) for p in self.place.pos]
        return self.acc.at[:, z, y, x]

    def last_copy(self):
        return remote(self.mine, self.other, self.send.at[5], self.recv.at[5], self.place.partner)

    def last(self):
        self.plane_all().wait_recv()
        self.mine[...] = functools.reduce(jnp.add, [self.got_p[k] for k in range(ONE, SIXTEEN)], self.own()[...])
        for step in range(TWO):
            for way in range(TWO):
                self.ring(step, way).wait_send()
        self.plane_all().wait_send()
        self.last_copy().start()

    def finish(self, store):
        self.last_copy().wait_recv()
        first = self.place.core == ZERO
        for u in range(self.units):
            own, came = self.mine[u, ZERO, ZERO, ZERO], self.other[u, ZERO, ZERO, ZERO]
            store(u, jnp.concatenate([jnp.where(first, own, came), jnp.where(first, came, own)], axis=ONE))
        self.last_copy().wait_send()


def landing_shapes(order, units):
    size = [FOUR, FOUR, FOUR]
    size[order[ZERO]] = ONE
    return (units, *size, EIGHT, WIDTH), (TWO, units, *size, EIGHT, WIDTH), (SIXTEEN, units, ONE, ONE, ONE, EIGHT, WIDTH), (units, ONE, ONE, ONE, EIGHT, WIDTH), (units, ONE, ONE, ONE, EIGHT, WIDTH)


class Small:
    def __init__(self, place, value, slots, send, recv):
        self.place, self.value, self.slots, self.send, self.recv = place, value, slots, send, recv

    def peers(self, stage):
        if stage == THREE:
            return [self.place.partner]
        return [self.place.device({stage: delta}) for delta in LINE]

    def copies(self, stage):
        return [remote(self.value, self.slots.at[THREE * stage + k], self.send.at[THREE * stage + k], self.recv.at[THREE * stage + k], peer)
                for k, peer in enumerate(self.peers(stage))]

    def start(self, stage):
        for copy in self.copies(stage):
            copy.start()

    def finish(self, stage):
        copies = self.copies(stage)
        for copy in copies:
            copy.wait()
        self.value[...] = functools.reduce(jnp.add, [self.slots[THREE * stage + k] for k in range(len(copies))], self.value[...])

    def turn(self, stage):
        def step():
            self.finish(stage)
            self.start(stage + ONE)
        return step

    def steps(self):
        return [lambda: self.start(ZERO), self.turn(ZERO), self.turn(ONE), self.turn(TWO), lambda: self.finish(THREE)]


class Late(Small):
    def __init__(self, place, value, slots, send, recv, planes, plane_send, plane_recv):
        super().__init__(place, value, slots, send, recv)
        self.planes, self.plane_send, self.plane_recv = planes, plane_send, plane_recv

    def peers(self, stage):
        return super().peers({ZERO: ORDERS[ZERO][ZERO], ONE: THREE}[stage])

    def plane(self, k, offsets):
        return remote(self.value, self.planes.at[k], self.plane_send, self.plane_recv, self.place.device(offsets))

    def steps(self):
        def first():
            each_of_plane(ORDERS[ZERO], lambda k, offsets: self.plane(k, offsets).start())

        def second():
            remote(self.planes.at[ONE:], self.planes.at[ONE:], self.plane_send, self.plane_recv, self.place.partner).wait()
            self.value[...] = functools.reduce(jnp.add, [self.planes[k] for k in range(ONE, SIXTEEN)], self.value[...])
            self.start(ZERO)

        return [first, second, self.turn(ZERO), lambda: self.finish(ONE)]


VMEM = pl.BlockSpec(memory_space=pltpu.VMEM)
HBM = pl.BlockSpec(memory_space=pl.ANY)
DMA = pltpu.SemaphoreType.DMA


COLOURS = ((THREE, FOUR, 5), (6, 7, EIGHT), (9, 10, 11))
GRID = (FOUR, FOUR, FOUR)


def spread(buf, u, out_ref, column_base):
    @pl.loop(ZERO, TWO)
    def _(half):
        for part in range(SIXTEEN):
            g = half * SIXTEEN + part
            tiles = [buf[half * TWO + part // EIGHT, part // TWO % FOUR, part % TWO * TWO + k // TWO, k % TWO, u].astype(F32) for k in range(FOUR)]
            rows = pl.ds(pl.multiple_of(g * SIXTEEN, SIXTEEN), SIXTEEN)
            for j, cols in enumerate(lane_tiles()):
                value = jnp.concatenate([t[FOUR * j:FOUR * j + FOUR] for t in tiles], axis=ZERO).astype(BF16)
                out_ref[rows, column_base + cols.start:column_base + cols.stop] = value


def spread_down(buf, u, out_ref, cols):
    @pl.loop(ZERO, SIXTEEN)
    def _(i):
        for k in range(EIGHT):
            d = i * EIGHT + k
            out_ref[pl.ds(pl.multiple_of(d * SIXTEEN, SIXTEEN), SIXTEEN), cols] = buf[i // FOUR, lax.rem(i, FOUR), k // TWO, k % TWO, u]


def same(shape, test):
    row = lax.broadcasted_iota(jnp.int32, shape, ZERO)
    col = lax.broadcasted_iota(jnp.int32, shape, ONE)
    return jnp.where(test(row, col), 1.0, 0.0)


def small_columns(small_ref, c_ref):
    rows = [small_ref[z, y, x, c, ZERO] for z in range(FOUR) for y in range(FOUR) for x in range(FOUR) for c in range(TWO)]
    table = jnp.concatenate(rows, axis=ZERO).astype(BF16)
    quads = nn(same((DIM, LANES), lambda r, c: r // FOUR == c).astype(BF16), table)
    quads = (quads * same((DIM, LANES), lambda r, c: r % FOUR == c % FOUR)).astype(BF16)
    mask = same((DIM, LANES), lambda r, c: r % SIXTEEN == c % SIXTEEN)
    pick = same((DIM, 32), lambda r, c: r // SIXTEEN == c).astype(BF16)
    ups = [(nn(pick, table[32 * k:32 * k + 32]) * mask).astype(BF16) for k in range(FOUR)]
    for layer in range(TWO):
        def is_up(r):
            return r // SIXTEEN == layer * FOUR + TWO

        value = nn(quads, same((LANES, LANES), lambda r, c: (r // 64 == layer) & (r % 64 // FOUR == c) & ~is_up(r)).astype(BF16))
        for k in range(FOUR):
            value = value + nn(ups[k], same((LANES, LANES), lambda r, c: is_up(r) & (c == B_UP + k)).astype(BF16))
        c_ref[layer] = value


def tile_of(rows):
    rows = rows.astype(F32)
    return jnp.concatenate([rows[:, cols] for cols in lane_tiles()], axis=ZERO).astype(BF16)


def small_row(b_attn, ln_par, b_up, b_down):
    lane = lax.broadcasted_iota(jnp.int32, (ONE, LANES), ONE)
    row = jnp.zeros((ONE, LANES), F32)
    pieces = []
    for l in range(TWO):
        for m in range(FOUR):
            pieces += [(b_attn[l, m:m + ONE, :], 64 * l + FOUR * m), (ln_par[l, m:m + ONE, :], 64 * l + FOUR * m + SIXTEEN)]
        pieces += [(b_up[l:l + ONE, :], 64 * l + 32), (b_down[l:l + ONE, :], 64 * l + 48)]
    for piece, at in pieces:
        n = piece.shape[ONE]
        wide = jnp.concatenate([piece.astype(F32), jnp.zeros((ONE, LANES - n), F32)], axis=ONE)
        wide = pltpu.roll(wide, at, ONE) if at else wide
        row = jnp.where((lane >= at) & (lane < at + n), wide, row)
    return row


def hooks(slot, plan):
    def hook(at):
        for slots, run in plan:
            mine = [when for when in slots if when % FOUR == at]
            if mine:
                pl.when(functools.reduce(jnp.logical_or, [slot + at == when for when in mine]))(run)
    return hook


def forward_kernel(len_ref, x_hbm, cos_ref, sin_ref, w_attn, b_attn, ln_par, w_up, b_up, w_down, b_down,
                   xs_out, q_ref, k_ref, v_ref, p_ref, ctx_ref, mid_ref, act_ref, slope_ref, st1_ref, st2_ref, c_ref,
                   nat_qkv, nat_wo, nat_up, nat_down,
                   xs, ctxb, n_qkv, n_wo, n_up, n_down, h_ref, s_a, s_b, s_c,
                   sbuf, q0, q1, q2, m0, m1, m2, stats, f0, f1, f2, send, recv, nat_sem, x_sem):
    step = pl.program_id(ZERO)
    phase, seq, layer = step // FOUR, lax.rem(step, FOUR), step // EIGHT
    place = Place()
    z, y, x = place.pos
    qkv_bufs, mo_bufs, fifteen = (q0, q1, q2), (m0, m1, m2), (f0, f1, f2)

    def group(bufs, base, l):
        return [Gather(place, b.at[l], fifteen[base // THREE], ORDERS[k], send.at[base + k, l], recv.at[base + k, l]) for k, b in enumerate(bufs)]

    little = Gather(place, sbuf, fifteen[TWO], ORDERS[ZERO], send.at[6, ZERO], recv.at[6, ZERO])

    def nat_copies(which, l):
        if which == ZERO:
            return [pltpu.make_async_copy(n_qkv, nat_qkv.at[l], nat_sem.at[ZERO])]
        return [pltpu.make_async_copy(src, dst.at[l], nat_sem.at[ONE + i]) for i, (src, dst) in enumerate(((n_wo, nat_wo), (n_up, nat_up), (n_down, nat_down)))]

    def wait(copies):
        for copy in copies:
            copy.wait()

    def start(copies):
        for copy in copies:
            copy.start()

    def take_qkv():
        pl.when(step > ZERO)(lambda: wait(nat_copies(ZERO, layer)))
        for m in range(THREE):
            spread(qkv_bufs[m].at[layer], ZERO, n_qkv.at[m], ZERO)
        start(nat_copies(ZERO, layer))

    def take_mo():
        pl.when(step > EIGHT)(lambda: wait(nat_copies(ONE, layer)))
        for colour in range(THREE):
            for u, unit in enumerate(COLOURS[colour]):
                buf = mo_bufs[colour].at[layer]
                if unit == THREE:
                    spread(buf, u, n_wo, ZERO)
                elif unit < EIGHT:
                    spread(buf, u, n_up, DIM * (unit - FOUR))
                else:
                    spread_down(buf, u, n_down, lane_tiles()[unit - EIGHT])
        start(nat_copies(ONE, layer))

    x_copies = [pltpu.make_async_copy(x_hbm.at[s], ctxb.at[s], x_sem.at[s]) for s in range(SEQS)]

    @pl.when(step == ZERO)
    def _():
        place.greet()
        start(x_copies)
        for l in range(TWO):
            for unit in range(12):
                if unit < FOUR:
                    tile = tile_of(w_attn[l, unit])
                elif unit < EIGHT:
                    tile = tile_of(w_up[l, :, DIM * (unit - FOUR):DIM * (unit - THREE)])
                else:
                    tile = w_down[l, :, lane_tiles()[unit - EIGHT]]
                if unit < THREE:
                    qkv_bufs[unit][l, z, y, x, place.core, ZERO] = tile
                else:
                    mo_bufs[(unit - THREE) // THREE][l, z, y, x, place.core, (unit - THREE) % THREE] = tile
        sbuf[z, y, x, place.core, ZERO] = small_row(b_attn, ln_par, b_up, b_down)
        parts = group(qkv_bufs, ZERO, ZERO)
        first, second = gather_steps([little] + parts), gather_steps(group(mo_bufs, THREE, ZERO))

        def ready(s):
            x_copies[s].wait()
            xs[s] = ctxb[s].T
            put_stats(stats.at[s], norm_stats(xs.at[s]))

        place.met()
        first[ZERO]()
        second[ZERO]()
        ready(ZERO)
        ready(ONE)
        first[ONE]()
        ready(TWO)
        ready(THREE)
        first[TWO]()
        second[ONE]()
        little.end()
        small_columns(sbuf, c_ref)
        for part in parts:
            part.end()

    attn_hook = hooks(step * FOUR, [((when, when + 32), run) for when, run in zip((9, 13), gather_steps(group(mo_bufs, THREE, layer))[TWO:])])
    mlp_steps = gather_steps(group(qkv_bufs, ZERO, ONE)) + gather_steps(group(mo_bufs, THREE, ONE))[:TWO]
    mlp_hook = hooks(step * FOUR, [((when,), run) for when, run in zip((SIXTEEN, 25, 30, 31, 17, 26), mlp_steps)])

    @pl.when(phase % TWO == ZERO)
    def _():
        pl.when(seq == ZERO)(take_qkv)

        @pl.when(step < FOUR)
        def _():
            xs_out[ZERO, ZERO] = xs[seq]

        @pl.when(step > 7)
        def _():
            put_stats(stats.at[seq], norm_stats(xs.at[seq]))

        attn_hook(ZERO)
        attn_forward(len_ref[seq], xs.at[seq], n_qkv, c_ref.at[layer], cos_ref, sin_ref, q_ref.at[ZERO, ZERO], k_ref.at[ZERO, ZERO],
                     v_ref.at[ZERO, ZERO], p_ref.at[ZERO, ZERO], ctx_ref.at[ZERO, ZERO], ctxb.at[seq], get_stats(stats.at[seq]), st1_ref.at[ZERO, ZERO], h_ref, s_a, s_b, s_c, attn_hook)
        attn_hook(THREE)

    @pl.when(phase % TWO == ONE)
    def _():
        pl.when(seq == ZERO)(take_mo)
        mlp_hook(ZERO)
        mlp_forward(layer, ctxb.at[seq], xs.at[seq], n_wo, n_up, n_down, c_ref.at[layer], mid_ref.at[ZERO, ZERO], act_ref.at[ZERO, ZERO], slope_ref.at[ZERO, ZERO],
                    st2_ref.at[ZERO, ZERO], h_ref, s_a, s_b, mlp_hook)

        @pl.when(layer == ZERO)
        def _():
            xs_out[ZERO, ZERO] = xs[seq]
        mlp_hook(THREE)

    @pl.when(step == 15)
    def _():
        for which in range(TWO):
            wait(nat_copies(which, ONE))


def attn_forward(length, xt, w, c_ref, cos_ref, sin_ref, q_ref, k_ref, v_ref, p_buf, ctx_ref, ctxb, stats, stat_ref, h_ref, s_a, s_b, s_c, hook):
    put_stats(stat_ref, stats)
    norm_to(xt, stats, c_ref, LN_PAR, h_ref)
    for m, acc in enumerate((s_a, s_b, s_c)):
        acc[...] = tn(w[m], h_ref[...])
    cos, sin = cos_ref[...], sin_ref[...]
    for m, (acc, out) in enumerate(((s_a, q_ref), (s_b, k_ref), (s_c, v_ref))):
        for head in range(HEADS):
            rows, one, two = head_rows(head)
            if m == TWO:
                out[rows, :] = (acc[rows, :] + column(c_ref, rows, B_ATTN + m)).astype(BF16)
                continue
            a, b = [acc[half, :] + column(c_ref, half, B_ATTN + m) for half in (one, two)]
            if m == ZERO:
                a, b = a * HEAD ** -0.5, b * HEAD ** -0.5
            out[one, :] = (a * cos - b * sin).astype(BF16)
            out[two, :] = (b * cos + a * sin).astype(BF16)
    hook(ONE)
    key = lax.broadcasted_iota(jnp.int32, (SIXTEEN, TOK), ONE)
    row = lax.broadcasted_iota(jnp.int32, (SIXTEEN, TOK), ZERO)
    bias_rows = jnp.where((row == ZERO) & (key >= length), NEG_BIG, 0.0).astype(BF16)
    one_rows = jnp.where(row == ZERO, 1.0, 0.0).astype(BF16)
    scores = (s_a, s_b)

    def open_head(head):
        rows = head_rows(head)[ZERO]
        keys = jnp.concatenate([k_ref[rows, :], bias_rows], axis=ZERO)
        queries = jnp.concatenate([q_ref[rows, :], one_rows], axis=ZERO)
        scores[head % TWO][...] = tn(keys, queries)

    def weigh(head):
        value, tops, sums = scores[head % TWO], [], []

        def top(rows):
            tops.append(jnp.max(value[rows, :], axis=ZERO, keepdims=True))
            if rows.stop == TOK:
                tops[:] = [functools.reduce(jnp.maximum, tops)]

        def power(rows):
            weight = jnp.exp(value[rows, :] - tops[ZERO])
            value[rows, :] = weight
            sums.append(total(weight))
            if rows.stop == TOK:
                sums[:] = [1.0 / functools.reduce(jnp.add, sums)]

        def share(rows):
            p_buf[head, rows, :] = (value[rows, :] * sums[ZERO]).astype(BF16)

        return [functools.partial(run, rows) for run in (top, power, share) for rows in row_chunks()]

    def close_head(head):
        rows = head_rows(head)[ZERO]
        ctx = nn(v_ref[rows, :], p_buf[head])
        ctx_ref[rows, :] = ctx
        ctxb[rows, :] = ctx.astype(BF16)

    open_head(ZERO)
    for head in range(HEADS):
        products = [functools.partial(open_head, head + ONE)] if head + ONE < HEADS else []
        if head:
            products.append(functools.partial(close_head, head - ONE))
        woven(products, weigh(head))
        if head == THREE:
            hook(TWO)
    close_head(HEADS - ONE)


def mlp_forward(layer, ctxb, xt, wo, up, down, c_ref, mid_ref, act_ref, slope_ref, stat_ref, h_ref, s_a, s_b, hook):
    s_a[...] = tn(wo[...], ctxb[...])
    for rows in row_chunks():
        mid_ref[rows, :] = (xt[rows, :].astype(F32) + s_a[rows, :] + column(c_ref, rows, B_ATTN + THREE)).astype(BF16)
    stats = norm_stats(mid_ref)
    put_stats(stat_ref, stats)
    norm_to(mid_ref, stats, c_ref, LN_PAR + TWO, h_ref)
    hook(ONE)
    pre = (s_a, s_b)
    parts = [slice(DIM * k, DIM * k + DIM) for k in range(FOUR)]

    def open_part(k):
        pre[k % TWO][...] = tn(up[:, parts[k]], h_ref[...])

    open_part(ZERO)
    for k, part in enumerate(parts):
        if k < THREE:
            open_part(k + ONE)
        for rows in row_chunks():
            value = pre[k % TWO][rows, :] + column(c_ref, rows, B_UP + k)
            scaled = value * math.sqrt(0.5)
            cdf = 0.5 + 0.5 * lax.erf(scaled)
            density = jnp.exp2(scaled * scaled * -math.log2(math.e) - 0.5 * math.log2(2.0 * math.pi))
            there = slice(part.start + rows.start, part.start + rows.stop)
            act_ref[there, :] = (value * cdf).astype(BF16)
            slope_ref[there, :] = cdf + value * density
        if k == ONE:
            hook(TWO)

    @pl.when(layer == ZERO)
    def _():
        s_a[...] = tn(down[...], act_ref[...])
        for rows in row_chunks():
            xt[rows, :] = (mid_ref[rows, :].astype(F32) + s_a[rows, :] + column(c_ref, rows, B_DOWN)).astype(BF16)


def forward(lengths, x, tables, params):
    def saved(index, rows, dtype):
        return jax.ShapeDtypeStruct((TWO, SEQS, rows, TOK), dtype), pl.BlockSpec((ONE, ONE, rows, TOK), index)

    def attn_at(s):
        return s // EIGHT, jnp.where(s // FOUR % TWO == ZERO, s % FOUR, THREE), ZERO, ZERO

    def mlp_at(s):
        odd = s // FOUR % TWO == ONE
        return jnp.where(s < 12, ZERO, ONE), jnp.where(odd, s % FOUR, jnp.where(s < FOUR, ZERO, THREE)), ZERO, ZERO

    def xs_at(s):
        return jnp.where(s < FOUR, ZERO, ONE), jnp.where(s < EIGHT, s % FOUR, THREE), ZERO, ZERO

    outs = [saved(xs_at, DIM, BF16)] + [saved(attn_at, DIM, BF16)] * THREE
    outs += [(jax.ShapeDtypeStruct((TWO, SEQS, HEADS, TOK, TOK), BF16), pl.BlockSpec((ONE, ONE, HEADS, TOK, TOK), lambda s: (*attn_at(s), ZERO))), saved(attn_at, DIM, F32)]
    outs += [saved(mlp_at, DIM, BF16), saved(mlp_at, FFN, BF16), saved(mlp_at, FFN, F32), saved(attn_at, EIGHT, F32), saved(mlp_at, EIGHT, F32)]
    outs += [(jax.ShapeDtypeStruct((TWO, *COLS), F32), once((TWO, *COLS)))]
    weights = ((THREE, DIM, DIM), (DIM, DIM), (DIM, FFN), (FFN, DIM))
    outs += [(jax.ShapeDtypeStruct((TWO, *w), BF16), HBM) for w in weights]
    scratch = [(SEQS, *SQUARE), (SEQS, *SQUARE), *weights, SQUARE]
    scratch = [pltpu.VMEM(s, BF16) for s in scratch] + [pltpu.VMEM(SQUARE, F32)] * THREE + [pltpu.VMEM((*GRID, TWO, ONE, ONE, LANES), F32)]
    scratch += [pltpu.VMEM((TWO, *GRID, TWO, n, SIXTEEN, LANES), BF16) for n in (ONE, THREE) for _ in range(THREE)]
    scratch += [pltpu.VMEM((SEQS, EIGHT, TOK), F32)] + [pltpu.VMEM((15, n, SIXTEEN, LANES), BF16) for n in (ONE, THREE)]
    scratch += [pltpu.VMEM((15, ONE, ONE, LANES), F32), DMA((7, TWO, 5)), DMA((7, TWO, 5)), DMA((FOUR,)), DMA((SEQS,))]
    return pl.pallas_call(
        forward_kernel, grid=(SIXTEEN,),
        out_shape=[o[ZERO] for o in outs], out_specs=[o[ONE] for o in outs],
        in_specs=[pl.BlockSpec(memory_space=pltpu.SMEM), HBM, once((HALF, TOK)), once((HALF, TOK))] + [once(p.shape) for p in params],
        scratch_shapes=scratch,
        compiler_params=pltpu.CompilerParams(collective_id=ZERO, has_side_effects=True, vmem_limit_bytes=67043328,
                                             dimension_semantics=("arbitrary",)),
        name="forward")(lengths, x, *tables, *params)


def norm_back(dh_ref, x_ref, stats, c_ref, lane, sums, at, write, beside):
    mean, rstd = stats
    means = [0.0, 0.0]

    def both(rows):
        dh = dh_ref[rows, :]
        return dh, dh * column(c_ref, rows, lane), (x_ref[rows, :].astype(F32) - mean) * rstd

    def first(rows):
        dh, dxhat, xhat = both(rows)
        means[ZERO], means[ONE] = means[ZERO] + total(dxhat), means[ONE] + total(dxhat * xhat)
        sums[at, rows, :] += fold(dh * xhat)
        sums[at + ONE, rows, :] += fold(dh)

    def second(rows):
        dh, dxhat, xhat = both(rows)
        write(rows, rstd * (dxhat - means[ZERO] * (1.0 / DIM) - xhat * (means[ONE] * (1.0 / DIM))))

    woven(beside, [functools.partial(run, rows) for run in (first, second) for rows in row_chunks()])


def columns_of(partials):
    lane = lax.broadcasted_iota(jnp.int32, COLS, ONE)
    value = jnp.zeros(COLS, F32)
    for at, partial in enumerate(partials):
        value = jnp.where(lane == at, jnp.sum(partial, axis=ONE, keepdims=True), value)
    return value.T[:EIGHT]


def head_rows(head):
    return slice(HEAD * head, HEAD * head + HEAD), slice(HEAD * head, HEAD * head + HALF), slice(HEAD * head + HALF, HEAD * head + HEAD)


class Reduce:
    def __init__(self, place, units, grads, buffers, send, recv):
        self.units = units
        self.scatters = [Scatter(place, (lambda u, k=k: grads(units[k][u])), *buffers[k], ORDERS[k], send.at[k], recv.at[k]) for k in range(THREE)]

    def steps(self, store):
        def each(*names):
            def step():
                for name in names:
                    for s in self.scatters:
                        getattr(s, name)()
            return step

        def finish():
            for units, s in zip(self.units, self.scatters):
                s.finish(lambda u, full, units=units: store(units[u], full))

        return [each("swap"), each("swapped", "ring_start"), each("ring_turn"), each("plane_start"), each("last"), finish]


def backward_kernel(dy_ref, mid_ref, ctx_ref, st2_ref, q_ref, k_ref, v_ref, x_ref, st1_ref, cos_ref, sin_ref, c_ref, p_hbm, slope_hbm, act_hbm,
                    qkv_hbm, wo_hbm, up_hbm, down_hbm,
                    dx_ref, attn_out, up_out, down_out, small_out, *refs):
    (grad, dctx, delta, big, wqkv, wo, slope, act, dpre, h_ref, s_a, s_b, d_a, d_b, sums,
     g_qkv, g_wo, g_up, g_down, *small_bufs), refs = refs[:28], refs[28:]
    qkv_bufs, mo_bufs, refs = [refs[6 * k:6 * k + 6] for k in range(THREE)], [refs[6 * k + 18:6 * k + 24] for k in range(THREE)], refs[36:]
    send, recv, late_sem, plane_sem, big_sem, w_sem, mlp_sem = refs
    step = pl.program_id(ZERO)
    phase, seq = step // FOUR, lax.rem(step, FOUR)
    layer = ONE - step // EIGHT
    place = Place()

    def grads(unit):
        if unit < THREE:
            return g_qkv.at[unit]
        if unit == THREE:
            return g_wo
        if unit < EIGHT:
            return g_up.at[unit - FOUR]
        return g_down.at[:, :, :, unit - EIGHT]

    live = step < SIXTEEN
    turn = jnp.where(live, ZERO, ONE)
    qkv_sums = Reduce(place, ((ZERO,), (ONE,), (TWO,)), grads, [(a, ra, rb, rp.at[turn], *last) for a, ra, rb, rp, *last in qkv_bufs], send.at[turn], recv.at[turn])
    mo_sums = Reduce(place, COLOURS, grads, mo_bufs, send.at[TWO], recv.at[TWO])

    def third(i):
        one = pl.ds(i, ONE)
        bufs = [(a.at[one], ra.at[one], rb.at[:, one], rp.at[:, one], mine.at[one], other.at[one]) for a, ra, rb, rp, mine, other in mo_bufs]
        return Reduce(place, [units[i:i + ONE] for units in COLOURS], grads, bufs, send.at[THREE + i], recv.at[THREE + i]).steps(store(ONE - turn))

    small_refs = small_bufs[::THREE]
    early, middle, late = [Late(place, small_refs[i], small_bufs[THREE * i + ONE], late_sem.at[i, ZERO], late_sem.at[i, ONE], small_bufs[THREE * i + TWO],
                                plane_sem.at[i, ZERO], plane_sem.at[i, ONE]).steps() for i in range(THREE)]
    first_core = place.core == ZERO

    def store(l):
        def put(unit, full):
            if unit < EIGHT:
                mine = jnp.where(first_core, full[:FOUR], full[FOUR:])
                if unit < FOUR:
                    attn_out[l, unit] = mine
                else:
                    up_out[l, :, DIM * (unit - FOUR):DIM * (unit - THREE)] = mine
            else:
                at = EIGHT * (unit % TWO)

                @pl.when(place.core == (unit - EIGHT) // TWO)
                def _():
                    down_out[l, at:at + EIGHT] = full
        return put

    def mlp_weights(l):
        parts = [pl.ds(DIM * k, DIM) for k in range(FOUR)]
        return ([pltpu.make_async_copy(down_hbm.at[l, part], big.at[k], big_sem.at[k]) for k, part in enumerate(parts)],
                [pltpu.make_async_copy(up_hbm.at[l, :, part], big.at[FOUR + k], big_sem.at[FOUR + k]) for k, part in enumerate(parts)] +
                [pltpu.make_async_copy(wo_hbm.at[l], wo, w_sem.at[ZERO])])

    def attn_weights(l):
        return [pltpu.make_async_copy(qkv_hbm.at[l], wqkv, w_sem.at[ONE])]

    def probs(l, s):
        return [pltpu.make_async_copy(p_hbm.at[l, s, k], big.at[k], big_sem.at[k]) for k in range(HEADS)]

    def saved_mlp(l, s):
        return [pltpu.make_async_copy(slope_hbm.at[l, s], slope, mlp_sem.at[ZERO]), pltpu.make_async_copy(act_hbm.at[l, s], act, mlp_sem.at[ONE])]

    def start(copies):
        for copy in copies:
            copy.start()

    def wait(copies):
        for copy in copies:
            copy.wait()

    @pl.when(step == ZERO)
    def _():
        place.greet()
        start(mlp_weights(ONE)[ZERO] + saved_mlp(ONE, ZERO) + mlp_weights(ONE)[ONE] + attn_weights(ONE))

    pl.when(step == ONE)(place.met)
    mo_steps, qkv_steps = mo_sums.steps(store(ONE - turn)), qkv_sums.steps(store(ONE - turn))

    def plan(slots, steps):
        return [((slot,), run) for slot, run in zip(slots, steps)]

    thirds = [], []
    for i, slots in enumerate(((48, 50, 54, 59, 73, 74), (48, 51, 55, 62, 73, 74), (48, 53, 57, 63, 73, 74))):
        steps = plan(slots, third(i))
        thirds[ZERO].extend(steps[:FOUR])
        thirds[ONE].extend(steps[FOUR:])
    attn_hook = hooks(step * FOUR, plan((48, 57, 61, 63), middle) + plan((SIXTEEN, 24, 28), mo_steps) + thirds[ZERO] +
                      plan((53, 53), qkv_steps[FOUR:]))
    mlp_plan = plan((37, 45, 46), mo_steps[THREE:]) + plan((32, 36, 40, 47), qkv_steps) + plan((34, 41, 45, 47), early)
    mlp_hook = hooks(step * FOUR, mlp_plan + plan((64, 66, 70, 72, 75), qkv_steps) + plan((65, 72, 74, 75), late) + thirds[ONE] +
                     plan((75,), qkv_steps[5:]))


    @pl.when(phase % TWO == ZERO)
    def _():
        @pl.when((seq == ZERO) & live)
        def _():
            for ref in (g_wo, g_up, g_down, sums):
                ref[...] = jnp.zeros_like(ref)

        @pl.when(step < FOUR)
        def _():
            grad[seq] = dy_ref[ZERO].T

        @pl.when((seq == ZERO) & live)
        def _():
            wait(mlp_weights(layer)[ZERO])

        mlp_hook(ZERO)

        @pl.when(step == SIXTEEN)
        def _():
            small_refs[TWO][...] = columns_of([sums[i] for i in range(5)])

        def after_first():
            pl.when(seq < THREE)(lambda: start(saved_mlp(layer, seq + ONE)))
            pl.when(seq == THREE)(lambda: start(probs(layer, ZERO)[:FOUR]))

        def before_second():
            pl.when(seq == ZERO)(lambda: wait(mlp_weights(layer)[ONE]))

        def after_second():
            pl.when(seq == THREE)(lambda: start(probs(layer, ZERO)[FOUR:]))

        pl.when(live)(lambda: wait(saved_mlp(layer, seq)))
        mlp_backward(grad.at[seq], slope, act, mid_ref, ctx_ref, st2_ref.at[ZERO], wo, big, c_ref, dctx.at[seq], delta.at[seq], g_wo, g_up, g_down,
                     dpre, h_ref, s_a, s_b, sums, pl.when(live), mlp_hook,
                     after_first, after_second, before_second)

        @pl.when((seq == THREE) & live)
        def _():
            value = columns_of([sums[i] for i in range(EIGHT)])

            @pl.when(layer == ONE)
            def _():
                small_refs[ZERO][:EIGHT, :] = value

            @pl.when(layer == ZERO)
            def _():
                small_refs[ONE][...] = value

        mlp_hook(THREE)

    @pl.when(phase % TWO == ONE)
    def _():
        @pl.when(seq == ZERO)
        def _():
            wait(attn_weights(layer))
            for ref in (g_qkv, sums):
                ref[...] = jnp.zeros_like(ref)

        @pl.when(step == FOUR)
        def _():
            start(saved_mlp(ZERO, ZERO))
        attn_hook(ZERO)

        def after_heads():
            pl.when(seq < THREE)(lambda: start(probs(layer, seq + ONE)))
            pl.when(step == 7)(lambda: start(mlp_weights(ZERO)[ZERO] + mlp_weights(ZERO)[ONE]))

        wait(probs(layer, seq))
        attn_backward(dctx.at[seq], delta.at[seq], big, q_ref, k_ref, v_ref, x_ref, st1_ref.at[ZERO], grad.at[seq], wqkv, c_ref, cos_ref, sin_ref,
                      g_qkv, dpre, h_ref, s_a, s_b, d_a, d_b, sums, attn_hook,
                      after_heads)

        @pl.when(step == 7)
        def _():
            small_refs[ZERO][EIGHT:, :] = columns_of([sums[i] for i in range(5)])

        @pl.when(step == 7)
        def _():
            start(attn_weights(ZERO))

        @pl.when(step > 11)
        def _():
            dx_ref[ZERO] = grad[seq].T
        attn_hook(THREE)

    @pl.when(step == 18)
    def _():
        small_out[:SIXTEEN, :], small_out[SIXTEEN:24, :], small_out[24:, :] = [ref[...] for ref in small_refs]


def add_to(ref, value):
    ref[...] = ref[...] + value.reshape(ref.shape)


def mlp_backward(grad, slope, act, mid_ref, ctx_ref, stat_ref, wo, big, c_ref, dctx, delta, g_wo, g_up, g_down, dpre, h_ref, s_a, s_b, sums, when, hook, after_first, after_second, before_second):
    parts = [slice(DIM * k, DIM * k + DIM) for k in range(FOUR)]
    pre = (s_a, s_b)

    def dact(k):
        pre[k % TWO][...] = nn(big[k], grad[...])

    @when
    def _():
        def scale(k, chunk):
            there = slice(parts[k].start + chunk.start, parts[k].start + chunk.stop)
            value = pre[k % TWO][chunk, :] * slope[there, :]
            sums[k, chunk, :] += fold(value)
            dpre[there, :] = value.astype(BF16)

        def down_product(k):
            add_to(g_down.at[k], nt(act[parts[k], :], grad[...]))

        dact(ZERO)
        norm_to(mid_ref.at[ZERO], get_stats(stat_ref), c_ref, LN_PAR + TWO, h_ref)
        for k in range(FOUR):
            products = [functools.partial(down_product, k)]
            if k < THREE:
                products = [functools.partial(dact, k + ONE)] + products
            woven(products, [functools.partial(scale, k, chunk) for chunk in row_chunks()])
        after_first()
    hook(ONE)

    @when
    def _():
        before_second()
        s_a[...] = functools.reduce(jnp.add, [nn(big[FOUR + k], dpre[rows, :]) for k, rows in enumerate(parts)])
        after_second()
    hook(TWO)

    @when
    def _():
        def write(rows, dx):
            dy = grad[rows, :].astype(F32)
            dmid = (dy + dx).astype(BF16)
            grad[rows, :] = dmid
            sums[6, rows, :] += fold(dy)
            sums[7, rows, :] += fold(dmid.astype(F32))

        norm_back(s_a, mid_ref.at[ZERO], get_stats(stat_ref), c_ref, LN_PAR + TWO, sums, FOUR, write,
                  [lambda k=k, rows=rows: add_to(g_up.at[k], nt(h_ref[...], dpre[rows, :])) for k, rows in enumerate(parts)])
        add_to(g_wo, nt(ctx_ref[ZERO].astype(BF16), grad[...]))
        s_b[...] = nn(wo[...], grad[...])
        for head in range(HEADS):
            rows = head_rows(head)[ZERO]
            value = s_b[rows, :].astype(BF16)
            dctx[rows, :] = value
            delta[head:head + ONE, :] = total(value.astype(F32) * ctx_ref[ZERO, rows, :])


def attn_backward(dctx, delta, probs, q_ref, k_ref, v_ref, x_ref, stat_ref, grad, wqkv, c_ref, cos_ref, sin_ref, g_qkv, dproj, h_ref, s_a, s_b, d_a, d_b,
                  sums, hook, prefetch):
    scores, dscores = (s_a, s_b), (d_a, d_b)
    q, k, v = q_ref.at[ZERO], k_ref.at[ZERO], v_ref.at[ZERO]

    def open_head(head):
        rows = head_rows(head)[ZERO]
        scores[head % TWO][...] = tn(v[rows, :], dctx[rows, :])

    def weigh(head, rows):
        dscores[head % TWO][rows, :] = (probs[head, rows, :].astype(F32) * (scores[head % TWO][rows, :] - delta[head:head + ONE, :])).astype(BF16)

    def values(head):
        rows = head_rows(head)[ZERO]
        dv = nt(dctx[rows, :], probs[head])
        sums[TWO, rows, :] += fold(dv)
        dproj[TWO * DIM + rows.start:TWO * DIM + rows.stop, :] = dv.astype(BF16)

    def close_head(head, m):
        rows, one, two = head_rows(head)
        ds = dscores[head % TWO][...]
        value = nn(k[rows, :], ds) * HEAD ** -0.5 if m == ZERO else nt(q[rows, :], ds)
        cos, sin = cos_ref[...], sin_ref[...]
        a, b = value[:HALF], value[HALF:]
        for at, out in ((one, a * cos + b * sin), (two, b * cos - a * sin)):
            dproj[m * DIM + at.start:m * DIM + at.stop, :] = out.astype(BF16)
            sums[m, at, :] += fold(out)

    open_head(ZERO)
    for head in range(HEADS):
        products = [functools.partial(values, head)]
        if head:
            products = [functools.partial(close_head, head - ONE, m) for m in range(TWO)] + products
        if head + ONE < HEADS:
            products = [functools.partial(open_head, head + ONE)] + products
        woven(products, [functools.partial(weigh, head, rows) for rows in row_chunks()])
        if head == THREE:
            hook(ONE)
    for m in range(TWO):
        close_head(HEADS - ONE, m)
    prefetch()
    hook(TWO)
    norm_to(x_ref.at[ZERO], get_stats(stat_ref), c_ref, LN_PAR, h_ref)
    parts = [slice(DIM * m, DIM * m + DIM) for m in range(THREE)]
    s_a[...] = functools.reduce(jnp.add, [nn(wqkv[m], dproj[rows, :]) for m, rows in enumerate(parts)])

    def write(rows, dx):
        grad[rows, :] = (grad[rows, :].astype(F32) + dx).astype(BF16)

    norm_back(s_a, x_ref.at[ZERO], get_stats(stat_ref), c_ref, LN_PAR, sums, THREE, write,
              [lambda m=m, rows=rows: add_to(g_qkv.at[m], nt(h_ref[...], dproj[rows, :])) for m, rows in enumerate(parts)])


def backward(dy, xs, q, k, v, probs, ctx, mid, act, slope, st1, st2, c, tables, w_qkv, w_o, w_up, w_down):
    def mlp_at(s):
        s = jnp.minimum(s, 15)
        odd = s // FOUR % TWO == ONE
        return ONE - s // EIGHT, jnp.where(odd, THREE, s % FOUR), ZERO, ZERO

    def attn_at(s):
        s = jnp.minimum(s, 15)
        odd = s // FOUR % TWO == ONE
        return jnp.where(s < EIGHT, ONE, ZERO) + jnp.where((s > 7) & (s < 12), ONE, ZERO), jnp.where(odd, s % FOUR, jnp.where(s < FOUR, ZERO, THREE)), ZERO, ZERO

    per_mlp = pl.BlockSpec((None, ONE, *SQUARE), mlp_at)
    per_attn = pl.BlockSpec((None, ONE, *SQUARE), attn_at)

    def stat(at):
        return pl.BlockSpec((None, ONE, EIGHT, TOK), at)

    acc = [(*GRID, EIGHT, WIDTH)]
    scratch = [pltpu.VMEM((SEQS, *SQUARE), BF16), pltpu.VMEM((SEQS, *SQUARE), BF16), pltpu.VMEM((SEQS, HEADS, TOK), F32),
               pltpu.VMEM((HEADS, TOK, TOK), BF16), pltpu.VMEM((THREE, DIM, DIM), BF16), pltpu.VMEM((DIM, DIM), BF16),
               pltpu.VMEM(TALL, F32), pltpu.VMEM(TALL, BF16), pltpu.VMEM(TALL, BF16), pltpu.VMEM(SQUARE, BF16),
               pltpu.VMEM(SQUARE, F32), pltpu.VMEM(SQUARE, F32), pltpu.VMEM((TOK, TOK), BF16), pltpu.VMEM((TOK, TOK), BF16),
               pltpu.VMEM((EIGHT, *COLS), F32), pltpu.VMEM((THREE, *GRID, EIGHT, DIM), F32), pltpu.VMEM((*GRID, EIGHT, DIM), F32),
               pltpu.VMEM((FOUR, *GRID, EIGHT, DIM), F32), pltpu.VMEM((*GRID, FOUR, EIGHT, DIM), F32), *[pltpu.VMEM((*lead, rows, DIM), F32) for rows in (SIXTEEN, EIGHT, EIGHT) for lead in ((), (6,), (SIXTEEN,))]]
    for n in (ONE, THREE):
        for order in ORDERS:
            ring_a, ring_b, plane, *last = landing_shapes(order, n)
            plane = (TWO, *plane) if n == ONE else plane
            scratch += [pltpu.VMEM(s, F32) for s in ((n, *GRID, EIGHT, WIDTH), ring_a, ring_b, plane, *last)]
    scratch += [DMA((6, THREE, 9)), DMA((6, THREE, 9)), DMA((THREE, TWO, 6)), DMA((THREE, TWO)), DMA((EIGHT,)), DMA((TWO,)), DMA((TWO,))]
    outs = ((TWO, FOUR, FOUR, DIM), (TWO, FOUR, FFN), (TWO, SIXTEEN, DIM), (32, DIM))
    whole = [pl.BlockSpec(s, lambda i, n=len(s): (ZERO,) * n, pipeline_mode=pl.Buffered(ONE)) for s in outs]
    dx_at = lambda s: (jnp.clip(s - 12, ZERO, THREE), ZERO, ZERO)
    return pl.pallas_call(
        backward_kernel, grid=(19,),
        out_shape=[jax.ShapeDtypeStruct((SEQS, TOK, DIM), BF16)] + [jax.ShapeDtypeStruct(s, F32) for s in outs],
        out_specs=[pl.BlockSpec((ONE, TOK, DIM), dx_at)] + whole,
        in_specs=[pl.BlockSpec((ONE, TOK, DIM), lambda s: (jnp.minimum(s, THREE), ZERO, ZERO)), per_mlp, per_mlp, stat(mlp_at)] + [per_attn] * FOUR + [stat(attn_at),
                  once((HALF, TOK)), once((HALF, TOK)), pl.BlockSpec((None, *COLS), lambda s: (ONE - jnp.minimum(s, 15) // EIGHT, ZERO, ZERO))] + [HBM] * 7,
        scratch_shapes=scratch,
        compiler_params=pltpu.CompilerParams(collective_id=ONE, has_side_effects=True, vmem_limit_bytes=67043328,
                                             dimension_semantics=("arbitrary",)),
        name="backward")(dy, mid, ctx, st2, q, k, v, xs, st1, *tables, c, probs, slope, act, w_qkv, w_o, w_up, w_down)


def results_kernel(dx_ref, attn_ref, up_ref, down_ref, small_ref, dx_out, attn_out, gb_attn, g_ln, up_out, gb_up, down_out, gb_down):
    dx_out[...] = dx_ref[...]

    @pl.when(pl.program_id(ZERO) == ZERO)
    def _():
        me = lax.axis_index(AXIS)
        attn_out[...], up_out[...], down_out[...] = attn_ref[...], up_ref[...], down_ref[...]
        mine = pltpu.roll(small_ref[...], lax.rem(DIM - FOUR * me + FOUR * LANES, DIM), ONE)
        for l in range(TWO):
            mlp = SIXTEEN - SIXTEEN * l
            attn = mlp + EIGHT
            gb_attn[l, :THREE], gb_attn[l, THREE:] = mine[attn:attn + THREE, :FOUR], mine[mlp + 7:mlp + EIGHT, :FOUR]
            g_ln[l, :TWO], g_ln[l, TWO:] = mine[attn + THREE:attn + 5, :FOUR], mine[mlp + FOUR:mlp + 6, :FOUR]
            gb_down[l:l + ONE, :] = mine[mlp + 6:mlp + 7, :FOUR]
            ups = small_ref[pl.ds(mlp + me // 32, ONE), :]
            gb_up[l:l + ONE, :] = pltpu.roll(ups, lax.rem(DIM - SIXTEEN * lax.rem(me, 32), DIM), ONE)[:, :SIXTEEN]


def results(dx, attn, up, down, small):
    shapes = [attn.shape, (TWO, FOUR, FOUR), (TWO, FOUR, FOUR), up.shape, (TWO, SIXTEEN), down.shape, (TWO, FOUR)]
    per = pl.BlockSpec((TWO, TOK, DIM), lambda s: (s, ZERO, ZERO))
    return pl.pallas_call(
        results_kernel, grid=(SEQS // TWO,), name="results",
        out_shape=[jax.ShapeDtypeStruct(dx.shape, BF16)] + [jax.ShapeDtypeStruct(s, F32) for s in shapes],
        in_specs=[per] + [once(a.shape) for a in (attn, up, down, small)],
        out_specs=[per] + [once(s) for s in shapes])(dx, attn, up, down, small)


def solution(mesh):
    batch_spec = P(AXIS)
    weight_specs = (P(None, None, AXIS, None), P(None, None, AXIS), P(None, None, AXIS),
                    P(None, AXIS, None), P(None, AXIS), P(None, AXIS, None), P(None, AXIS))

    def device_step(x, lengths, d_y, w_attn, b_attn, ln_par, w_up, b_up, w_down, b_down):
        tables = rotary_tables()
        xs, q, k, v, probs, ctx, mid, act, slope, st1, st2, c, w_qkv, w_o, w_up, w_down = forward(
            lengths, x, tables, (w_attn, b_attn, ln_par, w_up, b_up, w_down, b_down))
        return results(*backward(d_y, xs, q, k, v, probs, ctx, mid, act, slope, st1, st2, c, tables, w_qkv, w_o, w_up, w_down))

    return jax.shard_map(device_step, mesh=mesh,
                         in_specs=(batch_spec, batch_spec, batch_spec) + weight_specs,
                         out_specs=(batch_spec,) + weight_specs,
                         check_vma=False)
```
